16 devices in a mesh: dp: 2 (over z), dap: 8 (over y, x, core).
Axes of the slice: x: 2, y: 2, z: 2, core: 2. Of those that a mesh axis runs over, the one named last changes fastest.
Arguments:
- z_pair: bfloat16 [2, 256, 256, 128], P('dp', 'dap')
- pair_mask: int32 [2, 256, 256], P('dp', 'dap')
- dz_out: bfloat16 [2, 256, 256, 128], P('dp', 'dap')
- ln_in: bfloat16 [2, 2, 128], replicated
- w_proj: bfloat16 [2, 128, 640], replicated
- b_proj: bfloat16 [2, 640], replicated
- ln_mid: bfloat16 [2, 2, 128], replicated
- w_out: bfloat16 [2, 128, 128], replicated
- b_out: bfloat16 [2, 128], replicated
Outputs:
- output 1: bfloat16 [2, 256, 256, 128], P('dp', 'dap')
- output 2: bfloat16 [2, 256, 256, 128], P('dp', 'dap')
- output 3: float32 [2, 2, 128], replicated
- output 4: float32 [2, 128, 640], replicated
- output 5: float32 [2, 640], replicated
- output 6: float32 [2, 2, 128], replicated
- output 7: float32 [2, 128, 128], replicated
- output 8: float32 [2, 128], replicated
All inputs are finite; a program needn't handle non-finite values.
Results may differ from the reference program's by a relative error of at most 0.0119678.
Values are sent between devices in bfloat16 or wider.
A program may use at most 1 GiB of HBM per device.

```python
import jax
import jax.numpy as jnp
from jax import lax

PROTEINS = 2
N_RES = 256
C_Z = 128
C_HID = 128
LN_EPS = 1e-5


def layer_norm(values, ln_gain, ln_bias):
    mean_val = jnp.mean(values, axis=-1, keepdims=True)
    centered = values - mean_val
    variance = jnp.mean(centered * centered, axis=-1, keepdims=True)
    return centered * lax.rsqrt(variance + LN_EPS) * ln_gain + ln_bias


def to_bf16(values):
    return values.astype(jnp.bfloat16).astype(jnp.float32)


def tri_block(z_in, mask_f, weights, incoming):
    ln_in, w_proj, b_proj, ln_mid, w_out, b_out = weights
    z_f32 = z_in.astype(jnp.float32)
    z_hat = to_bf16(layer_norm(z_f32, ln_in[0], ln_in[1]))
    proj_all = jnp.dot(z_hat, w_proj) + b_proj
    a_side = to_bf16(jax.nn.sigmoid(proj_all[..., :C_HID]) * proj_all[..., C_HID:2 * C_HID] * mask_f)
    b_side = to_bf16(jax.nn.sigmoid(proj_all[..., 2 * C_HID:3 * C_HID]) * proj_all[..., 3 * C_HID:4 * C_HID] * mask_f)
    g_side = jax.nn.sigmoid(proj_all[..., 4 * C_HID:])
    if incoming:
        tri_x = jnp.einsum("kic,kjc->ijc", a_side, b_side)
    else:
        tri_x = jnp.einsum("ikc,jkc->ijc", a_side, b_side)
    x_hat = to_bf16(layer_norm(tri_x, ln_mid[0], ln_mid[1]))
    update = jnp.dot(x_hat, w_out) + b_out
    return (z_f32 + g_side * update).astype(jnp.bfloat16)


def protein_grads(z_one, mask_one, dz_one, weights_all):
    mask_f = mask_one.astype(jnp.float32)[:, :, None]

    def forward(z_in, weights):
        first_set = tuple(weight_arr[0] for weight_arr in weights)
        second_set = tuple(weight_arr[1] for weight_arr in weights)
        z_mid = tri_block(z_in, mask_f, first_set, False)
        return tri_block(z_mid, mask_f, second_set, True)

    z_new, pull_back = jax.vjp(forward, z_one, weights_all)
    dz_in, d_weights = pull_back(dz_one)
    return z_new, dz_in, d_weights


def setup_inputs(seed: int = 0) -> dict:
    key_list = jax.random.split(jax.random.key(seed), 12)
    pair_shape = (PROTEINS, N_RES, N_RES, C_Z)
    proj_width = 4 * C_HID + C_Z
    z_pair = jax.random.normal(key_list[0], pair_shape, jnp.float32).astype(jnp.bfloat16)
    lengths = jax.random.randint(key_list[1], (PROTEINS,), N_RES // 2, N_RES + 1)
    positions = jnp.arange(N_RES)
    valid_res = positions[None, :] < lengths[:, None]
    pair_mask = (valid_res[:, :, None] & valid_res[:, None, :]).astype(jnp.int32)
    dz_out = jax.random.normal(key_list[2], pair_shape, jnp.float32).astype(jnp.bfloat16)
    ln_in = jnp.stack([1.0 + 0.3 * jax.random.normal(key_list[3], (2, C_Z), jnp.float32), 0.3 * jax.random.normal(key_list[4], (2, C_Z), jnp.float32)], axis=1).astype(jnp.bfloat16)
    w_proj = (jax.random.normal(key_list[5], (2, C_Z, proj_width), jnp.float32) * C_Z ** -0.5).astype(jnp.bfloat16)
    b_proj = (0.5 * jax.random.normal(key_list[6], (2, proj_width), jnp.float32)).astype(jnp.bfloat16)
    ln_mid = jnp.stack([1.0 + 0.3 * jax.random.normal(key_list[7], (2, C_HID), jnp.float32), 0.3 * jax.random.normal(key_list[8], (2, C_HID), jnp.float32)], axis=1).astype(jnp.bfloat16)
    w_out = (jax.random.normal(key_list[9], (2, C_HID, C_Z), jnp.float32) * C_HID ** -0.5).astype(jnp.bfloat16)
    b_out = (0.5 * jax.random.normal(key_list[10], (2, C_Z), jnp.float32)).astype(jnp.bfloat16)
    return {"z_pair": z_pair, "pair_mask": pair_mask, "dz_out": dz_out, "ln_in": ln_in, "w_proj": w_proj, "b_proj": b_proj, "ln_mid": ln_mid, "w_out": w_out, "b_out": b_out}


def reference(z_pair, pair_mask, dz_out, ln_in, w_proj, b_proj, ln_mid, w_out, b_out):
    weights_all = (ln_in.astype(jnp.float32), w_proj.astype(jnp.float32), b_proj.astype(jnp.float32), ln_mid.astype(jnp.float32), w_out.astype(jnp.float32), b_out.astype(jnp.float32))

    def per_protein(operands):
        z_one, mask_one, dz_one = operands
        return protein_grads(z_one, mask_one, dz_one, weights_all)

    z_new, dz_in, d_weights = lax.map(per_protein, (z_pair, pair_mask, dz_out))
    d_ln_in, d_w_proj, d_b_proj, d_ln_mid, d_w_out, d_b_out = d_weights
    return (z_new, dz_in, jnp.sum(d_ln_in, axis=0), jnp.sum(d_w_proj, axis=0), jnp.sum(d_b_proj, axis=0), jnp.sum(d_ln_mid, axis=0), jnp.sum(d_w_out, axis=0), jnp.sum(d_b_out, axis=0))
```

```python
import functools

import jax
import jax.numpy as jnp
from jax import lax
from jax.experimental import pallas as pl
from jax.experimental.pallas import tpu as pltpu
from jax.sharding import PartitionSpec as P

LN_EPS = 1e-5
N = 256
C = 128
GROUP = 8
ROWS = N // GROUP
CH = C // GROUP
STEP = 8
SEND = 16
STEPS = ROWS // STEP
F32 = jnp.float32
BF16 = jnp.bfloat16
VMEM_LIMIT = 62 * 1024 * 1024


def dot(lhs, rhs, lhs_dim, rhs_dim):
    return lax.dot_general(lhs, rhs, (((lhs_dim,), (rhs_dim,)), ((), ())), preferred_element_type=F32)


def norm(values):
    mean = jnp.mean(values, axis=0, keepdims=True)
    cen = values - mean
    inv = lax.rsqrt(jnp.mean(cen * cen, axis=0, keepdims=True) + LN_EPS)
    return cen * inv, inv


def norm_back(d_hat, unit, inv, gain):
    d_unit = d_hat * gain
    mean_d = jnp.mean(d_unit, axis=0, keepdims=True)
    mean_du = jnp.mean(d_unit * unit, axis=0, keepdims=True)
    return inv * (d_unit - mean_d - unit * mean_du)


def fold(values):
    return values[:, :C] + values[:, C:]


def row_sums(acc):
    return jnp.sum(acc.T, axis=0, keepdims=True)


def sigmoid(values):
    return 0.5 * jnp.tanh(0.5 * values) + 0.5


def project(z_t, ln, w_t, bias):
    unit, inv = norm(z_t)
    z_hat = (unit * ln[0] + ln[1]).astype(BF16)
    return unit, inv, z_hat, dot(w_t, z_hat, 1, 0) + bias


def place():
    me = lax.axis_index("dap")
    return me, me // 4, (me // 2) % 2, me % 2


def enter():
    me = lax.axis_index("dap")
    sem = pltpu.get_barrier_semaphore()
    for k in range(1, GROUP):
        pl.semaphore_signal(sem, inc=1, device_id={"dap": (me + k) % GROUP}, device_id_type=pl.DeviceIdType.MESH)
    pl.semaphore_wait(sem, GROUP - 1)


def peers():
    me, cy, cx, core = place()
    out = []
    for dy, dx in ((1, 1), (1, 0), (0, 1), (0, 0)):
        for dc in (1, 0):
            out.append((((cy + dy) % 2) * 2 + (cx + dx) % 2) * 2 + (core + dc) % 2)
    return me, out


def spread(ref, value, row):
    for h in range(2):
        ref[pl.ds(h * C * STEP + row, C, stride=STEP), :] = value[:, h * C:(h + 1) * C]


def pack_rows(lo_ref, hi_ref, send_ref, slot):
    for h in range(2):
        for q in range(4):
            at = pl.ds((h * C + q * 32) * STEP, 32 * STEP)
            lo = lo_ref[at, :].reshape(32, STEP, C)
            hi = hi_ref[at, :].reshape(32, STEP, C)
            send_ref[slot, q * 32:(q + 1) * 32, :, h * C:(h + 1) * C] = jnp.concatenate([lo, hi], axis=1).astype(BF16)


def move(src_ref, dst_ref, send_sem, recv_sem, dest, own):
    if own:
        return pltpu.make_async_copy(src_ref, dst_ref, recv_sem)
    return pltpu.make_async_remote_copy(src_ref, dst_ref, send_sem, recv_sem, device_id={"dap": dest}, device_id_type=pl.DeviceIdType.MESH)


def wait_sends(copies):
    for copy in copies:
        if copy.is_remote:
            copy.wait_send()


def row_copies(send_ref, out_ref, send_sem, recv_sem, slot):
    me, dests = peers()
    start = pl.multiple_of(me * ROWS + slot * SEND, SEND)
    return [
        move(send_ref.at[slot, pl.ds(pl.multiple_of(dest * CH, CH), CH)], out_ref.at[:, pl.ds(start, SEND), :],
             send_sem.at[slot, k], recv_sem, dest, k == GROUP - 1)
        for k, dest in enumerate(dests)
    ]


def send_rows(step, jobs):
    for slot in range(ROWS // SEND):
        @pl.when(step == 2 * slot + 1)
        def _():
            for stage, send_ref, out_ref, send_sem, recv_sem in jobs:
                pack_rows(stage.at[0], stage.at[1], send_ref, slot)
                for copy in row_copies(send_ref, out_ref, send_sem, recv_sem, slot):
                    copy.start()

    @pl.when(step == STEPS - 1)
    def _():
        for stage, send_ref, out_ref, send_sem, recv_sem in jobs:
            for slot in range(ROWS // SEND):
                wait_sends(row_copies(send_ref, out_ref, send_sem, recv_sem, slot))
            pltpu.make_async_copy(out_ref, out_ref, recv_sem).wait()


def pre_row(r, z_t, mask_ref, ln_ref, w_t_ref, bias_ref, g_ref, a_stage, b_stage):
    _, _, _, p = project(z_t, ln_ref, w_t_ref[...], bias_ref[...])
    m = mask_ref[0, pl.ds(r, 1), :].astype(F32)
    spread(a_stage, sigmoid(p[:C]) * p[C:2 * C] * m, r)
    spread(b_stage, sigmoid(p[2 * C:3 * C]) * p[3 * C:4 * C] * m, r)
    g_ref[r] = sigmoid(p[4 * C:])


def pre_kernel(z_ref, mask_ref, ln_ref, w_t_ref, bias_ref, eye_ref, a_ref, b_ref, g_ref, a_st, b_st, a_send, b_send, a_ss, b_ss, rs):
    step = pl.program_id(0)
    pl.when(step == 0)(enter)
    half = step % 2

    def body(r, carry):
        z_t = dot(eye_ref[...], z_ref[r], 1, 1)
        pre_row(r, z_t, mask_ref, ln_ref, w_t_ref, bias_ref, g_ref, a_st.at[half], b_st.at[half])
        return carry

    lax.fori_loop(0, STEP, body, 0)
    send_rows(step, [(a_st, a_send, a_ref, a_ss, rs.at[0]), (b_st, b_send, b_ref, b_ss, rs.at[1])])


def mid_kernel(x_ref, z_ref, g0_ref, mask_ref, mln_ref, wo_t_ref, bo_ref, ln_ref, w_t_ref, bias_ref, eye_ref,
               a_ref, b_ref, g_ref, zm_ref, a_st, b_st, a_send, b_send, a_ss, b_ss, rs):
    step = pl.program_id(0)
    pl.when(step == 0)(enter)
    half = step % 2

    def body(r, carry):
        unit, _ = norm(x_ref[r].astype(F32))
        x_hat = (unit * mln_ref[0] + mln_ref[1]).astype(BF16)
        update = dot(wo_t_ref[...], x_hat, 1, 0) + bo_ref[...]
        z_new = (dot(eye_ref[...], z_ref[r], 1, 1) + g0_ref[r] * update).astype(BF16)
        zm_ref[r] = z_new
        pre_row(r, z_new.astype(F32), mask_ref, ln_ref, w_t_ref, bias_ref, g_ref, a_st.at[half], b_st.at[half])
        return carry

    lax.fori_loop(0, STEP, body, 0)
    send_rows(step, [(a_st, a_send, a_ref, a_ss, rs.at[0]), (b_st, b_send, b_ref, b_ss, rs.at[1])])


def post_back_row(x_t, g, dz, mln_ref, wo_t_ref, wo_ref, bo_ref, acc_ref):
    unit, inv = norm(x_t)
    x_hat = (unit * mln_ref[0] + mln_ref[1]).astype(BF16)
    update = dot(wo_t_ref[...], x_hat, 1, 0) + bo_ref[...]
    d_up = dz * g
    d_up_bf = d_up.astype(BF16)
    acc_ref[0] += dot(x_hat, d_up_bf, 1, 1)
    acc_ref[3] += fold(d_up)
    d_hat = dot(wo_ref[...], d_up_bf, 1, 0).astype(BF16).astype(F32)
    acc_ref[1] += fold(d_hat * unit)
    acc_ref[2] += fold(d_hat)
    dx = norm_back(d_hat, unit, inv, mln_ref[0])
    return update, dx, dz * update * g * (1.0 - g)


def put_post(grad_ref, acc_ref):
    grad_ref[0:C, :] = acc_ref[0]
    grad_ref[C:C + 8, :] = jnp.concatenate([row_sums(acc_ref[1]), row_sums(acc_ref[2]), row_sums(acc_ref[3]), jnp.zeros((5, C), F32)], axis=0)


def turn_kernel(x_ref, zm_ref, g_ref, dz_ref, mln_ref, wo_t_ref, wo_ref, bo_ref, eye_ref,
                dx_ref, z_out_ref, dpg_ref, grad_ref, d_st, d_send, acc_ref, d_ss, rs):
    step = pl.program_id(0)

    @pl.when(step == 0)
    def _():
        enter()
        acc_ref[...] = jnp.zeros_like(acc_ref)

    half = step % 2

    def body(r, carry):
        dz = dot(eye_ref[...], dz_ref[r], 1, 1)
        g = g_ref[r]
        update, dx, d_pg = post_back_row(x_ref[r].astype(F32), g, dz, mln_ref, wo_t_ref, wo_ref, bo_ref, acc_ref)
        dpg_ref[r] = d_pg
        z_out_ref[r] = (zm_ref[r].astype(F32) + g * update).T.astype(BF16)
        spread(d_st.at[half], dx, r)
        return carry

    lax.fori_loop(0, STEP, body, 0)

    @pl.when(step == STEPS - 1)
    def _():
        put_post(grad_ref, acc_ref)

    send_rows(step, [(d_st, d_send, dx_ref, d_ss, rs.at[0])])


def pre_back_row(r, z_t, da, db, d_pg, mask_ref, ln_ref, w_t_ref, w_ref, bias_ref, w_acc, b_acc, l_acc):
    unit, inv, z_hat, p = project(z_t, ln_ref, w_t_ref[...], bias_ref[...])
    m = mask_ref[0, pl.ds(r, 1), :].astype(F32)
    parts = []
    for side, d_side in ((0, da), (1, db)):
        s = sigmoid(p[2 * side * C:(2 * side + 1) * C])
        v = p[(2 * side + 1) * C:(2 * side + 2) * C]
        d_v = d_side * m * s
        parts += [d_v * v * (1.0 - s), d_v]
    parts.append(d_pg)
    for k, part in enumerate(parts):
        b_acc[k * C:(k + 1) * C, :] += fold(part)
    d_p = jnp.concatenate([part.astype(BF16) for part in parts], axis=0)
    w_acc[...] += dot(d_p, z_hat, 1, 1)
    d_hat = dot(w_ref[...], d_p, 1, 0).astype(BF16).astype(F32)
    l_acc[0] += fold(d_hat * unit)
    l_acc[1] += fold(d_hat)
    return norm_back(d_hat, unit, inv, ln_ref[0])


def put_pre(grad_ref, w_acc, b_acc, l_acc):
    grad_ref[0:5 * C, :] = w_acc[...]
    rows = [row_sums(b_acc[k * C:(k + 1) * C, :]) for k in range(5)]
    rows += [row_sums(l_acc[0]), row_sums(l_acc[1]), jnp.zeros((1, C), F32)]
    grad_ref[5 * C:5 * C + 8, :] = jnp.concatenate(rows, axis=0)


def back_kernel(da_ref, db_ref, dpg1_ref, zm_ref, mask_ref, dz_ref, x_ref, g_ref, ln_ref, w_t_ref, w_ref, bias_ref,
                mln_ref, wo_t_ref, wo_ref, bo_ref, eye_ref,
                dx_ref, dzm_ref, dpg_ref, grad1_ref, grad0_ref, d_st, d_send, w_acc, b_acc, l_acc, acc_ref, d_ss, rs):
    step = pl.program_id(0)

    @pl.when(step == 0)
    def _():
        enter()
        for ref in (w_acc, b_acc, l_acc, acc_ref):
            ref[...] = jnp.zeros_like(ref)

    half = step % 2

    def body(r, carry):
        dzn = pre_back_row(r, zm_ref[r].astype(F32), da_ref[r].astype(F32), db_ref[r].astype(F32), dpg1_ref[r], mask_ref,
                           ln_ref, w_t_ref, w_ref, bias_ref, w_acc, b_acc, l_acc)
        dzm = (dot(eye_ref[...], dz_ref[r], 1, 1) + dzn).astype(BF16)
        dzm_ref[r] = dzm
        _, dx, d_pg = post_back_row(x_ref[r].astype(F32), g_ref[r], dzm.astype(F32), mln_ref, wo_t_ref, wo_ref, bo_ref, acc_ref)
        dpg_ref[r] = d_pg
        spread(d_st.at[half], dx, r)
        return carry

    lax.fori_loop(0, STEP, body, 0)

    @pl.when(step == STEPS - 1)
    def _():
        put_pre(grad1_ref, w_acc, b_acc, l_acc)
        put_post(grad0_ref, acc_ref)

    send_rows(step, [(d_st, d_send, dx_ref, d_ss, rs.at[0])])


def last_kernel(da_ref, db_ref, dpg_ref, z_ref, mask_ref, dzm_ref, ln_ref, w_t_ref, w_ref, bias_ref, eye_ref,
                dz_ref, grad_ref, w_acc, b_acc, l_acc):
    step = pl.program_id(0)

    @pl.when(step == 0)
    def _():
        for ref in (w_acc, b_acc, l_acc):
            ref[...] = jnp.zeros_like(ref)

    def body(r, carry):
        z_t = dot(eye_ref[...], z_ref[r], 1, 1)
        dzn = pre_back_row(r, z_t, da_ref[r].astype(F32), db_ref[r].astype(F32), dpg_ref[r], mask_ref,
                           ln_ref, w_t_ref, w_ref, bias_ref, w_acc, b_acc, l_acc)
        dz_ref[r] = (dzm_ref[r].astype(F32) + dzn).T.astype(BF16)
        return carry

    lax.fori_loop(0, STEP, body, 0)

    @pl.when(step == STEPS - 1)
    def _():
        put_pre(grad_ref, w_acc, b_acc, l_acc)


HALF = N // 2


def spread_channel(stage, value, c):
    for h in range(2):
        stage[pl.ds((h * 2 + c // 8) * HALF * 8 + c % 8, HALF, stride=8), :] = value[:, h * C:(h + 1) * C]


def pack_channels(stage, send_ref, slot):
    for h in range(2):
        for q in range(4):
            lo = stage[pl.ds((h * 2) * HALF * 8 + q * 256, 256), :].reshape(32, 8, C)
            hi = stage[pl.ds((h * 2 + 1) * HALF * 8 + q * 256, 256), :].reshape(32, 8, C)
            send_ref[slot, q * 32:(q + 1) * 32, :, h * C:(h + 1) * C] = jnp.concatenate([lo, hi], axis=1).astype(BF16)


def channel_copies(send_ref, out_ref, send_sem, recv_sem, slot, top):
    me, cy, cx, core = place()
    out = []
    k = 0
    for dx in (1, 0):
        for dc in (1, 0):
            within = ((cx + dx) % 2) * 2 + (core + dc) % 2
            out.append(move(send_ref.at[slot, pl.ds(pl.multiple_of(within * ROWS, ROWS), ROWS)],
                            out_ref.at[:, pl.ds(pl.multiple_of(me * CH, CH), CH), :],
                            send_sem.at[slot, k], recv_sem, top * 4 + within, slot == 1 and k == 3))
            k += 1
    return out


def channel_kernel(products, n_in, n_out, *refs):
    ins, outs = refs[:n_in], refs[n_in:n_in + n_out]
    stages = refs[n_in + n_out:n_in + 2 * n_out]
    sends = refs[n_in + 2 * n_out:n_in + 3 * n_out]
    sems = refs[n_in + 3 * n_out:n_in + 4 * n_out]
    rs = refs[-1]
    step = pl.program_id(0)
    pl.when(step == 0)(enter)
    _, cy, _, _ = place()
    top = (cy + 1 + step) % 2
    rows = pl.ds(pl.multiple_of(top * HALF, HALF), HALF)
    for j in range(n_out):
        for c in range(CH):
            spread_channel(stages[j], products[j](ins, c, rows), c)
        for slot in range(2):
            @pl.when(step == slot)
            def _():
                pack_channels(stages[j], sends[j], slot)
                for copy in channel_copies(sends[j], outs[j], sems[j], rs.at[j], slot, top):
                    copy.start()

    @pl.when(step == 1)
    def _():
        for j in range(n_out):
            for slot in range(2):
                wait_sends(channel_copies(sends[j], outs[j], sems[j], rs.at[j], slot, (cy + 1 + slot) % 2))
            pltpu.make_async_copy(outs[j], outs[j], rs.at[j]).wait()


OUT_FWD = (lambda r, c, rows: dot(r[0][c, rows, :], r[1][c], 1, 1),)
IN_FWD = (lambda r, c, rows: dot(r[0][c, :, rows], r[1][c], 0, 0),)
IN_BWD = (lambda r, c, rows: dot(r[1][c, rows, :], r[2][c], 1, 1), lambda r, c, rows: dot(r[0][c, rows, :], r[2][c], 1, 0))
OUT_BWD = (lambda r, c, rows: dot(r[2][c, rows, :], r[1][c], 1, 0), lambda r, c, rows: dot(r[2][c, :, rows], r[0][c], 0, 0))

ANY = pl.BlockSpec(memory_space=pl.ANY)
TRI = jax.ShapeDtypeStruct((CH, N, N), BF16)
ROW = jax.ShapeDtypeStruct((ROWS, C, N), BF16)
ROW32 = jax.ShapeDtypeStruct((ROWS, C, N), F32)
NATIVE = jax.ShapeDtypeStruct((ROWS, N, C), BF16)
POST = jax.ShapeDtypeStruct((C + 8, C), F32)
PRE = jax.ShapeDtypeStruct((5 * C + 8, C), F32)


def by_row(array):
    tail = array.shape[1:]
    return pl.BlockSpec((array.shape[0] // STEPS,) + tail, lambda t: (t,) + (0,) * len(tail))


def whole(array):
    zeros = (0,) * len(array.shape)
    return pl.BlockSpec(array.shape, lambda t: zeros)


def params(collective_id):
    if collective_id is None:
        return pltpu.CompilerParams(dimension_semantics=("arbitrary",), vmem_limit_bytes=VMEM_LIMIT)
    return pltpu.CompilerParams(dimension_semantics=("arbitrary",), vmem_limit_bytes=VMEM_LIMIT, collective_id=collective_id, has_side_effects=True)


def row_call(kernel, name, collective_id, ins, consts, outs, specs, n_send, scratch):
    sent = [pltpu.VMEM((2, 2 * C * STEP, C), F32)] * n_send + [pltpu.VMEM((ROWS // SEND, C, SEND, N), BF16)] * n_send
    sems = [pltpu.SemaphoreType.DMA((ROWS // SEND, GROUP))] * n_send + ([pltpu.SemaphoreType.DMA((n_send,))] if n_send else [])
    return pl.pallas_call(
        kernel,
        grid=(STEPS,),
        in_specs=[by_row(x) for x in ins] + [whole(x) for x in consts],
        out_specs=specs,
        out_shape=outs,
        scratch_shapes=sent + scratch + sems,
        compiler_params=params(collective_id),
        name=name,
    )(*ins, *consts)


def channel_call(products, name, collective_id, ins, n_out):
    return pl.pallas_call(
        functools.partial(channel_kernel, products, len(ins), n_out),
        grid=(2,),
        in_specs=[whole(x) for x in ins],
        out_specs=[ANY] * n_out,
        out_shape=[ROW] * n_out,
        scratch_shapes=[pltpu.VMEM((4 * HALF * 8, C), F32)] * n_out + [pltpu.VMEM((2, HALF, CH, N), BF16)] * n_out
        + [pltpu.SemaphoreType.DMA((2, 4))] * n_out + [pltpu.SemaphoreType.DMA((n_out,))],
        compiler_params=params(collective_id),
        name=name,
    )(*ins)


def local_step(z_pair, pair_mask, dz_out, ln_in, w_proj, b_proj, ln_mid, w_out, b_out):
    z, dz = z_pair[0], dz_out[0]
    mask = pair_mask.reshape(STEPS, STEP, N)
    eye = jnp.eye(C, dtype=BF16)
    ln = jnp.broadcast_to(ln_in.astype(F32)[..., None], (2, 2, C, N))
    mln = jnp.broadcast_to(ln_mid.astype(F32)[..., None], (2, 2, C, N))
    bias = jnp.broadcast_to(b_proj.astype(F32)[..., None], (2, 5 * C, N))
    bo = jnp.broadcast_to(b_out.astype(F32)[..., None], (2, C, N))
    w_t = jnp.swapaxes(w_proj, 1, 2)
    wo_t = jnp.swapaxes(w_out, 1, 2)
    pre = [(ln[k], w_t[k], bias[k]) for k in range(2)]
    post = [(mln[k], wo_t[k], bo[k]) for k in range(2)]

    a0, b0, g0 = row_call(pre_kernel, "pre0", 0, [z, mask], [*pre[0], eye], [TRI, TRI, ROW32], [ANY, ANY, by_row(ROW32)], 2, [])
    x0, = channel_call(OUT_FWD, "tri0", 1, [a0, b0], 1)
    a1, b1, g1, zm = row_call(mid_kernel, "mid", 2, [x0, z, g0, mask], [*post[0], *pre[1], eye], [TRI, TRI, ROW32, ROW],
                              [ANY, ANY, by_row(ROW32), by_row(ROW)], 2, [])
    x1, = channel_call(IN_FWD, "tri1", 3, [a1, b1], 1)
    post_acc = [pltpu.VMEM((4, C, C), F32)]
    pre_acc = [pltpu.VMEM((5 * C, C), F32), pltpu.VMEM((5 * C, C), F32), pltpu.VMEM((2, C, C), F32)]
    dx1, z_new, dpg1, post_g1 = row_call(turn_kernel, "turn", 4, [x1, zm, g1, dz], [mln[1], wo_t[1], w_out[1], bo[1], eye],
                                         [TRI, NATIVE, ROW32, POST], [ANY, by_row(NATIVE), by_row(ROW32), whole(POST)], 1, post_acc)
    da1, db1 = channel_call(IN_BWD, "trib1", 5, [a1, b1, dx1], 2)
    dx0, dzm, dpg0, pre_g1, post_g0 = row_call(
        back_kernel, "back", 6, [da1, db1, dpg1, zm, mask, dz, x0, g0],
        [ln[1], w_t[1], w_proj[1], bias[1], mln[0], wo_t[0], w_out[0], bo[0], eye],
        [TRI, ROW, ROW32, PRE, POST], [ANY, by_row(ROW), by_row(ROW32), whole(PRE), whole(POST)], 1, pre_acc + post_acc)
    da0, db0 = channel_call(OUT_BWD, "trib0", 7, [a0, b0, dx0], 2)
    dz_new, pre_g0 = row_call(last_kernel, "last", None, [da0, db0, dpg0, z, mask, dzm], [ln[0], w_t[0], w_proj[0], bias[0], eye],
                              [NATIVE, PRE], [by_row(NATIVE), whole(PRE)], 0, pre_acc)

    total = lax.psum(jnp.concatenate([pre_g0, pre_g1, post_g0, post_g1]), ("dp", "dap"))
    pre_g = [total[:5 * C + 8], total[5 * C + 8:2 * (5 * C + 8)]]
    post_g = [total[2 * (5 * C + 8):2 * (5 * C + 8) + C + 8], total[2 * (5 * C + 8) + C + 8:]]
    d_w_proj = jnp.stack([g[:5 * C].T for g in pre_g])
    d_b_proj = jnp.stack([g[5 * C:5 * C + 5].reshape(5 * C) for g in pre_g])
    d_ln_in = jnp.stack([g[5 * C + 5:5 * C + 7] for g in pre_g])
    d_w_out = jnp.stack([g[:C] for g in post_g])
    d_ln_mid = jnp.stack([g[C:C + 2] for g in post_g])
    d_b_out = jnp.stack([g[C + 2] for g in post_g])
    return z_new[None], dz_new[None], d_ln_in, d_w_proj, d_b_proj, d_ln_mid, d_w_out, d_b_out


def solution(mesh):
    row_spec = P("dp", "dap")
    return jax.shard_map(local_step, mesh=mesh, in_specs=(row_spec,) * 3 + (P(),) * 6,
                         out_specs=(row_spec,) * 2 + (P(),) * 6, check_vma=False)
```

```python
import functools

import jax
import jax.numpy as jnp
from jax import lax
from jax.experimental import pallas as pl
from jax.experimental.pallas import tpu as pltpu
from jax.sharding import PartitionSpec as P

LN_EPS = 1e-5
N = 256
C = 128
GROUP = 8
ROWS = N // GROUP
CH = C // GROUP
STEP = 8
SEND = 16
STEPS = ROWS // STEP
F32 = jnp.float32
BF16 = jnp.bfloat16
VMEM_LIMIT = 62 * 1024 * 1024


def dot(lhs, rhs, lhs_dim, rhs_dim):
    return lax.dot_general(lhs, rhs, (((lhs_dim,), (rhs_dim,)), ((), ())), preferred_element_type=F32)


def norm(values):
    mean = jnp.mean(values, axis=0, keepdims=True)
    cen = values - mean
    inv = lax.rsqrt(jnp.mean(cen * cen, axis=0, keepdims=True) + LN_EPS)
    return cen * inv, inv


def norm_back(d_hat, unit, inv, gain):
    d_unit = d_hat * gain
    mean_d = jnp.mean(d_unit, axis=0, keepdims=True)
    mean_du = jnp.mean(d_unit * unit, axis=0, keepdims=True)
    return inv * (d_unit - mean_d - unit * mean_du)


def fold(values):
    return values[:, :C] + values[:, C:]


def row_sums(acc):
    return jnp.sum(acc.T, axis=0, keepdims=True)


def sigmoid(values):
    return 0.5 * jnp.tanh(0.5 * values) + 0.5


def project(z_t, ln, w_t, bias):
    unit, inv = norm(z_t)
    z_hat = (unit * ln[0] + ln[1]).astype(BF16)
    return unit, inv, z_hat, dot(w_t[...], z_hat, 1, 0) + bias[...]


def set_eye(eye):
    same = lax.broadcasted_iota(jnp.int32, (C, C), 0) == lax.broadcasted_iota(jnp.int32, (C, C), 1)
    eye[...] = jnp.where(same, 1.0, 0.0).astype(BF16)


def set_column(ref, row):
    column = jnp.broadcast_to(row.astype(F32), (C, C)).T
    ref[:, :C] = column
    ref[:, C:] = column


def set_pre(block, ln_in, w_proj, b_proj, ln, w_t, bias):
    for k in range(2):
        set_column(ln.at[k], ln_in[block, k:k + 1, :])
    for k in range(5):
        cols = slice(k * C, (k + 1) * C)
        set_column(bias.at[cols], b_proj[block:block + 1, cols])
        w_t[cols, :] = w_proj[block, :, cols].astype(F32).T.astype(BF16)


def set_post(block, ln_mid, w_out, b_out, mln, wo_t, bo):
    for k in range(2):
        set_column(mln.at[k], ln_mid[block, k:k + 1, :])
    set_column(bo, b_out[block:block + 1, :])
    wo_t[...] = w_out[block].astype(F32).T.astype(BF16)


def place():
    me = lax.axis_index("dap")
    return me, me // 4, (me // 2) % 2, me % 2


def enter():
    me = lax.axis_index("dap")
    sem = pltpu.get_barrier_semaphore()
    for k in range(1, GROUP):
        pl.semaphore_signal(sem, inc=1, device_id={"dap": (me + k) % GROUP}, device_id_type=pl.DeviceIdType.MESH)
    pl.semaphore_wait(sem, GROUP - 1)


def peers():
    me, cy, cx, core = place()
    out = []
    for dy, dx in ((1, 0), (0, 1), (1, 1), (0, 0)):
        for dc in (1, 0):
            out.append((((cy + dy) % 2) * 2 + (cx + dx) % 2) * 2 + (core + dc) % 2)
    return me, out


def spread(ref, value, row):
    for h in range(2):
        ref[pl.ds(h * C * STEP + row, C, stride=STEP), :] = value[:, h * C:(h + 1) * C]


def pack_rows(lo_ref, hi_ref, send_ref, slot):
    for h in range(2):
        for q in range(4):
            at = pl.ds((h * C + q * 32) * STEP, 32 * STEP)
            lo = lo_ref[at, :].reshape(32, STEP, C)
            hi = hi_ref[at, :].reshape(32, STEP, C)
            send_ref[slot, q * 32:(q + 1) * 32, :, h * C:(h + 1) * C] = jnp.concatenate([lo, hi], axis=1).astype(BF16)


def move(src_ref, dst_ref, send_sem, recv_sem, dest, own):
    if own:
        return pltpu.make_async_copy(src_ref, dst_ref, recv_sem)
    return pltpu.make_async_remote_copy(src_ref, dst_ref, send_sem, recv_sem, device_id={"dap": dest}, device_id_type=pl.DeviceIdType.MESH)


def wait_sends(copies):
    for copy in copies:
        if copy.is_remote:
            copy.wait_send()


def row_copies(send_ref, out_ref, send_sem, recv_sem, slot):
    me, dests = peers()
    start = pl.multiple_of(me * ROWS + slot * SEND, SEND)
    return [
        move(send_ref.at[slot, pl.ds(pl.multiple_of(dest * CH, CH), CH)], out_ref.at[:, pl.ds(start, SEND), :],
             send_sem.at[slot, k], recv_sem, dest, k == GROUP - 1)
        for k, dest in enumerate(dests)
    ]


def send_rows(step, jobs):
    for slot in range(ROWS // SEND):
        @pl.when(step == 2 * slot + 1)
        def _():
            for stage, send_ref, out_ref, send_sem, recv_sem in jobs:
                pack_rows(stage.at[0], stage.at[1], send_ref, slot)
                for copy in row_copies(send_ref, out_ref, send_sem, recv_sem, slot)[:4]:
                    copy.start()
            if slot == ROWS // SEND - 1:
                for stage, send_ref, out_ref, send_sem, recv_sem in jobs:
                    for past in range(ROWS // SEND):
                        for copy in row_copies(send_ref, out_ref, send_sem, recv_sem, past)[4:]:
                            copy.start()

    @pl.when(step == STEPS - 1)
    def _():
        for stage, send_ref, out_ref, send_sem, recv_sem in jobs:
            for slot in range(ROWS // SEND):
                wait_sends(row_copies(send_ref, out_ref, send_sem, recv_sem, slot))
            pltpu.make_async_copy(out_ref, out_ref, recv_sem).wait()


def pre_row(r, z_t, mask_ref, ln_ref, w_t_ref, bias_ref, g_ref, a_stage, b_stage):
    _, _, _, p = project(z_t, ln_ref, w_t_ref, bias_ref)
    m = mask_ref[0, pl.ds(r, 1), :].astype(F32)
    spread(a_stage, sigmoid(p[:C]) * p[C:2 * C] * m, r)
    spread(b_stage, sigmoid(p[2 * C:3 * C]) * p[3 * C:4 * C] * m, r)
    g_ref[r] = sigmoid(p[4 * C:])


def pre_kernel(z_ref, mask_ref, ln_in, w_proj, b_proj, a_ref, b_ref, g_ref, a_st, b_st, a_send, b_send,
               eye_ref, ln_ref, w_t_ref, bias_ref, a_ss, b_ss, rs):
    step = pl.program_id(0)

    @pl.when(step == 0)
    def _():
        enter()
        set_eye(eye_ref)
        set_pre(0, ln_in, w_proj, b_proj, ln_ref, w_t_ref, bias_ref)

    half = step % 2

    def body(r, carry):
        z_t = dot(eye_ref[...], z_ref[r], 1, 1)
        pre_row(r, z_t, mask_ref, ln_ref, w_t_ref, bias_ref, g_ref, a_st.at[half], b_st.at[half])
        return carry

    lax.fori_loop(0, STEP, body, 0)
    send_rows(step, [(a_st, a_send, a_ref, a_ss, rs.at[0]), (b_st, b_send, b_ref, b_ss, rs.at[1])])


def mid_kernel(x_ref, z_ref, g0_ref, mask_ref, ln_mid, w_out, b_out, ln_in, w_proj, b_proj,
               a_ref, b_ref, g_ref, zm_ref, a_st, b_st, a_send, b_send,
               eye_ref, ln_ref, w_t_ref, bias_ref, mln_ref, wo_t_ref, bo_ref, a_ss, b_ss, rs):
    step = pl.program_id(0)

    @pl.when(step == 0)
    def _():
        enter()
        set_eye(eye_ref)
        set_pre(1, ln_in, w_proj, b_proj, ln_ref, w_t_ref, bias_ref)
        set_post(0, ln_mid, w_out, b_out, mln_ref, wo_t_ref, bo_ref)

    half = step % 2

    def body(r, carry):
        unit, _ = norm(x_ref[r].astype(F32))
        x_hat = (unit * mln_ref[0] + mln_ref[1]).astype(BF16)
        update = dot(wo_t_ref[...], x_hat, 1, 0) + bo_ref[...]
        z_new = (dot(eye_ref[...], z_ref[r], 1, 1) + g0_ref[r] * update).astype(BF16)
        zm_ref[r] = z_new
        pre_row(r, z_new.astype(F32), mask_ref, ln_ref, w_t_ref, bias_ref, g_ref, a_st.at[half], b_st.at[half])
        return carry

    lax.fori_loop(0, STEP, body, 0)
    send_rows(step, [(a_st, a_send, a_ref, a_ss, rs.at[0]), (b_st, b_send, b_ref, b_ss, rs.at[1])])


def post_back_row(x_t, g, dz, mln_ref, wo_t_ref, wo_ref, bo_ref, acc_ref):
    unit, inv = norm(x_t)
    x_hat = (unit * mln_ref[0] + mln_ref[1]).astype(BF16)
    update = dot(wo_t_ref[...], x_hat, 1, 0) + bo_ref[...]
    d_up = dz * g
    d_up_bf = d_up.astype(BF16)
    acc_ref[0] += dot(x_hat, d_up_bf, 1, 1)
    acc_ref[3] += fold(d_up)
    d_hat = dot(wo_ref[...], d_up_bf, 1, 0).astype(BF16).astype(F32)
    acc_ref[1] += fold(d_hat * unit)
    acc_ref[2] += fold(d_hat)
    dx = norm_back(d_hat, unit, inv, mln_ref[0])
    return update, dx, dz * update * g * (1.0 - g)


def put_post(grad_ref, acc_ref):
    grad_ref[0:C, :] = acc_ref[0]
    grad_ref[C:C + 8, :] = jnp.concatenate([row_sums(acc_ref[1]), row_sums(acc_ref[2]), row_sums(acc_ref[3]), jnp.zeros((5, C), F32)], axis=0)
    grad_ref[C + 8:C + 16, :] = jnp.zeros((8, C), F32)


def turn_kernel(x_ref, zm_ref, g_ref, dz_ref, ln_mid, w_out, b_out,
                dx_ref, z_out_ref, dpg_ref, grad_ref, d_st, d_send, eye_ref, mln_ref, wo_t_ref, bo_ref, acc_ref, d_ss, rs):
    step = pl.program_id(0)
    wo_ref = w_out.at[1]

    @pl.when(step == 0)
    def _():
        enter()
        set_eye(eye_ref)
        set_post(1, ln_mid, w_out, b_out, mln_ref, wo_t_ref, bo_ref)
        acc_ref[...] = jnp.zeros_like(acc_ref)

    half = step % 2

    def body(r, carry):
        dz = dot(eye_ref[...], dz_ref[r], 1, 1)
        g = g_ref[r]
        update, dx, d_pg = post_back_row(x_ref[r].astype(F32), g, dz, mln_ref, wo_t_ref, wo_ref, bo_ref, acc_ref)
        dpg_ref[r] = d_pg
        z_out_ref[r] = (zm_ref[r].astype(F32) + g * update).T.astype(BF16)
        spread(d_st.at[half], dx, r)
        return carry

    lax.fori_loop(0, STEP, body, 0)

    @pl.when(step == STEPS - 1)
    def _():
        put_post(grad_ref, acc_ref)

    send_rows(step, [(d_st, d_send, dx_ref, d_ss, rs.at[0])])


def pre_back_row(r, z_t, da, db, d_pg, mask_ref, ln_ref, w_t_ref, w_ref, bias_ref, w_acc, b_acc, l_acc):
    unit, inv, z_hat, p = project(z_t, ln_ref, w_t_ref, bias_ref)
    m = mask_ref[0, pl.ds(r, 1), :].astype(F32)
    parts = []
    for side, d_side in ((0, da), (1, db)):
        s = sigmoid(p[2 * side * C:(2 * side + 1) * C])
        v = p[(2 * side + 1) * C:(2 * side + 2) * C]
        d_v = d_side * m * s
        parts += [d_v * v * (1.0 - s), d_v]
    parts.append(d_pg)
    for k, part in enumerate(parts):
        b_acc[k * C:(k + 1) * C, :] += fold(part)
    d_p = jnp.concatenate([part.astype(BF16) for part in parts], axis=0)
    w_acc[...] += dot(d_p, z_hat, 1, 1)
    d_hat = dot(w_ref[...], d_p, 1, 0).astype(BF16).astype(F32)
    l_acc[0] += fold(d_hat * unit)
    l_acc[1] += fold(d_hat)
    return norm_back(d_hat, unit, inv, ln_ref[0])


def put_pre(grad_ref, w_acc, b_acc, l_acc):
    grad_ref[0:5 * C, :] = w_acc[...]
    rows = [row_sums(b_acc[k * C:(k + 1) * C, :]) for k in range(5)]
    rows += [row_sums(l_acc[0]), row_sums(l_acc[1]), jnp.zeros((1, C), F32)]
    grad_ref[5 * C:5 * C + 8, :] = jnp.concatenate(rows, axis=0)
    grad_ref[5 * C + 8:5 * C + 16, :] = jnp.zeros((8, C), F32)


def back_kernel(da_ref, db_ref, dpg1_ref, zm_ref, mask_ref, dz_ref, x_ref, g_ref, ln_in, w_proj, b_proj, ln_mid, w_out, b_out,
                dx_ref, dzm_ref, dpg_ref, grad1_ref, grad0_ref, d_st, d_send,
                eye_ref, ln_ref, w_t_ref, bias_ref, mln_ref, wo_t_ref, bo_ref, w_acc, b_acc, l_acc, acc_ref, d_ss, rs):
    step = pl.program_id(0)
    w_ref, wo_ref = w_proj.at[1], w_out.at[0]

    @pl.when(step == 0)
    def _():
        enter()
        set_eye(eye_ref)
        set_pre(1, ln_in, w_proj, b_proj, ln_ref, w_t_ref, bias_ref)
        set_post(0, ln_mid, w_out, b_out, mln_ref, wo_t_ref, bo_ref)
        for ref in (w_acc, b_acc, l_acc, acc_ref):
            ref[...] = jnp.zeros_like(ref)

    half = step % 2

    def body(r, carry):
        dzn = pre_back_row(r, zm_ref[r].astype(F32), da_ref[r].astype(F32), db_ref[r].astype(F32), dpg1_ref[r], mask_ref,
                           ln_ref, w_t_ref, w_ref, bias_ref, w_acc, b_acc, l_acc)
        dzm = (dot(eye_ref[...], dz_ref[r], 1, 1) + dzn).astype(BF16)
        dzm_ref[r] = dzm
        _, dx, d_pg = post_back_row(x_ref[r].astype(F32), g_ref[r], dzm.astype(F32), mln_ref, wo_t_ref, wo_ref, bo_ref, acc_ref)
        dpg_ref[r] = d_pg
        spread(d_st.at[half], dx, r)
        return carry

    lax.fori_loop(0, STEP, body, 0)

    @pl.when(step == STEPS - 1)
    def _():
        put_pre(grad1_ref, w_acc, b_acc, l_acc)
        put_post(grad0_ref, acc_ref)

    send_rows(step, [(d_st, d_send, dx_ref, d_ss, rs.at[0])])


def last_kernel(da_ref, db_ref, dpg_ref, z_ref, mask_ref, dzm_ref, ln_in, w_proj, b_proj,
                dz_ref, grad_ref, eye_ref, ln_ref, w_t_ref, bias_ref, w_acc, b_acc, l_acc):
    step = pl.program_id(0)
    w_ref = w_proj.at[0]

    @pl.when(step == 0)
    def _():
        set_eye(eye_ref)
        set_pre(0, ln_in, w_proj, b_proj, ln_ref, w_t_ref, bias_ref)
        for ref in (w_acc, b_acc, l_acc):
            ref[...] = jnp.zeros_like(ref)

    def body(r, carry):
        z_t = dot(eye_ref[...], z_ref[r], 1, 1)
        dzn = pre_back_row(r, z_t, da_ref[r].astype(F32), db_ref[r].astype(F32), dpg_ref[r], mask_ref,
                           ln_ref, w_t_ref, w_ref, bias_ref, w_acc, b_acc, l_acc)
        dz_ref[r] = (dzm_ref[r].astype(F32) + dzn).T.astype(BF16)
        return carry

    lax.fori_loop(0, STEP, body, 0)

    @pl.when(step == STEPS - 1)
    def _():
        put_pre(grad_ref, w_acc, b_acc, l_acc)


HALF = N // 2


def spread_channel(stage, value, c):
    for h in range(2):
        stage[pl.ds((h * 2 + c // 8) * HALF * 8 + c % 8, HALF, stride=8), :] = value[:, h * C:(h + 1) * C]


def pack_channels(stage, send_ref, slot):
    for h in range(2):
        for q in range(4):
            lo = stage[pl.ds((h * 2) * HALF * 8 + q * 256, 256), :].reshape(32, 8, C)
            hi = stage[pl.ds((h * 2 + 1) * HALF * 8 + q * 256, 256), :].reshape(32, 8, C)
            send_ref[slot, q * 32:(q + 1) * 32, :, h * C:(h + 1) * C] = jnp.concatenate([lo, hi], axis=1).astype(BF16)


def channel_copies(send_ref, out_ref, send_sem, recv_sem, slot, top):
    me, cy, cx, core = place()
    out = []
    k = 0
    for dx in (1, 0):
        for dc in (1, 0):
            within = ((cx + dx) % 2) * 2 + (core + dc) % 2
            out.append(move(send_ref.at[slot, pl.ds(pl.multiple_of(within * ROWS, ROWS), ROWS)],
                            out_ref.at[:, pl.ds(pl.multiple_of(me * CH, CH), CH), :],
                            send_sem.at[slot, k], recv_sem, top * 4 + within, slot == 1 and k == 3))
            k += 1
    return out


def channel_kernel(products, n_in, n_out, *refs):
    ins, outs = refs[:n_in], refs[n_in:n_in + n_out]
    stages = refs[n_in + n_out:n_in + 2 * n_out]
    sends = refs[n_in + 2 * n_out:n_in + 3 * n_out]
    sems = refs[n_in + 3 * n_out:n_in + 4 * n_out]
    rs = refs[-1]
    step = pl.program_id(0)
    pl.when(step == 0)(enter)
    _, cy, _, _ = place()
    top = (cy + 1 + step) % 2
    rows = pl.ds(pl.multiple_of(top * HALF, HALF), HALF)
    for j in range(n_out):
        for c in range(CH):
            spread_channel(stages[j], products[j](ins, c, rows), c)
        for slot in range(2):
            @pl.when(step == slot)
            def _():
                pack_channels(stages[j], sends[j], slot)
                for copy in channel_copies(sends[j], outs[j], sems[j], rs.at[j], slot, top)[2 - 2 * slot:4 - 2 * slot]:
                    copy.start()

    @pl.when(step == 1)
    def _():
        for slot in range(2):
            for j in range(n_out):
                for copy in channel_copies(sends[j], outs[j], sems[j], rs.at[j], slot, (cy + 1 + slot) % 2)[2 * slot:2 + 2 * slot]:
                    copy.start()
        for j in range(n_out):
            for slot in range(2):
                wait_sends(channel_copies(sends[j], outs[j], sems[j], rs.at[j], slot, (cy + 1 + slot) % 2))
            pltpu.make_async_copy(outs[j], outs[j], rs.at[j]).wait()


OUT_FWD = (lambda r, c, rows: dot(r[0][c, rows, :], r[1][c], 1, 1),)
IN_FWD = (lambda r, c, rows: dot(r[0][c, :, rows], r[1][c], 0, 0),)
IN_BWD = (lambda r, c, rows: dot(r[1][c, rows, :], r[2][c], 1, 1), lambda r, c, rows: dot(r[0][c, rows, :], r[2][c], 1, 0))
OUT_BWD = (lambda r, c, rows: dot(r[2][c, rows, :], r[1][c], 1, 0), lambda r, c, rows: dot(r[2][c, :, rows], r[0][c], 0, 0))

ALL = 16
SHARE = 112
PACKS = (C + 16, C + 16, 5 * C + 16, 5 * C + 16)


def share(k):
    return pl.ds(pl.multiple_of(k * SHARE, SHARE), SHARE)


def sum_kernel(p0, p1, p2, p3, tot_ref, send_ref, got_ref, part_ref, ss, rs, ss2, rs2):
    dp, dap = lax.axis_index("dp"), lax.axis_index("dap")
    me = dp * GROUP + dap
    others = [(me + k) % ALL for k in range(1, ALL)]
    ids = [{"dp": o // GROUP, "dap": o % GROUP} for o in others]
    sem = pltpu.get_barrier_semaphore()
    for to in ids:
        pl.semaphore_signal(sem, inc=1, device_id=to, device_id_type=pl.DeviceIdType.MESH)
    at = 0
    for ref, rows in zip((p0, p1, p2, p3), PACKS):
        send_ref[at:at + rows, :] = ref[...].astype(BF16)
        at += rows
    send_ref[at:, :] = jnp.zeros((ALL * SHARE - at, C), BF16)
    pl.semaphore_wait(sem, ALL - 1)

    def first(to, k, frm):
        return pltpu.make_async_remote_copy(send_ref.at[share(others[k])], got_ref.at[frm], ss.at[k], rs.at[frm], device_id=to, device_id_type=pl.DeviceIdType.MESH)

    def second(to, k, frm):
        return pltpu.make_async_remote_copy(part_ref, tot_ref.at[share(frm)], ss2.at[k], rs2.at[frm], device_id=to, device_id_type=pl.DeviceIdType.MESH)

    for k, to in enumerate(ids):
        first(to, k, me).start()
    got_ref[me] = send_ref[share(me), :]
    for k, to in enumerate(ids):
        first(to, k, others[k]).wait_recv()
    total = got_ref[0].astype(F32)
    for k in range(1, ALL):
        total = total + got_ref[k].astype(F32)
    part_ref[...] = total
    for k, to in enumerate(ids):
        second(to, k, me).start()
    tot_ref[share(me), :] = total
    for k, to in enumerate(ids):
        second(to, k, others[k]).wait_recv()
    for k, to in enumerate(ids):
        first(to, k, me).wait_send()
        second(to, k, me).wait_send()


def split_kernel(tot, d_ln_in, d_w_proj, d_b_proj, d_ln_mid, d_w_out, d_b_out):
    at = 0
    for k in range(2):
        d_w_out[k] = tot[at:at + C, :]
        d_ln_mid[k] = tot[at + C:at + C + 2, :]
        d_b_out[k:k + 1, :] = tot[at + C + 2:at + C + 3, :]
        at += C + 16
    for k in range(2):
        for j in range(5):
            d_w_proj[k, :, j * C:(j + 1) * C] = tot[at + j * C:at + (j + 1) * C, :].T
            d_b_proj[k:k + 1, j * C:(j + 1) * C] = tot[at + 5 * C + j:at + 5 * C + j + 1, :]
        d_ln_in[k] = tot[at + 5 * C + 5:at + 5 * C + 7, :]
        at += 5 * C + 16


def sum_grads(packs):
    vmem = pl.BlockSpec(memory_space=pltpu.VMEM)
    dma = pltpu.SemaphoreType.DMA((ALL,))
    total = pl.pallas_call(
        sum_kernel,
        in_specs=[vmem] * 4,
        out_specs=vmem,
        out_shape=jax.ShapeDtypeStruct((ALL * SHARE, C), F32),
        scratch_shapes=[pltpu.VMEM((ALL * SHARE, C), BF16), pltpu.VMEM((ALL, SHARE, C), BF16), pltpu.VMEM((SHARE, C), F32), dma, dma, dma, dma],
        compiler_params=pltpu.CompilerParams(vmem_limit_bytes=VMEM_LIMIT, collective_id=8, has_side_effects=True),
        name="sum",
    )(*packs)
    shapes = ((2, 2, C), (2, C, 5 * C), (2, 5 * C), (2, 2, C), (2, C, C), (2, C))
    return pl.pallas_call(
        split_kernel,
        in_specs=[vmem],
        out_specs=[vmem] * 6,
        out_shape=[jax.ShapeDtypeStruct(shape, F32) for shape in shapes],
        name="split",
    )(total)


ANY = pl.BlockSpec(memory_space=pl.ANY)
TRI = jax.ShapeDtypeStruct((CH, N, N), BF16)
ROW = jax.ShapeDtypeStruct((ROWS, C, N), BF16)
ROW32 = jax.ShapeDtypeStruct((ROWS, C, N), F32)
NATIVE = jax.ShapeDtypeStruct((ROWS, N, C), BF16)
POST = jax.ShapeDtypeStruct((C + 16, C), F32)
PRE = jax.ShapeDtypeStruct((5 * C + 16, C), F32)


def by_row(array):
    tail = array.shape[1:]
    return pl.BlockSpec((array.shape[0] // STEPS,) + tail, lambda t: (t,) + (0,) * len(tail))


def whole(array):
    zeros = (0,) * len(array.shape)
    return pl.BlockSpec(array.shape, lambda t: zeros)


def params(collective_id):
    if collective_id is None:
        return pltpu.CompilerParams(dimension_semantics=("arbitrary",), vmem_limit_bytes=VMEM_LIMIT)
    return pltpu.CompilerParams(dimension_semantics=("arbitrary",), vmem_limit_bytes=VMEM_LIMIT, collective_id=collective_id, has_side_effects=True)


def row_call(kernel, name, collective_id, ins, consts, outs, specs, n_send, scratch):
    sent = [pltpu.VMEM((2, 2 * C * STEP, C), F32)] * n_send + [pltpu.VMEM((ROWS // SEND, C, SEND, N), BF16)] * n_send
    sems = [pltpu.SemaphoreType.DMA((ROWS // SEND, GROUP))] * n_send + ([pltpu.SemaphoreType.DMA((n_send,))] if n_send else [])
    return pl.pallas_call(
        kernel,
        grid=(STEPS,),
        in_specs=[by_row(x) for x in ins] + [whole(x) for x in consts],
        out_specs=specs,
        out_shape=outs,
        scratch_shapes=sent + scratch + sems,
        compiler_params=params(collective_id),
        name=name,
    )(*ins, *consts)


def channel_call(products, name, collective_id, ins, n_out):
    return pl.pallas_call(
        functools.partial(channel_kernel, products, len(ins), n_out),
        grid=(2,),
        in_specs=[whole(x) for x in ins],
        out_specs=[ANY] * n_out,
        out_shape=[ROW] * n_out,
        scratch_shapes=[pltpu.VMEM((4 * HALF * 8, C), F32)] * n_out + [pltpu.VMEM((2, HALF, CH, N), BF16)] * n_out
        + [pltpu.SemaphoreType.DMA((2, 4))] * n_out + [pltpu.SemaphoreType.DMA((n_out,))],
        compiler_params=params(collective_id),
        name=name,
    )(*ins)


def local_step(z_pair, pair_mask, dz_out, ln_in, w_proj, b_proj, ln_mid, w_out, b_out):
    z, dz = z_pair[0], dz_out[0]
    mask = pair_mask.reshape(STEPS, STEP, N)
    pre, post = [ln_in, w_proj, b_proj], [ln_mid, w_out, b_out]
    eye = [pltpu.VMEM((C, C), BF16)]
    pre_c = [pltpu.VMEM((2, C, N), F32), pltpu.VMEM((5 * C, C), BF16), pltpu.VMEM((5 * C, N), F32)]
    post_c = [pltpu.VMEM((2, C, N), F32), pltpu.VMEM((C, C), BF16), pltpu.VMEM((C, N), F32)]
    post_acc = [pltpu.VMEM((4, C, C), F32)]
    pre_acc = [pltpu.VMEM((5 * C, C), F32), pltpu.VMEM((5 * C, C), F32), pltpu.VMEM((2, C, C), F32)]

    a0, b0, g0 = row_call(pre_kernel, "pre0", 0, [z, mask], pre, [TRI, TRI, ROW32], [ANY, ANY, by_row(ROW32)], 2, eye + pre_c)
    x0, = channel_call(OUT_FWD, "tri0", 1, [a0, b0], 1)
    a1, b1, g1, zm = row_call(mid_kernel, "mid", 2, [x0, z, g0, mask], post + pre, [TRI, TRI, ROW32, ROW],
                              [ANY, ANY, by_row(ROW32), by_row(ROW)], 2, eye + pre_c + post_c)
    x1, = channel_call(IN_FWD, "tri1", 3, [a1, b1], 1)
    dx1, z_new, dpg1, post_g1 = row_call(turn_kernel, "turn", 4, [x1, zm, g1, dz], post, [TRI, NATIVE, ROW32, POST],
                                         [ANY, by_row(NATIVE), by_row(ROW32), whole(POST)], 1, eye + post_c + post_acc)
    da1, db1 = channel_call(IN_BWD, "trib1", 5, [a1, b1, dx1], 2)
    dx0, dzm, dpg0, pre_g1, post_g0 = row_call(
        back_kernel, "back", 6, [da1, db1, dpg1, zm, mask, dz, x0, g0], pre + post, [TRI, ROW, ROW32, PRE, POST],
        [ANY, by_row(ROW), by_row(ROW32), whole(PRE), whole(POST)], 1, eye + pre_c + post_c + pre_acc + post_acc)
    da0, db0 = channel_call(OUT_BWD, "trib0", 7, [a0, b0, dx0], 2)
    dz_new, pre_g0 = row_call(last_kernel, "last", None, [da0, db0, dpg0, z, mask, dzm], pre, [NATIVE, PRE],
                              [by_row(NATIVE), whole(PRE)], 0, eye + pre_c + pre_acc)
    return (z_new[None], dz_new[None], *sum_grads([post_g0, post_g1, pre_g0, pre_g1]))


def solution(mesh):
    row_spec = P("dp", "dap")
    return jax.shard_map(local_step, mesh=mesh, in_specs=(row_spec,) * 3 + (P(),) * 6,
                         out_specs=(row_spec,) * 2 + (P(),) * 6, check_vma=False)
```

```python
import functools

import jax
import jax.numpy as jnp
from jax import lax
from jax.experimental import pallas as pl
from jax.experimental.pallas import tpu as pltpu
from jax.sharding import PartitionSpec as P

LN_EPS = 1e-5
N = 256
C = 128
GROUP = 8
ROWS = N // GROUP
CH = C // GROUP
STEP = 8
UNROLL = 4
STEPS = ROWS // STEP
F32 = jnp.float32
BF16 = jnp.bfloat16
VMEM_LIMIT = 62 * 1024 * 1024


def dot(lhs, rhs, lhs_dim, rhs_dim):
    return lax.dot_general(lhs, rhs, (((lhs_dim,), (rhs_dim,)), ((), ())), preferred_element_type=F32)


def norm(values):
    mean = jnp.mean(values, axis=0, keepdims=True)
    cen = values - mean
    inv = lax.rsqrt(jnp.mean(cen * cen, axis=0, keepdims=True) + LN_EPS)
    return cen * inv, inv


def norm_back(d_hat, unit, inv, gain):
    d_unit = d_hat * gain
    mean_d = jnp.mean(d_unit, axis=0, keepdims=True)
    mean_du = jnp.mean(d_unit * unit, axis=0, keepdims=True)
    return inv * (d_unit - mean_d - unit * mean_du)


def fold(values):
    return values[:, :C] + values[:, C:]


def row_sums(acc):
    return jnp.sum(acc.T, axis=0, keepdims=True)


def sigmoid(values):
    return 0.5 * jnp.tanh(0.5 * values) + 0.5


def project(z_t, ln, w_t, bias):
    unit, inv = norm(z_t)
    z_hat = (unit * ln[0] + ln[1]).astype(BF16)
    return unit, inv, z_hat, dot(w_t[...], z_hat, 1, 0) + bias[...]


def set_eye(eye):
    same = lax.broadcasted_iota(jnp.int32, (C, C), 0) == lax.broadcasted_iota(jnp.int32, (C, C), 1)
    eye[...] = jnp.where(same, 1.0, 0.0).astype(BF16)


def set_column(ref, row):
    column = jnp.broadcast_to(row.astype(F32), (C, C)).T
    ref[:, :C] = column
    ref[:, C:] = column


def set_pre(block, ln_in, w_proj, b_proj, ln, w_t, bias):
    for k in range(2):
        set_column(ln.at[k], ln_in[block, k:k + 1, :])
    for k in range(5):
        cols = slice(k * C, (k + 1) * C)
        set_column(bias.at[cols], b_proj[block:block + 1, cols])
        w_t[cols, :] = w_proj[block, :, cols].astype(F32).T.astype(BF16)


def set_post(block, ln_mid, w_out, b_out, mln, wo_t, bo):
    for k in range(2):
        set_column(mln.at[k], ln_mid[block, k:k + 1, :])
    set_column(bo, b_out[block:block + 1, :])
    wo_t[...] = w_out[block].astype(F32).T.astype(BF16)


def place():
    me = lax.axis_index("dap")
    return me, me // 4, (me // 2) % 2, me % 2


def enter():
    me = lax.axis_index("dap")
    sem = pltpu.get_barrier_semaphore()
    for k in range(1, GROUP):
        pl.semaphore_signal(sem, inc=1, device_id={"dap": (me + k) % GROUP}, device_id_type=pl.DeviceIdType.MESH)


def all_in():
    pl.semaphore_wait(pltpu.get_barrier_semaphore(), GROUP - 1)


def peers():
    me, cy, cx, core = place()
    out = []
    for dy, dx in ((1, 1), (1, 0), (0, 1), (0, 0)):
        for dc in (1, 0):
            out.append((((cy + dy) % 2) * 2 + (cx + dx) % 2) * 2 + (core + dc) % 2)
    return me, out


def spread(ref, value, row):
    for h in range(2):
        ref[pl.ds(h * C * STEP + row, C, stride=STEP), :] = value[:, h * C:(h + 1) * C]


def pack_rows(stage, send_ref, slot):
    for h in range(2):
        for q in range(4):
            rows = stage[pl.ds((h * C + q * 32) * STEP, 32 * STEP), :].reshape(32, STEP, C)
            send_ref[slot, q * 32:(q + 1) * 32, :, h * C:(h + 1) * C] = rows.astype(BF16)


def move(src_ref, dst_ref, send_sem, recv_sem, dest, own):
    if own:
        return pltpu.make_async_copy(src_ref, dst_ref, recv_sem)
    return pltpu.make_async_remote_copy(src_ref, dst_ref, send_sem, recv_sem, device_id={"dap": dest}, device_id_type=pl.DeviceIdType.MESH)


def wait_sends(copies):
    for copy in copies:
        if copy.is_remote:
            copy.wait_send()


def row_copies(send_ref, out_ref, send_sem, recv_sem, slot):
    me, dests = peers()
    start = pl.multiple_of(me * ROWS + slot * STEP, STEP)
    return [
        move(send_ref.at[slot, pl.ds(pl.multiple_of(dest * CH, CH), CH)], out_ref.at[:, pl.ds(start, STEP), :],
             send_sem.at[slot, k], recv_sem, dest, k == GROUP - 1)
        for k, dest in enumerate(dests)
    ]


def send_rows(step, jobs):
    pl.when(step == 0)(all_in)
    for stage, send_ref, out_ref, send_sem, recv_sem in jobs:
        pack_rows(stage, send_ref, step)
        for copy in row_copies(send_ref, out_ref, send_sem, recv_sem, step):
            copy.start()

    @pl.when(step == STEPS - 1)
    def _():
        for stage, send_ref, out_ref, send_sem, recv_sem in jobs:
            for slot in range(STEPS):
                wait_sends(row_copies(send_ref, out_ref, send_sem, recv_sem, slot))
            pltpu.make_async_copy(out_ref, out_ref, recv_sem).wait()


def rows_loop(body):
    def step(r, carry):
        body(r)
        return carry

    lax.fori_loop(0, STEP, step, 0, unroll=UNROLL)


def pre_row(r, z_t, mask_ref, ln_ref, w_t_ref, bias_ref, g_ref, keep_ref, unit_ref, inv_ref, a_stage, b_stage):
    unit, inv, _, p = project(z_t, ln_ref, w_t_ref, bias_ref)
    unit_ref[r] = unit
    inv_ref[0, pl.ds(r, 1), :] = inv
    m = mask_ref[0, pl.ds(r, 1), :].astype(F32)
    for side, stage in ((0, a_stage), (1, b_stage)):
        s = sigmoid(p[2 * side * C:(2 * side + 1) * C])
        v = p[(2 * side + 1) * C:(2 * side + 2) * C]
        sm = s * m
        spread(stage, sm * v, r)
        keep_ref[r, 2 * side] = sm
        keep_ref[r, 2 * side + 1] = v * (1.0 - s)
    g_ref[r] = sigmoid(p[4 * C:])


def pre_kernel(z_ref, mask_ref, ln_in, w_proj, b_proj, a_ref, b_ref, g_ref, keep_ref, unit_ref, inv_ref, a_st, b_st, a_send, b_send,
               eye_ref, ln_ref, w_t_ref, bias_ref, a_ss, b_ss, rs):
    step = pl.program_id(0)

    @pl.when(step == 0)
    def _():
        enter()
        set_eye(eye_ref)
        set_pre(0, ln_in, w_proj, b_proj, ln_ref, w_t_ref, bias_ref)

    @rows_loop
    def _(r):
        z_t = dot(eye_ref[...], z_ref[r], 1, 1)
        pre_row(r, z_t, mask_ref, ln_ref, w_t_ref, bias_ref, g_ref, keep_ref, unit_ref, inv_ref, a_st, b_st)

    send_rows(step, [(a_st, a_send, a_ref, a_ss, rs.at[0]), (b_st, b_send, b_ref, b_ss, rs.at[1])])


def mid_kernel(x_ref, z_ref, g0_ref, mask_ref, ln_mid, w_out, b_out, ln_in, w_proj, b_proj,
               a_ref, b_ref, g_ref, keep_ref, unit_ref, inv_ref, zm_ref, gu_ref, munit_ref, minv_ref, a_st, b_st, a_send, b_send,
               eye_ref, ln_ref, w_t_ref, bias_ref, mln_ref, wo_t_ref, bo_ref, a_ss, b_ss, rs):
    step = pl.program_id(0)

    @pl.when(step == 0)
    def _():
        enter()
        set_eye(eye_ref)
        set_pre(1, ln_in, w_proj, b_proj, ln_ref, w_t_ref, bias_ref)
        set_post(0, ln_mid, w_out, b_out, mln_ref, wo_t_ref, bo_ref)

    @rows_loop
    def _(r):
        unit, inv = norm(x_ref[r].astype(F32))
        munit_ref[r] = unit
        minv_ref[0, pl.ds(r, 1), :] = inv
        x_hat = (unit * mln_ref[0] + mln_ref[1]).astype(BF16)
        update = dot(wo_t_ref[...], x_hat, 1, 0) + bo_ref[...]
        g = g0_ref[r]
        change = g * update
        gu_ref[r] = change * (1.0 - g)
        z_new = (dot(eye_ref[...], z_ref[r], 1, 1) + change).astype(BF16)
        zm_ref[r] = z_new
        pre_row(r, z_new.astype(F32), mask_ref, ln_ref, w_t_ref, bias_ref, g_ref, keep_ref, unit_ref, inv_ref, a_st, b_st)

    send_rows(step, [(a_st, a_send, a_ref, a_ss, rs.at[0]), (b_st, b_send, b_ref, b_ss, rs.at[1])])


def post_back_row(unit, inv, g, dz, mln_ref, wo_ref, acc_ref, x_hat=None):
    if x_hat is None:
        x_hat = (unit * mln_ref[0] + mln_ref[1]).astype(BF16)
    d_up = dz * g
    d_up_bf = d_up.astype(BF16)
    acc_ref[0] += dot(x_hat, d_up_bf, 1, 1)
    acc_ref[3] += fold(d_up)
    d_hat = dot(wo_ref[...], d_up_bf, 1, 0).astype(BF16).astype(F32)
    acc_ref[1] += fold(d_hat * unit)
    acc_ref[2] += fold(d_hat)
    return norm_back(d_hat, unit, inv, mln_ref[0])


def put_post(grad_ref, acc_ref):
    grad_ref[0:C, :] = acc_ref[0]
    grad_ref[C:C + 8, :] = jnp.concatenate([row_sums(acc_ref[1]), row_sums(acc_ref[2]), row_sums(acc_ref[3]), jnp.zeros((5, C), F32)], axis=0)
    grad_ref[C + 8:C + 16, :] = jnp.zeros((8, C), F32)


def turn_kernel(x_ref, zm_ref, g_ref, dz_ref, ln_mid, w_out, b_out,
                dx_ref, z_out_ref, dpg_ref, grad_ref, d_st, d_send, eye_ref, mln_ref, wo_t_ref, bo_ref, acc_ref, d_ss, rs):
    step = pl.program_id(0)
    wo_ref = w_out.at[1]

    @pl.when(step == 0)
    def _():
        enter()
        set_eye(eye_ref)
        set_post(1, ln_mid, w_out, b_out, mln_ref, wo_t_ref, bo_ref)
        acc_ref[...] = jnp.zeros_like(acc_ref)

    @rows_loop
    def _(r):
        dz = dot(eye_ref[...], dz_ref[r], 1, 1)
        g = g_ref[r]
        unit, inv = norm(x_ref[r].astype(F32))
        x_hat = (unit * mln_ref[0] + mln_ref[1]).astype(BF16)
        change = g * (dot(wo_t_ref[...], x_hat, 1, 0) + bo_ref[...])
        dpg_ref[r] = dz * change * (1.0 - g)
        z_out_ref[r] = (zm_ref[r].astype(F32) + change).T.astype(BF16)
        spread(d_st, post_back_row(unit, inv, g, dz, mln_ref, wo_ref, acc_ref, x_hat), r)

    @pl.when(step == STEPS - 1)
    def _():
        put_post(grad_ref, acc_ref)

    send_rows(step, [(d_st, d_send, dx_ref, d_ss, rs.at[0])])


def pre_back_row(unit, inv, keep, da, db, d_pg, ln_ref, w_ref, w_acc, b_acc, l_acc):
    z_hat = (unit * ln_ref[0] + ln_ref[1]).astype(BF16)
    parts = []
    for side, d_side in ((0, da), (1, db)):
        d_v = d_side * keep[2 * side]
        parts += [d_v * keep[2 * side + 1], d_v]
    parts.append(d_pg)
    for k, part in enumerate(parts):
        b_acc[k * C:(k + 1) * C, :] += fold(part)
    d_p = jnp.concatenate([part.astype(BF16) for part in parts], axis=0)
    w_acc[...] += dot(d_p, z_hat, 1, 1)
    d_hat = dot(w_ref[...], d_p, 1, 0).astype(BF16).astype(F32)
    l_acc[0] += fold(d_hat * unit)
    l_acc[1] += fold(d_hat)
    return norm_back(d_hat, unit, inv, ln_ref[0])


def put_pre(grad_ref, w_acc, b_acc, l_acc):
    grad_ref[0:5 * C, :] = w_acc[...]
    rows = [row_sums(b_acc[k * C:(k + 1) * C, :]) for k in range(5)]
    rows += [row_sums(l_acc[0]), row_sums(l_acc[1]), jnp.zeros((1, C), F32)]
    grad_ref[5 * C:5 * C + 8, :] = jnp.concatenate(rows, axis=0)
    grad_ref[5 * C + 8:5 * C + 16, :] = jnp.zeros((8, C), F32)


def set_gains(ref, ln, block):
    for k in range(2):
        set_column(ref.at[k], ln[block, k:k + 1, :])


def back_kernel(da_ref, db_ref, dpg1_ref, keep_ref, unit_ref, inv_ref, dz_ref, munit_ref, minv_ref, g_ref, gu_ref, ln_in, w_proj, ln_mid, w_out,
                dx_ref, dzm_ref, dpg_ref, grad1_ref, grad0_ref, d_st, d_send,
                eye_ref, ln_ref, mln_ref, w_acc, b_acc, l_acc, acc_ref, d_ss, rs):
    step = pl.program_id(0)
    w_ref, wo_ref = w_proj.at[1], w_out.at[0]

    @pl.when(step == 0)
    def _():
        enter()
        set_eye(eye_ref)
        set_gains(ln_ref, ln_in, 1)
        set_gains(mln_ref, ln_mid, 0)
        for ref in (w_acc, b_acc, l_acc, acc_ref):
            ref[...] = jnp.zeros_like(ref)

    @rows_loop
    def _(r):
        at = pl.ds(r, 1)
        dzn = pre_back_row(unit_ref[r], inv_ref[0, at, :], keep_ref.at[r], da_ref[r].astype(F32), db_ref[r].astype(F32), dpg1_ref[r],
                           ln_ref, w_ref, w_acc, b_acc, l_acc)
        dzm = (dot(eye_ref[...], dz_ref[r], 1, 1) + dzn).astype(BF16)
        dzm_ref[r] = dzm
        dzm = dzm.astype(F32)
        dpg_ref[r] = dzm * gu_ref[r]
        spread(d_st, post_back_row(munit_ref[r], minv_ref[0, at, :], g_ref[r], dzm, mln_ref, wo_ref, acc_ref), r)

    @pl.when(step == STEPS - 1)
    def _():
        put_pre(grad1_ref, w_acc, b_acc, l_acc)
        put_post(grad0_ref, acc_ref)

    send_rows(step, [(d_st, d_send, dx_ref, d_ss, rs.at[0])])


def last_kernel(da_ref, db_ref, dpg_ref, keep_ref, unit_ref, inv_ref, dzm_ref, ln_in, w_proj,
                dz_ref, grad_ref, ln_ref, w_acc, b_acc, l_acc):
    step = pl.program_id(0)
    w_ref = w_proj.at[0]

    @pl.when(step == 0)
    def _():
        set_gains(ln_ref, ln_in, 0)
        for ref in (w_acc, b_acc, l_acc):
            ref[...] = jnp.zeros_like(ref)

    @rows_loop
    def _(r):
        dzn = pre_back_row(unit_ref[r], inv_ref[0, pl.ds(r, 1), :], keep_ref.at[r], da_ref[r].astype(F32), db_ref[r].astype(F32), dpg_ref[r],
                           ln_ref, w_ref, w_acc, b_acc, l_acc)
        dz_ref[r] = (dzm_ref[r].astype(F32) + dzn).T.astype(BF16)

    @pl.when(step == STEPS - 1)
    def _():
        put_pre(grad_ref, w_acc, b_acc, l_acc)


HALF = N // 2


def spread_channel(stage, value, c):
    for h in range(2):
        stage[pl.ds((h * 2 + c // 8) * HALF * 8 + c % 8, HALF, stride=8), :] = value[:, h * C:(h + 1) * C]


def pack_channels(stage, send_ref, slot):
    for h in range(2):
        for q in range(4):
            lo = stage[pl.ds((h * 2) * HALF * 8 + q * 256, 256), :].reshape(32, 8, C)
            hi = stage[pl.ds((h * 2 + 1) * HALF * 8 + q * 256, 256), :].reshape(32, 8, C)
            send_ref[slot, q * 32:(q + 1) * 32, :, h * C:(h + 1) * C] = jnp.concatenate([lo, hi], axis=1).astype(BF16)


def channel_copies(send_ref, out_ref, send_sem, recv_sem, slot, top):
    me, cy, cx, core = place()
    out = []
    k = 0
    for dx in (1, 0):
        for dc in (1, 0):
            within = ((cx + dx) % 2) * 2 + (core + dc) % 2
            out.append(move(send_ref.at[slot, pl.ds(pl.multiple_of(within * ROWS, ROWS), ROWS)],
                            out_ref.at[:, pl.ds(pl.multiple_of(me * CH, CH), CH), :],
                            send_sem.at[slot, k], recv_sem, top * 4 + within, slot == 1 and k == 3))
            k += 1
    return out


def channel_kernel(products, n_in, n_out, *refs):
    ins, outs = refs[:n_in], refs[n_in:n_in + n_out]
    stages = refs[n_in + n_out:n_in + 2 * n_out]
    sends = refs[n_in + 2 * n_out:n_in + 3 * n_out]
    sems = refs[n_in + 3 * n_out:n_in + 4 * n_out]
    rs = refs[-1]
    step = pl.program_id(0)
    pl.when(step == 0)(enter)
    _, cy, _, _ = place()
    top = (cy + 1 + step) % 2
    rows = pl.ds(pl.multiple_of(top * HALF, HALF), HALF)
    for j in range(n_out):
        for c in range(CH):
            spread_channel(stages[j], products[j](ins, c, rows), c)
        for slot in range(2):
            @pl.when(step == slot)
            def _():
                pack_channels(stages[j], sends[j], slot)
                if slot == 0 and j == 0:
                    all_in()
                for copy in channel_copies(sends[j], outs[j], sems[j], rs.at[j], slot, top):
                    copy.start()

    @pl.when(step == 1)
    def _():
        for j in range(n_out):
            for slot in range(2):
                wait_sends(channel_copies(sends[j], outs[j], sems[j], rs.at[j], slot, (cy + 1 + slot) % 2))
            pltpu.make_async_copy(outs[j], outs[j], rs.at[j]).wait()


OUT_FWD = (lambda r, c, rows: dot(r[0][c, rows, :], r[1][c], 1, 1),)
IN_FWD = (lambda r, c, rows: dot(r[0][c, :, rows], r[1][c], 0, 0),)
IN_BWD = (lambda r, c, rows: dot(r[1][c, rows, :], r[2][c], 1, 1), lambda r, c, rows: dot(r[0][c, rows, :], r[2][c], 1, 0))
OUT_BWD = (lambda r, c, rows: dot(r[2][c, rows, :], r[1][c], 1, 0), lambda r, c, rows: dot(r[2][c, :, rows], r[0][c], 0, 0))

ALL = 16
SHARE = 112
PACKS = (C + 16, C + 16, 5 * C + 16, 5 * C + 16)


def share(k):
    return pl.ds(pl.multiple_of(k * SHARE, SHARE), SHARE)


def sum_kernel(p0, p1, p2, p3, tot_ref, send_ref, got_ref, part_ref, ss, rs, ss2, rs2):
    dp, dap = lax.axis_index("dp"), lax.axis_index("dap")
    me = dp * GROUP + dap
    others = [(me + k) % ALL for k in range(1, ALL)]
    ids = [{"dp": o // GROUP, "dap": o % GROUP} for o in others]
    sem = pltpu.get_barrier_semaphore()
    for to in ids:
        pl.semaphore_signal(sem, inc=1, device_id=to, device_id_type=pl.DeviceIdType.MESH)
    at = 0
    for ref, rows in zip((p0, p1, p2, p3), PACKS):
        send_ref[at:at + rows, :] = ref[...].astype(BF16)
        at += rows
    send_ref[at:, :] = jnp.zeros((ALL * SHARE - at, C), BF16)
    pl.semaphore_wait(sem, ALL - 1)

    def first(to, k, frm):
        return pltpu.make_async_remote_copy(send_ref.at[share(others[k])], got_ref.at[frm], ss.at[k], rs.at[frm], device_id=to, device_id_type=pl.DeviceIdType.MESH)

    def second(to, k, frm):
        return pltpu.make_async_remote_copy(part_ref, tot_ref.at[share(frm)], ss2.at[k], rs2.at[frm], device_id=to, device_id_type=pl.DeviceIdType.MESH)

    for k, to in enumerate(ids):
        first(to, k, me).start()
    got_ref[me] = send_ref[share(me), :]
    for k, to in enumerate(ids):
        first(to, k, others[k]).wait_recv()
    total = got_ref[0].astype(F32)
    for k in range(1, ALL):
        total = total + got_ref[k].astype(F32)
    part_ref[...] = total
    for k, to in enumerate(ids):
        second(to, k, me).start()
    tot_ref[share(me), :] = total
    for k, to in enumerate(ids):
        second(to, k, others[k]).wait_recv()
    for k, to in enumerate(ids):
        first(to, k, me).wait_send()
        second(to, k, me).wait_send()


def split_kernel(tot, d_ln_in, d_w_proj, d_b_proj, d_ln_mid, d_w_out, d_b_out):
    at = 0
    for k in range(2):
        d_w_out[k] = tot[at:at + C, :]
        d_ln_mid[k] = tot[at + C:at + C + 2, :]
        d_b_out[k:k + 1, :] = tot[at + C + 2:at + C + 3, :]
        at += C + 16
    for k in range(2):
        for j in range(5):
            d_w_proj[k, :, j * C:(j + 1) * C] = tot[at + j * C:at + (j + 1) * C, :].T
            d_b_proj[k:k + 1, j * C:(j + 1) * C] = tot[at + 5 * C + j:at + 5 * C + j + 1, :]
        d_ln_in[k] = tot[at + 5 * C + 5:at + 5 * C + 7, :]
        at += 5 * C + 16


def sum_grads(packs):
    vmem = pl.BlockSpec(memory_space=pltpu.VMEM)
    dma = pltpu.SemaphoreType.DMA((ALL,))
    total = pl.pallas_call(
        sum_kernel,
        in_specs=[vmem] * 4,
        out_specs=vmem,
        out_shape=jax.ShapeDtypeStruct((ALL * SHARE, C), F32),
        scratch_shapes=[pltpu.VMEM((ALL * SHARE, C), BF16), pltpu.VMEM((ALL, SHARE, C), BF16), pltpu.VMEM((SHARE, C), F32), dma, dma, dma, dma],
        compiler_params=pltpu.CompilerParams(vmem_limit_bytes=VMEM_LIMIT, collective_id=8, has_side_effects=True),
        name="sum",
    )(*packs)
    shapes = ((2, 2, C), (2, C, 5 * C), (2, 5 * C), (2, 2, C), (2, C, C), (2, C))
    return pl.pallas_call(
        split_kernel,
        in_specs=[vmem],
        out_specs=[vmem] * 6,
        out_shape=[jax.ShapeDtypeStruct(shape, F32) for shape in shapes],
        name="split",
    )(total)


ANY = pl.BlockSpec(memory_space=pl.ANY)
TRI = jax.ShapeDtypeStruct((CH, N, N), BF16)
ROW = jax.ShapeDtypeStruct((ROWS, C, N), BF16)
ROW32 = jax.ShapeDtypeStruct((ROWS, C, N), F32)
NATIVE = jax.ShapeDtypeStruct((ROWS, N, C), BF16)
POST = jax.ShapeDtypeStruct((C + 16, C), F32)
PRE = jax.ShapeDtypeStruct((5 * C + 16, C), F32)
KEEP = jax.ShapeDtypeStruct((ROWS, 4, C, N), F32)
INV = jax.ShapeDtypeStruct((STEPS, STEP, N), F32)


def by_row(array):
    tail = array.shape[1:]
    return pl.BlockSpec((array.shape[0] // STEPS,) + tail, lambda t: (t,) + (0,) * len(tail))


def whole(array):
    zeros = (0,) * len(array.shape)
    return pl.BlockSpec(array.shape, lambda t: zeros)


def params(collective_id):
    if collective_id is None:
        return pltpu.CompilerParams(dimension_semantics=("arbitrary",), vmem_limit_bytes=VMEM_LIMIT)
    return pltpu.CompilerParams(dimension_semantics=("arbitrary",), vmem_limit_bytes=VMEM_LIMIT, collective_id=collective_id, has_side_effects=True)


def row_call(kernel, name, collective_id, ins, consts, outs, specs, n_send, scratch):
    sent = [pltpu.VMEM((2 * C * STEP, C), F32)] * n_send + [pltpu.VMEM((STEPS, C, STEP, N), BF16)] * n_send
    sems = [pltpu.SemaphoreType.DMA((STEPS, GROUP))] * n_send + ([pltpu.SemaphoreType.DMA((n_send,))] if n_send else [])
    return pl.pallas_call(
        kernel,
        grid=(STEPS,),
        in_specs=[by_row(x) for x in ins] + [whole(x) for x in consts],
        out_specs=specs,
        out_shape=outs,
        scratch_shapes=sent + scratch + sems,
        compiler_params=params(collective_id),
        name=name,
    )(*ins, *consts)


def channel_call(products, name, collective_id, ins, n_out):
    return pl.pallas_call(
        functools.partial(channel_kernel, products, len(ins), n_out),
        grid=(2,),
        in_specs=[whole(x) for x in ins],
        out_specs=[ANY] * n_out,
        out_shape=[ROW] * n_out,
        scratch_shapes=[pltpu.VMEM((4 * HALF * 8, C), F32)] * n_out + [pltpu.VMEM((2, HALF, CH, N), BF16)] * n_out
        + [pltpu.SemaphoreType.DMA((2, 4))] * n_out + [pltpu.SemaphoreType.DMA((n_out,))],
        compiler_params=params(collective_id),
        name=name,
    )(*ins)


def local_step(z_pair, pair_mask, dz_out, ln_in, w_proj, b_proj, ln_mid, w_out, b_out):
    z, dz = z_pair[0], dz_out[0]
    mask = pair_mask.reshape(STEPS, STEP, N)
    pre, post = [ln_in, w_proj, b_proj], [ln_mid, w_out, b_out]
    eye = [pltpu.VMEM((C, C), BF16)]
    pre_c = [pltpu.VMEM((2, C, N), F32), pltpu.VMEM((5 * C, C), BF16), pltpu.VMEM((5 * C, N), F32)]
    post_c = [pltpu.VMEM((2, C, N), F32), pltpu.VMEM((C, C), BF16), pltpu.VMEM((C, N), F32)]
    post_acc = [pltpu.VMEM((4, C, C), F32)]
    pre_acc = [pltpu.VMEM((5 * C, C), F32), pltpu.VMEM((5 * C, C), F32), pltpu.VMEM((2, C, C), F32)]

    kept = [by_row(ROW32), by_row(KEEP), by_row(ROW32), by_row(INV)]
    a0, b0, g0, keep0, unit0, inv0 = row_call(pre_kernel, "pre0", 0, [z, mask], pre, [TRI, TRI, ROW32, KEEP, ROW32, INV],
                                              [ANY, ANY, *kept], 2, eye + pre_c)
    x0, = channel_call(OUT_FWD, "tri0", 1, [a0, b0], 1)
    a1, b1, g1, keep1, unit1, inv1, zm, gu0, munit0, minv0 = row_call(
        mid_kernel, "mid", 2, [x0, z, g0, mask], post + pre, [TRI, TRI, ROW32, KEEP, ROW32, INV, ROW, ROW32, ROW32, INV],
        [ANY, ANY, *kept, by_row(ROW), by_row(ROW32), by_row(ROW32), by_row(INV)], 2, eye + pre_c + post_c)
    x1, = channel_call(IN_FWD, "tri1", 3, [a1, b1], 1)
    dx1, z_new, dpg1, post_g1 = row_call(turn_kernel, "turn", 4, [x1, zm, g1, dz], post, [TRI, NATIVE, ROW32, POST],
                                         [ANY, by_row(NATIVE), by_row(ROW32), whole(POST)], 1, eye + post_c + post_acc)
    da1, db1 = channel_call(IN_BWD, "trib1", 5, [a1, b1, dx1], 2)
    gains = [pltpu.VMEM((2, C, N), F32)]
    dx0, dzm, dpg0, pre_g1, post_g0 = row_call(
        back_kernel, "back", 6, [da1, db1, dpg1, keep1, unit1, inv1, dz, munit0, minv0, g0, gu0], [ln_in, w_proj, ln_mid, w_out],
        [TRI, ROW, ROW32, PRE, POST], [ANY, by_row(ROW), by_row(ROW32), whole(PRE), whole(POST)], 1, eye + gains * 2 + pre_acc + post_acc)
    da0, db0 = channel_call(OUT_BWD, "trib0", 7, [a0, b0, dx0], 2)
    dz_new, pre_g0 = row_call(last_kernel, "last", None, [da0, db0, dpg0, keep0, unit0, inv0, dzm], [ln_in, w_proj], [NATIVE, PRE],
                              [by_row(NATIVE), whole(PRE)], 0, gains + pre_acc)
    return (z_new[None], dz_new[None], *sum_grads([post_g0, post_g1, pre_g0, pre_g1]))


def solution(mesh):
    row_spec = P("dp", "dap")
    return jax.shard_map(local_step, mesh=mesh, in_specs=(row_spec,) * 3 + (P(),) * 6,
                         out_specs=(row_spec,) * 2 + (P(),) * 6, check_vma=False)
```

```python
import functools

import jax
import jax.numpy as jnp
from jax import lax
from jax.experimental import pallas as pl
from jax.experimental.pallas import tpu as pltpu
from jax.sharding import PartitionSpec as P

LN_EPS = 1e-5
N = 256
C = 128
GROUP = 8
ROWS = N // GROUP
CH = C // GROUP
STEP = 8
UNROLL = 4
STEPS = ROWS // STEP
F32 = jnp.float32
BF16 = jnp.bfloat16
VMEM_LIMIT = 62 * 1024 * 1024


def dot(lhs, rhs, lhs_dim, rhs_dim):
    return lax.dot_general(lhs, rhs, (((lhs_dim,), (rhs_dim,)), ((), ())), preferred_element_type=F32)


def norm(values):
    mean = jnp.mean(values, axis=0, keepdims=True)
    cen = values - mean
    inv = lax.rsqrt(jnp.mean(cen * cen, axis=0, keepdims=True) + LN_EPS)
    return cen * inv, inv


def norm_back(d_hat, unit, inv, gain):
    d_unit = d_hat * gain
    mean_d = jnp.mean(d_unit, axis=0, keepdims=True)
    mean_du = jnp.mean(d_unit * unit, axis=0, keepdims=True)
    return inv * (d_unit - mean_d - unit * mean_du)


def fold(values):
    return values[:, :C] + values[:, C:]


def row_sums(acc):
    return jnp.sum(acc.T, axis=0, keepdims=True)


def sigmoid(values):
    return 0.5 * jnp.tanh(0.5 * values) + 0.5


def project(z_t, ln, w_t, bias):
    unit, inv = norm(z_t)
    z_hat = (unit * ln[0] + ln[1]).astype(BF16)
    return unit, inv, z_hat, dot(w_t[...], z_hat, 1, 0) + bias[...]


def set_eye(eye):
    same = lax.broadcasted_iota(jnp.int32, (C, C), 0) == lax.broadcasted_iota(jnp.int32, (C, C), 1)
    eye[...] = jnp.where(same, 1.0, 0.0).astype(BF16)


def set_column(ref, row):
    column = jnp.broadcast_to(row.astype(F32), (C, C)).T
    ref[:, :C] = column
    ref[:, C:] = column


def set_pre(block, ln_in, w_proj, b_proj, ln, w_t, bias):
    for k in range(2):
        set_column(ln.at[k], ln_in[block, k:k + 1, :])
    for k in range(5):
        cols = slice(k * C, (k + 1) * C)
        set_column(bias.at[cols], b_proj[block:block + 1, cols])
        w_t[cols, :] = w_proj[block, :, cols].astype(F32).T.astype(BF16)


def set_post(block, ln_mid, w_out, b_out, mln, wo_t, bo):
    for k in range(2):
        set_column(mln.at[k], ln_mid[block, k:k + 1, :])
    set_column(bo, b_out[block:block + 1, :])
    wo_t[...] = w_out[block].astype(F32).T.astype(BF16)


def place():
    me = lax.axis_index("dap")
    return me, me // 4, (me // 2) % 2, me % 2


def enter():
    me = lax.axis_index("dap")
    sem = pltpu.get_barrier_semaphore()
    for k in range(1, GROUP):
        pl.semaphore_signal(sem, inc=1, device_id={"dap": (me + k) % GROUP}, device_id_type=pl.DeviceIdType.MESH)


def all_in():
    pl.semaphore_wait(pltpu.get_barrier_semaphore(), GROUP - 1)


def peers():
    me, cy, cx, core = place()
    out = []
    for dy, dx in ((1, 1), (1, 0), (0, 1), (0, 0)):
        for dc in (1, 0):
            out.append((((cy + dy) % 2) * 2 + (cx + dx) % 2) * 2 + (core + dc) % 2)
    return me, out


def spread(ref, value, row):
    for h in range(2):
        ref[pl.ds(h * C * STEP + row, C, stride=STEP), :] = value[:, h * C:(h + 1) * C]


def pack_rows(stage, send_ref, slot):
    for h in range(2):
        for q in range(4):
            rows = stage[pl.ds((h * C + q * 32) * STEP, 32 * STEP), :].reshape(32, STEP, C)
            send_ref[slot, q * 32:(q + 1) * 32, :, h * C:(h + 1) * C] = rows.astype(BF16)


def move(src_ref, dst_ref, send_sem, recv_sem, dest, own):
    if own:
        return pltpu.make_async_copy(src_ref, dst_ref, recv_sem)
    return pltpu.make_async_remote_copy(src_ref, dst_ref, send_sem, recv_sem, device_id={"dap": dest}, device_id_type=pl.DeviceIdType.MESH)


def wait_sends(copies):
    for copy in copies:
        if copy.is_remote:
            copy.wait_send()


def row_copies(send_ref, out_ref, send_sem, recv_sem, slot):
    me, dests = peers()
    start = pl.multiple_of(me * ROWS + slot * STEP, STEP)
    return [
        move(send_ref.at[slot, pl.ds(pl.multiple_of(dest * CH, CH), CH)], out_ref.at[:, pl.ds(start, STEP), :],
             send_sem.at[slot, k], recv_sem, dest, k == GROUP - 1)
        for k, dest in enumerate(dests)
    ]


def send_rows(step, jobs):
    for stage, send_ref, out_ref, send_sem, recv_sem in jobs:
        pack_rows(stage, send_ref, step)
        for copy in row_copies(send_ref, out_ref, send_sem, recv_sem, step):
            copy.start()

    @pl.when(step == STEPS - 1)
    def _():
        for stage, send_ref, out_ref, send_sem, recv_sem in jobs:
            for slot in range(STEPS):
                wait_sends(row_copies(send_ref, out_ref, send_sem, recv_sem, slot))
            pltpu.make_async_copy(out_ref, out_ref, recv_sem).wait()


OUT_FWD = (lambda r, c: dot(r[0][c], r[1][c], 1, 1),)
IN_FWD = (lambda r, c: dot(r[0][c], r[1][c], 0, 0),)
IN_BWD = (lambda r, c: dot(r[1][c], r[2][c], 1, 1), lambda r, c: dot(r[0][c], r[2][c], 1, 0))
OUT_BWD = (lambda r, c: dot(r[2][c], r[1][c], 1, 0), lambda r, c: dot(r[2][c], r[0][c], 0, 0))


def back_copy(job, t, k, dest, frm):
    stage, send_ref, land_ref, send_sem, recv_sem = job
    return pltpu.make_async_remote_copy(
        send_ref.at[t, dest], land_ref.at[t, :, pl.ds(pl.multiple_of(frm * CH, CH), CH), :], send_sem.at[t, k], recv_sem.at[t, frm],
        device_id={"dap": dest}, device_id_type=pl.DeviceIdType.MESH)


def channel_part(products, ins, jobs):
    for product, job in zip(products, jobs):
        def body(c, carry):
            value = product(ins, c)
            for h in range(2):
                job[0][pl.ds((h * 2 + c // 8) * N * 8 + c % 8, N, stride=8), :] = value[:, h * C:(h + 1) * C]
            return carry

        lax.fori_loop(0, CH, body, 0, unroll=4)
    all_in()
    me, dests = peers()
    for t in range(STEPS):
        for job in jobs:
            stage, send_ref, land_ref = job[:3]
            for dest in range(GROUP):
                for h in range(2):
                    at = h * 2 * N * 8 + (dest * ROWS + t * STEP) * 8
                    lo = stage[pl.ds(at, 64), :].reshape(STEP, 8, C)
                    hi = stage[pl.ds(at + N * 8, 64), :].reshape(STEP, 8, C)
                    send_ref[t, dest, :, :, h * C:(h + 1) * C] = jnp.concatenate([lo, hi], axis=1).astype(BF16)
            for k, dest in enumerate(dests[:-1]):
                back_copy(job, t, k, dest, me).start()
            land_ref[t, :, pl.ds(pl.multiple_of(me * CH, CH), CH), :] = send_ref[t, me]


def arrive(t, jobs):
    me, dests = peers()
    for job in jobs:
        for k, frm in enumerate(dests[:-1]):
            back_copy(job, t, k, frm, frm).wait_recv()

    @pl.when(t == STEPS - 1)
    def _():
        for job in jobs:
            for slot in range(STEPS):
                for k, dest in enumerate(dests[:-1]):
                    back_copy(job, slot, k, dest, me).wait_send()


def rows_loop(body):
    def step(r, carry):
        body(r)
        return carry

    lax.fori_loop(0, STEP, step, 0, unroll=UNROLL)


def pre_row(r, z_t, mask_ref, ln_ref, w_t_ref, bias_ref, g_ref, keep_ref, unit_ref, inv_ref, a_stage, b_stage):
    unit, inv, _, p = project(z_t, ln_ref, w_t_ref, bias_ref)
    unit_ref[r] = unit
    inv_ref[0, pl.ds(r, 1), :] = inv
    m = mask_ref[0, pl.ds(r, 1), :].astype(F32)
    for side, stage in ((0, a_stage), (1, b_stage)):
        s = sigmoid(p[2 * side * C:(2 * side + 1) * C])
        v = p[(2 * side + 1) * C:(2 * side + 2) * C]
        sm = s * m
        spread(stage, sm * v, r)
        keep_ref[r, 2 * side] = sm
        keep_ref[r, 2 * side + 1] = v * (1.0 - s)
    g_ref[r] = sigmoid(p[4 * C:])


def pre_kernel(z_ref, mask_ref, ln_in, w_proj, b_proj, a_ref, b_ref, g_ref, keep_ref, unit_ref, inv_ref, a_st, b_st, a_send, b_send,
               eye_ref, ln_ref, w_t_ref, bias_ref, a_ss, b_ss, rs):
    step = pl.program_id(0)

    @pl.when(step == 0)
    def _():
        enter()
        set_eye(eye_ref)
        set_pre(0, ln_in, w_proj, b_proj, ln_ref, w_t_ref, bias_ref)

    @rows_loop
    def _(r):
        z_t = dot(eye_ref[...], z_ref[r], 1, 1)
        pre_row(r, z_t, mask_ref, ln_ref, w_t_ref, bias_ref, g_ref, keep_ref, unit_ref, inv_ref, a_st, b_st)

    pl.when(step == 0)(all_in)
    send_rows(step, [(a_st, a_send, a_ref, a_ss, rs.at[0]), (b_st, b_send, b_ref, b_ss, rs.at[1])])


def mid_kernel(a_in, b_in, z_ref, g0_ref, mask_ref, ln_mid, w_out, b_out, ln_in, w_proj, b_proj,
               a_ref, b_ref, g_ref, keep_ref, unit_ref, inv_ref, zm_ref, gu_ref, munit_ref, minv_ref, a_st, b_st, a_send, b_send,
               eye_ref, ln_ref, w_t_ref, bias_ref, mln_ref, wo_t_ref, bo_ref, a_ss, b_ss, rs,
               st0, se0, la0, ss0, rv0):
    step = pl.program_id(0)
    jobs = [(st0, se0, la0, ss0, rv0)]

    @pl.when(step == 0)
    def _():
        enter()
        set_eye(eye_ref)
        set_pre(1, ln_in, w_proj, b_proj, ln_ref, w_t_ref, bias_ref)
        set_post(0, ln_mid, w_out, b_out, mln_ref, wo_t_ref, bo_ref)
        channel_part(OUT_FWD, (a_in, b_in), jobs)

    @pl.when(step > 0)
    def _():
        t = step - 1
        arrive(t, jobs)
        x_ref = la0.at[t]

        @rows_loop
        def _(r):
            unit, inv = norm(x_ref[r].astype(F32))
            munit_ref[r] = unit
            minv_ref[0, pl.ds(r, 1), :] = inv
            x_hat = (unit * mln_ref[0] + mln_ref[1]).astype(BF16)
            update = dot(wo_t_ref[...], x_hat, 1, 0) + bo_ref[...]
            g = g0_ref[r]
            change = g * update
            gu_ref[r] = change * (1.0 - g)
            z_new = (dot(eye_ref[...], z_ref[r], 1, 1) + change).astype(BF16)
            zm_ref[r] = z_new
            pre_row(r, z_new.astype(F32), mask_ref, ln_ref, w_t_ref, bias_ref, g_ref, keep_ref, unit_ref, inv_ref, a_st, b_st)

        send_rows(t, [(a_st, a_send, a_ref, a_ss, rs.at[0]), (b_st, b_send, b_ref, b_ss, rs.at[1])])


def post_back_row(unit, inv, g, dz, mln_ref, wo_ref, acc_ref, x_hat=None):
    if x_hat is None:
        x_hat = (unit * mln_ref[0] + mln_ref[1]).astype(BF16)
    d_up = dz * g
    d_up_bf = d_up.astype(BF16)
    acc_ref[0] += dot(x_hat, d_up_bf, 1, 1)
    acc_ref[3] += fold(d_up)
    d_hat = dot(wo_ref[...], d_up_bf, 1, 0).astype(BF16).astype(F32)
    acc_ref[1] += fold(d_hat * unit)
    acc_ref[2] += fold(d_hat)
    return norm_back(d_hat, unit, inv, mln_ref[0])


def put_post(grad_ref, acc_ref):
    grad_ref[0:C, :] = acc_ref[0]
    grad_ref[C:C + 8, :] = jnp.concatenate([row_sums(acc_ref[1]), row_sums(acc_ref[2]), row_sums(acc_ref[3]), jnp.zeros((5, C), F32)], axis=0)
    grad_ref[C + 8:C + 16, :] = jnp.zeros((8, C), F32)


def turn_kernel(a_in, b_in, zm_ref, g_ref, dz_ref, ln_mid, w_out, b_out,
                dx_ref, z_out_ref, dpg_ref, grad_ref, d_st, d_send, eye_ref, mln_ref, wo_t_ref, bo_ref, acc_ref, d_ss, rs,
               st0, se0, la0, ss0, rv0):
    step = pl.program_id(0)
    jobs = [(st0, se0, la0, ss0, rv0)]
    wo_ref = w_out.at[1]

    @pl.when(step == 0)
    def _():
        enter()
        set_eye(eye_ref)
        set_post(1, ln_mid, w_out, b_out, mln_ref, wo_t_ref, bo_ref)
        acc_ref[...] = jnp.zeros_like(acc_ref)
        channel_part(IN_FWD, (a_in, b_in), jobs)

    @pl.when(step > 0)
    def _():
        t = step - 1
        arrive(t, jobs)
        x_ref = la0.at[t]

        @rows_loop
        def _(r):
            dz = dot(eye_ref[...], dz_ref[r], 1, 1)
            g = g_ref[r]
            unit, inv = norm(x_ref[r].astype(F32))
            x_hat = (unit * mln_ref[0] + mln_ref[1]).astype(BF16)
            change = g * (dot(wo_t_ref[...], x_hat, 1, 0) + bo_ref[...])
            dpg_ref[r] = dz * change * (1.0 - g)
            z_out_ref[r] = (zm_ref[r].astype(F32) + change).T.astype(BF16)
            spread(d_st, post_back_row(unit, inv, g, dz, mln_ref, wo_ref, acc_ref, x_hat), r)

        @pl.when(t == STEPS - 1)
        def _():
            put_post(grad_ref, acc_ref)

        send_rows(t, [(d_st, d_send, dx_ref, d_ss, rs.at[0])])


def pre_back_row(unit, inv, keep, da, db, d_pg, ln_ref, w_ref, w_acc, b_acc, l_acc):
    z_hat = (unit * ln_ref[0] + ln_ref[1]).astype(BF16)
    parts = []
    for side, d_side in ((0, da), (1, db)):
        d_v = d_side * keep[2 * side]
        parts += [d_v * keep[2 * side + 1], d_v]
    parts.append(d_pg)
    for k, part in enumerate(parts):
        b_acc[k * C:(k + 1) * C, :] += fold(part)
    d_p = jnp.concatenate([part.astype(BF16) for part in parts], axis=0)
    w_acc[...] += dot(d_p, z_hat, 1, 1)
    d_hat = dot(w_ref[...], d_p, 1, 0).astype(BF16).astype(F32)
    l_acc[0] += fold(d_hat * unit)
    l_acc[1] += fold(d_hat)
    return norm_back(d_hat, unit, inv, ln_ref[0])


def put_pre(grad_ref, w_acc, b_acc, l_acc):
    grad_ref[0:5 * C, :] = w_acc[...]
    rows = [row_sums(b_acc[k * C:(k + 1) * C, :]) for k in range(5)]
    rows += [row_sums(l_acc[0]), row_sums(l_acc[1]), jnp.zeros((1, C), F32)]
    grad_ref[5 * C:5 * C + 8, :] = jnp.concatenate(rows, axis=0)
    grad_ref[5 * C + 8:5 * C + 16, :] = jnp.zeros((8, C), F32)


def set_gains(ref, ln, block):
    for k in range(2):
        set_column(ref.at[k], ln[block, k:k + 1, :])


def back_kernel(a_in, b_in, dx_in, dpg1_ref, keep_ref, unit_ref, inv_ref, dz_ref, munit_ref, minv_ref, g_ref, gu_ref, ln_in, w_proj, ln_mid, w_out,
                dx_ref, dzm_ref, dpg_ref, grad1_ref, grad0_ref, d_st, d_send,
                eye_ref, ln_ref, mln_ref, w_acc, b_acc, l_acc, acc_ref, d_ss, rs,
               st0, st1, se0, se1, la0, la1, ss0, ss1, rv0, rv1):
    step = pl.program_id(0)
    jobs = [(st0, se0, la0, ss0, rv0), (st1, se1, la1, ss1, rv1)]
    w_ref, wo_ref = w_proj.at[1], w_out.at[0]

    @pl.when(step == 0)
    def _():
        enter()
        set_eye(eye_ref)
        set_gains(ln_ref, ln_in, 1)
        set_gains(mln_ref, ln_mid, 0)
        for ref in (w_acc, b_acc, l_acc, acc_ref):
            ref[...] = jnp.zeros_like(ref)
        channel_part(IN_BWD, (a_in, b_in, dx_in), jobs)

    @pl.when(step > 0)
    def _():
        t = step - 1
        arrive(t, jobs)
        da_ref, db_ref = la0.at[t], la1.at[t]

        @rows_loop
        def _(r):
            at = pl.ds(r, 1)
            dzn = pre_back_row(unit_ref[r], inv_ref[0, at, :], keep_ref.at[r], da_ref[r].astype(F32), db_ref[r].astype(F32), dpg1_ref[r],
                               ln_ref, w_ref, w_acc, b_acc, l_acc)
            dzm = (dot(eye_ref[...], dz_ref[r], 1, 1) + dzn).astype(BF16)
            dzm_ref[r] = dzm
            dzm = dzm.astype(F32)
            dpg_ref[r] = dzm * gu_ref[r]
            spread(d_st, post_back_row(munit_ref[r], minv_ref[0, at, :], g_ref[r], dzm, mln_ref, wo_ref, acc_ref), r)

        @pl.when(t == STEPS - 1)
        def _():
            put_pre(grad1_ref, w_acc, b_acc, l_acc)
            put_post(grad0_ref, acc_ref)

        send_rows(t, [(d_st, d_send, dx_ref, d_ss, rs.at[0])])


def last_kernel(a_in, b_in, dx_in, dpg_ref, keep_ref, unit_ref, inv_ref, dzm_ref, ln_in, w_proj,
                dz_ref, grad_ref, ln_ref, w_acc, b_acc, l_acc,
               st0, st1, se0, se1, la0, la1, ss0, ss1, rv0, rv1):
    step = pl.program_id(0)
    jobs = [(st0, se0, la0, ss0, rv0), (st1, se1, la1, ss1, rv1)]
    w_ref = w_proj.at[0]

    @pl.when(step == 0)
    def _():
        enter()
        set_gains(ln_ref, ln_in, 0)
        for ref in (w_acc, b_acc, l_acc):
            ref[...] = jnp.zeros_like(ref)
        channel_part(OUT_BWD, (a_in, b_in, dx_in), jobs)

    @pl.when(step > 0)
    def _():
        t = step - 1
        arrive(t, jobs)
        da_ref, db_ref = la0.at[t], la1.at[t]

        @rows_loop
        def _(r):
            dzn = pre_back_row(unit_ref[r], inv_ref[0, pl.ds(r, 1), :], keep_ref.at[r], da_ref[r].astype(F32), db_ref[r].astype(F32), dpg_ref[r],
                               ln_ref, w_ref, w_acc, b_acc, l_acc)
            dz_ref[r] = (dzm_ref[r].astype(F32) + dzn).T.astype(BF16)

        @pl.when(t == STEPS - 1)
        def _():
            put_pre(grad_ref, w_acc, b_acc, l_acc)


ALL = 16
SHARE = 112
PACKS = (C + 16, C + 16, 5 * C + 16, 5 * C + 16)


def share(k):
    return pl.ds(pl.multiple_of(k * SHARE, SHARE), SHARE)


def sum_kernel(p0, p1, p2, p3, tot_ref, send_ref, got_ref, part_ref, ss, rs, ss2, rs2):
    dp, dap = lax.axis_index("dp"), lax.axis_index("dap")
    me = dp * GROUP + dap
    others = [(me + k) % ALL for k in range(1, ALL)]
    ids = [{"dp": o // GROUP, "dap": o % GROUP} for o in others]
    sem = pltpu.get_barrier_semaphore()
    for to in ids:
        pl.semaphore_signal(sem, inc=1, device_id=to, device_id_type=pl.DeviceIdType.MESH)
    at = 0
    for ref, rows in zip((p0, p1, p2, p3), PACKS):
        send_ref[at:at + rows, :] = ref[...].astype(BF16)
        at += rows
    send_ref[at:, :] = jnp.zeros((ALL * SHARE - at, C), BF16)
    pl.semaphore_wait(sem, ALL - 1)

    def first(to, k, frm):
        return pltpu.make_async_remote_copy(send_ref.at[share(others[k])], got_ref.at[frm], ss.at[k], rs.at[frm], device_id=to, device_id_type=pl.DeviceIdType.MESH)

    def second(to, k, frm):
        return pltpu.make_async_remote_copy(part_ref, tot_ref.at[share(frm)], ss2.at[k], rs2.at[frm], device_id=to, device_id_type=pl.DeviceIdType.MESH)

    for k, to in enumerate(ids):
        first(to, k, me).start()
    got_ref[me] = send_ref[share(me), :]
    for k, to in enumerate(ids):
        first(to, k, others[k]).wait_recv()
    total = got_ref[0].astype(F32)
    for k in range(1, ALL):
        total = total + got_ref[k].astype(F32)
    part_ref[...] = total
    for k, to in enumerate(ids):
        second(to, k, me).start()
    tot_ref[share(me), :] = total
    for k, to in enumerate(ids):
        second(to, k, others[k]).wait_recv()
    for k, to in enumerate(ids):
        first(to, k, me).wait_send()
        second(to, k, me).wait_send()


def split_kernel(tot, d_ln_in, d_w_proj, d_b_proj, d_ln_mid, d_w_out, d_b_out):
    at = 0
    for k in range(2):
        d_w_out[k] = tot[at:at + C, :]
        d_ln_mid[k] = tot[at + C:at + C + 2, :]
        d_b_out[k:k + 1, :] = tot[at + C + 2:at + C + 3, :]
        at += C + 16
    for k in range(2):
        for j in range(5):
            d_w_proj[k, :, j * C:(j + 1) * C] = tot[at + j * C:at + (j + 1) * C, :].T
            d_b_proj[k:k + 1, j * C:(j + 1) * C] = tot[at + 5 * C + j:at + 5 * C + j + 1, :]
        d_ln_in[k] = tot[at + 5 * C + 5:at + 5 * C + 7, :]
        at += 5 * C + 16


def sum_grads(packs):
    vmem = pl.BlockSpec(memory_space=pltpu.VMEM)
    dma = pltpu.SemaphoreType.DMA((ALL,))
    total = pl.pallas_call(
        sum_kernel,
        in_specs=[vmem] * 4,
        out_specs=vmem,
        out_shape=jax.ShapeDtypeStruct((ALL * SHARE, C), F32),
        scratch_shapes=[pltpu.VMEM((ALL * SHARE, C), BF16), pltpu.VMEM((ALL, SHARE, C), BF16), pltpu.VMEM((SHARE, C), F32), dma, dma, dma, dma],
        compiler_params=pltpu.CompilerParams(vmem_limit_bytes=VMEM_LIMIT, collective_id=5, has_side_effects=True),
        name="sum",
    )(*packs)
    shapes = ((2, 2, C), (2, C, 5 * C), (2, 5 * C), (2, 2, C), (2, C, C), (2, C))
    return pl.pallas_call(
        split_kernel,
        in_specs=[vmem],
        out_specs=[vmem] * 6,
        out_shape=[jax.ShapeDtypeStruct(shape, F32) for shape in shapes],
        name="split",
    )(total)


TRI = jax.ShapeDtypeStruct((CH, N, N), BF16)
ROW = jax.ShapeDtypeStruct((ROWS, C, N), BF16)
ROW32 = jax.ShapeDtypeStruct((ROWS, C, N), F32)
NATIVE = jax.ShapeDtypeStruct((ROWS, N, C), BF16)
POST = jax.ShapeDtypeStruct((C + 16, C), F32)
PRE = jax.ShapeDtypeStruct((5 * C + 16, C), F32)
KEEP = jax.ShapeDtypeStruct((ROWS, 4, C, N), F32)
INV = jax.ShapeDtypeStruct((STEPS, STEP, N), F32)


def by_row(array, lead=0):
    tail = array.shape[1:]
    return pl.BlockSpec((array.shape[0] // STEPS,) + tail, lambda s: ((s * STEPS) // (STEPS + lead),) + (0,) * len(tail))


def whole(array):
    zeros = (0,) * len(array.shape)
    return pl.BlockSpec(array.shape, lambda t: zeros, pipeline_mode=pl.Buffered(1))


def out_spec(array, lead):
    if array is TRI:
        return pl.BlockSpec(memory_space=pl.ANY)
    if array in (PRE, POST):
        return pl.BlockSpec(array.shape, lambda t: (0, 0))
    return by_row(array, lead)


def row_call(kernel, name, collective_id, tris, ins, consts, outs, n_back, scratch):
    lead = 1 if tris else 0
    n_send = sum(out is TRI for out in outs)
    dma = pltpu.SemaphoreType.DMA
    sent = [pltpu.VMEM((2 * C * STEP, C), F32)] * n_send + [pltpu.VMEM((STEPS, C, STEP, N), BF16)] * n_send
    sems = [dma((STEPS, GROUP))] * n_send + ([dma((n_send,))] if n_send else [])
    back = [pltpu.VMEM((4 * N * 8, C), F32)] * n_back + [pltpu.VMEM((STEPS, GROUP, STEP, CH, N), BF16)] * n_back
    back += [pltpu.VMEM((STEPS, STEP, C, N), BF16)] * n_back + [dma((STEPS, GROUP))] * (2 * n_back)
    return pl.pallas_call(
        kernel,
        grid=(STEPS + lead,),
        in_specs=[whole(x) for x in tris] + [by_row(x, lead) for x in ins] + [whole(x) for x in consts],
        out_specs=[out_spec(out, lead) for out in outs],
        out_shape=outs,
        scratch_shapes=sent + scratch + sems + back,
        compiler_params=pltpu.CompilerParams(dimension_semantics=("arbitrary",), vmem_limit_bytes=VMEM_LIMIT, collective_id=collective_id, has_side_effects=True),
        name=name,
    )(*tris, *ins, *consts)


def local_step(z_pair, pair_mask, dz_out, ln_in, w_proj, b_proj, ln_mid, w_out, b_out):
    z, dz = z_pair[0], dz_out[0]
    mask = pair_mask.reshape(STEPS, STEP, N)
    pre, post = [ln_in, w_proj, b_proj], [ln_mid, w_out, b_out]
    eye = [pltpu.VMEM((C, C), BF16)]
    pre_c = [pltpu.VMEM((2, C, N), F32), pltpu.VMEM((5 * C, C), BF16), pltpu.VMEM((5 * C, N), F32)]
    post_c = [pltpu.VMEM((2, C, N), F32), pltpu.VMEM((C, C), BF16), pltpu.VMEM((C, N), F32)]
    post_acc = [pltpu.VMEM((4, C, C), F32)]
    pre_acc = [pltpu.VMEM((5 * C, C), F32), pltpu.VMEM((5 * C, C), F32), pltpu.VMEM((2, C, C), F32)]

    gains = [pltpu.VMEM((2, C, N), F32)]
    kept = [TRI, TRI, ROW32, KEEP, ROW32, INV]
    a0, b0, g0, keep0, unit0, inv0 = row_call(pre_kernel, "pre0", 0, [], [z, mask], pre, kept, 0, eye + pre_c)
    a1, b1, g1, keep1, unit1, inv1, zm, gu0, munit0, minv0 = row_call(
        mid_kernel, "mid", 1, [a0, b0], [z, g0, mask], post + pre, kept + [ROW, ROW32, ROW32, INV], 1, eye + pre_c + post_c)
    dx1, z_new, dpg1, post_g1 = row_call(
        turn_kernel, "turn", 2, [a1, b1], [zm, g1, dz], post, [TRI, NATIVE, ROW32, POST], 1, eye + post_c + post_acc)
    dx0, dzm, dpg0, pre_g1, post_g0 = row_call(
        back_kernel, "back", 3, [a1, b1, dx1], [dpg1, keep1, unit1, inv1, dz, munit0, minv0, g0, gu0], [ln_in, w_proj, ln_mid, w_out],
        [TRI, ROW, ROW32, PRE, POST], 2, eye + gains * 2 + pre_acc + post_acc)
    dz_new, pre_g0 = row_call(
        last_kernel, "last", 4, [a0, b0, dx0], [dpg0, keep0, unit0, inv0, dzm], [ln_in, w_proj], [NATIVE, PRE], 2, gains + pre_acc)
    return (z_new[None], dz_new[None], *sum_grads([post_g0, post_g1, pre_g0, pre_g1]))


def solution(mesh):
    row_spec = P("dp", "dap")
    return jax.shard_map(local_step, mesh=mesh, in_specs=(row_spec,) * 3 + (P(),) * 6,
                         out_specs=(row_spec,) * 2 + (P(),) * 6, check_vma=False)
```

```python
import functools

import jax
import jax.numpy as jnp
from jax import lax
from jax.experimental import pallas as pl
from jax.experimental.pallas import tpu as pltpu
from jax.sharding import PartitionSpec as P

LN_EPS = 1e-5
N = 256
C = 128
GROUP = 8
ROWS = N // GROUP
CH = C // GROUP
STEP = 8
UNROLL = 4
STEPS = ROWS // STEP
F32 = jnp.float32
BF16 = jnp.bfloat16
VMEM_LIMIT = 62 * 1024 * 1024


def dot(lhs, rhs, lhs_dim, rhs_dim):
    return lax.dot_general(lhs, rhs, (((lhs_dim,), (rhs_dim,)), ((), ())), preferred_element_type=F32)


def norm(values):
    mean = jnp.mean(values, axis=0, keepdims=True)
    cen = values - mean
    inv = lax.rsqrt(jnp.mean(cen * cen, axis=0, keepdims=True) + LN_EPS)
    return cen * inv, inv


def norm_back(d_hat, unit, inv, gain):
    d_unit = d_hat * gain
    mean_d = jnp.mean(d_unit, axis=0, keepdims=True)
    mean_du = jnp.mean(d_unit * unit, axis=0, keepdims=True)
    return inv * (d_unit - mean_d - unit * mean_du)


def fold(values):
    return values[:, :C] + values[:, C:]


def row_sums(acc):
    return jnp.sum(acc.T, axis=0, keepdims=True)


def sigmoid(values):
    return 0.5 * jnp.tanh(0.5 * values) + 0.5


def project(z_t, ln, w_t, bias):
    unit, inv = norm(z_t)
    z_hat = (unit * ln[0] + ln[1]).astype(BF16)
    return unit, inv, z_hat, dot(w_t[...], z_hat, 1, 0) + bias[...]


def set_eye(eye):
    same = lax.broadcasted_iota(jnp.int32, (C, C), 0) == lax.broadcasted_iota(jnp.int32, (C, C), 1)
    eye[...] = jnp.where(same, 1.0, 0.0).astype(BF16)


def set_column(ref, row):
    column = jnp.broadcast_to(row.astype(F32), (C, C)).T
    ref[:, :C] = column
    ref[:, C:] = column


def set_pre(block, ln_in, w_proj, b_proj, ln, w_t, bias):
    for k in range(2):
        set_column(ln.at[k], ln_in[block, k:k + 1, :])
    for k in range(5):
        cols = slice(k * C, (k + 1) * C)
        set_column(bias.at[cols], b_proj[block:block + 1, cols])
        w_t[cols, :] = w_proj[block, :, cols].astype(F32).T.astype(BF16)


def set_post(block, ln_mid, w_out, b_out, mln, wo_t, bo):
    for k in range(2):
        set_column(mln.at[k], ln_mid[block, k:k + 1, :])
    set_column(bo, b_out[block:block + 1, :])
    wo_t[...] = w_out[block].astype(F32).T.astype(BF16)


def place():
    me = lax.axis_index("dap")
    return me, me // 4, (me // 2) % 2, me % 2


def enter():
    me = lax.axis_index("dap")
    sem = pltpu.get_barrier_semaphore()
    for k in range(1, GROUP):
        pl.semaphore_signal(sem, inc=1, device_id={"dap": (me + k) % GROUP}, device_id_type=pl.DeviceIdType.MESH)


def all_in():
    pl.semaphore_wait(pltpu.get_barrier_semaphore(), GROUP - 1)


def peers():
    me, cy, cx, core = place()
    out = []
    for dy, dx in ((1, 1), (1, 0), (0, 1), (0, 0)):
        for dc in (1, 0):
            out.append((((cy + dy) % 2) * 2 + (cx + dx) % 2) * 2 + (core + dc) % 2)
    return me, out


def spread(ref, value, row):
    for h in range(2):
        ref[pl.ds(h * C * STEP + row, C, stride=STEP), :] = value[:, h * C:(h + 1) * C]


def pack_rows(stage, send_ref, slot):
    for h in range(2):
        for q in range(4):
            rows = stage[pl.ds((h * C + q * 32) * STEP, 32 * STEP), :].reshape(32, STEP, C)
            send_ref[slot, q * 32:(q + 1) * 32, :, h * C:(h + 1) * C] = rows.astype(BF16)


def move(src_ref, dst_ref, send_sem, recv_sem, dest, own):
    if own:
        return pltpu.make_async_copy(src_ref, dst_ref, recv_sem)
    return pltpu.make_async_remote_copy(src_ref, dst_ref, send_sem, recv_sem, device_id={"dap": dest}, device_id_type=pl.DeviceIdType.MESH)


def wait_sends(copies):
    for copy in copies:
        if copy.is_remote:
            copy.wait_send()


def row_copies(send_ref, out_ref, send_sem, recv_sem, slot):
    me, dests = peers()
    start = pl.multiple_of(me * ROWS + slot * STEP, STEP)
    return [
        move(send_ref.at[slot, pl.ds(pl.multiple_of(dest * CH, CH), CH)], out_ref.at[:, pl.ds(start, STEP), :],
             send_sem.at[slot, k], recv_sem, dest, k == GROUP - 1)
        for k, dest in enumerate(dests)
    ]


def send_rows(step, jobs):
    for stage, send_ref, out_ref, send_sem, recv_sem in jobs:
        pack_rows(stage, send_ref, step)
        for copy in row_copies(send_ref, out_ref, send_sem, recv_sem, step):
            copy.start()

    @pl.when(step == STEPS - 1)
    def _():
        for stage, send_ref, out_ref, send_sem, recv_sem in jobs:
            for slot in range(STEPS):
                wait_sends(row_copies(send_ref, out_ref, send_sem, recv_sem, slot))
            pltpu.make_async_copy(out_ref, out_ref, recv_sem).wait()


OUT_FWD = (lambda r, c: dot(r[0][c], r[1][c], 1, 1),)
IN_FWD = (lambda r, c: dot(r[0][c], r[1][c], 0, 0),)
IN_BWD = (lambda r, c: dot(r[1][c], r[2][c], 1, 1), lambda r, c: dot(r[0][c], r[2][c], 1, 0))
OUT_BWD = (lambda r, c: dot(r[2][c], r[1][c], 1, 0), lambda r, c: dot(r[2][c], r[0][c], 0, 0))


def back_copy(job, t, k, dest, frm):
    stage, send_ref, land_ref, send_sem, recv_sem = job
    return pltpu.make_async_remote_copy(
        send_ref.at[t, dest], land_ref.at[t, :, pl.ds(pl.multiple_of(frm * CH, CH), CH), :], send_sem.at[t, k], recv_sem.at[t, frm],
        device_id={"dap": dest}, device_id_type=pl.DeviceIdType.MESH)


GROUPS = 4


class Piecewise:
    def __init__(self, source, ref, sems):
        self.source, self.ref, self.sems = source, ref, sems

    def load(self, g):
        part = pl.ds(g * (CH // GROUPS), CH // GROUPS)
        return pltpu.make_async_copy(self.source.at[part], self.ref.at[part], self.sems.at[g])


def channel_part(products, ins, jobs):
    me, dests = peers()
    refs = [x.ref for x in ins]
    for j, (product, job) in enumerate(zip(products, jobs)):
        stage, send_ref, land_ref = job[:3]

        def body(c, carry):
            value = product(refs, c)
            for h in range(2):
                stage[pl.ds((h * 2 + c // 8) * N * 8 + c % 8, N, stride=8), :] = value[:, h * C:(h + 1) * C]
            return carry

        for g in range(GROUPS):
            if j == 0:
                for x in ins:
                    x.load(g).wait()
            lax.fori_loop(g * (CH // GROUPS), (g + 1) * (CH // GROUPS), body, 0, unroll=True)
        if j == 0:
            all_in()
        for t in range(STEPS):
            for dest in range(GROUP):
                for h in range(2):
                    at = h * 2 * N * 8 + (dest * ROWS + t * STEP) * 8
                    lo = stage[pl.ds(at, 64), :].reshape(STEP, 8, C)
                    hi = stage[pl.ds(at + N * 8, 64), :].reshape(STEP, 8, C)
                    send_ref[t, dest, :, :, h * C:(h + 1) * C] = jnp.concatenate([lo, hi], axis=1).astype(BF16)
            for k, dest in enumerate(dests[:-1]):
                back_copy(job, t, k, dest, me).start()
            land_ref[t, :, pl.ds(pl.multiple_of(me * CH, CH), CH), :] = send_ref[t, me]


def staged_kernel(inner, n_tri, n_in, *refs):
    far, refs = refs[:n_tri + n_in], refs[n_tri + n_in:]
    near, refs = refs[-2 - n_tri - n_in:-2], refs[:-2 - n_tri - n_in] + refs[-2:]
    refs, (tri_sem, row_sem) = refs[:-2], refs[-2:]
    step = pl.program_id(0)
    tris = [Piecewise(far[k], near[k], tri_sem.at[k]) for k in range(n_tri)]

    def fetch(t, slot):
        out = []
        for k in range(n_in):
            size = far[n_tri + k].shape[0] // STEPS
            out.append(pltpu.make_async_copy(far[n_tri + k].at[pl.ds(t * size, size)], near[n_tri + k].at[slot], row_sem.at[slot, k]))
        return out

    @pl.when(step == 0)
    def _():
        for g in range(GROUPS):
            for x in tris:
                x.load(g).start()
        for copy in fetch(0, 0):
            copy.start()

    slot = (step + 1) % 2

    @pl.when(step > 0)
    def _():
        for copy in fetch(step - 1, slot):
            copy.wait()

    @pl.when((step > 0) & (step < STEPS))
    def _():
        for copy in fetch(step, 1 - slot):
            copy.start()

    inner(*tris, *[ref.at[slot] for ref in near[n_tri:]], *refs)


def arrive(t, jobs):
    me, dests = peers()
    for job in jobs:
        for k, frm in enumerate(dests[:-1]):
            back_copy(job, t, k, frm, frm).wait_recv()

    @pl.when(t == STEPS - 1)
    def _():
        for job in jobs:
            for slot in range(STEPS):
                for k, dest in enumerate(dests[:-1]):
                    back_copy(job, slot, k, dest, me).wait_send()


def rows_loop(body):
    def step(r, carry):
        body(r)
        return carry

    lax.fori_loop(0, STEP, step, 0, unroll=UNROLL)


def pre_row(r, z_t, mask_ref, ln_ref, w_t_ref, bias_ref, g_ref, keep_ref, unit_ref, inv_ref, a_stage, b_stage):
    unit, inv, _, p = project(z_t, ln_ref, w_t_ref, bias_ref)
    unit_ref[r] = unit
    inv_ref[0, pl.ds(r, 1), :] = inv
    m = mask_ref[0, pl.ds(r, 1), :].astype(F32)
    for side, stage in ((0, a_stage), (1, b_stage)):
        s = sigmoid(p[2 * side * C:(2 * side + 1) * C])
        v = p[(2 * side + 1) * C:(2 * side + 2) * C]
        sm = s * m
        spread(stage, sm * v, r)
        keep_ref[r, 2 * side] = sm
        keep_ref[r, 2 * side + 1] = v * (1.0 - s)
    g_ref[r] = sigmoid(p[4 * C:])


def pre_kernel(z_ref, mask_ref, ln_in, w_proj, b_proj, a_ref, b_ref, g_ref, keep_ref, unit_ref, inv_ref, a_st, b_st, a_send, b_send,
               eye_ref, ln_ref, w_t_ref, bias_ref, a_ss, b_ss, rs):
    step = pl.program_id(0)

    @pl.when(step == 0)
    def _():
        enter()
        set_eye(eye_ref)
        set_pre(0, ln_in, w_proj, b_proj, ln_ref, w_t_ref, bias_ref)

    @rows_loop
    def _(r):
        z_t = dot(eye_ref[...], z_ref[r], 1, 1)
        pre_row(r, z_t, mask_ref, ln_ref, w_t_ref, bias_ref, g_ref, keep_ref, unit_ref, inv_ref, a_st, b_st)

    pl.when(step == 0)(all_in)
    send_rows(step, [(a_st, a_send, a_ref, a_ss, rs.at[0]), (b_st, b_send, b_ref, b_ss, rs.at[1])])


def mid_kernel(a_in, b_in, z_ref, g0_ref, mask_ref, ln_mid, w_out, b_out, ln_in, w_proj, b_proj,
               a_ref, b_ref, g_ref, keep_ref, unit_ref, inv_ref, zm_ref, gu_ref, munit_ref, minv_ref, a_st, b_st, a_send, b_send,
               eye_ref, ln_ref, w_t_ref, bias_ref, mln_ref, wo_t_ref, bo_ref, a_ss, b_ss, rs,
               st0, se0, la0, ss0, rv0):
    step = pl.program_id(0)
    jobs = [(st0, se0, la0, ss0, rv0)]

    @pl.when(step == 0)
    def _():
        enter()
        set_eye(eye_ref)
        set_pre(1, ln_in, w_proj, b_proj, ln_ref, w_t_ref, bias_ref)
        set_post(0, ln_mid, w_out, b_out, mln_ref, wo_t_ref, bo_ref)
        channel_part(OUT_FWD, (a_in, b_in), jobs)

    @pl.when(step > 0)
    def _():
        t = step - 1
        arrive(t, jobs)
        x_ref = la0.at[t]

        @rows_loop
        def _(r):
            unit, inv = norm(x_ref[r].astype(F32))
            munit_ref[r] = unit
            minv_ref[0, pl.ds(r, 1), :] = inv
            x_hat = (unit * mln_ref[0] + mln_ref[1]).astype(BF16)
            update = dot(wo_t_ref[...], x_hat, 1, 0) + bo_ref[...]
            g = g0_ref[r]
            change = g * update
            gu_ref[r] = change * (1.0 - g)
            z_new = (dot(eye_ref[...], z_ref[r], 1, 1) + change).astype(BF16)
            zm_ref[r] = z_new
            pre_row(r, z_new.astype(F32), mask_ref, ln_ref, w_t_ref, bias_ref, g_ref, keep_ref, unit_ref, inv_ref, a_st, b_st)

        send_rows(t, [(a_st, a_send, a_ref, a_ss, rs.at[0]), (b_st, b_send, b_ref, b_ss, rs.at[1])])


def post_back_row(unit, inv, g, dz, mln_ref, wo_ref, acc_ref, x_hat=None):
    if x_hat is None:
        x_hat = (unit * mln_ref[0] + mln_ref[1]).astype(BF16)
    d_up = dz * g
    d_up_bf = d_up.astype(BF16)
    acc_ref[0] += dot(x_hat, d_up_bf, 1, 1)
    acc_ref[3] += fold(d_up)
    d_hat = dot(wo_ref[...], d_up_bf, 1, 0).astype(BF16).astype(F32)
    acc_ref[1] += fold(d_hat * unit)
    acc_ref[2] += fold(d_hat)
    return norm_back(d_hat, unit, inv, mln_ref[0])


def put_post(grad_ref, acc_ref):
    grad_ref[0:C, :] = acc_ref[0]
    grad_ref[C:C + 8, :] = jnp.concatenate([row_sums(acc_ref[1]), row_sums(acc_ref[2]), row_sums(acc_ref[3]), jnp.zeros((5, C), F32)], axis=0)
    grad_ref[C + 8:C + 16, :] = jnp.zeros((8, C), F32)


def turn_kernel(a_in, b_in, zm_ref, g_ref, dz_ref, ln_mid, w_out, b_out,
                dx_ref, z_out_ref, dpg_ref, grad_ref, d_st, d_send, eye_ref, mln_ref, wo_t_ref, bo_ref, acc_ref, d_ss, rs,
               st0, se0, la0, ss0, rv0):
    step = pl.program_id(0)
    jobs = [(st0, se0, la0, ss0, rv0)]
    wo_ref = w_out.at[1]

    @pl.when(step == 0)
    def _():
        enter()
        set_eye(eye_ref)
        set_post(1, ln_mid, w_out, b_out, mln_ref, wo_t_ref, bo_ref)
        acc_ref[...] = jnp.zeros_like(acc_ref)
        channel_part(IN_FWD, (a_in, b_in), jobs)

    @pl.when(step > 0)
    def _():
        t = step - 1
        arrive(t, jobs)
        x_ref = la0.at[t]

        @rows_loop
        def _(r):
            dz = dot(eye_ref[...], dz_ref[r], 1, 1)
            g = g_ref[r]
            unit, inv = norm(x_ref[r].astype(F32))
            x_hat = (unit * mln_ref[0] + mln_ref[1]).astype(BF16)
            change = g * (dot(wo_t_ref[...], x_hat, 1, 0) + bo_ref[...])
            dpg_ref[r] = dz * change * (1.0 - g)
            z_out_ref[r] = (zm_ref[r].astype(F32) + change).astype(BF16)
            spread(d_st, post_back_row(unit, inv, g, dz, mln_ref, wo_ref, acc_ref, x_hat), r)

        @pl.when(t == STEPS - 1)
        def _():
            put_post(grad_ref, acc_ref)

        send_rows(t, [(d_st, d_send, dx_ref, d_ss, rs.at[0])])


def pre_back_row(unit, inv, keep, da, db, d_pg, ln_ref, w_ref, w_acc, b_acc, l_acc):
    z_hat = (unit * ln_ref[0] + ln_ref[1]).astype(BF16)
    parts = []
    for side, d_side in ((0, da), (1, db)):
        d_v = d_side * keep[2 * side]
        parts += [d_v * keep[2 * side + 1], d_v]
    parts.append(d_pg)
    for k, part in enumerate(parts):
        b_acc[k * C:(k + 1) * C, :] += fold(part)
    d_p = jnp.concatenate([part.astype(BF16) for part in parts], axis=0)
    w_acc[...] += dot(d_p, z_hat, 1, 1)
    d_hat = dot(w_ref[...], d_p, 1, 0).astype(BF16).astype(F32)
    l_acc[0] += fold(d_hat * unit)
    l_acc[1] += fold(d_hat)
    return norm_back(d_hat, unit, inv, ln_ref[0])


def put_pre(grad_ref, w_acc, b_acc, l_acc):
    grad_ref[0:5 * C, :] = w_acc[...]
    rows = [row_sums(b_acc[k * C:(k + 1) * C, :]) for k in range(5)]
    rows += [row_sums(l_acc[0]), row_sums(l_acc[1]), jnp.zeros((1, C), F32)]
    grad_ref[5 * C:5 * C + 8, :] = jnp.concatenate(rows, axis=0)
    grad_ref[5 * C + 8:5 * C + 16, :] = jnp.zeros((8, C), F32)


def set_gains(ref, ln, block):
    for k in range(2):
        set_column(ref.at[k], ln[block, k:k + 1, :])


def back_kernel(a_in, b_in, dx_in, dpg1_ref, keep_ref, unit_ref, inv_ref, dz_ref, munit_ref, minv_ref, g_ref, gu_ref, ln_in, w_proj, ln_mid, w_out,
                dx_ref, dzm_ref, dpg_ref, grad1_ref, grad0_ref, d_st, d_send,
                eye_ref, ln_ref, mln_ref, w_acc, b_acc, l_acc, acc_ref, d_ss, rs,
               st0, st1, se0, se1, la0, la1, ss0, ss1, rv0, rv1):
    step = pl.program_id(0)
    jobs = [(st0, se0, la0, ss0, rv0), (st1, se1, la1, ss1, rv1)]
    w_ref, wo_ref = w_proj.at[1], w_out.at[0]

    @pl.when(step == 0)
    def _():
        enter()
        set_eye(eye_ref)
        set_gains(ln_ref, ln_in, 1)
        set_gains(mln_ref, ln_mid, 0)
        for ref in (w_acc, b_acc, l_acc, acc_ref):
            ref[...] = jnp.zeros_like(ref)
        channel_part(IN_BWD, (a_in, b_in, dx_in), jobs)

    @pl.when(step > 0)
    def _():
        t = step - 1
        arrive(t, jobs)
        da_ref, db_ref = la0.at[t], la1.at[t]

        @rows_loop
        def _(r):
            at = pl.ds(r, 1)
            dzn = pre_back_row(unit_ref[r], inv_ref[0, at, :], keep_ref.at[r], da_ref[r].astype(F32), db_ref[r].astype(F32), dpg1_ref[r],
                               ln_ref, w_ref, w_acc, b_acc, l_acc)
            dzm = (dot(eye_ref[...], dz_ref[r], 1, 1) + dzn).astype(BF16)
            dzm_ref[r] = dzm
            dzm = dzm.astype(F32)
            dpg_ref[r] = dzm * gu_ref[r]
            spread(d_st, post_back_row(munit_ref[r], minv_ref[0, at, :], g_ref[r], dzm, mln_ref, wo_ref, acc_ref), r)

        @pl.when(t == STEPS - 1)
        def _():
            put_pre(grad1_ref, w_acc, b_acc, l_acc)
            put_post(grad0_ref, acc_ref)

        send_rows(t, [(d_st, d_send, dx_ref, d_ss, rs.at[0])])


def last_kernel(a_in, b_in, dx_in, dpg_ref, keep_ref, unit_ref, inv_ref, dzm_ref, ln_in, w_proj,
                dz_ref, grad_ref, ln_ref, w_acc, b_acc, l_acc,
               st0, st1, se0, se1, la0, la1, ss0, ss1, rv0, rv1):
    step = pl.program_id(0)
    jobs = [(st0, se0, la0, ss0, rv0), (st1, se1, la1, ss1, rv1)]
    w_ref = w_proj.at[0]

    @pl.when(step == 0)
    def _():
        enter()
        set_gains(ln_ref, ln_in, 0)
        for ref in (w_acc, b_acc, l_acc):
            ref[...] = jnp.zeros_like(ref)
        channel_part(OUT_BWD, (a_in, b_in, dx_in), jobs)

    @pl.when(step > 0)
    def _():
        t = step - 1
        arrive(t, jobs)
        da_ref, db_ref = la0.at[t], la1.at[t]

        @rows_loop
        def _(r):
            dzn = pre_back_row(unit_ref[r], inv_ref[0, pl.ds(r, 1), :], keep_ref.at[r], da_ref[r].astype(F32), db_ref[r].astype(F32), dpg_ref[r],
                               ln_ref, w_ref, w_acc, b_acc, l_acc)
            dz_ref[r] = (dzm_ref[r].astype(F32) + dzn).astype(BF16)

        @pl.when(t == STEPS - 1)
        def _():
            put_pre(grad_ref, w_acc, b_acc, l_acc)


ALL = 16
SHARE = 112
PACKS = (C + 16, C + 16, 5 * C + 16, 5 * C + 16)


def share(k):
    return pl.ds(pl.multiple_of(k * SHARE, SHARE), SHARE)


def sum_kernel(p0, p1, p2, p3, tot_ref, send_ref, got_ref, part_ref, ss, rs, ss2, rs2):
    dp, dap = lax.axis_index("dp"), lax.axis_index("dap")
    me = dp * GROUP + dap
    others = [(me + k) % ALL for k in range(1, ALL)]
    ids = [{"dp": o // GROUP, "dap": o % GROUP} for o in others]
    sem = pltpu.get_barrier_semaphore()
    for to in ids:
        pl.semaphore_signal(sem, inc=1, device_id=to, device_id_type=pl.DeviceIdType.MESH)
    at = 0
    for ref, rows in zip((p0, p1, p2, p3), PACKS):
        send_ref[at:at + rows, :] = ref[...].astype(BF16)
        at += rows
    send_ref[at:, :] = jnp.zeros((ALL * SHARE - at, C), BF16)
    pl.semaphore_wait(sem, ALL - 1)

    def first(to, k, frm):
        return pltpu.make_async_remote_copy(send_ref.at[share(others[k])], got_ref.at[frm], ss.at[k], rs.at[frm], device_id=to, device_id_type=pl.DeviceIdType.MESH)

    def second(to, k, frm):
        return pltpu.make_async_remote_copy(part_ref, tot_ref.at[share(frm)], ss2.at[k], rs2.at[frm], device_id=to, device_id_type=pl.DeviceIdType.MESH)

    for k, to in enumerate(ids):
        first(to, k, me).start()
    got_ref[me] = send_ref[share(me), :]
    for k, to in enumerate(ids):
        first(to, k, others[k]).wait_recv()
    total = got_ref[0].astype(F32)
    for k in range(1, ALL):
        total = total + got_ref[k].astype(F32)
    part_ref[...] = total
    for k, to in enumerate(ids):
        second(to, k, me).start()
    tot_ref[share(me), :] = total
    for k, to in enumerate(ids):
        second(to, k, others[k]).wait_recv()
    for k, to in enumerate(ids):
        first(to, k, me).wait_send()
        second(to, k, me).wait_send()


def split_kernel(z_t, dz_t, tot, z_out, dz_out, *grads):
    for r in range(STEP):
        z_out[r] = z_t[r].astype(F32).T.astype(BF16)
        dz_out[r] = dz_t[r].astype(F32).T.astype(BF16)
    pl.when(pl.program_id(0) == 0)(lambda: split_grads(tot, *grads))


def split_grads(tot, d_ln_in, d_w_proj, d_b_proj, d_ln_mid, d_w_out, d_b_out):
    at = 0
    for k in range(2):
        d_w_out[k] = tot[at:at + C, :]
        d_ln_mid[k] = tot[at + C:at + C + 2, :]
        d_b_out[k:k + 1, :] = tot[at + C + 2:at + C + 3, :]
        at += C + 16
    for k in range(2):
        for j in range(5):
            d_w_proj[k, :, j * C:(j + 1) * C] = tot[at + j * C:at + (j + 1) * C, :].T
            d_b_proj[k:k + 1, j * C:(j + 1) * C] = tot[at + 5 * C + j:at + 5 * C + j + 1, :]
        d_ln_in[k] = tot[at + 5 * C + 5:at + 5 * C + 7, :]
        at += 5 * C + 16


def finish(z_t, dz_t, packs):
    vmem = pl.BlockSpec(memory_space=pltpu.VMEM)
    dma = pltpu.SemaphoreType.DMA((ALL,))
    total = pl.pallas_call(
        sum_kernel,
        in_specs=[vmem] * 4,
        out_specs=vmem,
        out_shape=jax.ShapeDtypeStruct((ALL * SHARE, C), F32),
        scratch_shapes=[pltpu.VMEM((ALL * SHARE, C), BF16), pltpu.VMEM((ALL, SHARE, C), BF16), pltpu.VMEM((SHARE, C), F32), dma, dma, dma, dma],
        compiler_params=pltpu.CompilerParams(vmem_limit_bytes=VMEM_LIMIT, collective_id=5, has_side_effects=True),
        name="sum",
    )(*packs)
    shapes = ((2, 2, C), (2, C, 5 * C), (2, 5 * C), (2, 2, C), (2, C, C), (2, C))
    grads = [jax.ShapeDtypeStruct(shape, F32) for shape in shapes]
    return pl.pallas_call(
        split_kernel,
        grid=(STEPS,),
        in_specs=[by_row(z_t), by_row(dz_t), whole(total)],
        out_specs=[by_row(NATIVE)] * 2 + [pl.BlockSpec(x.shape, lambda t, n=len(x.shape): (0,) * n) for x in grads],
        out_shape=[NATIVE] * 2 + grads,
        compiler_params=pltpu.CompilerParams(dimension_semantics=("arbitrary",)),
        name="split",
    )(z_t, dz_t, total)


TRI = jax.ShapeDtypeStruct((CH, N, N), BF16)
ROW = jax.ShapeDtypeStruct((ROWS, C, N), BF16)
ROW32 = jax.ShapeDtypeStruct((ROWS, C, N), F32)
NATIVE = jax.ShapeDtypeStruct((ROWS, N, C), BF16)
POST = jax.ShapeDtypeStruct((C + 16, C), F32)
PRE = jax.ShapeDtypeStruct((5 * C + 16, C), F32)
KEEP = jax.ShapeDtypeStruct((ROWS, 4, C, N), F32)
INV = jax.ShapeDtypeStruct((STEPS, STEP, N), F32)


def by_row(array, lead=0):
    tail = array.shape[1:]
    return pl.BlockSpec((array.shape[0] // STEPS,) + tail, lambda s: ((s * STEPS) // (STEPS + lead),) + (0,) * len(tail))


def whole(array):
    zeros = (0,) * len(array.shape)
    return pl.BlockSpec(array.shape, lambda t: zeros, pipeline_mode=pl.Buffered(1))


def out_spec(array, lead):
    if array is TRI:
        return pl.BlockSpec(memory_space=pl.ANY)
    if array in (PRE, POST):
        return pl.BlockSpec(array.shape, lambda t: (0, 0))
    return by_row(array, lead)


def row_call(kernel, name, collective_id, tris, ins, consts, outs, n_back, scratch):
    lead = 1 if tris else 0
    n_send = sum(out is TRI for out in outs)
    dma = pltpu.SemaphoreType.DMA
    sent = [pltpu.VMEM((2 * C * STEP, C), F32)] * n_send + [pltpu.VMEM((STEPS, C, STEP, N), BF16)] * n_send
    sems = [dma((STEPS, GROUP))] * n_send + ([dma((n_send,))] if n_send else [])
    back = [pltpu.VMEM((4 * N * 8, C), F32)] * n_back + [pltpu.VMEM((STEPS, GROUP, STEP, CH, N), BF16)] * n_back
    back += [pltpu.VMEM((STEPS, STEP, C, N), BF16)] * n_back + [dma((STEPS, GROUP))] * (2 * n_back)
    far = pl.BlockSpec(memory_space=pl.ANY)
    near = []
    if tris:
        near = [pltpu.VMEM(x.shape, x.dtype) for x in tris] + [pltpu.VMEM((2, x.shape[0] // STEPS) + x.shape[1:], x.dtype) for x in ins]
        near += [dma((len(tris), GROUPS)), dma((2, len(ins)))]
        kernel = functools.partial(staged_kernel, kernel, len(tris), len(ins))
    return pl.pallas_call(
        kernel,
        grid=(STEPS + lead,),
        in_specs=[far if tris else by_row(x) for x in [*tris, *ins]] + [whole(x) for x in consts],
        out_specs=[out_spec(out, lead) for out in outs],
        out_shape=outs,
        scratch_shapes=sent + scratch + sems + back + near,
        compiler_params=pltpu.CompilerParams(dimension_semantics=("arbitrary",), vmem_limit_bytes=VMEM_LIMIT, collective_id=collective_id, has_side_effects=True),
        name=name,
    )(*tris, *ins, *consts)


def local_step(z_pair, pair_mask, dz_out, ln_in, w_proj, b_proj, ln_mid, w_out, b_out):
    z, dz = z_pair[0], dz_out[0]
    mask = pair_mask.reshape(STEPS, STEP, N)
    pre, post = [ln_in, w_proj, b_proj], [ln_mid, w_out, b_out]
    eye = [pltpu.VMEM((C, C), BF16)]
    pre_c = [pltpu.VMEM((2, C, N), F32), pltpu.VMEM((5 * C, C), BF16), pltpu.VMEM((5 * C, N), F32)]
    post_c = [pltpu.VMEM((2, C, N), F32), pltpu.VMEM((C, C), BF16), pltpu.VMEM((C, N), F32)]
    post_acc = [pltpu.VMEM((4, C, C), F32)]
    pre_acc = [pltpu.VMEM((5 * C, C), F32), pltpu.VMEM((5 * C, C), F32), pltpu.VMEM((2, C, C), F32)]

    gains = [pltpu.VMEM((2, C, N), F32)]
    kept = [TRI, TRI, ROW32, KEEP, ROW32, INV]
    a0, b0, g0, keep0, unit0, inv0 = row_call(pre_kernel, "pre0", 0, [], [z, mask], pre, kept, 0, eye + pre_c)
    a1, b1, g1, keep1, unit1, inv1, zm, gu0, munit0, minv0 = row_call(
        mid_kernel, "mid", 1, [a0, b0], [z, g0, mask], post + pre, kept + [ROW, ROW32, ROW32, INV], 1, eye + pre_c + post_c)
    dx1, z_new, dpg1, post_g1 = row_call(
        turn_kernel, "turn", 2, [a1, b1], [zm, g1, dz], post, [TRI, ROW, ROW32, POST], 1, eye + post_c + post_acc)
    dx0, dzm, dpg0, pre_g1, post_g0 = row_call(
        back_kernel, "back", 3, [a1, b1, dx1], [dpg1, keep1, unit1, inv1, dz, munit0, minv0, g0, gu0], [ln_in, w_proj, ln_mid, w_out],
        [TRI, ROW, ROW32, PRE, POST], 2, eye + gains * 2 + pre_acc + post_acc)
    dz_new, pre_g0 = row_call(
        last_kernel, "last", 4, [a0, b0, dx0], [dpg0, keep0, unit0, inv0, dzm], [ln_in, w_proj], [ROW, PRE], 2, gains + pre_acc)
    z_out, dz_pair, *grads = finish(z_new, dz_new, [post_g0, post_g1, pre_g0, pre_g1])
    return z_out[None], dz_pair[None], *grads


def solution(mesh):
    row_spec = P("dp", "dap")
    return jax.shard_map(local_step, mesh=mesh, in_specs=(row_spec,) * 3 + (P(),) * 6,
                         out_specs=(row_spec,) * 2 + (P(),) * 6, check_vma=False)
```

```python
import functools

import jax
import jax.numpy as jnp
from jax import lax
from jax.experimental import pallas as pl
from jax.experimental.pallas import tpu as pltpu
from jax.sharding import PartitionSpec as P

LN_EPS = 1e-5
N = 256
C = 128
GROUP = 8
ROWS = N // GROUP
CH = C // GROUP
STEP = 8
UNROLL = 4
STEPS = ROWS // STEP
F32 = jnp.float32
BF16 = jnp.bfloat16
VMEM_LIMIT = 62 * 1024 * 1024


def dot(lhs, rhs, lhs_dim, rhs_dim):
    return lax.dot_general(lhs, rhs, (((lhs_dim,), (rhs_dim,)), ((), ())), preferred_element_type=F32)


def norm(values):
    mean = jnp.mean(values, axis=0, keepdims=True)
    cen = values - mean
    inv = lax.rsqrt(jnp.mean(cen * cen, axis=0, keepdims=True) + LN_EPS)
    return cen * inv, inv


def norm_back(d_hat, unit, inv, gain):
    d_unit = d_hat * gain
    mean_d = jnp.mean(d_unit, axis=0, keepdims=True)
    mean_du = jnp.mean(d_unit * unit, axis=0, keepdims=True)
    return inv * (d_unit - mean_d - unit * mean_du)


def fold(values):
    return values[:, :C] + values[:, C:]


def row_sums(acc):
    return jnp.sum(acc.T, axis=0, keepdims=True)


def sigmoid(values):
    return 0.5 * jnp.tanh(0.5 * values) + 0.5


def project(z_t, ln, w_t, bias):
    unit, inv = norm(z_t)
    z_hat = (unit * ln[0] + ln[1]).astype(BF16)
    return unit, inv, z_hat, dot(w_t[...], z_hat, 1, 0) + bias[...]


def set_eye(eye):
    same = lax.broadcasted_iota(jnp.int32, (C, C), 0) == lax.broadcasted_iota(jnp.int32, (C, C), 1)
    eye[...] = jnp.where(same, 1.0, 0.0).astype(BF16)


def set_column(ref, row):
    column = jnp.broadcast_to(row.astype(F32), (C, C)).T
    ref[:, :C] = column
    ref[:, C:] = column


def set_pre(block, ln_in, w_proj, b_proj, ln, w_t, bias):
    for k in range(2):
        set_column(ln.at[k], ln_in[block, k:k + 1, :])
    for k in range(5):
        cols = slice(k * C, (k + 1) * C)
        set_column(bias.at[cols], b_proj[block:block + 1, cols])
        w_t[cols, :] = w_proj[block, :, cols].astype(F32).T.astype(BF16)


def set_post(block, ln_mid, w_out, b_out, mln, wo_t, bo):
    for k in range(2):
        set_column(mln.at[k], ln_mid[block, k:k + 1, :])
    set_column(bo, b_out[block:block + 1, :])
    wo_t[...] = w_out[block].astype(F32).T.astype(BF16)


def place():
    me = lax.axis_index("dap")
    return me, me // 4, (me // 2) % 2, me % 2


def enter():
    me = lax.axis_index("dap")
    sem = pltpu.get_barrier_semaphore()
    for k in range(1, GROUP):
        pl.semaphore_signal(sem, inc=1, device_id={"dap": (me + k) % GROUP}, device_id_type=pl.DeviceIdType.MESH)


def all_in():
    pl.semaphore_wait(pltpu.get_barrier_semaphore(), GROUP - 1)


def peers():
    me, cy, cx, core = place()
    out = []
    for dy, dx in ((1, 1), (1, 0), (0, 1), (0, 0)):
        for dc in (1, 0):
            out.append((((cy + dy) % 2) * 2 + (cx + dx) % 2) * 2 + (core + dc) % 2)
    return me, out


def spread(ref, value, row):
    for h in range(2):
        ref[pl.ds(h * C * STEP + row, C, stride=STEP), :] = value[:, h * C:(h + 1) * C]


def pack_rows(stage, send_ref, slot):
    for h in range(2):
        for q in range(4):
            rows = stage[pl.ds((h * C + q * 32) * STEP, 32 * STEP), :].reshape(32, STEP, C)
            send_ref[slot, q * 32:(q + 1) * 32, :, h * C:(h + 1) * C] = rows.astype(BF16)


def move(src_ref, dst_ref, send_sem, recv_sem, dest, own):
    if own:
        return pltpu.make_async_copy(src_ref, dst_ref, recv_sem)
    return pltpu.make_async_remote_copy(src_ref, dst_ref, send_sem, recv_sem, device_id={"dap": dest}, device_id_type=pl.DeviceIdType.MESH)


def wait_sends(copies):
    for copy in copies:
        if copy.is_remote:
            copy.wait_send()


def row_copies(send_ref, out_ref, send_sem, recv_sem, slot):
    me, dests = peers()
    start = pl.multiple_of(me * ROWS + slot * STEP, STEP)
    return [
        move(send_ref.at[slot, pl.ds(pl.multiple_of(dest * CH, CH), CH)], out_ref.at[:, pl.ds(start, STEP), :],
             send_sem.at[slot, k], recv_sem, dest, k == GROUP - 1)
        for k, dest in enumerate(dests)
    ]


def send_rows(step, jobs):
    for stage, send_ref, out_ref, send_sem, recv_sem in jobs:
        pack_rows(stage, send_ref, step)
        for copy in row_copies(send_ref, out_ref, send_sem, recv_sem, step):
            copy.start()

    @pl.when(step == STEPS - 1)
    def _():
        for stage, send_ref, out_ref, send_sem, recv_sem in jobs:
            for slot in range(STEPS):
                wait_sends(row_copies(send_ref, out_ref, send_sem, recv_sem, slot))
            pltpu.make_async_copy(out_ref, out_ref, recv_sem).wait()


OUT_FWD = (lambda r, c: dot(r[0][c], r[1][c], 1, 1),)
IN_FWD = (lambda r, c: dot(r[0][c], r[1][c], 0, 0),)
IN_BWD = (lambda r, c: dot(r[1][c], r[2][c], 1, 1), lambda r, c: dot(r[0][c], r[2][c], 1, 0))
OUT_BWD = (lambda r, c: dot(r[2][c], r[1][c], 1, 0), lambda r, c: dot(r[2][c], r[0][c], 0, 0))


def back_copy(job, t, k, dest, frm):
    stage, send_ref, land_ref, send_sem, recv_sem = job
    return pltpu.make_async_remote_copy(
        send_ref.at[t, dest], land_ref.at[t, :, pl.ds(pl.multiple_of(frm * CH, CH), CH), :], send_sem.at[t, k], recv_sem.at[t, frm],
        device_id={"dap": dest}, device_id_type=pl.DeviceIdType.MESH)


GROUPS = 4


class Piecewise:
    def __init__(self, source, ref, sems):
        self.source, self.ref, self.sems = source, ref, sems

    def load(self, g):
        part = pl.ds(g * (CH // GROUPS), CH // GROUPS)
        return pltpu.make_async_copy(self.source.at[part], self.ref.at[part], self.sems.at[g])


def channel_part(products, ins, jobs):
    me, dests = peers()
    refs = [x.ref for x in ins]
    for j, (product, job) in enumerate(zip(products, jobs)):
        stage, send_ref, land_ref = job[:3]

        def body(c, carry):
            value = product(refs, c)
            for h in range(2):
                stage[pl.ds((h * 2 + c // 8) * N * 8 + c % 8, N, stride=8), :] = value[:, h * C:(h + 1) * C]
            return carry

        for g in range(GROUPS):
            if j == 0:
                for x in ins:
                    x.load(g).wait()
            lax.fori_loop(g * (CH // GROUPS), (g + 1) * (CH // GROUPS), body, 0, unroll=True)
        if j == 0:
            all_in()
        for t in range(STEPS):
            for dest in range(GROUP):
                for h in range(2):
                    at = h * 2 * N * 8 + (dest * ROWS + t * STEP) * 8
                    lo = stage[pl.ds(at, 64), :].reshape(STEP, 8, C)
                    hi = stage[pl.ds(at + N * 8, 64), :].reshape(STEP, 8, C)
                    send_ref[t, dest, :, :, h * C:(h + 1) * C] = jnp.concatenate([lo, hi], axis=1).astype(BF16)
            for k, dest in enumerate(dests[:-1]):
                back_copy(job, t, k, dest, me).start()
            land_ref[t, :, pl.ds(pl.multiple_of(me * CH, CH), CH), :] = send_ref[t, me]


def staged_kernel(inner, n_tri, n_in, *refs):
    far, refs = refs[:n_tri + n_in], refs[n_tri + n_in:]
    near, refs = refs[-2 - n_tri - n_in:-2], refs[:-2 - n_tri - n_in] + refs[-2:]
    refs, (tri_sem, row_sem) = refs[:-2], refs[-2:]
    step = pl.program_id(0)
    tris = [Piecewise(far[k], near[k], tri_sem.at[k]) for k in range(n_tri)]

    def fetch(t, slot):
        out = []
        for k in range(n_in):
            size = far[n_tri + k].shape[0] // STEPS
            out.append(pltpu.make_async_copy(far[n_tri + k].at[pl.ds(t * size, size)], near[n_tri + k].at[slot], row_sem.at[slot, k]))
        return out

    @pl.when(step == 0)
    def _():
        for g in range(GROUPS):
            for x in tris:
                x.load(g).start()
        for copy in fetch(0, 0):
            copy.start()

    slot = (step + 1) % 2

    @pl.when(step > 0)
    def _():
        for copy in fetch(step - 1, slot):
            copy.wait()

    @pl.when((step > 0) & (step < STEPS))
    def _():
        for copy in fetch(step, 1 - slot):
            copy.start()

    inner(*tris, *[ref.at[slot] for ref in near[n_tri:]], *refs)


def arrive(t, jobs):
    me, dests = peers()
    for job in jobs:
        for k, frm in enumerate(dests[:-1]):
            back_copy(job, t, k, frm, frm).wait_recv()

    @pl.when(t == STEPS - 1)
    def _():
        for job in jobs:
            for slot in range(STEPS):
                for k, dest in enumerate(dests[:-1]):
                    back_copy(job, slot, k, dest, me).wait_send()


def rows_loop(body):
    def step(r, carry):
        body(r)
        return carry

    lax.fori_loop(0, STEP, step, 0, unroll=UNROLL)


def pre_row(r, z_t, mask_ref, ln_ref, w_t_ref, bias_ref, g_ref, keep_ref, unit_ref, inv_ref, a_stage, b_stage):
    unit, inv, _, p = project(z_t, ln_ref, w_t_ref, bias_ref)
    unit_ref[r] = unit
    inv_ref[0, pl.ds(r, 1), :] = inv
    m = mask_ref[0, pl.ds(r, 1), :].astype(F32)
    for side, stage in ((0, a_stage), (1, b_stage)):
        s = sigmoid(p[2 * side * C:(2 * side + 1) * C])
        v = p[(2 * side + 1) * C:(2 * side + 2) * C]
        sm = s * m
        spread(stage, sm * v, r)
        keep_ref[r, 2 * side] = sm
        keep_ref[r, 2 * side + 1] = v * (1.0 - s)
    g_ref[r] = sigmoid(p[4 * C:])


def pre_kernel(z_ref, mask_ref, ln_in, w_proj, b_proj, a_ref, b_ref, g_ref, keep_ref, unit_ref, inv_ref, a_st, b_st, a_send, b_send,
               eye_ref, ln_ref, w_t_ref, bias_ref, a_ss, b_ss, rs):
    step = pl.program_id(0)

    @pl.when(step == 0)
    def _():
        enter()
        set_eye(eye_ref)
        set_pre(0, ln_in, w_proj, b_proj, ln_ref, w_t_ref, bias_ref)

    @rows_loop
    def _(r):
        z_t = dot(eye_ref[...], z_ref[r], 1, 1)
        pre_row(r, z_t, mask_ref, ln_ref, w_t_ref, bias_ref, g_ref, keep_ref, unit_ref, inv_ref, a_st, b_st)

    pl.when(step == 0)(all_in)
    send_rows(step, [(a_st, a_send, a_ref, a_ss, rs.at[0]), (b_st, b_send, b_ref, b_ss, rs.at[1])])


def mid_kernel(a_in, b_in, z_ref, g0_ref, mask_ref, ln_mid, w_out, b_out, ln_in, w_proj, b_proj,
               a_ref, b_ref, g_ref, keep_ref, unit_ref, inv_ref, zm_ref, gu_ref, munit_ref, minv_ref, a_st, b_st, a_send, b_send,
               eye_ref, ln_ref, w_t_ref, bias_ref, mln_ref, wo_t_ref, bo_ref, a_ss, b_ss, rs,
               st0, se0, la0, ss0, rv0):
    step = pl.program_id(0)
    jobs = [(st0, se0, la0, ss0, rv0)]

    @pl.when(step == 0)
    def _():
        enter()
        set_eye(eye_ref)
        set_pre(1, ln_in, w_proj, b_proj, ln_ref, w_t_ref, bias_ref)
        set_post(0, ln_mid, w_out, b_out, mln_ref, wo_t_ref, bo_ref)
        channel_part(OUT_FWD, (a_in, b_in), jobs)

    @pl.when(step > 0)
    def _():
        t = step - 1
        arrive(t, jobs)
        x_ref = la0.at[t]

        @rows_loop
        def _(r):
            unit, inv = norm(x_ref[r].astype(F32))
            munit_ref[r] = unit
            minv_ref[0, pl.ds(r, 1), :] = inv
            x_hat = (unit * mln_ref[0] + mln_ref[1]).astype(BF16)
            update = dot(wo_t_ref[...], x_hat, 1, 0) + bo_ref[...]
            g = g0_ref[r]
            change = g * update
            gu_ref[r] = change * (1.0 - g)
            z_new = (dot(eye_ref[...], z_ref[r], 1, 1) + change).astype(BF16)
            zm_ref[r] = z_new
            pre_row(r, z_new.astype(F32), mask_ref, ln_ref, w_t_ref, bias_ref, g_ref, keep_ref, unit_ref, inv_ref, a_st, b_st)

        send_rows(t, [(a_st, a_send, a_ref, a_ss, rs.at[0]), (b_st, b_send, b_ref, b_ss, rs.at[1])])


def post_back_row(unit, inv, g, dz, mln_ref, wo_ref, acc_ref, x_hat=None):
    if x_hat is None:
        x_hat = (unit * mln_ref[0] + mln_ref[1]).astype(BF16)
    d_up = dz * g
    d_up_bf = d_up.astype(BF16)
    acc_ref[0] += dot(x_hat, d_up_bf, 1, 1)
    acc_ref[3] += fold(d_up)
    d_hat = dot(wo_ref[...], d_up_bf, 1, 0).astype(BF16).astype(F32)
    acc_ref[1] += fold(d_hat * unit)
    acc_ref[2] += fold(d_hat)
    return norm_back(d_hat, unit, inv, mln_ref[0])


def put_post(grad_ref, acc_ref):
    grad_ref[0:C, :] = acc_ref[0]
    grad_ref[C:C + 8, :] = jnp.concatenate([row_sums(acc_ref[1]), row_sums(acc_ref[2]), row_sums(acc_ref[3]), jnp.zeros((5, C), F32)], axis=0)
    grad_ref[C + 8:C + 16, :] = jnp.zeros((8, C), F32)


def turn_kernel(a_in, b_in, zm_ref, g_ref, dz_ref, ln_mid, w_out, b_out,
                dx_ref, z_out_ref, dpg_ref, grad_ref, d_st, d_send, eye_ref, mln_ref, wo_t_ref, bo_ref, acc_ref, d_ss, rs,
               st0, se0, la0, ss0, rv0):
    step = pl.program_id(0)
    jobs = [(st0, se0, la0, ss0, rv0)]
    wo_ref = w_out.at[1]

    @pl.when(step == 0)
    def _():
        enter()
        set_eye(eye_ref)
        set_post(1, ln_mid, w_out, b_out, mln_ref, wo_t_ref, bo_ref)
        acc_ref[...] = jnp.zeros_like(acc_ref)
        channel_part(IN_FWD, (a_in, b_in), jobs)

    @pl.when(step > 0)
    def _():
        t = step - 1
        arrive(t, jobs)
        x_ref = la0.at[t]

        @rows_loop
        def _(r):
            dz = dot(eye_ref[...], dz_ref[r], 1, 1)
            g = g_ref[r]
            unit, inv = norm(x_ref[r].astype(F32))
            x_hat = (unit * mln_ref[0] + mln_ref[1]).astype(BF16)
            change = g * (dot(wo_t_ref[...], x_hat, 1, 0) + bo_ref[...])
            dpg_ref[r] = dz * change * (1.0 - g)
            z_out_ref[r] = (zm_ref[r].astype(F32) + change).T.astype(BF16)
            spread(d_st, post_back_row(unit, inv, g, dz, mln_ref, wo_ref, acc_ref, x_hat), r)

        @pl.when(t == STEPS - 1)
        def _():
            put_post(grad_ref, acc_ref)

        send_rows(t, [(d_st, d_send, dx_ref, d_ss, rs.at[0])])


def pre_back_row(unit, inv, keep, da, db, d_pg, ln_ref, w_ref, w_acc, b_acc, l_acc):
    z_hat = (unit * ln_ref[0] + ln_ref[1]).astype(BF16)
    parts = []
    for side, d_side in ((0, da), (1, db)):
        d_v = d_side * keep[2 * side]
        parts += [d_v * keep[2 * side + 1], d_v]
    parts.append(d_pg)
    for k, part in enumerate(parts):
        b_acc[k * C:(k + 1) * C, :] += fold(part)
    d_p = jnp.concatenate([part.astype(BF16) for part in parts], axis=0)
    w_acc[...] += dot(d_p, z_hat, 1, 1)
    d_hat = dot(w_ref[...], d_p, 1, 0).astype(BF16).astype(F32)
    l_acc[0] += fold(d_hat * unit)
    l_acc[1] += fold(d_hat)
    return norm_back(d_hat, unit, inv, ln_ref[0])


def put_pre(grad_ref, w_acc, b_acc, l_acc):
    grad_ref[0:5 * C, :] = w_acc[...]
    rows = [row_sums(b_acc[k * C:(k + 1) * C, :]) for k in range(5)]
    rows += [row_sums(l_acc[0]), row_sums(l_acc[1]), jnp.zeros((1, C), F32)]
    grad_ref[5 * C:5 * C + 8, :] = jnp.concatenate(rows, axis=0)
    grad_ref[5 * C + 8:5 * C + 16, :] = jnp.zeros((8, C), F32)


def set_gains(ref, ln, block):
    for k in range(2):
        set_column(ref.at[k], ln[block, k:k + 1, :])


def back_kernel(a_in, b_in, dx_in, dpg1_ref, keep_ref, unit_ref, inv_ref, dz_ref, munit_ref, minv_ref, g_ref, gu_ref, ln_in, w_proj, ln_mid, w_out,
                dx_ref, dzm_ref, dpg_ref, grad1_ref, grad0_ref, d_st, d_send,
                eye_ref, ln_ref, mln_ref, w_acc, b_acc, l_acc, acc_ref, d_ss, rs,
               st0, st1, se0, se1, la0, la1, ss0, ss1, rv0, rv1):
    step = pl.program_id(0)
    jobs = [(st0, se0, la0, ss0, rv0), (st1, se1, la1, ss1, rv1)]
    w_ref, wo_ref = w_proj.at[1], w_out.at[0]

    @pl.when(step == 0)
    def _():
        enter()
        set_eye(eye_ref)
        set_gains(ln_ref, ln_in, 1)
        set_gains(mln_ref, ln_mid, 0)
        for ref in (w_acc, b_acc, l_acc, acc_ref):
            ref[...] = jnp.zeros_like(ref)
        channel_part(IN_BWD, (a_in, b_in, dx_in), jobs)

    @pl.when(step > 0)
    def _():
        t = step - 1
        arrive(t, jobs)
        da_ref, db_ref = la0.at[t], la1.at[t]

        @rows_loop
        def _(r):
            at = pl.ds(r, 1)
            dzn = pre_back_row(unit_ref[r], inv_ref[0, at, :], keep_ref.at[r], da_ref[r].astype(F32), db_ref[r].astype(F32), dpg1_ref[r],
                               ln_ref, w_ref, w_acc, b_acc, l_acc)
            dzm = (dot(eye_ref[...], dz_ref[r], 1, 1) + dzn).astype(BF16)
            dzm_ref[r] = dzm
            dzm = dzm.astype(F32)
            dpg_ref[r] = dzm * gu_ref[r]
            spread(d_st, post_back_row(munit_ref[r], minv_ref[0, at, :], g_ref[r], dzm, mln_ref, wo_ref, acc_ref), r)

        @pl.when(t == STEPS - 1)
        def _():
            put_pre(grad1_ref, w_acc, b_acc, l_acc)
            put_post(grad0_ref, acc_ref)

        send_rows(t, [(d_st, d_send, dx_ref, d_ss, rs.at[0])])


def last_kernel(a_in, b_in, dx_in, dpg_ref, keep_ref, unit_ref, inv_ref, dzm_ref, ln_in, w_proj,
                dz_ref, grad_ref, ln_ref, w_acc, b_acc, l_acc,
               st0, st1, se0, se1, la0, la1, ss0, ss1, rv0, rv1):
    step = pl.program_id(0)
    jobs = [(st0, se0, la0, ss0, rv0), (st1, se1, la1, ss1, rv1)]
    w_ref = w_proj.at[0]

    @pl.when(step == 0)
    def _():
        enter()
        set_gains(ln_ref, ln_in, 0)
        for ref in (w_acc, b_acc, l_acc):
            ref[...] = jnp.zeros_like(ref)
        channel_part(OUT_BWD, (a_in, b_in, dx_in), jobs)

    @pl.when(step > 0)
    def _():
        t = step - 1
        arrive(t, jobs)
        da_ref, db_ref = la0.at[t], la1.at[t]

        @rows_loop
        def _(r):
            dzn = pre_back_row(unit_ref[r], inv_ref[0, pl.ds(r, 1), :], keep_ref.at[r], da_ref[r].astype(F32), db_ref[r].astype(F32), dpg_ref[r],
                               ln_ref, w_ref, w_acc, b_acc, l_acc)
            dz_ref[r] = (dzm_ref[r].astype(F32) + dzn).T.astype(BF16)

        @pl.when(t == STEPS - 1)
        def _():
            put_pre(grad_ref, w_acc, b_acc, l_acc)


ALL = 16
SHARE = 112
PACKS = (C + 16, C + 16, 5 * C + 16, 5 * C + 16)


def share(k):
    return pl.ds(pl.multiple_of(k * SHARE, SHARE), SHARE)


def sum_kernel(p0, p1, p2, p3, tot_ref, send_ref, got_ref, part_ref, ss, rs, ss2, rs2, ss3, rs3):
    dp, dap = lax.axis_index("dp"), lax.axis_index("dap")
    me = dp * GROUP + dap
    core = dap % 2
    twin = me + 1 - 2 * core
    others = [(me + k) % ALL for k in range(1, ALL)]
    chips = [(me + 2 * k) % ALL for k in range(1, ALL // 2)]

    def device(o):
        return {"dp": o // GROUP, "dap": o % GROUP}

    def remote(src, dst, send_sem, recv_sem, to):
        return pltpu.make_async_remote_copy(src, dst, send_sem, recv_sem, device_id=device(to), device_id_type=pl.DeviceIdType.MESH)

    sem = pltpu.get_barrier_semaphore()
    for to in others:
        pl.semaphore_signal(sem, inc=1, device_id=device(to), device_id_type=pl.DeviceIdType.MESH)
    at = 0
    for ref, rows in zip((p0, p1, p2, p3), PACKS):
        send_ref[at:at + rows, :] = ref[...].astype(BF16)
        at += rows
    send_ref[at:, :] = jnp.zeros((ALL * SHARE - at, C), BF16)
    pl.semaphore_wait(sem, ALL - 1)

    def first(k, frm):
        return remote(send_ref.at[share(others[k])], got_ref.at[frm], ss.at[k], rs.at[frm], others[k])

    def second(k, frm):
        return remote(part_ref, tot_ref.at[share(frm)], ss2.at[k], rs2.at[frm], chips[k])

    def third(k, block):
        return remote(tot_ref.at[share(block)], tot_ref.at[share(block)], ss3.at[k], rs3.at[k], twin)

    for k in range(ALL - 1):
        first(k, me).start()
    got_ref[me] = send_ref[share(me), :]
    for k in range(ALL - 1):
        first(k, others[k]).wait_recv()
    total = got_ref[0].astype(F32)
    for k in range(1, ALL):
        total = total + got_ref[k].astype(F32)
    part_ref[...] = total
    for k in range(ALL // 2 - 1):
        second(k, me).start()
    own = remote(part_ref, tot_ref.at[share(me)], ss3.at[7], rs3.at[7], twin)
    own.start()
    tot_ref[share(me), :] = total
    for k in range(ALL // 2 - 2, -1, -1):
        back = (me + ALL - 2 * (k + 1)) % ALL
        second(k, back).wait_recv()
        third(k, back).start()
    for k in range(ALL // 2 - 1):
        third(k, (twin + ALL - 2 * (k + 1)) % ALL).wait_recv()
    remote(part_ref, tot_ref.at[share(twin)], ss3.at[7], rs3.at[7], twin).wait_recv()
    own.wait_send()
    for k in range(ALL - 1):
        first(k, me).wait_send()
    for k in range(ALL // 2 - 1):
        second(k, me).wait_send()
        third(k, (me + ALL - 2 * (k + 1)) % ALL).wait_send()


def split_kernel(z_in, dz_in, tot, z_out, dz_out, *grads):
    z_out[...] = z_in[...]
    dz_out[...] = dz_in[...]
    pl.when(pl.program_id(0) == 0)(lambda: split_grads(tot, *grads))


def split_grads(tot, d_ln_in, d_w_proj, d_b_proj, d_ln_mid, d_w_out, d_b_out):
    at = 0
    for k in range(2):
        d_w_out[k] = tot[at:at + C, :]
        d_ln_mid[k] = tot[at + C:at + C + 2, :]
        d_b_out[k:k + 1, :] = tot[at + C + 2:at + C + 3, :]
        at += C + 16
    for k in range(2):
        for j in range(5):
            d_w_proj[k, :, j * C:(j + 1) * C] = tot[at + j * C:at + (j + 1) * C, :].T
            d_b_proj[k:k + 1, j * C:(j + 1) * C] = tot[at + 5 * C + j:at + 5 * C + j + 1, :]
        d_ln_in[k] = tot[at + 5 * C + 5:at + 5 * C + 7, :]
        at += 5 * C + 16


def finish(z_new, dz_new, packs):
    vmem = pl.BlockSpec(memory_space=pltpu.VMEM)
    dma = pltpu.SemaphoreType.DMA((ALL,))
    total = pl.pallas_call(
        sum_kernel,
        in_specs=[vmem] * 4,
        out_specs=vmem,
        out_shape=jax.ShapeDtypeStruct((ALL * SHARE, C), F32),
        scratch_shapes=[pltpu.VMEM((ALL * SHARE, C), BF16), pltpu.VMEM((ALL, SHARE, C), BF16), pltpu.VMEM((SHARE, C), F32), dma, dma, dma, dma, dma, dma],
        compiler_params=pltpu.CompilerParams(vmem_limit_bytes=VMEM_LIMIT, collective_id=5, has_side_effects=True),
        name="sum",
    )(*packs)
    shapes = ((2, 2, C), (2, C, 5 * C), (2, 5 * C), (2, 2, C), (2, C, C), (2, C))
    grads = [jax.ShapeDtypeStruct(shape, F32) for shape in shapes]
    return pl.pallas_call(
        split_kernel,
        grid=(STEPS,),
        in_specs=[by_row(z_new), by_row(dz_new), whole(total)],
        out_specs=[by_row(NATIVE)] * 2 + [pl.BlockSpec(x.shape, lambda t, n=len(x.shape): (0,) * n) for x in grads],
        out_shape=[NATIVE] * 2 + grads,
        compiler_params=pltpu.CompilerParams(dimension_semantics=("arbitrary",)),
        name="split",
    )(z_new, dz_new, total)


TRI = jax.ShapeDtypeStruct((CH, N, N), BF16)
ROW = jax.ShapeDtypeStruct((ROWS, C, N), BF16)
ROW32 = jax.ShapeDtypeStruct((ROWS, C, N), F32)
NATIVE = jax.ShapeDtypeStruct((ROWS, N, C), BF16)
POST = jax.ShapeDtypeStruct((C + 16, C), F32)
PRE = jax.ShapeDtypeStruct((5 * C + 16, C), F32)
KEEP = jax.ShapeDtypeStruct((ROWS, 4, C, N), F32)
INV = jax.ShapeDtypeStruct((STEPS, STEP, N), F32)


def by_row(array, lead=0):
    tail = array.shape[1:]
    return pl.BlockSpec((array.shape[0] // STEPS,) + tail, lambda s: ((s * STEPS) // (STEPS + lead),) + (0,) * len(tail))


def whole(array):
    zeros = (0,) * len(array.shape)
    return pl.BlockSpec(array.shape, lambda t: zeros, pipeline_mode=pl.Buffered(1))


def out_spec(array, lead):
    if array is TRI:
        return pl.BlockSpec(memory_space=pl.ANY)
    if array in (PRE, POST):
        return pl.BlockSpec(array.shape, lambda t: (0, 0))
    return by_row(array, lead)


def row_call(kernel, name, collective_id, tris, ins, consts, outs, n_back, scratch):
    lead = 1 if tris else 0
    n_send = sum(out is TRI for out in outs)
    dma = pltpu.SemaphoreType.DMA
    sent = [pltpu.VMEM((2 * C * STEP, C), F32)] * n_send + [pltpu.VMEM((STEPS, C, STEP, N), BF16)] * n_send
    sems = [dma((STEPS, GROUP))] * n_send + ([dma((n_send,))] if n_send else [])
    back = [pltpu.VMEM((4 * N * 8, C), F32)] * n_back + [pltpu.VMEM((STEPS, GROUP, STEP, CH, N), BF16)] * n_back
    back += [pltpu.VMEM((STEPS, STEP, C, N), BF16)] * n_back + [dma((STEPS, GROUP))] * (2 * n_back)
    far = pl.BlockSpec(memory_space=pl.ANY)
    near = []
    if tris:
        near = [pltpu.VMEM(x.shape, x.dtype) for x in tris] + [pltpu.VMEM((2, x.shape[0] // STEPS) + x.shape[1:], x.dtype) for x in ins]
        near += [dma((len(tris), GROUPS)), dma((2, len(ins)))]
        kernel = functools.partial(staged_kernel, kernel, len(tris), len(ins))
    return pl.pallas_call(
        kernel,
        grid=(STEPS + lead,),
        in_specs=[far if tris else by_row(x) for x in [*tris, *ins]] + [whole(x) for x in consts],
        out_specs=[out_spec(out, lead) for out in outs],
        out_shape=outs,
        scratch_shapes=sent + scratch + sems + back + near,
        compiler_params=pltpu.CompilerParams(dimension_semantics=("arbitrary",), vmem_limit_bytes=VMEM_LIMIT, collective_id=collective_id, has_side_effects=True),
        name=name,
    )(*tris, *ins, *consts)


def local_step(z_pair, pair_mask, dz_out, ln_in, w_proj, b_proj, ln_mid, w_out, b_out):
    z, dz = z_pair[0], dz_out[0]
    mask = pair_mask.reshape(STEPS, STEP, N)
    pre, post = [ln_in, w_proj, b_proj], [ln_mid, w_out, b_out]
    eye = [pltpu.VMEM((C, C), BF16)]
    pre_c = [pltpu.VMEM((2, C, N), F32), pltpu.VMEM((5 * C, C), BF16), pltpu.VMEM((5 * C, N), F32)]
    post_c = [pltpu.VMEM((2, C, N), F32), pltpu.VMEM((C, C), BF16), pltpu.VMEM((C, N), F32)]
    post_acc = [pltpu.VMEM((4, C, C), F32)]
    pre_acc = [pltpu.VMEM((5 * C, C), F32), pltpu.VMEM((5 * C, C), F32), pltpu.VMEM((2, C, C), F32)]

    gains = [pltpu.VMEM((2, C, N), F32)]
    kept = [TRI, TRI, ROW32, KEEP, ROW32, INV]
    a0, b0, g0, keep0, unit0, inv0 = row_call(pre_kernel, "pre0", 0, [], [z, mask], pre, kept, 0, eye + pre_c)
    a1, b1, g1, keep1, unit1, inv1, zm, gu0, munit0, minv0 = row_call(
        mid_kernel, "mid", 1, [a0, b0], [z, g0, mask], post + pre, kept + [ROW, ROW32, ROW32, INV], 1, eye + pre_c + post_c)
    dx1, z_new, dpg1, post_g1 = row_call(
        turn_kernel, "turn", 2, [a1, b1], [zm, g1, dz], post, [TRI, NATIVE, ROW32, POST], 1, eye + post_c + post_acc)
    dx0, dzm, dpg0, pre_g1, post_g0 = row_call(
        back_kernel, "back", 3, [a1, b1, dx1], [dpg1, keep1, unit1, inv1, dz, munit0, minv0, g0, gu0], [ln_in, w_proj, ln_mid, w_out],
        [TRI, ROW, ROW32, PRE, POST], 2, eye + gains * 2 + pre_acc + post_acc)
    dz_new, pre_g0 = row_call(
        last_kernel, "last", 4, [a0, b0, dx0], [dpg0, keep0, unit0, inv0, dzm], [ln_in, w_proj], [NATIVE, PRE], 2, gains + pre_acc)
    z_out, dz_pair, *grads = finish(z_new, dz_new, [post_g0, post_g1, pre_g0, pre_g1])
    return z_out[None], dz_pair[None], *grads


def solution(mesh):
    row_spec = P("dp", "dap")
    return jax.shard_map(local_step, mesh=mesh, in_specs=(row_spec,) * 3 + (P(),) * 6,
                         out_specs=(row_spec,) * 2 + (P(),) * 6, check_vma=False)
```

```python
import functools

import jax
import jax.numpy as jnp
from jax import lax
from jax.experimental import pallas as pl
from jax.experimental.pallas import tpu as pltpu
from jax.sharding import PartitionSpec as P

LN_EPS = 1e-5
N = 256
C = 128
GROUP = 8
ROWS = N // GROUP
CH = C // GROUP
STEP = 8
UNROLL = 4
STEPS = ROWS // STEP
PROJ = 5 * C
HAT = 16
F32 = jnp.float32
BF16 = jnp.bfloat16
VMEM_LIMIT = 62 * 1024 * 1024


def dot(lhs, rhs, lhs_dim, rhs_dim):
    return lax.dot_general(lhs, rhs, (((lhs_dim,), (rhs_dim,)), ((), ())), preferred_element_type=F32)


nn = functools.partial(dot, lhs_dim=1, rhs_dim=0)
nt = functools.partial(dot, lhs_dim=1, rhs_dim=1)
tn = functools.partial(dot, lhs_dim=0, rhs_dim=0)


def step_now():
    return pl.program_id(0)


def mean(values):
    return jnp.mean(values, axis=0, keepdims=True)


def norm(values):
    cen = values - mean(values)
    inv = lax.rsqrt(mean(cen * cen) + LN_EPS)
    return cen * inv, inv


def norm_back(d_hat, unit, inv, gain):
    d_unit = d_hat * gain
    mean_d = mean(d_unit)
    mean_du = mean(d_unit * unit)
    return inv * (d_unit - mean_d - unit * mean_du)


def fold(values):
    return values[:, :C] + values[:, C:]


def row_sums(acc):
    return jnp.sum(acc.T, axis=0, keepdims=True)


def sigmoid(values):
    return 0.5 * jnp.tanh(0.5 * values) + 0.5


def project(z_t, ln, w_t, bias):
    unit, inv = norm(z_t)
    z_hat = (unit * ln[0] + ln[1]).astype(BF16)
    return unit, inv, z_hat, nn(w_t[...], z_hat) + bias[...]


def set_eye(eye):
    same = lax.broadcasted_iota(jnp.int32, (C, C), 0) == lax.broadcasted_iota(jnp.int32, (C, C), 1)
    eye[...] = jnp.where(same, 1.0, 0.0).astype(BF16)


def set_column(ref, row):
    column = jnp.broadcast_to(row.astype(F32), (C, C)).T
    ref[:, :C] = column
    ref[:, C:] = column


def set_pre(block, ln_in, w_proj, b_proj, ln, w_t, bias):
    for k in range(2):
        set_column(ln.at[k], ln_in[block, k:k + 1, :])
    for k in range(5):
        cols = slice(k * C, (k + 1) * C)
        set_column(bias.at[cols], b_proj[block:block + 1, cols])
        w_t[cols, :] = w_proj[block, :, cols].astype(F32).T.astype(BF16)


def set_post(block, ln_mid, w_out, b_out, mln, wo_t, bo):
    for k in range(2):
        set_column(mln.at[k], ln_mid[block, k:k + 1, :])
    set_column(bo, b_out[block:block + 1, :])
    wo_t[...] = w_out[block].astype(F32).T.astype(BF16)


def place():
    me = lax.axis_index("dap")
    return me, me // 4, (me // 2) % 2, me % 2


def enter():
    me = lax.axis_index("dap")
    sem = pltpu.get_barrier_semaphore()
    for k in range(1, GROUP):
        pl.semaphore_signal(sem, inc=1, device_id={"dap": (me + k) % GROUP}, device_id_type=pl.DeviceIdType.MESH)


def all_in():
    pl.semaphore_wait(pltpu.get_barrier_semaphore(), GROUP - 1)


def peers():
    me, cy, cx, core = place()
    out = []
    for dy, dx in ((1, 1), (1, 0), (0, 1), (0, 0)):
        for dc in (1, 0):
            out.append((((cy + dy) % 2) * 2 + (cx + dx) % 2) * 2 + (core + dc) % 2)
    return me, out


def spread(ref, value, row):
    for h in range(2):
        ref[pl.ds(h * C * STEP + row, C, stride=STEP), :] = value[:, h * C:(h + 1) * C]


def pack_rows(stage, send_ref, slot):
    for h in range(2):
        for q in range(4):
            rows = stage[pl.ds((h * C + q * 32) * STEP, 32 * STEP), :].reshape(32, STEP, C)
            send_ref[slot, q * 32:(q + 1) * 32, :, h * C:(h + 1) * C] = rows.astype(BF16)


def move(src_ref, dst_ref, send_sem, recv_sem, dest, own):
    if own:
        return pltpu.make_async_copy(src_ref, dst_ref, recv_sem)
    return pltpu.make_async_remote_copy(src_ref, dst_ref, send_sem, recv_sem, device_id={"dap": dest}, device_id_type=pl.DeviceIdType.MESH)


def wait_sends(copies):
    for copy in copies:
        if copy.is_remote:
            copy.wait_send()


def row_copies(send_ref, out_ref, send_sem, recv_sem, slot):
    me, dests = peers()
    start = pl.multiple_of(me * ROWS + slot * STEP, STEP)
    return [
        move(send_ref.at[slot, pl.ds(pl.multiple_of(dest * CH, CH), CH)], out_ref.at[:, pl.ds(start, STEP), :],
             send_sem.at[slot, k], recv_sem, dest, k == GROUP - 1)
        for k, dest in enumerate(dests)
    ]


BCH = C // 2
BLOCK = N // 2


def by_column(kind, core):
    return core if kind else 1 - core


def pick(column, on_column, on_row):
    return column * on_column + (1 - column) * on_row


def channels(core):
    return pl.ds(pl.multiple_of(core * BCH, BCH), BCH)


def swap(lo, hi):
    first = lax.broadcasted_iota(jnp.int32, lo.shape, 1) < BLOCK // 2
    return jnp.where(first, lo, pltpu.roll(hi, BLOCK // 2, 1)), jnp.where(first, pltpu.roll(lo, BLOCK // 2, 1), hi)


def swap_core1(value):
    lo, hi = swap(value[BCH:, :BLOCK], value[BCH:, BLOCK:])
    return jnp.concatenate([value[:BCH], jnp.concatenate([lo, hi], axis=1)], axis=0)


def block_copies(kind, halves, send_ref, out_ref, send_sem, recv_sem, slot):
    me, cy, cx, core = place()
    out = []
    for k, (to, far) in enumerate(((0, 1), (1, 1), (1 - core, 0), (core, 0))):
        column = by_column(kind, to)
        y, x = cy, cx
        if far:
            y, x = (1 - cy, cx) if column else (cy, 1 - cx)
        start = pick(column, cy, cx) * 2 * ROWS + core * ROWS + slot * STEP
        src = send_ref.at[slot, pick(column, y, x), channels(to)] if halves else send_ref.at[slot, channels(to)]
        out.append(move(src, out_ref.at[:, pl.ds(pl.multiple_of(start, STEP), STEP), :], send_sem.at[slot, k], recv_sem, (y * 2 + x) * 2 + to, k == 3))
    return out


def pack_halves(stage, send_ref, slot):
    for h in range(2):
        for q in range(4):
            rows = stage[pl.ds((h * C + q * 32) * STEP, 32 * STEP), :].reshape(32, STEP, C)
            send_ref[slot, h, q * 32:(q + 1) * 32] = rows.astype(BF16)


A_ROWS = (pack_rows, functools.partial(block_copies, 0, False))
B_ROWS = (pack_rows, functools.partial(block_copies, 1, False))
ROWS_ALL = (pack_rows, row_copies)
DX_ROWS = (pack_halves, functools.partial(block_copies, 0, True))


def send_rows(step, jobs):
    for (pack, copies), stage, send_ref, out_ref, send_sem, recv_sem in jobs:
        pack(stage, send_ref, step)
        for copy in copies(send_ref, out_ref, send_sem, recv_sem, step):
            copy.start()

    @pl.when(step == STEPS - 1)
    def _():
        for (pack, copies), stage, send_ref, out_ref, send_sem, recv_sem in jobs:
            for slot in range(STEPS):
                wait_sends(copies(send_ref, out_ref, send_sem, recv_sem, slot))
            pltpu.make_async_copy(out_ref, out_ref, recv_sem).wait()


OUT_FWD = (lambda c, a, b: nt(a[c], b[c]),)
IN_FWD = (lambda c, a, b: tn(a[c], b[c]),)
IN_BWD = (lambda c, a, b, dx: nt(b[c], dx[c]), lambda c, a, b, dx: nn(a[c], dx[c]))
OUT_BWD = (lambda c, a, b, dx: nn(dx[c], b[c]), lambda c, a, b, dx: tn(dx[c], a[c]))


def back_copy(job, t, k, dest, frm):
    stage, send_ref, land_ref, send_sem, recv_sem = job
    return pltpu.make_async_remote_copy(
        send_ref.at[t, dest], land_ref.at[t, :, pl.ds(pl.multiple_of(frm * CH, CH), CH), :], send_sem.at[t, k], recv_sem.at[t, frm],
        device_id={"dap": dest}, device_id_type=pl.DeviceIdType.MESH)


GROUPS = 4


class Piecewise:
    def __init__(self, source, ref, sems):
        self.source, self.ref, self.sems = source, ref, sems

    def load(self, g):
        size = self.ref.shape[0] // GROUPS
        part = pl.ds(g * size, size)
        return pltpu.make_async_copy(self.source.at[part], self.ref.at[part], self.sems.at[g])


def channel_part(products, ins, jobs):
    me, dests = peers()
    refs = [x.ref for x in ins]
    for j, (product, job) in enumerate(zip(products, jobs)):
        stage, send_ref, land_ref = job[:3]

        def body(c, carry):
            value = product(c, *refs)
            for h in range(2):
                stage[pl.ds((h * 2 + c // 8) * N * 8 + c % 8, N, stride=8), :] = value[:, h * C:(h + 1) * C]
            return carry

        for g in range(GROUPS):
            if j == 0:
                for x in ins:
                    x.load(g).wait()
            lax.fori_loop(g * (CH // GROUPS), (g + 1) * (CH // GROUPS), body, 0, unroll=True)
        if j == 0:
            all_in()
        for t in range(STEPS):
            for dest in range(GROUP):
                for h in range(2):
                    at = h * 2 * N * 8 + (dest * ROWS + t * STEP) * 8
                    lo = stage[pl.ds(at, 64), :].reshape(STEP, 8, C)
                    hi = stage[pl.ds(at + N * 8, 64), :].reshape(STEP, 8, C)
                    send_ref[t, dest, :, :, h * C:(h + 1) * C] = jnp.concatenate([lo, hi], axis=1).astype(BF16)
            for k, dest in enumerate(dests[:-1]):
                back_copy(job, t, k, dest, me).start()
            land_ref[t, :, pl.ds(pl.multiple_of(me * CH, CH), CH), :] = send_ref[t, me]


def block_sends(kind, job, t):
    stage, send_ref, land_ref, send_sem, recv_sem = job
    me, cy, cx, core = place()
    column = by_column(kind, core)
    mine = pick(column, cy, cx)
    y, x = cy + column * (1 - 2 * cy), cx + (1 - column) * (1 - 2 * cx)
    land = land_ref.at[t, mine, :, channels(core), :]
    out = []
    for k, (dest, member, slot) in enumerate((((y * 2 + x) * 2, pick(column, y, x) * 2, core), ((y * 2 + x) * 2 + 1, pick(column, y, x) * 2 + 1, core),
                                              (me + 1 - 2 * core, mine * 2 + 1 - core, 2))):
        out.append(pltpu.make_async_remote_copy(send_ref.at[t, member], land, send_sem.at[t, k], recv_sem.at[t, slot],
                                                device_id={"dap": dest}, device_id_type=pl.DeviceIdType.MESH))
    return out


def block_receives(kind, job, t):
    stage, send_ref, land_ref, send_sem, recv_sem = job
    me, cy, cx, core = place()
    out = []
    for slot, (frm, far) in enumerate(((0, 1), (1, 1), (1 - core, 0))):
        column = by_column(kind, frm)
        y, x = cy, cx
        if far:
            y, x = (1 - cy, cx) if column else (cy, 1 - cx)
        out.append(pltpu.make_async_remote_copy(send_ref.at[t, 0], land_ref.at[t, pick(column, y, x), :, channels(frm), :], send_sem.at[t, slot],
                                                recv_sem.at[t, slot], device_id={"dap": (y * 2 + x) * 2 + frm}, device_id_type=pl.DeviceIdType.MESH))
    return out


def block_part(products, kinds, ins, jobs):
    me, cy, cx, core = place()
    refs = [x.ref for x in ins]
    for j, (product, kind, job) in enumerate(zip(products, kinds, jobs)):
        stage, send_ref, land_ref = job[:3]
        tiles = send_ref.shape[-1] // C

        def body(c, carry):
            value = product(c, *refs)
            for h in range(tiles):
                stage[pl.ds((h * (BCH // 8) + c // 8) * BLOCK * 8 + c % 8, BLOCK, stride=8), :] = value[:, h * C:(h + 1) * C]
            return carry

        for g in range(GROUPS):
            if j == 0:
                for x in ins:
                    x.load(g).wait()
            lax.fori_loop(g * (BCH // GROUPS), (g + 1) * (BCH // GROUPS), body, 0, unroll=4)
        if j == 0:
            all_in()
        mine = pick(by_column(kind, core), cy, cx)

        def turn(t, carry):
            for member in range(4):
                for h in range(tiles):
                    for q in range(BCH // 16):
                        at = (h * (BCH // 8) + 2 * q) * BLOCK * 8 + (member * ROWS + t * STEP) * 8
                        lo = stage[pl.ds(pl.multiple_of(at, 64), 64), :].reshape(STEP, 8, C)
                        hi = stage[pl.ds(pl.multiple_of(at + BLOCK * 8, 64), 64), :].reshape(STEP, 8, C)
                        send_ref[t, member, :, q * 16:(q + 1) * 16, h * C:(h + 1) * C] = jnp.concatenate([lo, hi], axis=1).astype(BF16)
            for copy in block_sends(kind, job, t):
                copy.start()
            land_ref[t, mine, :, channels(core), :] = send_ref[t, mine * 2 + core]
            return carry

        lax.fori_loop(0, STEPS, turn, 0)


def block_arrive(t, kinds, jobs):
    for kind, job in zip(kinds, jobs):
        for copy in block_receives(kind, job, t):
            copy.wait_recv()

    @pl.when(t == STEPS - 1)
    def _():
        for kind, job in zip(kinds, jobs):
            for slot in range(STEPS):
                for copy in block_sends(kind, job, slot):
                    copy.wait_send()


def both(land_ref, t, r):
    return land_ref[t, 0, r].astype(F32) + land_ref[t, 1, r].astype(F32)


def staged_kernel(inner, n_tri, n_in, *refs):
    far, refs = refs[:n_tri + n_in], refs[n_tri + n_in:]
    near, refs = refs[-2 - n_tri - n_in:-2], refs[:-2 - n_tri - n_in] + refs[-2:]
    refs, (tri_sem, row_sem) = refs[:-2], refs[-2:]
    step = step_now()
    tris = [Piecewise(far[k], near[k], tri_sem.at[k]) for k in range(n_tri)]

    def fetch(t, slot):
        out = []
        for k in range(n_in):
            size = far[n_tri + k].shape[0] // STEPS
            out.append(pltpu.make_async_copy(far[n_tri + k].at[pl.ds(t * size, size)], near[n_tri + k].at[slot], row_sem.at[slot, k]))
        return out

    @pl.when(step == 0)
    def _():
        for g in range(GROUPS):
            for x in tris:
                x.load(g).start()
        for copy in fetch(0, 0):
            copy.start()

    slot = (step + 1) % 2

    @pl.when(step > 0)
    def _():
        for copy in fetch(step - 1, slot):
            copy.wait()

    @pl.when((step > 0) & (step < STEPS))
    def _():
        for copy in fetch(step, 1 - slot):
            copy.start()

    inner(*tris, *[ref.at[slot] for ref in near[n_tri:]], *refs)


def arrive(t, jobs):
    me, dests = peers()
    for job in jobs:
        for k, frm in enumerate(dests[:-1]):
            back_copy(job, t, k, frm, frm).wait_recv()

    @pl.when(t == STEPS - 1)
    def _():
        for job in jobs:
            for slot in range(STEPS):
                for k, dest in enumerate(dests[:-1]):
                    back_copy(job, slot, k, dest, me).wait_send()


def rows_loop(body):
    def step(r, carry):
        body(r)
        return carry

    lax.fori_loop(0, STEP, step, 0, unroll=UNROLL)


def pre_row(r, z_t, mask_ref, ln_ref, w_t_ref, bias_ref, g_ref, keep_ref, unit_ref, inv_ref, a_stage, b_stage):
    unit, inv, _, p = project(z_t, ln_ref, w_t_ref, bias_ref)
    unit_ref[r] = unit
    inv_ref[0, pl.ds(r, 1), :] = inv
    m = mask_ref[0, pl.ds(r, 1), :].astype(F32)
    for side, stage in ((0, a_stage), (1, b_stage)):
        s = sigmoid(p[2 * side * C:(2 * side + 1) * C])
        v = p[(2 * side + 1) * C:(2 * side + 2) * C]
        sm = s * m
        spread(stage, sm * v, r)
        keep_ref[r, 2 * side] = sm
        keep_ref[r, 2 * side + 1] = v * (1.0 - s)
    g_ref[r] = sigmoid(p[4 * C:])


def pre_kernel(z_ref, mask_ref, ln_in, w_proj, b_proj, a_ref, b_ref, g_ref, keep_ref, unit_ref, inv_ref, a_st, b_st, a_send, b_send,
               eye_ref, ln_ref, w_t_ref, bias_ref, a_ss, b_ss, rs):
    step = step_now()

    @pl.when(step == 0)
    def _():
        enter()
        set_eye(eye_ref)
        set_pre(0, ln_in, w_proj, b_proj, ln_ref, w_t_ref, bias_ref)

    @rows_loop
    def _(r):
        z_t = nt(eye_ref[...], z_ref[r])
        pre_row(r, z_t, mask_ref, ln_ref, w_t_ref, bias_ref, g_ref, keep_ref, unit_ref, inv_ref, a_st, b_st)

    pl.when(step == 0)(all_in)
    send_rows(step, [(A_ROWS, a_st, a_send, a_ref, a_ss, rs.at[0]), (B_ROWS, b_st, b_send, b_ref, b_ss, rs.at[1])])


def mid_kernel(a_in, b_in, z_ref, g0_ref, mask_ref, ln_mid, w_out, b_out, ln_in, w_proj, b_proj,
               a_ref, b_ref, g_ref, keep_ref, unit_ref, inv_ref, zm_ref, gu_ref, munit_ref, minv_ref, a_st, b_st, a_send, b_send,
               eye_ref, ln_ref, w_t_ref, bias_ref, mln_ref, wo_t_ref, bo_ref, a_ss, b_ss, rs,
               st0, se0, la0, ss0, rv0):
    step = step_now()
    jobs = [(st0, se0, la0, ss0, rv0)]

    @pl.when(step == 0)
    def _():
        enter()
        set_eye(eye_ref)
        set_pre(1, ln_in, w_proj, b_proj, ln_ref, w_t_ref, bias_ref)
        set_post(0, ln_mid, w_out, b_out, mln_ref, wo_t_ref, bo_ref)
        block_part(OUT_FWD, (0,), (a_in, b_in), jobs)

    @pl.when(step > 0)
    def _():
        t = step - 1
        block_arrive(t, (0,), jobs)

        @rows_loop
        def _(r):
            unit, inv = norm(swap_core1(jnp.concatenate([la0[t, 0, r], la0[t, 1, r]], axis=1).astype(F32)))
            munit_ref[r] = unit
            minv_ref[0, pl.ds(r, 1), :] = inv
            x_hat = (unit * mln_ref[0] + mln_ref[1]).astype(BF16)
            update = nn(wo_t_ref[...], x_hat) + bo_ref[...]
            g = g0_ref[r]
            change = g * update
            gu_ref[r] = change * (1.0 - g)
            z_new = (nt(eye_ref[...], z_ref[r]) + change).astype(BF16)
            zm_ref[r] = z_new
            pre_row(r, z_new.astype(F32), mask_ref, ln_ref, w_t_ref, bias_ref, g_ref, keep_ref, unit_ref, inv_ref, a_st, b_st)

        send_rows(t, [(ROWS_ALL, a_st, a_send, a_ref, a_ss, rs.at[0]), (ROWS_ALL, b_st, b_send, b_ref, b_ss, rs.at[1])])


def post_back_row(unit, inv, g, dz, mln_ref, wo_ref, acc_ref, x_hat=None):
    if x_hat is None:
        x_hat = (unit * mln_ref[0] + mln_ref[1]).astype(BF16)
    d_up = dz * g
    d_up_bf = d_up.astype(BF16)
    acc_ref[0] += nt(x_hat, d_up_bf)
    acc_ref[3] += fold(d_up)
    d_hat = nn(wo_ref[...], d_up_bf).astype(BF16).astype(F32)
    acc_ref[1] += fold(d_hat * unit)
    acc_ref[2] += fold(d_hat)
    return norm_back(d_hat, unit, inv, mln_ref[0])


def put_post(grad_ref, acc_ref):
    grad_ref[0:C, :] = acc_ref[0]
    grad_ref[C:C + 8, :] = jnp.concatenate([row_sums(acc_ref[1]), row_sums(acc_ref[2]), row_sums(acc_ref[3]), jnp.zeros((5, C), F32)], axis=0)
    grad_ref[C + 8:C + HAT, :] = jnp.zeros((8, C), F32)


def turn_kernel(a_in, b_in, zm_ref, g_ref, dz_ref, ln_mid, w_out, b_out,
                dx_ref, z_out_ref, dpg_ref, grad_ref, d_st, d_send, eye_ref, mln_ref, wo_t_ref, bo_ref, acc_ref, d_ss, rs,
               st0, se0, la0, ss0, rv0):
    step = step_now()
    jobs = [(st0, se0, la0, ss0, rv0)]
    wo_ref = w_out.at[1]

    @pl.when(step == 0)
    def _():
        enter()
        set_eye(eye_ref)
        set_post(1, ln_mid, w_out, b_out, mln_ref, wo_t_ref, bo_ref)
        acc_ref[...] = jnp.zeros_like(acc_ref)
        channel_part(IN_FWD, (a_in, b_in), jobs)

    @pl.when(step > 0)
    def _():
        t = step - 1
        arrive(t, jobs)
        x_ref = la0.at[t]

        @rows_loop
        def _(r):
            dz = nt(eye_ref[...], dz_ref[r])
            g = g_ref[r]
            unit, inv = norm(x_ref[r].astype(F32))
            x_hat = (unit * mln_ref[0] + mln_ref[1]).astype(BF16)
            change = g * (nn(wo_t_ref[...], x_hat) + bo_ref[...])
            dpg_ref[r] = dz * change * (1.0 - g)
            z_out_ref[r] = (zm_ref[r].astype(F32) + change).T.astype(BF16)
            spread(d_st, post_back_row(unit, inv, g, dz, mln_ref, wo_ref, acc_ref, x_hat), r)

        @pl.when(t == STEPS - 1)
        def _():
            put_post(grad_ref, acc_ref)

        send_rows(t, [(ROWS_ALL, d_st, d_send, dx_ref, d_ss, rs.at[0])])


def pre_back_row(unit, inv, keep, da, db, d_pg, ln_ref, w_ref, w_acc, b_acc, l_acc):
    z_hat = (unit * ln_ref[0] + ln_ref[1]).astype(BF16)
    parts = []
    for side, d_side in ((0, da), (1, db)):
        d_v = d_side * keep[2 * side]
        parts += [d_v * keep[2 * side + 1], d_v]
    parts.append(d_pg)
    for k, part in enumerate(parts):
        b_acc[k * C:(k + 1) * C, :] += fold(part)
    d_p = jnp.concatenate([part.astype(BF16) for part in parts], axis=0)
    w_acc[...] += nt(d_p, z_hat)
    d_hat = nn(w_ref[...], d_p).astype(BF16).astype(F32)
    l_acc[0] += fold(d_hat * unit)
    l_acc[1] += fold(d_hat)
    return norm_back(d_hat, unit, inv, ln_ref[0])


def put_pre(grad_ref, w_acc, b_acc, l_acc):
    grad_ref[0:PROJ, :] = w_acc[...]
    rows = [row_sums(b_acc[k * C:(k + 1) * C, :]) for k in range(5)]
    rows += [row_sums(l_acc[0]), row_sums(l_acc[1]), jnp.zeros((1, C), F32)]
    grad_ref[PROJ:PROJ + 8, :] = jnp.concatenate(rows, axis=0)
    grad_ref[PROJ + 8:PROJ + HAT, :] = jnp.zeros((8, C), F32)


def set_gains(ref, ln, block):
    for k in range(2):
        set_column(ref.at[k], ln[block, k:k + 1, :])


def back_kernel(a_in, b_in, dx_in, dpg1_ref, keep_ref, unit_ref, inv_ref, dz_ref, munit_ref, minv_ref, g_ref, gu_ref, ln_in, w_proj, ln_mid, w_out,
                dx_ref, dzm_ref, dpg_ref, grad1_ref, grad0_ref, d_st, d_send,
                eye_ref, ln_ref, mln_ref, w_acc, b_acc, l_acc, acc_ref, d_ss, rs,
               st0, st1, se0, se1, la0, la1, ss0, ss1, rv0, rv1):
    step = step_now()
    jobs = [(st0, se0, la0, ss0, rv0), (st1, se1, la1, ss1, rv1)]
    w_ref, wo_ref = w_proj.at[1], w_out.at[0]

    @pl.when(step == 0)
    def _():
        enter()
        set_eye(eye_ref)
        set_gains(ln_ref, ln_in, 1)
        set_gains(mln_ref, ln_mid, 0)
        for ref in (w_acc, b_acc, l_acc, acc_ref):
            ref[...] = jnp.zeros_like(ref)
        channel_part(IN_BWD, (a_in, b_in, dx_in), jobs)

    @pl.when(step > 0)
    def _():
        t = step - 1
        arrive(t, jobs)
        da_ref, db_ref = la0.at[t], la1.at[t]

        @rows_loop
        def _(r):
            at = pl.ds(r, 1)
            dzn = pre_back_row(unit_ref[r], inv_ref[0, at, :], keep_ref.at[r], da_ref[r].astype(F32), db_ref[r].astype(F32), dpg1_ref[r],
                               ln_ref, w_ref, w_acc, b_acc, l_acc)
            dzm = (nt(eye_ref[...], dz_ref[r]) + dzn).astype(BF16)
            dzm_ref[r] = dzm
            dzm = dzm.astype(F32)
            dpg_ref[r] = dzm * gu_ref[r]
            spread(d_st, swap_core1(post_back_row(munit_ref[r], minv_ref[0, at, :], g_ref[r], dzm, mln_ref, wo_ref, acc_ref)), r)

        @pl.when(t == STEPS - 1)
        def _():
            put_pre(grad1_ref, w_acc, b_acc, l_acc)
            put_post(grad0_ref, acc_ref)

        send_rows(t, [(DX_ROWS, d_st, d_send, dx_ref, d_ss, rs.at[0])])


def last_kernel(a_in, b_in, dx_in, dpg_ref, keep_ref, unit_ref, inv_ref, dzm_ref, ln_in, w_proj,
                dz_ref, grad_ref, ln_ref, w_acc, b_acc, l_acc,
               st0, st1, se0, se1, la0, la1, ss0, ss1, rv0, rv1):
    step = step_now()
    jobs = [(st0, se0, la0, ss0, rv0), (st0, se1, la1, ss1, rv1)]
    w_ref = w_proj.at[0]

    @pl.when(step == 0)
    def _():
        enter()
        set_gains(ln_ref, ln_in, 0)
        for ref in (w_acc, b_acc, l_acc):
            ref[...] = jnp.zeros_like(ref)
        block_part(OUT_BWD, (0, 1), (a_in, b_in, dx_in), jobs)

    @pl.when(step > 0)
    def _():
        t = step - 1
        block_arrive(t, (0, 1), jobs)

        @rows_loop
        def _(r):
            dzn = pre_back_row(unit_ref[r], inv_ref[0, pl.ds(r, 1), :], keep_ref.at[r], both(la0, t, r), both(la1, t, r), dpg_ref[r],
                               ln_ref, w_ref, w_acc, b_acc, l_acc)
            dz_ref[r] = (dzm_ref[r].astype(F32) + dzn).T.astype(BF16)

        @pl.when(t == STEPS - 1)
        def _():
            put_pre(grad_ref, w_acc, b_acc, l_acc)


ALL = 16
SHARE = 112
PACKS = (C + HAT, C + HAT, PROJ + HAT, PROJ + HAT)


def share(k):
    return pl.ds(pl.multiple_of(k * SHARE, SHARE), SHARE)


def sum_kernel(p0, p1, p2, p3, tot_ref, send_ref, got_ref, part_ref, ss, rs, ss2, rs2, ss3, rs3):
    dp, dap = lax.axis_index("dp"), lax.axis_index("dap")
    me = dp * GROUP + dap
    core = dap % 2
    twin = me + 1 - 2 * core
    others = [(me + k) % ALL for k in range(1, ALL)]
    chips = [(me + 2 * k) % ALL for k in range(1, ALL // 2)]

    def device(o):
        return {"dp": o // GROUP, "dap": o % GROUP}

    def remote(src, dst, send_sem, recv_sem, to):
        return pltpu.make_async_remote_copy(src, dst, send_sem, recv_sem, device_id=device(to), device_id_type=pl.DeviceIdType.MESH)

    sem = pltpu.get_barrier_semaphore()
    for to in others:
        pl.semaphore_signal(sem, inc=1, device_id=device(to), device_id_type=pl.DeviceIdType.MESH)
    at = 0
    for ref, rows in zip((p0, p1, p2, p3), PACKS):
        send_ref[at:at + rows, :] = ref[...].astype(BF16)
        at += rows
    send_ref[at:, :] = jnp.zeros((ALL * SHARE - at, C), BF16)
    pl.semaphore_wait(sem, ALL - 1)

    def first(k, frm):
        return remote(send_ref.at[share(others[k])], got_ref.at[frm], ss.at[k], rs.at[frm], others[k])

    def second(k, frm):
        return remote(part_ref, tot_ref.at[share(frm)], ss2.at[k], rs2.at[frm], chips[k])

    def third(k, block):
        return remote(tot_ref.at[share(block)], tot_ref.at[share(block)], ss3.at[k], rs3.at[k], twin)

    for k in range(ALL - 1):
        first(k, me).start()
    got_ref[me] = send_ref[share(me), :]
    for k in range(ALL - 1):
        first(k, others[k]).wait_recv()
    total = got_ref[0].astype(F32)
    for k in range(1, ALL):
        total = total + got_ref[k].astype(F32)
    part_ref[...] = total
    for k in range(ALL // 2 - 1):
        second(k, me).start()
    own = remote(part_ref, tot_ref.at[share(me)], ss3.at[7], rs3.at[7], twin)
    own.start()
    tot_ref[share(me), :] = total
    for k in range(ALL // 2 - 2, -1, -1):
        back = (me + ALL - 2 * (k + 1)) % ALL
        second(k, back).wait_recv()
        third(k, back).start()
    for k in range(ALL // 2 - 1):
        third(k, (twin + ALL - 2 * (k + 1)) % ALL).wait_recv()
    remote(part_ref, tot_ref.at[share(twin)], ss3.at[7], rs3.at[7], twin).wait_recv()
    own.wait_send()
    for k in range(ALL - 1):
        first(k, me).wait_send()
    for k in range(ALL // 2 - 1):
        second(k, me).wait_send()
        third(k, (me + ALL - 2 * (k + 1)) % ALL).wait_send()


def split_kernel(z_in, dz_in, tot, z_out, dz_out, *grads):
    z_out[...] = z_in[...]
    dz_out[...] = dz_in[...]
    pl.when(step_now() == 0)(lambda: split_grads(tot, *grads))


def split_grads(tot, d_ln_in, d_w_proj, d_b_proj, d_ln_mid, d_w_out, d_b_out):
    at = 0
    for k in range(2):
        d_w_out[k] = tot[at:at + C, :]
        d_ln_mid[k] = tot[at + C:at + C + 2, :]
        d_b_out[k:k + 1, :] = tot[at + C + 2:at + C + 3, :]
        at += C + HAT
    for k in range(2):
        for j in range(5):
            d_w_proj[k, :, j * C:(j + 1) * C] = tot[at + j * C:at + (j + 1) * C, :].T
            d_b_proj[k:k + 1, j * C:(j + 1) * C] = tot[at + PROJ + j:at + PROJ + j + 1, :]
        d_ln_in[k] = tot[at + PROJ + 5:at + PROJ + 7, :]
        at += PROJ + HAT


def finish(z_new, dz_new, packs):
    vmem = pl.BlockSpec(memory_space=pltpu.VMEM)
    dma = pltpu.SemaphoreType.DMA((ALL,))
    total = pl.pallas_call(
        sum_kernel,
        in_specs=[vmem] * 4,
        out_specs=vmem,
        out_shape=jax.ShapeDtypeStruct((ALL * SHARE, C), F32),
        scratch_shapes=[pltpu.VMEM((ALL * SHARE, C), BF16), pltpu.VMEM((ALL, SHARE, C), BF16), pltpu.VMEM((SHARE, C), F32), dma, dma, dma, dma, dma, dma],
        compiler_params=pltpu.CompilerParams(vmem_limit_bytes=VMEM_LIMIT, collective_id=5, has_side_effects=True),
        name="sum",
    )(*packs)
    shapes = ((2, 2, C), (2, C, PROJ), (2, PROJ), (2, 2, C), (2, C, C), (2, C))
    grads = [jax.ShapeDtypeStruct(shape, F32) for shape in shapes]
    return pl.pallas_call(
        split_kernel,
        grid=(STEPS,),
        in_specs=[by_row(z_new), by_row(dz_new), whole(total)],
        out_specs=[by_row(NATIVE)] * 2 + [pl.BlockSpec(x.shape, lambda t, n=len(x.shape): (0,) * n) for x in grads],
        out_shape=[NATIVE] * 2 + grads,
        compiler_params=pltpu.CompilerParams(dimension_semantics=("arbitrary",)),
        name="split",
    )(z_new, dz_new, total)


TRI = jax.ShapeDtypeStruct((CH, N, N), BF16)
BTRI = jax.ShapeDtypeStruct((BCH, BLOCK, N), BF16)
BDX = jax.ShapeDtypeStruct((BCH, BLOCK, BLOCK), BF16)
SENT = (TRI, BTRI, BDX)
ROW = jax.ShapeDtypeStruct((ROWS, C, N), BF16)
ROW32 = jax.ShapeDtypeStruct((ROWS, C, N), F32)
NATIVE = jax.ShapeDtypeStruct((ROWS, N, C), BF16)
POST = jax.ShapeDtypeStruct((C + HAT, C), F32)
PRE = jax.ShapeDtypeStruct((PROJ + HAT, C), F32)
KEEP = jax.ShapeDtypeStruct((ROWS, 4, C, N), F32)
INV = jax.ShapeDtypeStruct((STEPS, STEP, N), F32)


def by_row(array, lead=0):
    tail = array.shape[1:]
    return pl.BlockSpec((array.shape[0] // STEPS,) + tail, lambda s: ((s * STEPS) // (STEPS + lead),) + (0,) * len(tail))


def whole(array):
    zeros = (0,) * len(array.shape)
    return pl.BlockSpec(array.shape, lambda t: zeros, pipeline_mode=pl.Buffered(1))


def out_spec(array, lead):
    if array in SENT:
        return pl.BlockSpec(memory_space=pl.ANY)
    if array in (PRE, POST):
        return pl.BlockSpec(array.shape, lambda t: (0, 0))
    return by_row(array, lead)


def row_call(kernel, name, collective_id, tris, ins, consts, outs, n_back, scratch, width=0):
    lead = 1 if tris else 0
    n_send = sum(out in SENT for out in outs)
    packed = (STEPS, 2, C, STEP, BLOCK) if BDX in outs else (STEPS, C, STEP, N)
    dma = pltpu.SemaphoreType.DMA
    sent = [pltpu.VMEM((2 * C * STEP, C), F32)] * n_send + [pltpu.VMEM(packed, BF16)] * n_send
    sems = [dma((STEPS, GROUP))] * n_send + ([dma((n_send,))] if n_send else [])
    back = [pltpu.VMEM((4 * N * 8, C), F32)] * n_back + [pltpu.VMEM((STEPS, GROUP, STEP, CH, N), BF16)] * n_back
    back += [pltpu.VMEM((STEPS, STEP, C, N), BF16)] * n_back
    if width:
        back = [pltpu.VMEM((BCH * BLOCK * width // C if k == 0 else 8, C), F32) for k in range(n_back)]
        back += [pltpu.VMEM((STEPS, 4, STEP, BCH, width), BF16)] * n_back + [pltpu.VMEM((STEPS, 2, STEP, C, width), BF16)] * n_back
    back += [dma((STEPS, GROUP))] * (2 * n_back)
    far = pl.BlockSpec(memory_space=pl.ANY)
    near = []
    if tris:
        near = [pltpu.VMEM(x.shape, x.dtype) for x in tris] + [pltpu.VMEM((2, x.shape[0] // STEPS) + x.shape[1:], x.dtype) for x in ins]
        near += [dma((len(tris), GROUPS)), dma((2, len(ins)))]
        kernel = functools.partial(staged_kernel, kernel, len(tris), len(ins))
    return pl.pallas_call(
        kernel,
        grid=(STEPS + lead,),
        in_specs=[far if tris else by_row(x) for x in [*tris, *ins]] + [whole(x) for x in consts],
        out_specs=[out_spec(out, lead) for out in outs],
        out_shape=outs,
        scratch_shapes=sent + scratch + sems + back + near,
        compiler_params=pltpu.CompilerParams(dimension_semantics=("arbitrary",), vmem_limit_bytes=VMEM_LIMIT, collective_id=collective_id, has_side_effects=True),
        name=name,
    )(*tris, *ins, *consts)


def local_step(z_pair, pair_mask, dz_out, ln_in, w_proj, b_proj, ln_mid, w_out, b_out):
    z, dz = z_pair[0], dz_out[0]
    mask = pair_mask.reshape(STEPS, STEP, N)
    pre, post = [ln_in, w_proj, b_proj], [ln_mid, w_out, b_out]
    eye = [pltpu.VMEM((C, C), BF16)]
    pre_c = [pltpu.VMEM((2, C, N), F32), pltpu.VMEM((PROJ, C), BF16), pltpu.VMEM((PROJ, N), F32)]
    post_c = [pltpu.VMEM((2, C, N), F32), pltpu.VMEM((C, C), BF16), pltpu.VMEM((C, N), F32)]
    post_acc = [pltpu.VMEM((4, C, C), F32)]
    pre_acc = [pltpu.VMEM((PROJ, C), F32), pltpu.VMEM((PROJ, C), F32), pltpu.VMEM((2, C, C), F32)]

    gains = [pltpu.VMEM((2, C, N), F32)]
    kept = [TRI, TRI, ROW32, KEEP, ROW32, INV]
    a0, b0, g0, keep0, unit0, inv0 = row_call(pre_kernel, "pre0", 0, [], [z, mask], pre, [BTRI, BTRI] + kept[2:], 0, eye + pre_c)
    a1, b1, g1, keep1, unit1, inv1, zm, gu0, munit0, minv0 = row_call(
        mid_kernel, "mid", 1, [a0, b0], [z, g0, mask], post + pre, kept + [ROW, ROW32, ROW32, INV], 1, eye + pre_c + post_c, BLOCK)
    dx1, z_new, dpg1, post_g1 = row_call(
        turn_kernel, "turn", 2, [a1, b1], [zm, g1, dz], post, [TRI, NATIVE, ROW32, POST], 1, eye + post_c + post_acc)
    dx0, dzm, dpg0, pre_g1, post_g0 = row_call(
        back_kernel, "back", 3, [a1, b1, dx1], [dpg1, keep1, unit1, inv1, dz, munit0, minv0, g0, gu0], [ln_in, w_proj, ln_mid, w_out],
        [BDX, ROW, ROW32, PRE, POST], 2, eye + gains * 2 + pre_acc + post_acc)
    dz_new, pre_g0 = row_call(
        last_kernel, "last", 4, [a0, b0, dx0], [dpg0, keep0, unit0, inv0, dzm], [ln_in, w_proj], [NATIVE, PRE], 2, gains + pre_acc, N)
    z_out, dz_pair, *grads = finish(z_new, dz_new, [post_g0, post_g1, pre_g0, pre_g1])
    return z_out[None], dz_pair[None], *grads


def solution(mesh):
    row_spec = P("dp", "dap")
    return jax.shard_map(local_step, mesh=mesh, in_specs=(row_spec,) * 3 + (P(),) * 6,
                         out_specs=(row_spec,) * 2 + (P(),) * 6, check_vma=False)
```

```python
import functools

import jax
import jax.numpy as jnp
from jax import lax
from jax.experimental import pallas as pl
from jax.experimental.pallas import tpu as pltpu
from jax.sharding import PartitionSpec as P

LN_EPS = 1e-5
N = 256
C = 128
GROUP = 8
ROWS = N // GROUP
CH = C // GROUP
STEP = 8
UNROLL = 4
STEPS = ROWS // STEP
PROJ = 5 * C
HAT = 16
F32 = jnp.float32
BF16 = jnp.bfloat16
VMEM_LIMIT = 62 * 1024 * 1024


def dot(lhs, rhs, lhs_dim, rhs_dim):
    return lax.dot_general(lhs, rhs, (((lhs_dim,), (rhs_dim,)), ((), ())), preferred_element_type=F32)


nn = functools.partial(dot, lhs_dim=1, rhs_dim=0)
nt = functools.partial(dot, lhs_dim=1, rhs_dim=1)
tn = functools.partial(dot, lhs_dim=0, rhs_dim=0)


def step_now():
    return pl.program_id(0)


def mean(values):
    return jnp.mean(values, axis=0, keepdims=True)


def norm(values):
    cen = values - mean(values)
    inv = lax.rsqrt(mean(cen * cen) + LN_EPS)
    return cen * inv, inv


def norm_back(d_hat, unit, inv, gain):
    d_unit = d_hat * gain
    mean_d = mean(d_unit)
    mean_du = mean(d_unit * unit)
    return inv * (d_unit - mean_d - unit * mean_du)


def fold(values):
    return values[:, :C] + values[:, C:]


def row_sums(acc):
    return jnp.sum(acc.T, axis=0, keepdims=True)


def sigmoid(values):
    return 0.5 * jnp.tanh(0.5 * values) + 0.5


def project(z_t, ln, w_t, bias):
    unit, inv = norm(z_t)
    z_hat = (unit * ln[0] + ln[1]).astype(BF16)
    return unit, inv, z_hat, nn(w_t[...], z_hat) + bias[...]


def set_eye(eye):
    same = lax.broadcasted_iota(jnp.int32, (C, C), 0) == lax.broadcasted_iota(jnp.int32, (C, C), 1)
    eye[...] = jnp.where(same, 1.0, 0.0).astype(BF16)


def set_column(ref, row):
    column = jnp.broadcast_to(row.astype(F32), (C, C)).T
    ref[:, :C] = column
    ref[:, C:] = column


def set_pre(block, ln_in, w_proj, b_proj, ln, w_t, bias):
    for k in range(2):
        set_column(ln.at[k], ln_in[block, k:k + 1, :])
    for k in range(5):
        cols = slice(k * C, (k + 1) * C)
        set_column(bias.at[cols], b_proj[block:block + 1, cols])
        w_t[cols, :] = w_proj[block, :, cols].astype(F32).T.astype(BF16)


def set_post(block, ln_mid, w_out, b_out, mln, wo_t, bo):
    for k in range(2):
        set_column(mln.at[k], ln_mid[block, k:k + 1, :])
    set_column(bo, b_out[block:block + 1, :])
    wo_t[...] = w_out[block].astype(F32).T.astype(BF16)


def place():
    me = lax.axis_index("dap")
    return me, me // 4, (me // 2) % 2, me % 2


def enter():
    me = lax.axis_index("dap")
    sem = pltpu.get_barrier_semaphore()
    for k in range(1, GROUP):
        pl.semaphore_signal(sem, inc=1, device_id={"dap": (me + k) % GROUP}, device_id_type=pl.DeviceIdType.MESH)


def all_in():
    pl.semaphore_wait(pltpu.get_barrier_semaphore(), GROUP - 1)


def peers():
    me, cy, cx, core = place()
    out = []
    for dy, dx in ((1, 1), (1, 0), (0, 1), (0, 0)):
        for dc in (1, 0):
            out.append((((cy + dy) % 2) * 2 + (cx + dx) % 2) * 2 + (core + dc) % 2)
    return me, out


def spread(ref, value, row):
    for h in range(2):
        ref[pl.ds(h * C * STEP + row, C, stride=STEP), :] = value[:, h * C:(h + 1) * C]


def pack_rows(stage, send_ref, slot):
    for h in range(2):
        for q in range(4):
            rows = stage[pl.ds((h * C + q * 32) * STEP, 32 * STEP), :].reshape(32, STEP, C)
            send_ref[slot, q * 32:(q + 1) * 32, :, h * C:(h + 1) * C] = rows.astype(BF16)


def move(src_ref, dst_ref, send_sem, recv_sem, dest, own):
    if own:
        return pltpu.make_async_copy(src_ref, dst_ref, recv_sem)
    return pltpu.make_async_remote_copy(src_ref, dst_ref, send_sem, recv_sem, device_id={"dap": dest}, device_id_type=pl.DeviceIdType.MESH)


def wait_sends(copies):
    for copy in copies:
        if copy.is_remote:
            copy.wait_send()


def row_copies(send_ref, out_ref, send_sem, recv_sem, slot):
    me, dests = peers()
    start = pl.multiple_of(me * ROWS + slot * STEP, STEP)
    return [
        move(send_ref.at[slot, pl.ds(pl.multiple_of(dest * CH, CH), CH)], out_ref.at[:, pl.ds(start, STEP), :],
             send_sem.at[slot, k], recv_sem, dest, k == GROUP - 1)
        for k, dest in enumerate(dests)
    ]


BCH = C // 2
BLOCK = N // 2


def by_column(kind, core):
    return core if kind else 1 - core


def pick(column, on_column, on_row):
    return column * on_column + (1 - column) * on_row


def channels(core):
    return pl.ds(pl.multiple_of(core * BCH, BCH), BCH)


def swap(lo, hi):
    first = lax.broadcasted_iota(jnp.int32, lo.shape, 1) < BLOCK // 2
    return jnp.where(first, lo, pltpu.roll(hi, BLOCK // 2, 1)), jnp.where(first, pltpu.roll(lo, BLOCK // 2, 1), hi)


def swap_core1(value):
    lo, hi = swap(value[BCH:, :BLOCK], value[BCH:, BLOCK:])
    return jnp.concatenate([value[:BCH], jnp.concatenate([lo, hi], axis=1)], axis=0)


def block_copies(kind, halves, send_ref, out_ref, send_sem, recv_sem, slot):
    me, cy, cx, core = place()
    out = []
    for k, (to, far) in enumerate(((0, 1), (1, 1), (1 - core, 0), (core, 0))):
        column = by_column(kind, to)
        y, x = cy, cx
        if far:
            y, x = (1 - cy, cx) if column else (cy, 1 - cx)
        start = pick(column, cy, cx) * 2 * ROWS + core * ROWS + slot * STEP
        src = send_ref.at[slot, pick(column, y, x), channels(to)] if halves else send_ref.at[slot, channels(to)]
        out.append(move(src, out_ref.at[:, pl.ds(pl.multiple_of(start, STEP), STEP), :], send_sem.at[slot, k], recv_sem, (y * 2 + x) * 2 + to, k == 3))
    return out


def pack_halves(stage, send_ref, slot):
    for h in range(2):
        for q in range(4):
            rows = stage[pl.ds((h * C + q * 32) * STEP, 32 * STEP), :].reshape(32, STEP, C)
            send_ref[slot, h, q * 32:(q + 1) * 32] = rows.astype(BF16)


A_ROWS = (pack_rows, functools.partial(block_copies, 0, False))
B_ROWS = (pack_rows, functools.partial(block_copies, 1, False))
ROWS_ALL = (pack_rows, row_copies)
DX_ROWS = (pack_halves, functools.partial(block_copies, 0, True))


def send_rows(step, jobs):
    for (pack, copies), stage, send_ref, out_ref, send_sem, recv_sem in jobs:
        pack(stage, send_ref, step)
        for copy in copies(send_ref, out_ref, send_sem, recv_sem, step):
            copy.start()

    @pl.when(step == STEPS - 1)
    def _():
        for (pack, copies), stage, send_ref, out_ref, send_sem, recv_sem in jobs:
            for slot in range(STEPS):
                wait_sends(copies(send_ref, out_ref, send_sem, recv_sem, slot))
            pltpu.make_async_copy(out_ref, out_ref, recv_sem).wait()


OUT_FWD = (lambda c, a, b: nt(a[c], b[c]),)
IN_FWD = (lambda c, a, b: tn(a[c], b[c]),)
IN_BWD = (lambda c, a, b, dx: nt(b[c], dx[c]), lambda c, a, b, dx: nn(a[c], dx[c]))
OUT_BWD = (lambda c, a, b, dx: nn(dx[c], b[c]), lambda c, a, b, dx: tn(dx[c], a[c]))


def back_copy(job, t, k, dest, frm):
    stage, send_ref, land_ref, send_sem, recv_sem = job
    return pltpu.make_async_remote_copy(
        send_ref.at[t, dest], land_ref.at[t, :, pl.ds(pl.multiple_of(frm * CH, CH), CH), :], send_sem.at[t, k], recv_sem.at[t, frm],
        device_id={"dap": dest}, device_id_type=pl.DeviceIdType.MESH)


EARLY = 2
GROUPS = 4


class Piecewise:
    def __init__(self, source, ref, sems):
        self.source, self.ref, self.sems = source, ref, sems

    def load(self, g):
        size = self.ref.shape[0] // GROUPS
        part = pl.ds(g * size, size)
        return pltpu.make_async_copy(self.source.at[part], self.ref.at[part], self.sems.at[g])


def channel_part(products, ins, jobs):
    me, dests = peers()
    refs = [x.ref for x in ins]
    for j, (product, job) in enumerate(zip(products, jobs)):
        stage, send_ref, land_ref = job[:3]

        def body(c, carry):
            value = product(c, *refs)
            for h in range(2):
                stage[pl.ds((h * 2 + c // 8) * N * 8 + c % 8, N, stride=8), :] = value[:, h * C:(h + 1) * C]
            return carry

        for g in range(GROUPS):
            if j == 0:
                for x in ins:
                    x.load(g).wait()
            lax.fori_loop(g * (CH // GROUPS), (g + 1) * (CH // GROUPS), body, 0, unroll=True)
        if j == 0:
            all_in()
        for t in range(STEPS):
            for dest in range(GROUP):
                for h in range(2):
                    at = h * 2 * N * 8 + (dest * ROWS + t * STEP) * 8
                    lo = stage[pl.ds(at, 64), :].reshape(STEP, 8, C)
                    hi = stage[pl.ds(at + N * 8, 64), :].reshape(STEP, 8, C)
                    send_ref[t, dest, :, :, h * C:(h + 1) * C] = jnp.concatenate([lo, hi], axis=1).astype(BF16)
            for k, dest in enumerate(dests[:-1]):
                back_copy(job, t, k, dest, me).start()
            land_ref[t, :, pl.ds(pl.multiple_of(me * CH, CH), CH), :] = send_ref[t, me]


def block_sends(kind, job, t, piece=None):
    stage, send_ref, land_ref, send_sem, recv_sem = job
    me, cy, cx, core = place()
    column = by_column(kind, core)
    mine = pick(column, cy, cx)
    y, x = cy + column * (1 - 2 * cy), cx + (1 - column) * (1 - 2 * cx)
    size = BCH if piece is None else BCH // GROUPS
    at = (piece or 0) * size
    land = land_ref.at[t, mine, :, pl.ds(pl.multiple_of(core * BCH + at, size), size), :]
    out = []
    for k, (dest, member, slot) in enumerate((((y * 2 + x) * 2, pick(column, y, x) * 2, core), ((y * 2 + x) * 2 + 1, pick(column, y, x) * 2 + 1, core),
                                              (me + 1 - 2 * core, mine * 2 + 1 - core, 2))):
        out.append(pltpu.make_async_remote_copy(send_ref.at[t, member, :, pl.ds(at, size), :], land, send_sem.at[t, k], recv_sem.at[t, slot],
                                                device_id={"dap": dest}, device_id_type=pl.DeviceIdType.MESH))
    return out


def block_receives(kind, job, t):
    stage, send_ref, land_ref, send_sem, recv_sem = job
    me, cy, cx, core = place()
    out = []
    for slot, (frm, far) in enumerate(((0, 1), (1, 1), (1 - core, 0))):
        column = by_column(kind, frm)
        y, x = cy, cx
        if far:
            y, x = (1 - cy, cx) if column else (cy, 1 - cx)
        out.append(pltpu.make_async_remote_copy(send_ref.at[t, 0], land_ref.at[t, pick(column, y, x), :, channels(frm), :], send_sem.at[t, slot],
                                                recv_sem.at[t, slot], device_id={"dap": (y * 2 + x) * 2 + frm}, device_id_type=pl.DeviceIdType.MESH))
    return out


def block_part(products, kinds, ins, jobs):
    me, cy, cx, core = place()
    refs = [x.ref for x in ins]
    for j, (product, kind, job) in enumerate(zip(products, kinds, jobs)):
        stage, send_ref, land_ref = job[:3]
        tiles = send_ref.shape[-1] // C

        def body(c, carry):
            value = product(c, *refs)
            for h in range(tiles):
                stage[pl.ds((h * (BCH // 8) + c // 8) * BLOCK * 8 + c % 8, BLOCK, stride=8), :] = value[:, h * C:(h + 1) * C]
            return carry

        mine = pick(by_column(kind, core), cy, cx)

        def pack(t, q):
            for member in range(4):
                for h in range(tiles):
                    at = (h * (BCH // 8) + q * 2) * BLOCK * 8 + (member * ROWS + t * STEP) * 8
                    lo = stage[pl.ds(at, 64), :].reshape(STEP, 8, C)
                    hi = stage[pl.ds(at + BLOCK * 8, 64), :].reshape(STEP, 8, C)
                    send_ref[t, member, :, q * CH:(q + 1) * CH, h * C:(h + 1) * C] = jnp.concatenate([lo, hi], axis=1).astype(BF16)

        def keep(t):
            land_ref[t, mine, :, channels(core), :] = send_ref[t, mine * 2 + core]

        for g in range(GROUPS):
            if j == 0:
                for x in ins:
                    x.load(g).wait()
            lax.fori_loop(g * CH, (g + 1) * CH, body, 0, unroll=4)
            if g == j == 0:
                all_in()
            for t in range(EARLY):
                pack(t, g)
                for copy in block_sends(kind, job, t, g):
                    copy.start()
        for t in range(EARLY, STEPS):
            for g in range(GROUPS):
                pack(t, g)
            for copy in block_sends(kind, job, t):
                copy.start()
        for t in range(STEPS):
            keep(t)


def block_arrive(t, kinds, jobs):
    for kind, job in zip(kinds, jobs):
        for copy in block_receives(kind, job, t):
            copy.wait_recv()

    @pl.when(t == STEPS - 1)
    def _():
        for kind, job in zip(kinds, jobs):
            for slot in range(STEPS):
                for copy in block_sends(kind, job, slot):
                    copy.wait_send()


def both(land_ref, t, r):
    return land_ref[t, 0, r].astype(F32) + land_ref[t, 1, r].astype(F32)


def staged_kernel(inner, n_tri, n_in, *refs):
    far, refs = refs[:n_tri + n_in], refs[n_tri + n_in:]
    near, refs = refs[-2 - n_tri - n_in:-2], refs[:-2 - n_tri - n_in] + refs[-2:]
    refs, (tri_sem, row_sem) = refs[:-2], refs[-2:]
    step = step_now()
    tris = [Piecewise(far[k], near[k], tri_sem.at[k]) for k in range(n_tri)]

    def fetch(t, slot):
        out = []
        for k in range(n_in):
            size = far[n_tri + k].shape[0] // STEPS
            out.append(pltpu.make_async_copy(far[n_tri + k].at[pl.ds(t * size, size)], near[n_tri + k].at[slot], row_sem.at[slot, k]))
        return out

    @pl.when(step == 0)
    def _():
        for g in range(GROUPS):
            for x in tris:
                x.load(g).start()
        for copy in fetch(0, 0):
            copy.start()

    slot = (step + 1) % 2

    @pl.when(step > 0)
    def _():
        for copy in fetch(step - 1, slot):
            copy.wait()

    @pl.when((step > 0) & (step < STEPS))
    def _():
        for copy in fetch(step, 1 - slot):
            copy.start()

    inner(*tris, *[ref.at[slot] for ref in near[n_tri:]], *refs)


def arrive(t, jobs):
    me, dests = peers()
    for job in jobs:
        for k, frm in enumerate(dests[:-1]):
            back_copy(job, t, k, frm, frm).wait_recv()

    @pl.when(t == STEPS - 1)
    def _():
        for job in jobs:
            for slot in range(STEPS):
                for k, dest in enumerate(dests[:-1]):
                    back_copy(job, slot, k, dest, me).wait_send()


def rows_loop(body):
    def step(r, carry):
        body(r)
        return carry

    lax.fori_loop(0, STEP, step, 0, unroll=UNROLL)


def pre_row(r, z_t, mask_ref, ln_ref, w_t_ref, bias_ref, g_ref, keep_ref, unit_ref, inv_ref, a_stage, b_stage):
    unit, inv, _, p = project(z_t, ln_ref, w_t_ref, bias_ref)
    unit_ref[r] = unit
    inv_ref[0, pl.ds(r, 1), :] = inv
    m = mask_ref[0, pl.ds(r, 1), :].astype(F32)
    for side, stage in ((0, a_stage), (1, b_stage)):
        s = sigmoid(p[2 * side * C:(2 * side + 1) * C])
        v = p[(2 * side + 1) * C:(2 * side + 2) * C]
        sm = s * m
        spread(stage, sm * v, r)
        keep_ref[r, 2 * side] = sm
        keep_ref[r, 2 * side + 1] = v * (1.0 - s)
    g_ref[r] = sigmoid(p[4 * C:])


def pre_kernel(z_ref, mask_ref, ln_in, w_proj, b_proj, a_ref, b_ref, g_ref, keep_ref, unit_ref, inv_ref, a_st, b_st, a_send, b_send,
               eye_ref, ln_ref, w_t_ref, bias_ref, a_ss, b_ss, rs):
    step = step_now()

    @pl.when(step == 0)
    def _():
        enter()
        set_eye(eye_ref)
        set_pre(0, ln_in, w_proj, b_proj, ln_ref, w_t_ref, bias_ref)

    @rows_loop
    def _(r):
        z_t = nt(eye_ref[...], z_ref[r])
        pre_row(r, z_t, mask_ref, ln_ref, w_t_ref, bias_ref, g_ref, keep_ref, unit_ref, inv_ref, a_st, b_st)

    pl.when(step == 0)(all_in)
    send_rows(step, [(A_ROWS, a_st, a_send, a_ref, a_ss, rs.at[0]), (B_ROWS, b_st, b_send, b_ref, b_ss, rs.at[1])])


def mid_kernel(a_in, b_in, z_ref, g0_ref, mask_ref, ln_mid, w_out, b_out, ln_in, w_proj, b_proj,
               a_ref, b_ref, g_ref, keep_ref, unit_ref, inv_ref, zm_ref, gu_ref, munit_ref, minv_ref, a_st, b_st, a_send, b_send,
               eye_ref, ln_ref, w_t_ref, bias_ref, mln_ref, wo_t_ref, bo_ref, a_ss, b_ss, rs,
               st0, se0, la0, ss0, rv0):
    step = step_now()
    jobs = [(st0, se0, la0, ss0, rv0)]

    @pl.when(step == 0)
    def _():
        enter()
        set_eye(eye_ref)
        set_pre(1, ln_in, w_proj, b_proj, ln_ref, w_t_ref, bias_ref)
        set_post(0, ln_mid, w_out, b_out, mln_ref, wo_t_ref, bo_ref)
        block_part(OUT_FWD, (0,), (a_in, b_in), jobs)

    @pl.when(step > 0)
    def _():
        t = step - 1
        block_arrive(t, (0,), jobs)

        @rows_loop
        def _(r):
            unit, inv = norm(swap_core1(jnp.concatenate([la0[t, 0, r], la0[t, 1, r]], axis=1).astype(F32)))
            munit_ref[r] = unit
            minv_ref[0, pl.ds(r, 1), :] = inv
            x_hat = (unit * mln_ref[0] + mln_ref[1]).astype(BF16)
            update = nn(wo_t_ref[...], x_hat) + bo_ref[...]
            g = g0_ref[r]
            change = g * update
            gu_ref[r] = change * (1.0 - g)
            z_new = (nt(eye_ref[...], z_ref[r]) + change).astype(BF16)
            zm_ref[r] = z_new
            pre_row(r, z_new.astype(F32), mask_ref, ln_ref, w_t_ref, bias_ref, g_ref, keep_ref, unit_ref, inv_ref, a_st, b_st)

        send_rows(t, [(ROWS_ALL, a_st, a_send, a_ref, a_ss, rs.at[0]), (ROWS_ALL, b_st, b_send, b_ref, b_ss, rs.at[1])])


def post_back_row(unit, inv, g, dz, mln_ref, wo_ref, acc_ref, x_hat=None):
    if x_hat is None:
        x_hat = (unit * mln_ref[0] + mln_ref[1]).astype(BF16)
    d_up = dz * g
    d_up_bf = d_up.astype(BF16)
    acc_ref[0] += nt(x_hat, d_up_bf)
    acc_ref[3] += fold(d_up)
    d_hat = nn(wo_ref[...], d_up_bf).astype(BF16).astype(F32)
    acc_ref[1] += fold(d_hat * unit)
    acc_ref[2] += fold(d_hat)
    return norm_back(d_hat, unit, inv, mln_ref[0])


def put_post(grad_ref, acc_ref):
    grad_ref[0:C, :] = acc_ref[0]
    grad_ref[C:C + 8, :] = jnp.concatenate([row_sums(acc_ref[1]), row_sums(acc_ref[2]), row_sums(acc_ref[3]), jnp.zeros((5, C), F32)], axis=0)
    grad_ref[C + 8:C + HAT, :] = jnp.zeros((8, C), F32)


def turn_kernel(a_in, b_in, zm_ref, g_ref, dz_ref, ln_mid, w_out, b_out,
                dx_ref, z_out_ref, dpg_ref, grad_ref, d_st, d_send, eye_ref, mln_ref, wo_t_ref, bo_ref, acc_ref, d_ss, rs,
               st0, se0, la0, ss0, rv0):
    step = step_now()
    jobs = [(st0, se0, la0, ss0, rv0)]
    wo_ref = w_out.at[1]

    @pl.when(step == 0)
    def _():
        enter()
        set_eye(eye_ref)
        set_post(1, ln_mid, w_out, b_out, mln_ref, wo_t_ref, bo_ref)
        acc_ref[...] = jnp.zeros_like(acc_ref)
        channel_part(IN_FWD, (a_in, b_in), jobs)

    @pl.when(step > 0)
    def _():
        t = step - 1
        arrive(t, jobs)
        x_ref = la0.at[t]

        @rows_loop
        def _(r):
            dz = nt(eye_ref[...], dz_ref[r])
            g = g_ref[r]
            unit, inv = norm(x_ref[r].astype(F32))
            x_hat = (unit * mln_ref[0] + mln_ref[1]).astype(BF16)
            change = g * (nn(wo_t_ref[...], x_hat) + bo_ref[...])
            dpg_ref[r] = dz * change * (1.0 - g)
            z_out_ref[r] = (zm_ref[r].astype(F32) + change).T.astype(BF16)
            spread(d_st, post_back_row(unit, inv, g, dz, mln_ref, wo_ref, acc_ref, x_hat), r)

        @pl.when(t == STEPS - 1)
        def _():
            put_post(grad_ref, acc_ref)

        send_rows(t, [(ROWS_ALL, d_st, d_send, dx_ref, d_ss, rs.at[0])])


def pre_back_row(unit, inv, keep, da, db, d_pg, ln_ref, w_ref, w_acc, b_acc, l_acc):
    z_hat = (unit * ln_ref[0] + ln_ref[1]).astype(BF16)
    parts = []
    for side, d_side in ((0, da), (1, db)):
        d_v = d_side * keep[2 * side]
        parts += [d_v * keep[2 * side + 1], d_v]
    parts.append(d_pg)
    for k, part in enumerate(parts):
        b_acc[k * C:(k + 1) * C, :] += fold(part)
    d_p = jnp.concatenate([part.astype(BF16) for part in parts], axis=0)
    w_acc[...] += nt(d_p, z_hat)
    d_hat = nn(w_ref[...], d_p).astype(BF16).astype(F32)
    l_acc[0] += fold(d_hat * unit)
    l_acc[1] += fold(d_hat)
    return norm_back(d_hat, unit, inv, ln_ref[0])


def put_pre(grad_ref, w_acc, b_acc, l_acc):
    grad_ref[0:PROJ, :] = w_acc[...]
    rows = [row_sums(b_acc[k * C:(k + 1) * C, :]) for k in range(5)]
    rows += [row_sums(l_acc[0]), row_sums(l_acc[1]), jnp.zeros((1, C), F32)]
    grad_ref[PROJ:PROJ + 8, :] = jnp.concatenate(rows, axis=0)
    grad_ref[PROJ + 8:PROJ + HAT, :] = jnp.zeros((8, C), F32)


def set_gains(ref, ln, block):
    for k in range(2):
        set_column(ref.at[k], ln[block, k:k + 1, :])


def back_kernel(a_in, b_in, dx_in, dpg1_ref, keep_ref, unit_ref, inv_ref, dz_ref, munit_ref, minv_ref, g_ref, gu_ref, ln_in, w_proj, ln_mid, w_out,
                dx_ref, dzm_ref, dpg_ref, grad1_ref, grad0_ref, d_st, d_send,
                eye_ref, ln_ref, mln_ref, w_acc, b_acc, l_acc, acc_ref, d_ss, rs,
               st0, st1, se0, se1, la0, la1, ss0, ss1, rv0, rv1):
    step = step_now()
    jobs = [(st0, se0, la0, ss0, rv0), (st1, se1, la1, ss1, rv1)]
    w_ref, wo_ref = w_proj.at[1], w_out.at[0]

    @pl.when(step == 0)
    def _():
        enter()
        set_eye(eye_ref)
        set_gains(ln_ref, ln_in, 1)
        set_gains(mln_ref, ln_mid, 0)
        for ref in (w_acc, b_acc, l_acc, acc_ref):
            ref[...] = jnp.zeros_like(ref)
        channel_part(IN_BWD, (a_in, b_in, dx_in), jobs)

    @pl.when(step > 0)
    def _():
        t = step - 1
        arrive(t, jobs)
        da_ref, db_ref = la0.at[t], la1.at[t]

        @rows_loop
        def _(r):
            at = pl.ds(r, 1)
            dzn = pre_back_row(unit_ref[r], inv_ref[0, at, :], keep_ref.at[r], da_ref[r].astype(F32), db_ref[r].astype(F32), dpg1_ref[r],
                               ln_ref, w_ref, w_acc, b_acc, l_acc)
            dzm = (nt(eye_ref[...], dz_ref[r]) + dzn).astype(BF16)
            dzm_ref[r] = dzm
            dzm = dzm.astype(F32)
            dpg_ref[r] = dzm * gu_ref[r]
            spread(d_st, swap_core1(post_back_row(munit_ref[r], minv_ref[0, at, :], g_ref[r], dzm, mln_ref, wo_ref, acc_ref)), r)

        @pl.when(t == STEPS - 1)
        def _():
            put_pre(grad1_ref, w_acc, b_acc, l_acc)
            put_post(grad0_ref, acc_ref)

        send_rows(t, [(DX_ROWS, d_st, d_send, dx_ref, d_ss, rs.at[0])])


def last_kernel(a_in, b_in, dx_in, dpg_ref, keep_ref, unit_ref, inv_ref, dzm_ref, ln_in, w_proj,
                dz_ref, grad_ref, ln_ref, w_acc, b_acc, l_acc,
               st0, st1, se0, se1, la0, la1, ss0, ss1, rv0, rv1):
    step = step_now()
    jobs = [(st0, se0, la0, ss0, rv0), (st0, se1, la1, ss1, rv1)]
    w_ref = w_proj.at[0]

    @pl.when(step == 0)
    def _():
        enter()
        set_gains(ln_ref, ln_in, 0)
        for ref in (w_acc, b_acc, l_acc):
            ref[...] = jnp.zeros_like(ref)
        block_part(OUT_BWD, (0, 1), (a_in, b_in, dx_in), jobs)

    @pl.when(step > 0)
    def _():
        t = step - 1
        block_arrive(t, (0, 1), jobs)

        @rows_loop
        def _(r):
            dzn = pre_back_row(unit_ref[r], inv_ref[0, pl.ds(r, 1), :], keep_ref.at[r], both(la0, t, r), both(la1, t, r), dpg_ref[r],
                               ln_ref, w_ref, w_acc, b_acc, l_acc)
            dz_ref[r] = (dzm_ref[r].astype(F32) + dzn).T.astype(BF16)

        @pl.when(t == STEPS - 1)
        def _():
            put_pre(grad_ref, w_acc, b_acc, l_acc)


ALL = 16
SHARE = 112
PACKS = (C + HAT, C + HAT, PROJ + HAT, PROJ + HAT)


def share(k):
    return pl.ds(pl.multiple_of(k * SHARE, SHARE), SHARE)


def sum_kernel(p0, p1, p2, p3, tot_ref, send_ref, got_ref, part_ref, ss, rs, ss2, rs2, ss3, rs3):
    dp, dap = lax.axis_index("dp"), lax.axis_index("dap")
    me = dp * GROUP + dap
    core = dap % 2
    twin = me + 1 - 2 * core
    others = [(me + k) % ALL for k in range(1, ALL)]
    chips = [(me + 2 * k) % ALL for k in range(1, ALL // 2)]

    def device(o):
        return {"dp": o // GROUP, "dap": o % GROUP}

    def remote(src, dst, send_sem, recv_sem, to):
        return pltpu.make_async_remote_copy(src, dst, send_sem, recv_sem, device_id=device(to), device_id_type=pl.DeviceIdType.MESH)

    sem = pltpu.get_barrier_semaphore()
    for to in others:
        pl.semaphore_signal(sem, inc=1, device_id=device(to), device_id_type=pl.DeviceIdType.MESH)
    at = 0
    for ref, rows in zip((p0, p1, p2, p3), PACKS):
        send_ref[at:at + rows, :] = ref[...].astype(BF16)
        at += rows
    send_ref[at:, :] = jnp.zeros((ALL * SHARE - at, C), BF16)
    pl.semaphore_wait(sem, ALL - 1)

    def first(k, frm):
        return remote(send_ref.at[share(others[k])], got_ref.at[frm], ss.at[k], rs.at[frm], others[k])

    def second(k, frm):
        return remote(part_ref, tot_ref.at[share(frm)], ss2.at[k], rs2.at[frm], chips[k])

    def third(k, block):
        return remote(tot_ref.at[share(block)], tot_ref.at[share(block)], ss3.at[k], rs3.at[k], twin)

    for k in range(ALL - 1):
        first(k, me).start()
    got_ref[me] = send_ref[share(me), :]
    for k in range(ALL - 1):
        first(k, others[k]).wait_recv()
    total = got_ref[0].astype(F32)
    for k in range(1, ALL):
        total = total + got_ref[k].astype(F32)
    part_ref[...] = total
    for k in range(ALL // 2 - 1):
        second(k, me).start()
    own = remote(part_ref, tot_ref.at[share(me)], ss3.at[7], rs3.at[7], twin)
    own.start()
    tot_ref[share(me), :] = total
    for k in range(ALL // 2 - 2, -1, -1):
        back = (me + ALL - 2 * (k + 1)) % ALL
        second(k, back).wait_recv()
        third(k, back).start()
    for k in range(ALL // 2 - 1):
        third(k, (twin + ALL - 2 * (k + 1)) % ALL).wait_recv()
    remote(part_ref, tot_ref.at[share(twin)], ss3.at[7], rs3.at[7], twin).wait_recv()
    own.wait_send()
    for k in range(ALL - 1):
        first(k, me).wait_send()
    for k in range(ALL // 2 - 1):
        second(k, me).wait_send()
        third(k, (me + ALL - 2 * (k + 1)) % ALL).wait_send()


def split_kernel(z_in, dz_in, tot, z_out, dz_out, *grads):
    z_out[...] = z_in[...]
    dz_out[...] = dz_in[...]
    pl.when(step_now() == 0)(lambda: split_grads(tot, *grads))


def split_grads(tot, d_ln_in, d_w_proj, d_b_proj, d_ln_mid, d_w_out, d_b_out):
    at = 0
    for k in range(2):
        d_w_out[k] = tot[at:at + C, :]
        d_ln_mid[k] = tot[at + C:at + C + 2, :]
        d_b_out[k:k + 1, :] = tot[at + C + 2:at + C + 3, :]
        at += C + HAT
    for k in range(2):
        for j in range(5):
            d_w_proj[k, :, j * C:(j + 1) * C] = tot[at + j * C:at + (j + 1) * C, :].T
            d_b_proj[k:k + 1, j * C:(j + 1) * C] = tot[at + PROJ + j:at + PROJ + j + 1, :]
        d_ln_in[k] = tot[at + PROJ + 5:at + PROJ + 7, :]
        at += PROJ + HAT


def finish(z_new, dz_new, packs):
    vmem = pl.BlockSpec(memory_space=pltpu.VMEM)
    dma = pltpu.SemaphoreType.DMA((ALL,))
    total = pl.pallas_call(
        sum_kernel,
        in_specs=[vmem] * 4,
        out_specs=vmem,
        out_shape=jax.ShapeDtypeStruct((ALL * SHARE, C), F32),
        scratch_shapes=[pltpu.VMEM((ALL * SHARE, C), BF16), pltpu.VMEM((ALL, SHARE, C), BF16), pltpu.VMEM((SHARE, C), F32), dma, dma, dma, dma, dma, dma],
        compiler_params=pltpu.CompilerParams(vmem_limit_bytes=VMEM_LIMIT, collective_id=5, has_side_effects=True),
        name="sum",
    )(*packs)
    shapes = ((2, 2, C), (2, C, PROJ), (2, PROJ), (2, 2, C), (2, C, C), (2, C))
    grads = [jax.ShapeDtypeStruct(shape, F32) for shape in shapes]
    return pl.pallas_call(
        split_kernel,
        grid=(STEPS,),
        in_specs=[by_row(z_new), by_row(dz_new), whole(total)],
        out_specs=[by_row(NATIVE)] * 2 + [pl.BlockSpec(x.shape, lambda t, n=len(x.shape): (0,) * n) for x in grads],
        out_shape=[NATIVE] * 2 + grads,
        compiler_params=pltpu.CompilerParams(dimension_semantics=("arbitrary",)),
        name="split",
    )(z_new, dz_new, total)


TRI = jax.ShapeDtypeStruct((CH, N, N), BF16)
BTRI = jax.ShapeDtypeStruct((BCH, BLOCK, N), BF16)
BDX = jax.ShapeDtypeStruct((BCH, BLOCK, BLOCK), BF16)
SENT = (TRI, BTRI, BDX)
ROW = jax.ShapeDtypeStruct((ROWS, C, N), BF16)
ROW32 = jax.ShapeDtypeStruct((ROWS, C, N), F32)
NATIVE = jax.ShapeDtypeStruct((ROWS, N, C), BF16)
POST = jax.ShapeDtypeStruct((C + HAT, C), F32)
PRE = jax.ShapeDtypeStruct((PROJ + HAT, C), F32)
KEEP = jax.ShapeDtypeStruct((ROWS, 4, C, N), F32)
INV = jax.ShapeDtypeStruct((STEPS, STEP, N), F32)


def by_row(array, lead=0):
    tail = array.shape[1:]
    return pl.BlockSpec((array.shape[0] // STEPS,) + tail, lambda s: ((s * STEPS) // (STEPS + lead),) + (0,) * len(tail))


def whole(array):
    zeros = (0,) * len(array.shape)
    return pl.BlockSpec(array.shape, lambda t: zeros, pipeline_mode=pl.Buffered(1))


def out_spec(array, lead):
    if array in SENT:
        return pl.BlockSpec(memory_space=pl.ANY)
    if array in (PRE, POST):
        return pl.BlockSpec(array.shape, lambda t: (0, 0))
    return by_row(array, lead)


def row_call(kernel, name, collective_id, tris, ins, consts, outs, n_back, scratch, width=0):
    lead = 1 if tris else 0
    n_send = sum(out in SENT for out in outs)
    packed = (STEPS, 2, C, STEP, BLOCK) if BDX in outs else (STEPS, C, STEP, N)
    dma = pltpu.SemaphoreType.DMA
    sent = [pltpu.VMEM((2 * C * STEP, C), F32)] * n_send + [pltpu.VMEM(packed, BF16)] * n_send
    sems = [dma((STEPS, GROUP))] * n_send + ([dma((n_send,))] if n_send else [])
    back = [pltpu.VMEM((4 * N * 8, C), F32)] * n_back + [pltpu.VMEM((STEPS, GROUP, STEP, CH, N), BF16)] * n_back
    back += [pltpu.VMEM((STEPS, STEP, C, N), BF16)] * n_back
    if width:
        back = [pltpu.VMEM((BCH * BLOCK * width // C if k == 0 else 8, C), F32) for k in range(n_back)]
        back += [pltpu.VMEM((STEPS, 4, STEP, BCH, width), BF16)] * n_back + [pltpu.VMEM((STEPS, 2, STEP, C, width), BF16)] * n_back
    back += [dma((STEPS, GROUP))] * (2 * n_back)
    far = pl.BlockSpec(memory_space=pl.ANY)
    near = []
    if tris:
        near = [pltpu.VMEM(x.shape, x.dtype) for x in tris] + [pltpu.VMEM((2, x.shape[0] // STEPS) + x.shape[1:], x.dtype) for x in ins]
        near += [dma((len(tris), GROUPS)), dma((2, len(ins)))]
        kernel = functools.partial(staged_kernel, kernel, len(tris), len(ins))
    return pl.pallas_call(
        kernel,
        grid=(STEPS + lead,),
        in_specs=[far if tris else by_row(x) for x in [*tris, *ins]] + [whole(x) for x in consts],
        out_specs=[out_spec(out, lead) for out in outs],
        out_shape=outs,
        scratch_shapes=sent + scratch + sems + back + near,
        compiler_params=pltpu.CompilerParams(dimension_semantics=("arbitrary",), vmem_limit_bytes=VMEM_LIMIT, collective_id=collective_id, has_side_effects=True),
        name=name,
    )(*tris, *ins, *consts)


def local_step(z_pair, pair_mask, dz_out, ln_in, w_proj, b_proj, ln_mid, w_out, b_out):
    z, dz = z_pair[0], dz_out[0]
    mask = pair_mask.reshape(STEPS, STEP, N)
    pre, post = [ln_in, w_proj, b_proj], [ln_mid, w_out, b_out]
    eye = [pltpu.VMEM((C, C), BF16)]
    pre_c = [pltpu.VMEM((2, C, N), F32), pltpu.VMEM((PROJ, C), BF16), pltpu.VMEM((PROJ, N), F32)]
    post_c = [pltpu.VMEM((2, C, N), F32), pltpu.VMEM((C, C), BF16), pltpu.VMEM((C, N), F32)]
    post_acc = [pltpu.VMEM((4, C, C), F32)]
    pre_acc = [pltpu.VMEM((PROJ, C), F32), pltpu.VMEM((PROJ, C), F32), pltpu.VMEM((2, C, C), F32)]

    gains = [pltpu.VMEM((2, C, N), F32)]
    kept = [TRI, TRI, ROW32, KEEP, ROW32, INV]
    a0, b0, g0, keep0, unit0, inv0 = row_call(pre_kernel, "pre0", 0, [], [z, mask], pre, [BTRI, BTRI] + kept[2:], 0, eye + pre_c)
    a1, b1, g1, keep1, unit1, inv1, zm, gu0, munit0, minv0 = row_call(
        mid_kernel, "mid", 1, [a0, b0], [z, g0, mask], post + pre, kept + [ROW, ROW32, ROW32, INV], 1, eye + pre_c + post_c, BLOCK)
    dx1, z_new, dpg1, post_g1 = row_call(
        turn_kernel, "turn", 2, [a1, b1], [zm, g1, dz], post, [TRI, NATIVE, ROW32, POST], 1, eye + post_c + post_acc)
    dx0, dzm, dpg0, pre_g1, post_g0 = row_call(
        back_kernel, "back", 3, [a1, b1, dx1], [dpg1, keep1, unit1, inv1, dz, munit0, minv0, g0, gu0], [ln_in, w_proj, ln_mid, w_out],
        [BDX, ROW, ROW32, PRE, POST], 2, eye + gains * 2 + pre_acc + post_acc)
    dz_new, pre_g0 = row_call(
        last_kernel, "last", 4, [a0, b0, dx0], [dpg0, keep0, unit0, inv0, dzm], [ln_in, w_proj], [NATIVE, PRE], 2, gains + pre_acc, N)
    z_out, dz_pair, *grads = finish(z_new, dz_new, [post_g0, post_g1, pre_g0, pre_g1])
    return z_out[None], dz_pair[None], *grads


def solution(mesh):
    row_spec = P("dp", "dap")
    return jax.shard_map(local_step, mesh=mesh, in_specs=(row_spec,) * 3 + (P(),) * 6,
                         out_specs=(row_spec,) * 2 + (P(),) * 6, check_vma=False)
```

```python
import functools

import jax
import jax.numpy as jnp
from jax import lax
from jax.experimental import pallas as pl
from jax.experimental.pallas import tpu as pltpu
from jax.sharding import PartitionSpec as P

LN_EPS = 1e-5
N = 256
C = 128
GROUP = 8
ROWS = N // GROUP
CH = C // GROUP
STEP = 8
UNROLL = 4
STEPS = ROWS // STEP
PROJ = 5 * C
HAT = 16
F32 = jnp.float32
BF16 = jnp.bfloat16
VMEM_LIMIT = 62 * 1024 * 1024


def dot(lhs, rhs, lhs_dim, rhs_dim):
    return lax.dot_general(lhs, rhs, (((lhs_dim,), (rhs_dim,)), ((), ())), preferred_element_type=F32)


nn = functools.partial(dot, lhs_dim=1, rhs_dim=0)
nt = functools.partial(dot, lhs_dim=1, rhs_dim=1)
tn = functools.partial(dot, lhs_dim=0, rhs_dim=0)


def step_now():
    return pl.program_id(0)


def mean(values):
    return jnp.mean(values, axis=0, keepdims=True)


def norm(values):
    cen = values - mean(values)
    inv = lax.rsqrt(mean(cen * cen) + LN_EPS)
    return cen * inv, inv


def norm_back(d_hat, unit, inv, gain):
    d_unit = d_hat * gain
    mean_d = mean(d_unit)
    mean_du = mean(d_unit * unit)
    return inv * (d_unit - mean_d - unit * mean_du)


def fold(values):
    return values[:, :C] + values[:, C:]


def row_sums(acc):
    return jnp.sum(acc.T, axis=0, keepdims=True)


def sigmoid(values):
    return 0.5 * jnp.tanh(0.5 * values) + 0.5


def project(z_t, ln, w_t, bias):
    unit, inv = norm(z_t)
    z_hat = (unit * ln[0] + ln[1]).astype(BF16)
    return unit, inv, z_hat, nn(w_t[...], z_hat) + bias[...]


def set_eye(eye):
    same = lax.broadcasted_iota(jnp.int32, (C, C), 0) == lax.broadcasted_iota(jnp.int32, (C, C), 1)
    eye[...] = jnp.where(same, 1.0, 0.0).astype(BF16)


def set_column(ref, row):
    column = jnp.broadcast_to(row.astype(F32), (C, C)).T
    ref[:, :C] = column
    ref[:, C:] = column


def set_pre(block, ln_in, w_proj, b_proj, ln, w_t, bias):
    for k in range(2):
        set_column(ln.at[k], ln_in[block, k:k + 1, :])
    for k in range(5):
        cols = slice(k * C, (k + 1) * C)
        set_column(bias.at[cols], b_proj[block:block + 1, cols])
        w_t[cols, :] = w_proj[block, :, cols].astype(F32).T.astype(BF16)


def set_post(block, ln_mid, w_out, b_out, mln, wo_t, bo):
    for k in range(2):
        set_column(mln.at[k], ln_mid[block, k:k + 1, :])
    set_column(bo, b_out[block:block + 1, :])
    wo_t[...] = w_out[block].astype(F32).T.astype(BF16)


def place():
    me = lax.axis_index("dap")
    return me, me // 4, (me // 2) % 2, me % 2


def enter():
    me = lax.axis_index("dap")
    sem = pltpu.get_barrier_semaphore()
    for k in range(1, GROUP):
        pl.semaphore_signal(sem, inc=1, device_id={"dap": (me + k) % GROUP}, device_id_type=pl.DeviceIdType.MESH)


def all_in(others=GROUP - 1):
    pl.semaphore_wait(pltpu.get_barrier_semaphore(), others)


def peers():
    me, cy, cx, core = place()
    out = []
    for dy, dx in ((1, 1), (1, 0), (0, 1), (0, 0)):
        for dc in (1, 0):
            out.append((((cy + dy) % 2) * 2 + (cx + dx) % 2) * 2 + (core + dc) % 2)
    return me, out


def spread(ref, value, row):
    for h in range(2):
        ref[pl.ds(h * C * STEP + row, C, stride=STEP), :] = value[:, h * C:(h + 1) * C]


def pack_rows(stage, send_ref, slot):
    for h in range(2):
        for q in range(4):
            rows = stage[pl.ds((h * C + q * 32) * STEP, 32 * STEP), :].reshape(32, STEP, C)
            send_ref[slot, q * 32:(q + 1) * 32, :, h * C:(h + 1) * C] = rows.astype(BF16)


def move(src_ref, dst_ref, send_sem, recv_sem, dest, own):
    if own:
        return pltpu.make_async_copy(src_ref, dst_ref, recv_sem)
    return pltpu.make_async_remote_copy(src_ref, dst_ref, send_sem, recv_sem, device_id={"dap": dest}, device_id_type=pl.DeviceIdType.MESH)


def wait_sends(copies):
    for copy in copies:
        if copy.is_remote:
            copy.wait_send()


def row_copies(send_ref, out_ref, send_sem, recv_sem, slot):
    me, dests = peers()
    start = pl.multiple_of(me * ROWS + slot * STEP, STEP)
    return [
        move(send_ref.at[slot, pl.ds(pl.multiple_of(dest * CH, CH), CH)], out_ref.at[:, pl.ds(start, STEP), :],
             send_sem.at[slot, k], recv_sem, dest, k == GROUP - 1)
        for k, dest in enumerate(dests)
    ]


BCH = C // 2
BLOCK = N // 2


def by_column(kind, core):
    return core if kind else 1 - core


def pick(column, on_column, on_row):
    return column * on_column + (1 - column) * on_row


def channels(core):
    return pl.ds(pl.multiple_of(core * BCH, BCH), BCH)


def swap(lo, hi):
    first = lax.broadcasted_iota(jnp.int32, lo.shape, 1) < BLOCK // 2
    return jnp.where(first, lo, pltpu.roll(hi, BLOCK // 2, 1)), jnp.where(first, pltpu.roll(lo, BLOCK // 2, 1), hi)


def swap_core1(value):
    lo, hi = swap(value[BCH:, :BLOCK], value[BCH:, BLOCK:])
    return jnp.concatenate([value[:BCH], jnp.concatenate([lo, hi], axis=1)], axis=0)


def block_copies(kind, halves, send_ref, out_ref, send_sem, recv_sem, slot):
    me, cy, cx, core = place()
    out = []
    for k, (to, far) in enumerate(((0, 1), (1, 1), (1 - core, 0), (core, 0))):
        column = by_column(kind, to)
        y, x = cy, cx
        if far:
            y, x = (1 - cy, cx) if column else (cy, 1 - cx)
        start = pick(column, cy, cx) * 2 * ROWS + core * ROWS + slot * STEP
        src = send_ref.at[slot, pick(column, y, x), channels(to)] if halves else send_ref.at[slot, channels(to)]
        out.append(move(src, out_ref.at[:, pl.ds(pl.multiple_of(start, STEP), STEP), :], send_sem.at[slot, k], recv_sem, (y * 2 + x) * 2 + to, k == 3))
    return out


def pack_halves(stage, send_ref, slot):
    for h in range(2):
        for q in range(4):
            rows = stage[pl.ds((h * C + q * 32) * STEP, 32 * STEP), :].reshape(32, STEP, C)
            send_ref[slot, h, q * 32:(q + 1) * 32] = rows.astype(BF16)


A_ROWS = (pack_rows, functools.partial(block_copies, 0, False))
B_ROWS = (pack_rows, functools.partial(block_copies, 1, False))
ROWS_ALL = (pack_rows, row_copies)
DX_ROWS = (pack_halves, functools.partial(block_copies, 0, True))


def send_rows(step, jobs):
    for (pack, copies), stage, send_ref, out_ref, send_sem, recv_sem in jobs:
        pack(stage, send_ref, step)
        for copy in copies(send_ref, out_ref, send_sem, recv_sem, step):
            copy.start()

    @pl.when(step == STEPS - 1)
    def _():
        for (pack, copies), stage, send_ref, out_ref, send_sem, recv_sem in jobs:
            for slot in range(STEPS):
                wait_sends(copies(send_ref, out_ref, send_sem, recv_sem, slot))
            pltpu.make_async_copy(out_ref, out_ref, recv_sem).wait()


OUT_FWD = (lambda c, a, b: nt(a[c], b[c]),)
IN_FWD = (lambda c, a, b: tn(a[c], b[c]),)
IN_BWD = (lambda c, a, b, dx: nt(b[c], dx[c]), lambda c, a, b, dx: nn(a[c], dx[c]))
OUT_BWD = (lambda c, a, b, dx: nn(dx[c], b[c]), lambda c, a, b, dx: tn(dx[c], a[c]))


def back_copy(job, t, k, dest, frm):
    stage, send_ref, land_ref, send_sem, recv_sem = job
    return pltpu.make_async_remote_copy(
        send_ref.at[t, dest], land_ref.at[t, :, pl.ds(pl.multiple_of(frm * CH, CH), CH), :], send_sem.at[t, k], recv_sem.at[t, frm],
        device_id={"dap": dest}, device_id_type=pl.DeviceIdType.MESH)


EARLY = 2
GROUPS = 4


class Piecewise:
    def __init__(self, source, ref, sems):
        self.source, self.ref, self.sems = source, ref, sems

    def load(self, g):
        size = self.ref.shape[0] // GROUPS
        part = pl.ds(g * size, size)
        return pltpu.make_async_copy(self.source.at[part], self.ref.at[part], self.sems.at[g])


def channel_part(products, ins, jobs):
    me, dests = peers()
    refs = [x.ref for x in ins]
    for j, (product, job) in enumerate(zip(products, jobs)):
        stage, send_ref, land_ref = job[:3]

        def body(c, carry):
            value = product(c, *refs)
            for h in range(2):
                stage[pl.ds((h * 2 + c // 8) * N * 8 + c % 8, N, stride=8), :] = value[:, h * C:(h + 1) * C]
            return carry

        for g in range(GROUPS):
            if j == 0:
                for x in ins:
                    x.load(g).wait()
            lax.fori_loop(g * (CH // GROUPS), (g + 1) * (CH // GROUPS), body, 0, unroll=True)
        if j == 0:
            all_in()
        for t in range(STEPS):
            for dest in range(GROUP):
                for h in range(2):
                    at = h * 2 * N * 8 + (dest * ROWS + t * STEP) * 8
                    lo = stage[pl.ds(at, 64), :].reshape(STEP, 8, C)
                    hi = stage[pl.ds(at + N * 8, 64), :].reshape(STEP, 8, C)
                    send_ref[t, dest, :, :, h * C:(h + 1) * C] = jnp.concatenate([lo, hi], axis=1).astype(BF16)
            for k, dest in enumerate(dests[:-1]):
                back_copy(job, t, k, dest, me).start()
            land_ref[t, :, pl.ds(pl.multiple_of(me * CH, CH), CH), :] = send_ref[t, me]


def block_sends(kind, job, t, piece=None):
    stage, send_ref, land_ref, send_sem, recv_sem = job
    me, cy, cx, core = place()
    column = by_column(kind, core)
    mine = pick(column, cy, cx)
    y, x = cy + column * (1 - 2 * cy), cx + (1 - column) * (1 - 2 * cx)
    size = BCH if piece is None else BCH // GROUPS
    at = (piece or 0) * size
    land = land_ref.at[t, mine, :, pl.ds(pl.multiple_of(core * BCH + at, size), size), :]
    out = []
    for k, (dest, member, slot) in enumerate((((y * 2 + x) * 2, pick(column, y, x) * 2, core), ((y * 2 + x) * 2 + 1, pick(column, y, x) * 2 + 1, core),
                                              (me + 1 - 2 * core, mine * 2 + 1 - core, 2))):
        out.append(pltpu.make_async_remote_copy(send_ref.at[t, member, :, pl.ds(at, size), :], land, send_sem.at[t, k], recv_sem.at[t, slot],
                                                device_id={"dap": dest}, device_id_type=pl.DeviceIdType.MESH))
    return out


def block_receives(kind, job, t):
    stage, send_ref, land_ref, send_sem, recv_sem = job
    me, cy, cx, core = place()
    out = []
    for slot, (frm, far) in enumerate(((0, 1), (1, 1), (1 - core, 0))):
        column = by_column(kind, frm)
        y, x = cy, cx
        if far:
            y, x = (1 - cy, cx) if column else (cy, 1 - cx)
        out.append(pltpu.make_async_remote_copy(send_ref.at[t, 0], land_ref.at[t, pick(column, y, x), :, channels(frm), :], send_sem.at[t, slot],
                                                recv_sem.at[t, slot], device_id={"dap": (y * 2 + x) * 2 + frm}, device_id_type=pl.DeviceIdType.MESH))
    return out


def block_part(products, kinds, ins, jobs, others=GROUP - 1):
    me, cy, cx, core = place()
    refs = [x.ref for x in ins]
    for j, (product, kind, job) in enumerate(zip(products, kinds, jobs)):
        stage, send_ref, land_ref = job[:3]
        tiles = send_ref.shape[-1] // C

        def body(c, carry):
            value = product(c, *refs)
            for h in range(tiles):
                stage[pl.ds((h * (BCH // 8) + c // 8) * BLOCK * 8 + c % 8, BLOCK, stride=8), :] = value[:, h * C:(h + 1) * C]
            return carry

        mine = pick(by_column(kind, core), cy, cx)

        def pack(t, q):
            for member in range(4):
                for h in range(tiles):
                    at = (h * (BCH // 8) + q * 2) * BLOCK * 8 + (member * ROWS + t * STEP) * 8
                    lo = stage[pl.ds(at, 64), :].reshape(STEP, 8, C)
                    hi = stage[pl.ds(at + BLOCK * 8, 64), :].reshape(STEP, 8, C)
                    send_ref[t, member, :, q * CH:(q + 1) * CH, h * C:(h + 1) * C] = jnp.concatenate([lo, hi], axis=1).astype(BF16)

        def keep(t):
            land_ref[t, mine, :, channels(core), :] = send_ref[t, mine * 2 + core]

        for g in range(GROUPS):
            if j == 0:
                for x in ins:
                    x.load(g).wait()
            lax.fori_loop(g * CH, (g + 1) * CH, body, 0, unroll=4)
            if g == j == 0:
                all_in(others)
            for t in range(EARLY):
                pack(t, g)
                for copy in block_sends(kind, job, t, g):
                    copy.start()
        for t in range(EARLY, STEPS):
            for g in range(GROUPS):
                pack(t, g)
            for copy in block_sends(kind, job, t):
                copy.start()
        for t in range(STEPS):
            keep(t)


def block_arrive(t, kinds, jobs):
    for kind, job in zip(kinds, jobs):
        for copy in block_receives(kind, job, t):
            copy.wait_recv()

    @pl.when(t == STEPS - 1)
    def _():
        for kind, job in zip(kinds, jobs):
            for slot in range(STEPS):
                for copy in block_sends(kind, job, slot):
                    copy.wait_send()


def both(land_ref, t, r):
    return land_ref[t, 0, r].astype(F32) + land_ref[t, 1, r].astype(F32)


def staged_kernel(inner, n_tri, n_in, *refs):
    far, refs = refs[:n_tri + n_in], refs[n_tri + n_in:]
    near, refs = refs[-2 - n_tri - n_in:-2], refs[:-2 - n_tri - n_in] + refs[-2:]
    refs, (tri_sem, row_sem) = refs[:-2], refs[-2:]
    step = step_now()
    tris = [Piecewise(far[k], near[k], tri_sem.at[k]) for k in range(n_tri)]

    def fetch(t, slot):
        out = []
        for k in range(n_in):
            size = far[n_tri + k].shape[0] // STEPS
            out.append(pltpu.make_async_copy(far[n_tri + k].at[pl.ds(t * size, size)], near[n_tri + k].at[slot], row_sem.at[slot, k]))
        return out

    @pl.when(step == 0)
    def _():
        for g in range(GROUPS):
            for x in tris:
                x.load(g).start()
        for copy in fetch(0, 0):
            copy.start()

    slot = (step + 1) % 2

    @pl.when(step > 0)
    def _():
        for copy in fetch(step - 1, slot):
            copy.wait()

    @pl.when((step > 0) & (step < STEPS))
    def _():
        for copy in fetch(step, 1 - slot):
            copy.start()

    inner(*tris, *[ref.at[slot] for ref in near[n_tri:]], *refs)


def arrive(t, jobs):
    me, dests = peers()
    for job in jobs:
        for k, frm in enumerate(dests[:-1]):
            back_copy(job, t, k, frm, frm).wait_recv()

    @pl.when(t == STEPS - 1)
    def _():
        for job in jobs:
            for slot in range(STEPS):
                for k, dest in enumerate(dests[:-1]):
                    back_copy(job, slot, k, dest, me).wait_send()


def rows_loop(body):
    def step(r, carry):
        body(r)
        return carry

    lax.fori_loop(0, STEP, step, 0, unroll=UNROLL)


def pre_row(r, z_t, mask_ref, ln_ref, w_t_ref, bias_ref, g_ref, keep_ref, unit_ref, inv_ref, a_stage, b_stage):
    unit, inv, _, p = project(z_t, ln_ref, w_t_ref, bias_ref)
    unit_ref[r] = unit
    inv_ref[0, pl.ds(r, 1), :] = inv
    m = mask_ref[0, pl.ds(r, 1), :].astype(F32)
    for side, stage in ((0, a_stage), (1, b_stage)):
        s = sigmoid(p[2 * side * C:(2 * side + 1) * C])
        v = p[(2 * side + 1) * C:(2 * side + 2) * C]
        sm = s * m
        spread(stage, sm * v, r)
        keep_ref[r, 2 * side] = sm
        keep_ref[r, 2 * side + 1] = v * (1.0 - s)
    g_ref[r] = sigmoid(p[4 * C:])


def pre_kernel(z_ref, mask_ref, ln_in, w_proj, b_proj, a_ref, b_ref, g_ref, keep_ref, unit_ref, inv_ref, a_st, b_st, a_send, b_send,
               eye_ref, ln_ref, w_t_ref, bias_ref, a_ss, b_ss, rs):
    step = step_now()

    @pl.when(step == 0)
    def _():
        enter()
        set_eye(eye_ref)
        set_pre(0, ln_in, w_proj, b_proj, ln_ref, w_t_ref, bias_ref)

    @rows_loop
    def _(r):
        z_t = nt(eye_ref[...], z_ref[r])
        pre_row(r, z_t, mask_ref, ln_ref, w_t_ref, bias_ref, g_ref, keep_ref, unit_ref, inv_ref, a_st, b_st)

    pl.when(step == 0)(all_in)
    send_rows(step, [(A_ROWS, a_st, a_send, a_ref, a_ss, rs.at[0]), (B_ROWS, b_st, b_send, b_ref, b_ss, rs.at[1])])


def mid_kernel(a_in, b_in, z_ref, g0_ref, mask_ref, ln_mid, w_out, b_out, ln_in, w_proj, b_proj,
               a_ref, b_ref, g_ref, keep_ref, unit_ref, inv_ref, zm_ref, gu_ref, munit_ref, minv_ref, a_st, b_st, a_send, b_send,
               eye_ref, ln_ref, w_t_ref, bias_ref, mln_ref, wo_t_ref, bo_ref, a_ss, b_ss, rs,
               st0, se0, la0, ss0, rv0):
    step = step_now()
    jobs = [(st0, se0, la0, ss0, rv0)]

    @pl.when(step == 0)
    def _():
        enter()
        set_eye(eye_ref)
        set_pre(1, ln_in, w_proj, b_proj, ln_ref, w_t_ref, bias_ref)
        set_post(0, ln_mid, w_out, b_out, mln_ref, wo_t_ref, bo_ref)
        block_part(OUT_FWD, (0,), (a_in, b_in), jobs)

    @pl.when(step > 0)
    def _():
        t = step - 1
        block_arrive(t, (0,), jobs)

        @rows_loop
        def _(r):
            unit, inv = norm(swap_core1(jnp.concatenate([la0[t, 0, r], la0[t, 1, r]], axis=1).astype(F32)))
            munit_ref[r] = unit
            minv_ref[0, pl.ds(r, 1), :] = inv
            x_hat = (unit * mln_ref[0] + mln_ref[1]).astype(BF16)
            update = nn(wo_t_ref[...], x_hat) + bo_ref[...]
            g = g0_ref[r]
            change = g * update
            gu_ref[r] = change * (1.0 - g)
            z_new = (nt(eye_ref[...], z_ref[r]) + change).astype(BF16)
            zm_ref[r] = z_new
            pre_row(r, z_new.astype(F32), mask_ref, ln_ref, w_t_ref, bias_ref, g_ref, keep_ref, unit_ref, inv_ref, a_st, b_st)

        send_rows(t, [(ROWS_ALL, a_st, a_send, a_ref, a_ss, rs.at[0]), (ROWS_ALL, b_st, b_send, b_ref, b_ss, rs.at[1])])


def post_back_row(unit, inv, g, dz, mln_ref, wo_ref, acc_ref, x_hat=None):
    if x_hat is None:
        x_hat = (unit * mln_ref[0] + mln_ref[1]).astype(BF16)
    d_up = dz * g
    d_up_bf = d_up.astype(BF16)
    acc_ref[0] += nt(x_hat, d_up_bf)
    acc_ref[3] += fold(d_up)
    d_hat = nn(wo_ref[...], d_up_bf).astype(BF16).astype(F32)
    acc_ref[1] += fold(d_hat * unit)
    acc_ref[2] += fold(d_hat)
    return norm_back(d_hat, unit, inv, mln_ref[0])


def put_post(grad_ref, acc_ref):
    grad_ref[0:C, :] = acc_ref[0]
    grad_ref[C:C + 8, :] = jnp.concatenate([row_sums(acc_ref[1]), row_sums(acc_ref[2]), row_sums(acc_ref[3]), jnp.zeros((5, C), F32)], axis=0)
    grad_ref[C + 8:C + HAT, :] = jnp.zeros((8, C), F32)


def turn_kernel(a_in, b_in, zm_ref, g_ref, dz_ref, ln_mid, w_out, b_out,
                dx_ref, z_out_ref, dpg_ref, grad_ref, d_st, d_send, eye_ref, mln_ref, wo_t_ref, bo_ref, acc_ref, d_ss, rs,
               st0, se0, la0, ss0, rv0):
    step = step_now()
    jobs = [(st0, se0, la0, ss0, rv0)]
    wo_ref = w_out.at[1]

    @pl.when(step == 0)
    def _():
        enter()
        set_eye(eye_ref)
        set_post(1, ln_mid, w_out, b_out, mln_ref, wo_t_ref, bo_ref)
        acc_ref[...] = jnp.zeros_like(acc_ref)
        channel_part(IN_FWD, (a_in, b_in), jobs)

    @pl.when(step > 0)
    def _():
        t = step - 1
        arrive(t, jobs)
        x_ref = la0.at[t]

        @rows_loop
        def _(r):
            dz = nt(eye_ref[...], dz_ref[r])
            g = g_ref[r]
            unit, inv = norm(x_ref[r].astype(F32))
            x_hat = (unit * mln_ref[0] + mln_ref[1]).astype(BF16)
            change = g * (nn(wo_t_ref[...], x_hat) + bo_ref[...])
            dpg_ref[r] = dz * change * (1.0 - g)
            z_out_ref[r] = (zm_ref[r].astype(F32) + change).T.astype(BF16)
            spread(d_st, post_back_row(unit, inv, g, dz, mln_ref, wo_ref, acc_ref, x_hat), r)

        @pl.when(t == STEPS - 1)
        def _():
            put_post(grad_ref, acc_ref)

        send_rows(t, [(ROWS_ALL, d_st, d_send, dx_ref, d_ss, rs.at[0])])


def pre_back_row(unit, inv, keep, da, db, d_pg, ln_ref, w_ref, w_acc, b_acc, l_acc):
    z_hat = (unit * ln_ref[0] + ln_ref[1]).astype(BF16)
    parts = []
    for side, d_side in ((0, da), (1, db)):
        d_v = d_side * keep[2 * side]
        parts += [d_v * keep[2 * side + 1], d_v]
    parts.append(d_pg)
    for k, part in enumerate(parts):
        b_acc[k * C:(k + 1) * C, :] += fold(part)
    d_p = jnp.concatenate([part.astype(BF16) for part in parts], axis=0)
    w_acc[...] += nt(d_p, z_hat)
    d_hat = nn(w_ref[...], d_p).astype(BF16).astype(F32)
    l_acc[0] += fold(d_hat * unit)
    l_acc[1] += fold(d_hat)
    return norm_back(d_hat, unit, inv, ln_ref[0])


def put_pre(grad_ref, w_acc, b_acc, l_acc):
    grad_ref[0:PROJ, :] = w_acc[...]
    rows = [row_sums(b_acc[k * C:(k + 1) * C, :]) for k in range(5)]
    rows += [row_sums(l_acc[0]), row_sums(l_acc[1]), jnp.zeros((1, C), F32)]
    grad_ref[PROJ:PROJ + 8, :] = jnp.concatenate(rows, axis=0)
    grad_ref[PROJ + 8:PROJ + HAT, :] = jnp.zeros((8, C), F32)


def set_gains(ref, ln, block):
    for k in range(2):
        set_column(ref.at[k], ln[block, k:k + 1, :])


def back_kernel(a_in, b_in, dx_in, dpg1_ref, keep_ref, unit_ref, inv_ref, dz_ref, munit_ref, minv_ref, g_ref, gu_ref, ln_in, w_proj, ln_mid, w_out,
                dx_ref, dzm_ref, dpg_ref, grad1_ref, grad0_ref, d_st, d_send,
                eye_ref, ln_ref, mln_ref, w_acc, b_acc, l_acc, acc_ref, d_ss, rs,
               st0, st1, se0, se1, la0, la1, ss0, ss1, rv0, rv1):
    step = step_now()
    jobs = [(st0, se0, la0, ss0, rv0), (st1, se1, la1, ss1, rv1)]
    w_ref, wo_ref = w_proj.at[1], w_out.at[0]

    @pl.when(step == 0)
    def _():
        enter()
        set_eye(eye_ref)
        set_gains(ln_ref, ln_in, 1)
        set_gains(mln_ref, ln_mid, 0)
        for ref in (w_acc, b_acc, l_acc, acc_ref):
            ref[...] = jnp.zeros_like(ref)
        channel_part(IN_BWD, (a_in, b_in, dx_in), jobs)

    @pl.when(step > 0)
    def _():
        t = step - 1
        arrive(t, jobs)
        da_ref, db_ref = la0.at[t], la1.at[t]

        @rows_loop
        def _(r):
            at = pl.ds(r, 1)
            dzn = pre_back_row(unit_ref[r], inv_ref[0, at, :], keep_ref.at[r], da_ref[r].astype(F32), db_ref[r].astype(F32), dpg1_ref[r],
                               ln_ref, w_ref, w_acc, b_acc, l_acc)
            dzm = (nt(eye_ref[...], dz_ref[r]) + dzn).astype(BF16)
            dzm_ref[r] = dzm
            dzm = dzm.astype(F32)
            dpg_ref[r] = dzm * gu_ref[r]
            spread(d_st, swap_core1(post_back_row(munit_ref[r], minv_ref[0, at, :], g_ref[r], dzm, mln_ref, wo_ref, acc_ref)), r)

        @pl.when(t == STEPS - 1)
        def _():
            put_pre(grad1_ref, w_acc, b_acc, l_acc)
            put_post(grad0_ref, acc_ref)

        send_rows(t, [(DX_ROWS, d_st, d_send, dx_ref, d_ss, rs.at[0])])


ALL = 16
EARLY_SHARE, LATE_SHARE = 64, 48


def device(o):
    return {"dp": o // GROUP, "dap": o % GROUP}


def everyone():
    dap = lax.axis_index("dap")
    me = lax.axis_index("dp") * GROUP + dap
    twin = me + 1 - dap % 2 * 2
    return me, twin, [(me + k) % ALL for k in range(1, ALL)], [(me + 2 * k) % ALL for k in range(1, GROUP)]


def enter_all():
    for to in everyone()[2]:
        pl.semaphore_signal(pltpu.get_barrier_semaphore(), inc=1, device_id=device(to), device_id_type=pl.DeviceIdType.MESH)


class Adder:
    def __init__(self, base, send_ref, got_ref, part_ref, tot_ref, sems):
        self.base, self.send_ref, self.got_ref, self.part_ref, self.tot_ref, self.sems = base, send_ref, got_ref, part_ref, tot_ref, sems
        self.size = part_ref.shape[0]

    def share(self, k, base=0):
        return pl.ds(pl.multiple_of(base + k * self.size, HAT), self.size)

    def sums(self, k):
        return self.tot_ref.at[self.share(k, self.base)]

    def remote(self, src, dst, phase, k, slot, to):
        return pltpu.make_async_remote_copy(src, dst, self.sems.at[2 * phase, k], self.sems.at[2 * phase + 1, slot], device_id=device(to),
                                            device_id_type=pl.DeviceIdType.MESH)

    def first(self, k, frm):
        other = everyone()[2][k]
        return self.remote(self.send_ref.at[self.share(other)], self.got_ref.at[frm], 0, k, frm, other)

    def second(self, k, frm):
        return self.remote(self.part_ref, self.sums(frm), 1, k, frm, everyone()[3][k])

    def third(self, k, block):
        return self.remote(self.sums(block), self.sums(block), 2, k, k, everyone()[1])

    def own(self, block):
        return self.remote(self.part_ref, self.sums(block), 2, GROUP, GROUP, everyone()[1])

    def before(self, device_number, k):
        return (device_number + ALL - 2 * (k + 1)) % ALL

    def fill(self, *packs):
        at = 0
        for ref in packs:
            self.send_ref[at:at + ref.shape[0], :] = ref[...].astype(BF16)
            at += ref.shape[0]
        self.send_ref[at:, :] = jnp.zeros((self.send_ref.shape[0] - at, C), BF16)

    def scatter(self):
        me = everyone()[0]
        for k in range(ALL - 1):
            self.first(k, me).start()
        self.got_ref[me] = self.send_ref[self.share(me), :]

    def add(self):
        me, twin, others, chips = everyone()
        for k in range(ALL - 1):
            self.first(k, others[k]).wait_recv()
        total = self.got_ref[0].astype(F32)
        for k in range(1, ALL):
            total = total + self.got_ref[k].astype(F32)
        self.part_ref[...] = total
        for k in range(GROUP - 1):
            self.second(k, me).start()
        self.own(me).start()
        self.tot_ref[self.share(me, self.base), :] = total

    def hand_on(self):
        me = everyone()[0]
        for k in range(GROUP - 1):
            self.second(k, self.before(me, k)).wait_recv()
            self.third(k, self.before(me, k)).start()

    def finish(self):
        me, twin, others, chips = everyone()
        for k in range(GROUP - 1):
            self.third(k, self.before(twin, k)).wait_recv()
        self.own(twin).wait_recv()
        self.own(me).wait_send()
        for k in range(ALL - 1):
            self.first(k, me).wait_send()
        for k in range(GROUP - 1):
            self.second(k, me).wait_send()
            self.third(k, self.before(me, k)).wait_send()


def last_kernel(a_in, b_in, dx_in, dpg_ref, keep_ref, unit_ref, inv_ref, dzm_ref, ln_in, w_proj, post0, post1, pre1,
                dz_ref, tot_out, ln_ref, w_acc, b_acc, l_acc, grad_ref, send_e, got_e, part_e, send_l, got_l, part_l, tot_ref, sems,
                st0, st1, se0, se1, la0, la1, ss0, ss1, rv0, rv1):
    step = step_now()
    jobs = [(st0, se0, la0, ss0, rv0), (st0, se1, la1, ss1, rv1)]
    w_ref = w_proj.at[0]
    early = Adder(0, send_e, got_e, part_e, tot_ref, sems.at[0])
    late = Adder(send_e.shape[0], send_l, got_l, part_l, tot_ref, sems.at[1])

    @pl.when(step == 0)
    def _():
        enter_all()
        set_gains(ln_ref, ln_in, 0)
        for ref in (w_acc, b_acc, l_acc):
            ref[...] = jnp.zeros_like(ref)
        block_part(OUT_BWD, (0, 1), (a_in, b_in, dx_in), jobs, ALL - 1)
        early.fill(post0, post1, pre1)
        early.scatter()

    @pl.when(step > 0)
    def _():
        t = step - 1
        block_arrive(t, (0, 1), jobs)

        @rows_loop
        def _(r):
            dzn = pre_back_row(unit_ref[r], inv_ref[0, pl.ds(r, 1), :], keep_ref.at[r], both(la0, t, r), both(la1, t, r), dpg_ref[r],
                               ln_ref, w_ref, w_acc, b_acc, l_acc)
            dz_ref[r] = (dzm_ref[r].astype(F32) + dzn).T.astype(BF16)

        @pl.when(t == STEPS - 1)
        def _():
            put_pre(grad_ref, w_acc, b_acc, l_acc)
            late.fill(grad_ref)
            late.scatter()
            early.add()
            late.add()
            early.hand_on()
            late.hand_on()
            early.finish()
            late.finish()
            tot_out[...] = tot_ref[...]


def split_kernel(z_in, dz_in, tot, z_out, dz_out, *grads):
    z_out[...] = z_in[...]
    dz_out[...] = dz_in[...]
    pl.when(step_now() == 0)(lambda: split_grads(tot, *grads))


def split_grads(tot, d_ln_in, d_w_proj, d_b_proj, d_ln_mid, d_w_out, d_b_out):
    at = 0
    for k in range(2):
        d_w_out[k] = tot[at:at + C, :]
        d_ln_mid[k] = tot[at + C:at + C + 2, :]
        d_b_out[k:k + 1, :] = tot[at + C + 2:at + C + 3, :]
        at += C + HAT
    for k, at in enumerate((ALL * EARLY_SHARE, at)):
        for j in range(5):
            d_w_proj[k, :, j * C:(j + 1) * C] = tot[at + j * C:at + (j + 1) * C, :].T
            d_b_proj[k:k + 1, j * C:(j + 1) * C] = tot[at + PROJ + j:at + PROJ + j + 1, :]
        d_ln_in[k] = tot[at + PROJ + 5:at + PROJ + 7, :]


def finish(z_new, dz_new, total):
    shapes = ((2, 2, C), (2, C, PROJ), (2, PROJ), (2, 2, C), (2, C, C), (2, C))
    grads = [jax.ShapeDtypeStruct(shape, F32) for shape in shapes]
    return pl.pallas_call(
        split_kernel,
        grid=(STEPS,),
        in_specs=[by_row(z_new), by_row(dz_new), whole(total)],
        out_specs=[by_row(NATIVE)] * 2 + [pl.BlockSpec(x.shape, lambda t, n=len(x.shape): (0,) * n) for x in grads],
        out_shape=[NATIVE] * 2 + grads,
        compiler_params=pltpu.CompilerParams(dimension_semantics=("arbitrary",)),
        name="split",
    )(z_new, dz_new, total)


TRI = jax.ShapeDtypeStruct((CH, N, N), BF16)
BTRI = jax.ShapeDtypeStruct((BCH, BLOCK, N), BF16)
BDX = jax.ShapeDtypeStruct((BCH, BLOCK, BLOCK), BF16)
SENT = (TRI, BTRI, BDX)
ROW = jax.ShapeDtypeStruct((ROWS, C, N), BF16)
ROW32 = jax.ShapeDtypeStruct((ROWS, C, N), F32)
NATIVE = jax.ShapeDtypeStruct((ROWS, N, C), BF16)
POST = jax.ShapeDtypeStruct((C + HAT, C), F32)
PRE = jax.ShapeDtypeStruct((PROJ + HAT, C), F32)
TOT = jax.ShapeDtypeStruct((ALL * (EARLY_SHARE + LATE_SHARE), C), F32)
KEEP = jax.ShapeDtypeStruct((ROWS, 4, C, N), F32)
INV = jax.ShapeDtypeStruct((STEPS, STEP, N), F32)


def by_row(array, lead=0):
    tail = array.shape[1:]
    return pl.BlockSpec((array.shape[0] // STEPS,) + tail, lambda s: ((s * STEPS) // (STEPS + lead),) + (0,) * len(tail))


def whole(array):
    zeros = (0,) * len(array.shape)
    return pl.BlockSpec(array.shape, lambda t: zeros, pipeline_mode=pl.Buffered(1))


def out_spec(array, lead):
    if array in SENT:
        return pl.BlockSpec(memory_space=pl.ANY)
    if array in (PRE, POST, TOT):
        return pl.BlockSpec(array.shape, lambda t: (0, 0))
    return by_row(array, lead)


def row_call(kernel, name, collective_id, tris, ins, consts, outs, n_back, scratch, width=0):
    lead = 1 if tris else 0
    n_send = sum(out in SENT for out in outs)
    packed = (STEPS, 2, C, STEP, BLOCK) if BDX in outs else (STEPS, C, STEP, N)
    dma = pltpu.SemaphoreType.DMA
    sent = [pltpu.VMEM((2 * C * STEP, C), F32)] * n_send + [pltpu.VMEM(packed, BF16)] * n_send
    sems = [dma((STEPS, GROUP))] * n_send + ([dma((n_send,))] if n_send else [])
    back = [pltpu.VMEM((4 * N * 8, C), F32)] * n_back + [pltpu.VMEM((STEPS, GROUP, STEP, CH, N), BF16)] * n_back
    back += [pltpu.VMEM((STEPS, STEP, C, N), BF16)] * n_back
    if width:
        back = [pltpu.VMEM((BCH * BLOCK * width // C if k == 0 else 8, C), F32) for k in range(n_back)]
        back += [pltpu.VMEM((STEPS, 4, STEP, BCH, width), BF16)] * n_back + [pltpu.VMEM((STEPS, 2, STEP, C, width), BF16)] * n_back
    back += [dma((STEPS, GROUP))] * (2 * n_back)
    far = pl.BlockSpec(memory_space=pl.ANY)
    near = []
    if tris:
        near = [pltpu.VMEM(x.shape, x.dtype) for x in tris] + [pltpu.VMEM((2, x.shape[0] // STEPS) + x.shape[1:], x.dtype) for x in ins]
        near += [dma((len(tris), GROUPS)), dma((2, len(ins)))]
        kernel = functools.partial(staged_kernel, kernel, len(tris), len(ins))
    return pl.pallas_call(
        kernel,
        grid=(STEPS + lead,),
        in_specs=[far if tris else by_row(x) for x in [*tris, *ins]] + [whole(x) for x in consts],
        out_specs=[out_spec(out, lead) for out in outs],
        out_shape=outs,
        scratch_shapes=sent + scratch + sems + back + near,
        compiler_params=pltpu.CompilerParams(dimension_semantics=("arbitrary",), vmem_limit_bytes=VMEM_LIMIT, collective_id=collective_id, has_side_effects=True),
        name=name,
    )(*tris, *ins, *consts)


def local_step(z_pair, pair_mask, dz_out, ln_in, w_proj, b_proj, ln_mid, w_out, b_out):
    z, dz = z_pair[0], dz_out[0]
    mask = pair_mask.reshape(STEPS, STEP, N)
    pre, post = [ln_in, w_proj, b_proj], [ln_mid, w_out, b_out]
    eye = [pltpu.VMEM((C, C), BF16)]
    pre_c = [pltpu.VMEM((2, C, N), F32), pltpu.VMEM((PROJ, C), BF16), pltpu.VMEM((PROJ, N), F32)]
    post_c = [pltpu.VMEM((2, C, N), F32), pltpu.VMEM((C, C), BF16), pltpu.VMEM((C, N), F32)]
    post_acc = [pltpu.VMEM((4, C, C), F32)]
    pre_acc = [pltpu.VMEM((PROJ, C), F32), pltpu.VMEM((PROJ, C), F32), pltpu.VMEM((2, C, C), F32)]

    gains = [pltpu.VMEM((2, C, N), F32)]
    kept = [TRI, TRI, ROW32, KEEP, ROW32, INV]
    a0, b0, g0, keep0, unit0, inv0 = row_call(pre_kernel, "pre0", 0, [], [z, mask], pre, [BTRI, BTRI] + kept[2:], 0, eye + pre_c)
    a1, b1, g1, keep1, unit1, inv1, zm, gu0, munit0, minv0 = row_call(
        mid_kernel, "mid", 1, [a0, b0], [z, g0, mask], post + pre, kept + [ROW, ROW32, ROW32, INV], 1, eye + pre_c + post_c, BLOCK)
    dx1, z_new, dpg1, post_g1 = row_call(
        turn_kernel, "turn", 2, [a1, b1], [zm, g1, dz], post, [TRI, NATIVE, ROW32, POST], 1, eye + post_c + post_acc)
    dx0, dzm, dpg0, pre_g1, post_g0 = row_call(
        back_kernel, "back", 3, [a1, b1, dx1], [dpg1, keep1, unit1, inv1, dz, munit0, minv0, g0, gu0], [ln_in, w_proj, ln_mid, w_out],
        [BDX, ROW, ROW32, PRE, POST], 2, eye + gains * 2 + pre_acc + post_acc)
    adders = [pltpu.VMEM(PRE.shape, F32)]
    for size in (EARLY_SHARE, LATE_SHARE):
        adders += [pltpu.VMEM((ALL * size, C), BF16), pltpu.VMEM((ALL, size, C), BF16), pltpu.VMEM((size, C), F32)]
    adders += [pltpu.VMEM(TOT.shape, F32), pltpu.SemaphoreType.DMA((2, 6, ALL))]
    dz_new, total = row_call(
        last_kernel, "last", 4, [a0, b0, dx0], [dpg0, keep0, unit0, inv0, dzm], [ln_in, w_proj, post_g0, post_g1, pre_g1],
        [NATIVE, TOT], 2, gains + pre_acc + adders, N)
    z_out, dz_pair, *grads = finish(z_new, dz_new, total)
    return z_out[None], dz_pair[None], *grads


def solution(mesh):
    row_spec = P("dp", "dap")
    return jax.shard_map(local_step, mesh=mesh, in_specs=(row_spec,) * 3 + (P(),) * 6,
                         out_specs=(row_spec,) * 2 + (P(),) * 6, check_vma=False)
```

```python
import functools

import jax
import jax.numpy as jnp
from jax import lax
from jax.experimental import pallas as pl
from jax.experimental.pallas import tpu as pltpu
from jax.sharding import PartitionSpec as P

LN_EPS = 1e-5
N = 256
C = 128
GROUP = 8
ROWS = N // GROUP
CH = C // GROUP
STEP = 8
UNROLL = 4
STEPS = ROWS // STEP
PROJ = 5 * C
HAT = 16
F32 = jnp.float32
BF16 = jnp.bfloat16
VMEM_LIMIT = 62 * 1024 * 1024


def dot(lhs, rhs, lhs_dim, rhs_dim):
    return lax.dot_general(lhs, rhs, (((lhs_dim,), (rhs_dim,)), ((), ())), preferred_element_type=F32)


nn = functools.partial(dot, lhs_dim=1, rhs_dim=0)
nt = functools.partial(dot, lhs_dim=1, rhs_dim=1)
tn = functools.partial(dot, lhs_dim=0, rhs_dim=0)


def step_now():
    return pl.program_id(0)


def mean(values):
    return jnp.mean(values, axis=0, keepdims=True)


def norm(values):
    cen = values - mean(values)
    inv = lax.rsqrt(mean(cen * cen) + LN_EPS)
    return cen * inv, inv


def norm_back(d_hat, unit, inv, gain):
    d_unit = d_hat * gain
    mean_d = mean(d_unit)
    mean_du = mean(d_unit * unit)
    return inv * (d_unit - mean_d - unit * mean_du)


def fold(values):
    return values[:, :C] + values[:, C:]


def row_sums(acc):
    return jnp.sum(acc.T, axis=0, keepdims=True)


def sigmoid(values):
    return 0.5 * jnp.tanh(0.5 * values) + 0.5


def project(z_t, ln, w_t, bias):
    unit, inv = norm(z_t)
    z_hat = (unit * ln[0] + ln[1]).astype(BF16)
    return unit, inv, z_hat, nn(w_t[...], z_hat) + bias[...]


def set_eye(eye):
    same = lax.broadcasted_iota(jnp.int32, (C, C), 0) == lax.broadcasted_iota(jnp.int32, (C, C), 1)
    eye[...] = jnp.where(same, 1.0, 0.0).astype(BF16)


def set_column(ref, row):
    column = jnp.broadcast_to(row.astype(F32), (C, C)).T
    ref[:, :C] = column
    ref[:, C:] = column


def set_pre(block, ln_in, w_proj, b_proj, ln, w_t, bias):
    for k in range(2):
        set_column(ln.at[k], ln_in[block, k:k + 1, :])
    for k in range(5):
        cols = slice(k * C, (k + 1) * C)
        set_column(bias.at[cols], b_proj[block:block + 1, cols])
        w_t[cols, :] = w_proj[block, :, cols].astype(F32).T.astype(BF16)


def set_post(block, ln_mid, w_out, b_out, mln, wo_t, bo):
    for k in range(2):
        set_column(mln.at[k], ln_mid[block, k:k + 1, :])
    set_column(bo, b_out[block:block + 1, :])
    wo_t[...] = w_out[block].astype(F32).T.astype(BF16)


def place():
    me = lax.axis_index("dap")
    return me, me // 4, (me // 2) % 2, me % 2


def enter():
    me = lax.axis_index("dap")
    sem = pltpu.get_barrier_semaphore()
    for k in range(1, GROUP):
        pl.semaphore_signal(sem, inc=1, device_id={"dap": (me + k) % GROUP}, device_id_type=pl.DeviceIdType.MESH)


def all_in(others=GROUP - 1):
    pl.semaphore_wait(pltpu.get_barrier_semaphore(), others)


def peers():
    me, cy, cx, core = place()
    out = []
    for dy, dx in ((1, 1), (1, 0), (0, 1), (0, 0)):
        for dc in (1, 0):
            out.append((((cy + dy) % 2) * 2 + (cx + dx) % 2) * 2 + (core + dc) % 2)
    return me, out


def spread(ref, value, row):
    for h in range(2):
        ref[pl.ds(h * C * STEP + row, C, stride=STEP), :] = value[:, h * C:(h + 1) * C]


def pack_rows(stage, send_ref, slot):
    for h in range(2):
        for q in range(4):
            rows = stage[pl.ds((h * C + q * 32) * STEP, 32 * STEP), :].reshape(32, STEP, C)
            send_ref[slot, q * 32:(q + 1) * 32, :, h * C:(h + 1) * C] = rows.astype(BF16)


def move(src_ref, dst_ref, send_sem, recv_sem, dest, own):
    if own:
        return pltpu.make_async_copy(src_ref, dst_ref, recv_sem)
    return pltpu.make_async_remote_copy(src_ref, dst_ref, send_sem, recv_sem, device_id={"dap": dest}, device_id_type=pl.DeviceIdType.MESH)


def wait_sends(copies):
    for copy in copies:
        if copy.is_remote:
            copy.wait_send()


def row_copies(send_ref, out_ref, send_sem, recv_sem, slot):
    me, dests = peers()
    start = pl.multiple_of(me * ROWS + slot * STEP, STEP)
    return [
        move(send_ref.at[slot, pl.ds(pl.multiple_of(dest * CH, CH), CH)], out_ref.at[:, pl.ds(start, STEP), :],
             send_sem.at[slot, k], recv_sem, dest, k == GROUP - 1)
        for k, dest in enumerate(dests)
    ]


BCH = C // 2
BLOCK = N // 2


def by_column(kind, core):
    return core if kind else 1 - core


def pick(column, on_column, on_row):
    return column * on_column + (1 - column) * on_row


def channels(core):
    return pl.ds(pl.multiple_of(core * BCH, BCH), BCH)


def swap(lo, hi):
    first = lax.broadcasted_iota(jnp.int32, lo.shape, 1) < BLOCK // 2
    return jnp.where(first, lo, pltpu.roll(hi, BLOCK // 2, 1)), jnp.where(first, pltpu.roll(lo, BLOCK // 2, 1), hi)


def swap_core1(value):
    lo, hi = swap(value[BCH:, :BLOCK], value[BCH:, BLOCK:])
    return jnp.concatenate([value[:BCH], jnp.concatenate([lo, hi], axis=1)], axis=0)


def block_copies(kind, halves, send_ref, out_ref, send_sem, recv_sem, slot):
    me, cy, cx, core = place()
    out = []
    for k, (to, far) in enumerate(((0, 1), (1, 1), (1 - core, 0), (core, 0))):
        column = by_column(kind, to)
        y, x = cy, cx
        if far:
            y, x = (1 - cy, cx) if column else (cy, 1 - cx)
        start = pick(column, cy, cx) * 2 * ROWS + core * ROWS + slot * STEP
        src = send_ref.at[slot, pick(column, y, x), channels(to)] if halves else send_ref.at[slot, channels(to)]
        out.append(move(src, out_ref.at[:, pl.ds(pl.multiple_of(start, STEP), STEP), :], send_sem.at[slot, k], recv_sem, (y * 2 + x) * 2 + to, k == 3))
    return out


def pack_halves(stage, send_ref, slot):
    for h in range(2):
        for q in range(4):
            rows = stage[pl.ds((h * C + q * 32) * STEP, 32 * STEP), :].reshape(32, STEP, C)
            send_ref[slot, h, q * 32:(q + 1) * 32] = rows.astype(BF16)


A_ROWS = (pack_rows, functools.partial(block_copies, 0, False))
B_ROWS = (pack_rows, functools.partial(block_copies, 1, False))
ROWS_ALL = (pack_rows, row_copies)
DX_ROWS = (pack_halves, functools.partial(block_copies, 0, True))


def send_rows(step, jobs):
    for (pack, copies), stage, send_ref, out_ref, send_sem, recv_sems, k in jobs:
        pack(stage, send_ref, step)
        for copy in copies(send_ref, out_ref, send_sem, recv_sems.at[k], step):
            copy.start()
    PENDING.extend(jobs)


PENDING = []


def finish_rows(jobs):
    for (pack, copies), stage, send_ref, out_ref, send_sem, recv_sems, k in jobs:
        for slot in range(STEPS):
            wait_sends(copies(send_ref, out_ref, send_sem, recv_sems.at[k], slot))
        pltpu.make_async_copy(out_ref, out_ref, recv_sems.at[k]).wait()


OUT_FWD = (lambda c, a, b: nt(a[c], b[c]),)
IN_FWD = (lambda c, a, b: tn(a[c], b[c]),)
IN_BWD = (lambda c, a, b, dx: nt(b[c], dx[c]), lambda c, a, b, dx: nn(a[c], dx[c]))
OUT_BWD = (lambda c, a, b, dx: nn(dx[c], b[c]), lambda c, a, b, dx: tn(dx[c], a[c]))


def back_copy(job, t, k, dest, frm):
    stage, send_ref, land_ref, send_sem, recv_sem = job
    return pltpu.make_async_remote_copy(
        send_ref.at[t, dest], land_ref.at[t, :, pl.ds(pl.multiple_of(frm * CH, CH), CH), :], send_sem.at[t, k], recv_sem.at[t, frm],
        device_id={"dap": dest}, device_id_type=pl.DeviceIdType.MESH)


EARLY = 2
GROUPS = 4


class Piecewise:
    def __init__(self, source, ref, sems):
        self.source, self.ref, self.sems = source, ref, sems

    def load(self, g):
        size = self.ref.shape[0] // GROUPS
        part = pl.ds(g * size, size)
        return pltpu.make_async_copy(self.source.at[part], self.ref.at[part], self.sems.at[g])


def channel_part(products, ins, jobs):
    me, dests = peers()
    refs = [x.ref for x in ins]
    for j, (product, job) in enumerate(zip(products, jobs)):
        stage, send_ref, land_ref = job[:3]

        def body(c, carry):
            value = product(c, *refs)
            for h in range(2):
                stage[pl.ds((h * 2 + c // 8) * N * 8 + c % 8, N, stride=8), :] = value[:, h * C:(h + 1) * C]
            return carry

        for g in range(GROUPS):
            if j == 0:
                for x in ins:
                    x.load(g).wait()
            lax.fori_loop(g * (CH // GROUPS), (g + 1) * (CH // GROUPS), body, 0, unroll=True)
        if j == 0:
            all_in()
        for t in range(STEPS):
            for dest in range(GROUP):
                for h in range(2):
                    at = h * 2 * N * 8 + (dest * ROWS + t * STEP) * 8
                    lo = stage[pl.ds(at, 64), :].reshape(STEP, 8, C)
                    hi = stage[pl.ds(at + N * 8, 64), :].reshape(STEP, 8, C)
                    send_ref[t, dest, :, :, h * C:(h + 1) * C] = jnp.concatenate([lo, hi], axis=1).astype(BF16)
            for k, dest in enumerate(dests[:-1]):
                back_copy(job, t, k, dest, me).start()
            land_ref[t, :, pl.ds(pl.multiple_of(me * CH, CH), CH), :] = send_ref[t, me]


def block_sends(kind, job, t, piece=None):
    stage, send_ref, land_ref, send_sem, recv_sem = job
    me, cy, cx, core = place()
    column = by_column(kind, core)
    mine = pick(column, cy, cx)
    y, x = cy + column * (1 - 2 * cy), cx + (1 - column) * (1 - 2 * cx)
    size = BCH if piece is None else BCH // GROUPS
    at = (piece or 0) * size
    land = land_ref.at[t, mine, :, pl.ds(pl.multiple_of(core * BCH + at, size), size), :]
    out = []
    for k, (dest, member, slot) in enumerate((((y * 2 + x) * 2, pick(column, y, x) * 2, core), ((y * 2 + x) * 2 + 1, pick(column, y, x) * 2 + 1, core),
                                              (me + 1 - 2 * core, mine * 2 + 1 - core, 2))):
        out.append(pltpu.make_async_remote_copy(send_ref.at[t, member, :, pl.ds(at, size), :], land, send_sem.at[t, k], recv_sem.at[t, slot],
                                                device_id={"dap": dest}, device_id_type=pl.DeviceIdType.MESH))
    return out


def block_receives(kind, job, t):
    stage, send_ref, land_ref, send_sem, recv_sem = job
    me, cy, cx, core = place()
    out = []
    for slot, (frm, far) in enumerate(((0, 1), (1, 1), (1 - core, 0))):
        column = by_column(kind, frm)
        y, x = cy, cx
        if far:
            y, x = (1 - cy, cx) if column else (cy, 1 - cx)
        out.append(pltpu.make_async_remote_copy(send_ref.at[t, 0], land_ref.at[t, pick(column, y, x), :, channels(frm), :], send_sem.at[t, slot],
                                                recv_sem.at[t, slot], device_id={"dap": (y * 2 + x) * 2 + frm}, device_id_type=pl.DeviceIdType.MESH))
    return out


def block_part(products, kinds, ins, jobs, others=GROUP - 1):
    me, cy, cx, core = place()
    refs = [x.ref for x in ins]
    for j, (product, kind, job) in enumerate(zip(products, kinds, jobs)):
        stage, send_ref, land_ref = job[:3]
        tiles = send_ref.shape[-1] // C

        def body(c, carry):
            value = product(c, *refs)
            for h in range(tiles):
                stage[pl.ds((h * (BCH // 8) + c // 8) * BLOCK * 8 + c % 8, BLOCK, stride=8), :] = value[:, h * C:(h + 1) * C]
            return carry

        mine = pick(by_column(kind, core), cy, cx)

        def pack(t, q):
            for member in range(4):
                for h in range(tiles):
                    at = (h * (BCH // 8) + q * 2) * BLOCK * 8 + (member * ROWS + t * STEP) * 8
                    lo = stage[pl.ds(at, 64), :].reshape(STEP, 8, C)
                    hi = stage[pl.ds(at + BLOCK * 8, 64), :].reshape(STEP, 8, C)
                    send_ref[t, member, :, q * CH:(q + 1) * CH, h * C:(h + 1) * C] = jnp.concatenate([lo, hi], axis=1).astype(BF16)

        def keep(t):
            land_ref[t, mine, :, channels(core), :] = send_ref[t, mine * 2 + core]

        for g in range(GROUPS):
            if j == 0:
                for x in ins:
                    x.load(g).wait()
            lax.fori_loop(g * CH, (g + 1) * CH, body, 0, unroll=4)
            if g == j == 0:
                all_in(others)
            for t in range(EARLY):
                pack(t, g)
                for copy in block_sends(kind, job, t, g):
                    copy.start()
        for t in range(EARLY, STEPS):
            for g in range(GROUPS):
                pack(t, g)
            for copy in block_sends(kind, job, t):
                copy.start()
        for t in range(STEPS):
            keep(t)


def block_arrive(t, kinds, jobs):
    for kind, job in zip(kinds, jobs):
        for copy in block_receives(kind, job, t):
            copy.wait_recv()

    @pl.when(t == STEPS - 1)
    def _():
        for kind, job in zip(kinds, jobs):
            for slot in range(STEPS):
                for copy in block_sends(kind, job, slot):
                    copy.wait_send()


def both(land_ref, t, r):
    return land_ref[t, 0, r].astype(F32) + land_ref[t, 1, r].astype(F32)


def staged_kernel(inner, n_tri, n_in, n_const, outs, *refs):
    n_far = n_tri + n_in
    far, consts, refs = refs[:n_far], refs[n_far:n_far + n_const], refs[n_far + n_const:]
    results, refs = list(refs[:len(outs)]), refs[len(outs):]
    tri_sem, row_sem, out_sem = refs[-3:]
    rows_out = [k for k, out in enumerate(outs) if is_rows(out)]
    n_near = n_far + len(rows_out)
    refs, near = refs[:-3 - n_near], refs[-3 - n_near:-3]
    step = step_now()
    slot = (step + 1) % 2
    tris = [Piecewise(far[k], near[k], tri_sem.at[k]) for k in range(n_tri)]
    targets = [results[k] for k in rows_out]
    for k, ref in zip(rows_out, near[n_far:]):
        results[k] = ref.at[slot]

    def fetch(t, slot):
        return [pltpu.make_async_copy(block_of(whole_ref, t), ref.at[slot], row_sem.at[slot, k])
                for k, (whole_ref, ref) in enumerate(zip(far[n_tri:], near[n_tri:n_far]))]

    def store(t, slot):
        return [pltpu.make_async_copy(ref.at[slot], block_of(whole_ref, t), out_sem.at[slot, k])
                for k, (whole_ref, ref) in enumerate(zip(targets, near[n_far:]))]

    @pl.when(step == 0)
    def _():
        for g in range(GROUPS):
            for x in tris:
                x.load(g).start()
        for copy in fetch(0, 0):
            copy.start()

    @pl.when(step > 0)
    def _():
        for copy in fetch(step - 1, slot):
            copy.wait()

    @pl.when((step > 0) & (step < STEPS))
    def _():
        for copy in fetch(step, 1 - slot):
            copy.start()

    @pl.when(step > 2)
    def _():
        for copy in store(step - 3, slot):
            copy.wait()

    PENDING.clear()
    inner(*tris, *[ref.at[slot] for ref in near[n_tri:n_far]], *consts, *results, *refs)
    jobs = list(PENDING)

    @pl.when(step > 0)
    def _():
        for copy in store(step - 1, slot):
            copy.start()

    @pl.when(step == STEPS)
    def _():
        finish_rows(jobs)
        for copy in store(step - 2, 1 - slot) + store(step - 1, slot):
            copy.wait()


def block_of(ref, t):
    size = ref.shape[0] // STEPS
    return ref.at[pl.ds(t * size, size)]


def is_rows(out):
    return out not in (PRE, POST, TOT, *SENT)


def arrive(t, jobs):
    me, dests = peers()
    for job in jobs:
        for k, frm in enumerate(dests[:-1]):
            back_copy(job, t, k, frm, frm).wait_recv()

    @pl.when(t == STEPS - 1)
    def _():
        for job in jobs:
            for slot in range(STEPS):
                for k, dest in enumerate(dests[:-1]):
                    back_copy(job, slot, k, dest, me).wait_send()


def rows_loop(body):
    def step(r, carry):
        body(r)
        return carry

    lax.fori_loop(0, STEP, step, 0, unroll=UNROLL)


def pre_row(r, z_t, mask_ref, ln_ref, w_t_ref, bias_ref, g_ref, keep_ref, unit_ref, inv_ref, a_stage, b_stage):
    unit, inv, _, p = project(z_t, ln_ref, w_t_ref, bias_ref)
    unit_ref[r] = unit
    inv_ref[0, pl.ds(r, 1), :] = inv
    m = mask_ref[0, pl.ds(r, 1), :].astype(F32)
    for side, stage in ((0, a_stage), (1, b_stage)):
        s = sigmoid(p[2 * side * C:(2 * side + 1) * C])
        v = p[(2 * side + 1) * C:(2 * side + 2) * C]
        sm = s * m
        spread(stage, sm * v, r)
        keep_ref[r, 2 * side] = sm
        keep_ref[r, 2 * side + 1] = v * (1.0 - s)
    g_ref[r] = sigmoid(p[4 * C:])


def pre_kernel(z_ref, mask_ref, ln_in, w_proj, b_proj, a_ref, b_ref, g_ref, keep_ref, unit_ref, inv_ref, a_st, b_st, a_send, b_send,
               eye_ref, ln_ref, w_t_ref, bias_ref, a_ss, b_ss, rs):
    step = step_now()

    @pl.when(step == 0)
    def _():
        enter()
        set_eye(eye_ref)
        set_pre(0, ln_in, w_proj, b_proj, ln_ref, w_t_ref, bias_ref)
        all_in()

    @pl.when(step > 0)
    def _():
        t = step - 1

        @rows_loop
        def _(r):
            z_t = nt(eye_ref[...], z_ref[r])
            pre_row(r, z_t, mask_ref, ln_ref, w_t_ref, bias_ref, g_ref, keep_ref, unit_ref, inv_ref, a_st, b_st)

        send_rows(t, [(A_ROWS, a_st, a_send, a_ref, a_ss, rs, 0), (B_ROWS, b_st, b_send, b_ref, b_ss, rs, 1)])


def mid_kernel(a_in, b_in, z_ref, g0_ref, mask_ref, ln_mid, w_out, b_out, ln_in, w_proj, b_proj,
               a_ref, b_ref, g_ref, keep_ref, unit_ref, inv_ref, zm_ref, gu_ref, munit_ref, minv_ref, a_st, b_st, a_send, b_send,
               eye_ref, ln_ref, w_t_ref, bias_ref, mln_ref, wo_t_ref, bo_ref, a_ss, b_ss, rs,
               st0, se0, la0, ss0, rv0):
    step = step_now()
    jobs = [(st0, se0, la0, ss0, rv0)]

    @pl.when(step == 0)
    def _():
        enter()
        set_eye(eye_ref)
        set_pre(1, ln_in, w_proj, b_proj, ln_ref, w_t_ref, bias_ref)
        set_post(0, ln_mid, w_out, b_out, mln_ref, wo_t_ref, bo_ref)
        block_part(OUT_FWD, (0,), (a_in, b_in), jobs)

    @pl.when(step > 0)
    def _():
        t = step - 1
        block_arrive(t, (0,), jobs)

        @rows_loop
        def _(r):
            unit, inv = norm(swap_core1(jnp.concatenate([la0[t, 0, r], la0[t, 1, r]], axis=1).astype(F32)))
            munit_ref[r] = unit
            minv_ref[0, pl.ds(r, 1), :] = inv
            x_hat = (unit * mln_ref[0] + mln_ref[1]).astype(BF16)
            update = nn(wo_t_ref[...], x_hat) + bo_ref[...]
            g = g0_ref[r]
            change = g * update
            gu_ref[r] = change * (1.0 - g)
            z_new = (nt(eye_ref[...], z_ref[r]) + change).astype(BF16)
            zm_ref[r] = z_new
            pre_row(r, z_new.astype(F32), mask_ref, ln_ref, w_t_ref, bias_ref, g_ref, keep_ref, unit_ref, inv_ref, a_st, b_st)

        send_rows(t, [(ROWS_ALL, a_st, a_send, a_ref, a_ss, rs, 0), (ROWS_ALL, b_st, b_send, b_ref, b_ss, rs, 1)])


def post_back_row(unit, inv, g, dz, mln_ref, wo_ref, acc_ref, x_hat=None):
    if x_hat is None:
        x_hat = (unit * mln_ref[0] + mln_ref[1]).astype(BF16)
    d_up = dz * g
    d_up_bf = d_up.astype(BF16)
    acc_ref[0] += nt(x_hat, d_up_bf)
    acc_ref[3] += fold(d_up)
    d_hat = nn(wo_ref[...], d_up_bf).astype(BF16).astype(F32)
    acc_ref[1] += fold(d_hat * unit)
    acc_ref[2] += fold(d_hat)
    return norm_back(d_hat, unit, inv, mln_ref[0])


def put_post(grad_ref, acc_ref):
    grad_ref[0:C, :] = acc_ref[0]
    grad_ref[C:C + 8, :] = jnp.concatenate([row_sums(acc_ref[1]), row_sums(acc_ref[2]), row_sums(acc_ref[3]), jnp.zeros((5, C), F32)], axis=0)
    grad_ref[C + 8:C + HAT, :] = jnp.zeros((8, C), F32)


def turn_kernel(a_in, b_in, zm_ref, g_ref, dz_ref, ln_mid, w_out, b_out,
                dx_ref, z_out_ref, dpg_ref, grad_ref, d_st, d_send, eye_ref, mln_ref, wo_t_ref, bo_ref, acc_ref, d_ss, rs,
               st0, se0, la0, ss0, rv0):
    step = step_now()
    jobs = [(st0, se0, la0, ss0, rv0)]
    wo_ref = w_out.at[1]

    @pl.when(step == 0)
    def _():
        enter()
        set_eye(eye_ref)
        set_post(1, ln_mid, w_out, b_out, mln_ref, wo_t_ref, bo_ref)
        acc_ref[...] = jnp.zeros_like(acc_ref)
        channel_part(IN_FWD, (a_in, b_in), jobs)

    @pl.when(step > 0)
    def _():
        t = step - 1
        arrive(t, jobs)
        x_ref = la0.at[t]

        @rows_loop
        def _(r):
            dz = nt(eye_ref[...], dz_ref[r])
            g = g_ref[r]
            unit, inv = norm(x_ref[r].astype(F32))
            x_hat = (unit * mln_ref[0] + mln_ref[1]).astype(BF16)
            change = g * (nn(wo_t_ref[...], x_hat) + bo_ref[...])
            dpg_ref[r] = dz * change * (1.0 - g)
            z_out_ref[r] = (zm_ref[r].astype(F32) + change).T.astype(BF16)
            spread(d_st, post_back_row(unit, inv, g, dz, mln_ref, wo_ref, acc_ref, x_hat), r)

        @pl.when(t == STEPS - 1)
        def _():
            put_post(grad_ref, acc_ref)

        send_rows(t, [(ROWS_ALL, d_st, d_send, dx_ref, d_ss, rs, 0)])


def pre_back_row(unit, inv, keep, da, db, d_pg, ln_ref, w_ref, w_acc, b_acc, l_acc):
    z_hat = (unit * ln_ref[0] + ln_ref[1]).astype(BF16)
    parts = []
    for side, d_side in ((0, da), (1, db)):
        d_v = d_side * keep[2 * side]
        parts += [d_v * keep[2 * side + 1], d_v]
    parts.append(d_pg)
    for k, part in enumerate(parts):
        b_acc[k * C:(k + 1) * C, :] += fold(part)
    d_p = jnp.concatenate([part.astype(BF16) for part in parts], axis=0)
    w_acc[...] += nt(d_p, z_hat)
    d_hat = nn(w_ref[...], d_p).astype(BF16).astype(F32)
    l_acc[0] += fold(d_hat * unit)
    l_acc[1] += fold(d_hat)
    return norm_back(d_hat, unit, inv, ln_ref[0])


def put_pre(grad_ref, w_acc, b_acc, l_acc):
    grad_ref[0:PROJ, :] = w_acc[...]
    rows = [row_sums(b_acc[k * C:(k + 1) * C, :]) for k in range(5)]
    rows += [row_sums(l_acc[0]), row_sums(l_acc[1]), jnp.zeros((1, C), F32)]
    grad_ref[PROJ:PROJ + 8, :] = jnp.concatenate(rows, axis=0)
    grad_ref[PROJ + 8:PROJ + HAT, :] = jnp.zeros((8, C), F32)


def set_gains(ref, ln, block):
    for k in range(2):
        set_column(ref.at[k], ln[block, k:k + 1, :])


def back_kernel(a_in, b_in, dx_in, dpg1_ref, keep_ref, unit_ref, inv_ref, dz_ref, munit_ref, minv_ref, g_ref, gu_ref, ln_in, w_proj, ln_mid, w_out,
                dx_ref, dzm_ref, dpg_ref, grad1_ref, grad0_ref, d_st, d_send,
                eye_ref, ln_ref, mln_ref, w_acc, b_acc, l_acc, acc_ref, d_ss, rs,
               st0, st1, se0, se1, la0, la1, ss0, ss1, rv0, rv1):
    step = step_now()
    jobs = [(st0, se0, la0, ss0, rv0), (st1, se1, la1, ss1, rv1)]
    w_ref, wo_ref = w_proj.at[1], w_out.at[0]

    @pl.when(step == 0)
    def _():
        enter()
        set_eye(eye_ref)
        set_gains(ln_ref, ln_in, 1)
        set_gains(mln_ref, ln_mid, 0)
        for ref in (w_acc, b_acc, l_acc, acc_ref):
            ref[...] = jnp.zeros_like(ref)
        channel_part(IN_BWD, (a_in, b_in, dx_in), jobs)

    @pl.when(step > 0)
    def _():
        t = step - 1
        arrive(t, jobs)
        da_ref, db_ref = la0.at[t], la1.at[t]

        @rows_loop
        def _(r):
            at = pl.ds(r, 1)
            dzn = pre_back_row(unit_ref[r], inv_ref[0, at, :], keep_ref.at[r], da_ref[r].astype(F32), db_ref[r].astype(F32), dpg1_ref[r],
                               ln_ref, w_ref, w_acc, b_acc, l_acc)
            dzm = (nt(eye_ref[...], dz_ref[r]) + dzn).astype(BF16)
            dzm_ref[r] = dzm
            dzm = dzm.astype(F32)
            dpg_ref[r] = dzm * gu_ref[r]
            spread(d_st, swap_core1(post_back_row(munit_ref[r], minv_ref[0, at, :], g_ref[r], dzm, mln_ref, wo_ref, acc_ref)), r)

        @pl.when(t == STEPS - 1)
        def _():
            put_pre(grad1_ref, w_acc, b_acc, l_acc)
            put_post(grad0_ref, acc_ref)

        send_rows(t, [(DX_ROWS, d_st, d_send, dx_ref, d_ss, rs, 0)])


ALL = 16
EARLY_SHARE, LATE_SHARE = 64, 48


def device(o):
    return {"dp": o // GROUP, "dap": o % GROUP}


def everyone():
    dap = lax.axis_index("dap")
    me = lax.axis_index("dp") * GROUP + dap
    twin = me + 1 - dap % 2 * 2
    return me, twin, [(me + k) % ALL for k in range(1, ALL)], [(me + 2 * k) % ALL for k in range(1, GROUP)]


def enter_all():
    for to in everyone()[2]:
        pl.semaphore_signal(pltpu.get_barrier_semaphore(), inc=1, device_id=device(to), device_id_type=pl.DeviceIdType.MESH)


class Adder:
    def __init__(self, base, send_ref, got_ref, part_ref, tot_ref, sems):
        self.base, self.send_ref, self.got_ref, self.part_ref, self.tot_ref, self.sems = base, send_ref, got_ref, part_ref, tot_ref, sems
        self.size = part_ref.shape[0]

    def share(self, k, base=0):
        return pl.ds(pl.multiple_of(base + k * self.size, HAT), self.size)

    def sums(self, k):
        return self.tot_ref.at[self.share(k, self.base)]

    def remote(self, src, dst, phase, k, slot, to):
        return pltpu.make_async_remote_copy(src, dst, self.sems.at[2 * phase, k], self.sems.at[2 * phase + 1, slot], device_id=device(to),
                                            device_id_type=pl.DeviceIdType.MESH)

    def first(self, k, frm):
        other = everyone()[2][k]
        return self.remote(self.send_ref.at[self.share(other)], self.got_ref.at[frm], 0, k, frm, other)

    def second(self, k, frm):
        return self.remote(self.part_ref, self.sums(frm), 1, k, frm, everyone()[3][k])

    def third(self, k, block):
        return self.remote(self.sums(block), self.sums(block), 2, k, k, everyone()[1])

    def own(self, block):
        return self.remote(self.part_ref, self.sums(block), 2, GROUP, GROUP, everyone()[1])

    def before(self, device_number, k):
        return (device_number + ALL - 2 * (k + 1)) % ALL

    def fill(self, *packs):
        at = 0
        for ref in packs:
            self.send_ref[at:at + ref.shape[0], :] = ref[...].astype(BF16)
            at += ref.shape[0]
        self.send_ref[at:, :] = jnp.zeros((self.send_ref.shape[0] - at, C), BF16)

    def scatter(self):
        me = everyone()[0]
        for k in range(ALL - 1):
            self.first(k, me).start()
        self.got_ref[me] = self.send_ref[self.share(me), :]

    def add(self):
        me, twin, others, chips = everyone()
        for k in range(ALL - 1):
            self.first(k, others[k]).wait_recv()
        total = self.got_ref[0].astype(F32)
        for k in range(1, ALL):
            total = total + self.got_ref[k].astype(F32)
        self.part_ref[...] = total
        for k in range(GROUP - 1):
            self.second(k, me).start()
        self.own(me).start()
        self.tot_ref[self.share(me, self.base), :] = total

    def hand_on(self):
        me = everyone()[0]
        for k in range(GROUP - 1):
            self.second(k, self.before(me, k)).wait_recv()
            self.third(k, self.before(me, k)).start()

    def finish(self):
        me, twin, others, chips = everyone()
        for k in range(GROUP - 1):
            self.third(k, self.before(twin, k)).wait_recv()
        self.own(twin).wait_recv()
        self.own(me).wait_send()
        for k in range(ALL - 1):
            self.first(k, me).wait_send()
        for k in range(GROUP - 1):
            self.second(k, me).wait_send()
            self.third(k, self.before(me, k)).wait_send()


def last_kernel(a_in, b_in, dx_in, dpg_ref, keep_ref, unit_ref, inv_ref, dzm_ref, ln_in, w_proj, post0, post1, pre1,
                dz_ref, tot_out, ln_ref, w_acc, b_acc, l_acc, grad_ref, send_e, got_e, part_e, send_l, got_l, part_l, tot_ref, sems,
                st0, st1, se0, se1, la0, la1, ss0, ss1, rv0, rv1):
    step = step_now()
    jobs = [(st0, se0, la0, ss0, rv0), (st0, se1, la1, ss1, rv1)]
    w_ref = w_proj.at[0]
    early = Adder(0, send_e, got_e, part_e, tot_ref, sems.at[0])
    late = Adder(send_e.shape[0], send_l, got_l, part_l, tot_ref, sems.at[1])

    @pl.when(step == 0)
    def _():
        enter_all()
        set_gains(ln_ref, ln_in, 0)
        for ref in (w_acc, b_acc, l_acc):
            ref[...] = jnp.zeros_like(ref)
        block_part(OUT_BWD, (0, 1), (a_in, b_in, dx_in), jobs, ALL - 1)
        early.fill(post0, post1, pre1)
        early.scatter()

    @pl.when(step > 0)
    def _():
        t = step - 1
        block_arrive(t, (0, 1), jobs)

        @rows_loop
        def _(r):
            dzn = pre_back_row(unit_ref[r], inv_ref[0, pl.ds(r, 1), :], keep_ref.at[r], both(la0, t, r), both(la1, t, r), dpg_ref[r],
                               ln_ref, w_ref, w_acc, b_acc, l_acc)
            dz_ref[r] = (dzm_ref[r].astype(F32) + dzn).T.astype(BF16)

        @pl.when(t == STEPS - 1)
        def _():
            put_pre(grad_ref, w_acc, b_acc, l_acc)
            late.fill(grad_ref)
            late.scatter()
            early.add()
            late.add()
            early.hand_on()
            late.hand_on()
            early.finish()
            late.finish()
            tot_out[...] = tot_ref[...]


def split_kernel(z_in, dz_in, tot, z_out, dz_out, *grads):
    z_out[...] = z_in[...]
    dz_out[...] = dz_in[...]
    pl.when(step_now() == 0)(lambda: split_grads(tot, *grads))


def split_grads(tot, d_ln_in, d_w_proj, d_b_proj, d_ln_mid, d_w_out, d_b_out):
    at = 0
    for k in range(2):
        d_w_out[k] = tot[at:at + C, :]
        d_ln_mid[k] = tot[at + C:at + C + 2, :]
        d_b_out[k:k + 1, :] = tot[at + C + 2:at + C + 3, :]
        at += C + HAT
    for k, at in enumerate((ALL * EARLY_SHARE, at)):
        for j in range(5):
            d_w_proj[k, :, j * C:(j + 1) * C] = tot[at + j * C:at + (j + 1) * C, :].T
            d_b_proj[k:k + 1, j * C:(j + 1) * C] = tot[at + PROJ + j:at + PROJ + j + 1, :]
        d_ln_in[k] = tot[at + PROJ + 5:at + PROJ + 7, :]


def finish(z_new, dz_new, total):
    shapes = ((2, 2, C), (2, C, PROJ), (2, PROJ), (2, 2, C), (2, C, C), (2, C))
    grads = [jax.ShapeDtypeStruct(shape, F32) for shape in shapes]
    return pl.pallas_call(
        split_kernel,
        grid=(STEPS,),
        in_specs=[by_row(z_new), by_row(dz_new), whole(total)],
        out_specs=[by_row(NATIVE)] * 2 + [pl.BlockSpec(x.shape, lambda t, n=len(x.shape): (0,) * n) for x in grads],
        out_shape=[NATIVE] * 2 + grads,
        compiler_params=pltpu.CompilerParams(dimension_semantics=("arbitrary",)),
        name="split",
    )(z_new, dz_new, total)


TRI = jax.ShapeDtypeStruct((CH, N, N), BF16)
BTRI = jax.ShapeDtypeStruct((BCH, BLOCK, N), BF16)
BDX = jax.ShapeDtypeStruct((BCH, BLOCK, BLOCK), BF16)
SENT = (TRI, BTRI, BDX)
ROW = jax.ShapeDtypeStruct((ROWS, C, N), BF16)
ROW32 = jax.ShapeDtypeStruct((ROWS, C, N), F32)
NATIVE = jax.ShapeDtypeStruct((ROWS, N, C), BF16)
POST = jax.ShapeDtypeStruct((C + HAT, C), F32)
PRE = jax.ShapeDtypeStruct((PROJ + HAT, C), F32)
TOT = jax.ShapeDtypeStruct((ALL * (EARLY_SHARE + LATE_SHARE), C), F32)
KEEP = jax.ShapeDtypeStruct((ROWS, 4, C, N), F32)
INV = jax.ShapeDtypeStruct((STEPS, STEP, N), F32)


def by_row(array):
    tail = array.shape[1:]
    return pl.BlockSpec((array.shape[0] // STEPS,) + tail, lambda t: (t,) + (0,) * len(tail))


def whole(array):
    zeros = (0,) * len(array.shape)
    return pl.BlockSpec(array.shape, lambda t: zeros, pipeline_mode=pl.Buffered(1))


def row_call(kernel, name, collective_id, tris, ins, consts, outs, n_back, scratch, width=0):
    n_send = sum(out in SENT for out in outs)
    packed = (STEPS, 2, C, STEP, BLOCK) if BDX in outs else (STEPS, C, STEP, N)
    dma = pltpu.SemaphoreType.DMA
    sent = [pltpu.VMEM((2 * C * STEP, C), F32)] * n_send + [pltpu.VMEM(packed, BF16)] * n_send
    sems = [dma((STEPS, GROUP))] * n_send + ([dma((n_send,))] if n_send else [])
    back = [pltpu.VMEM((4 * N * 8, C), F32)] * n_back + [pltpu.VMEM((STEPS, GROUP, STEP, CH, N), BF16)] * n_back
    back += [pltpu.VMEM((STEPS, STEP, C, N), BF16)] * n_back
    if width:
        back = [pltpu.VMEM((BCH * BLOCK * width // C if k == 0 else 8, C), F32) for k in range(n_back)]
        back += [pltpu.VMEM((STEPS, 4, STEP, BCH, width), BF16)] * n_back + [pltpu.VMEM((STEPS, 2, STEP, C, width), BF16)] * n_back
    back += [dma((STEPS, GROUP))] * (2 * n_back)
    far = pl.BlockSpec(memory_space=pl.ANY)
    rows_out = [out for out in outs if is_rows(out)]
    near = [pltpu.VMEM(x.shape, x.dtype) for x in tris]
    near += [pltpu.VMEM((2, x.shape[0] // STEPS) + x.shape[1:], x.dtype) for x in [*ins, *rows_out]]
    near += [dma((max(len(tris), 1), GROUPS)), dma((2, len(ins))), dma((2, len(rows_out)))]
    return pl.pallas_call(
        functools.partial(staged_kernel, kernel, len(tris), len(ins), len(consts), outs),
        grid=(STEPS + 1,),
        in_specs=[far] * (len(tris) + len(ins)) + [whole(x) for x in consts],
        out_specs=[pl.BlockSpec(out.shape, lambda t: (0, 0)) if out in (PRE, POST, TOT) else far for out in outs],
        out_shape=outs,
        scratch_shapes=sent + scratch + sems + back + near,
        compiler_params=pltpu.CompilerParams(dimension_semantics=("arbitrary",), vmem_limit_bytes=VMEM_LIMIT, collective_id=collective_id, has_side_effects=True),
        name=name,
    )(*tris, *ins, *consts)


def local_step(z_pair, pair_mask, dz_out, ln_in, w_proj, b_proj, ln_mid, w_out, b_out):
    z, dz = z_pair[0], dz_out[0]
    mask = pair_mask.reshape(STEPS, STEP, N)
    pre, post = [ln_in, w_proj, b_proj], [ln_mid, w_out, b_out]
    eye = [pltpu.VMEM((C, C), BF16)]
    pre_c = [pltpu.VMEM((2, C, N), F32), pltpu.VMEM((PROJ, C), BF16), pltpu.VMEM((PROJ, N), F32)]
    post_c = [pltpu.VMEM((2, C, N), F32), pltpu.VMEM((C, C), BF16), pltpu.VMEM((C, N), F32)]
    post_acc = [pltpu.VMEM((4, C, C), F32)]
    pre_acc = [pltpu.VMEM((PROJ, C), F32), pltpu.VMEM((PROJ, C), F32), pltpu.VMEM((2, C, C), F32)]

    gains = [pltpu.VMEM((2, C, N), F32)]
    kept = [TRI, TRI, ROW32, KEEP, ROW32, INV]
    a0, b0, g0, keep0, unit0, inv0 = row_call(pre_kernel, "pre0", 0, [], [z, mask], pre, [BTRI, BTRI] + kept[2:], 0, eye + pre_c)
    a1, b1, g1, keep1, unit1, inv1, zm, gu0, munit0, minv0 = row_call(
        mid_kernel, "mid", 1, [a0, b0], [z, g0, mask], post + pre, kept + [ROW, ROW32, ROW32, INV], 1, eye + pre_c + post_c, BLOCK)
    dx1, z_new, dpg1, post_g1 = row_call(
        turn_kernel, "turn", 2, [a1, b1], [zm, g1, dz], post, [TRI, NATIVE, ROW32, POST], 1, eye + post_c + post_acc)
    dx0, dzm, dpg0, pre_g1, post_g0 = row_call(
        back_kernel, "back", 3, [a1, b1, dx1], [dpg1, keep1, unit1, inv1, dz, munit0, minv0, g0, gu0], [ln_in, w_proj, ln_mid, w_out],
        [BDX, ROW, ROW32, PRE, POST], 2, eye + gains * 2 + pre_acc + post_acc)
    adders = [pltpu.VMEM(PRE.shape, F32)]
    for size in (EARLY_SHARE, LATE_SHARE):
        adders += [pltpu.VMEM((ALL * size, C), BF16), pltpu.VMEM((ALL, size, C), BF16), pltpu.VMEM((size, C), F32)]
    adders += [pltpu.VMEM(TOT.shape, F32), pltpu.SemaphoreType.DMA((2, 6, ALL))]
    dz_new, total = row_call(
        last_kernel, "last", 4, [a0, b0, dx0], [dpg0, keep0, unit0, inv0, dzm], [ln_in, w_proj, post_g0, post_g1, pre_g1],
        [NATIVE, TOT], 2, gains + pre_acc + adders, N)
    z_out, dz_pair, *grads = finish(z_new, dz_new, total)
    return z_out[None], dz_pair[None], *grads


def solution(mesh):
    row_spec = P("dp", "dap")
    return jax.shard_map(local_step, mesh=mesh, in_specs=(row_spec,) * 3 + (P(),) * 6,
                         out_specs=(row_spec,) * 2 + (P(),) * 6, check_vma=False)
```

```python
import functools

import jax
import jax.numpy as jnp
from jax import lax
from jax.experimental import pallas as pl
from jax.experimental.pallas import tpu as pltpu
from jax.sharding import PartitionSpec as P

LN_EPS = 1e-5
N = 256
C = 128
GROUP = 8
ROWS = N // GROUP
CH = C // GROUP
STEP = 8
UNROLL = 4
STEPS = ROWS // STEP
PROJ = 5 * C
HAT = 16
F32 = jnp.float32
BF16 = jnp.bfloat16
VMEM_LIMIT = 62 * 1024 * 1024


def dot(lhs, rhs, lhs_dim, rhs_dim):
    return lax.dot_general(lhs, rhs, (((lhs_dim,), (rhs_dim,)), ((), ())), preferred_element_type=F32)


nn = functools.partial(dot, lhs_dim=1, rhs_dim=0)
nt = functools.partial(dot, lhs_dim=1, rhs_dim=1)
tn = functools.partial(dot, lhs_dim=0, rhs_dim=0)


def step_now():
    return pl.program_id(0)


def mean(values):
    return jnp.mean(values, axis=0, keepdims=True)


def norm(values):
    cen = values - mean(values)
    inv = lax.rsqrt(mean(cen * cen) + LN_EPS)
    return cen * inv, inv


def norm_back(d_hat, unit, inv, gain):
    d_unit = d_hat * gain
    mean_d = mean(d_unit)
    mean_du = mean(d_unit * unit)
    return inv * (d_unit - mean_d - unit * mean_du)


def fold(values):
    return values[:, :C] + values[:, C:]


def row_sums(acc):
    return jnp.sum(acc.T, axis=0, keepdims=True)


def sigmoid(values):
    return 0.5 * jnp.tanh(0.5 * values) + 0.5


def project(z_t, ln, w_t, bias):
    unit, inv = norm(z_t)
    z_hat = (unit * ln[0] + ln[1]).astype(BF16)
    return unit, inv, z_hat, nn(w_t[...], z_hat) + bias[...]


def set_eye(eye):
    same = lax.broadcasted_iota(jnp.int32, (C, C), 0) == lax.broadcasted_iota(jnp.int32, (C, C), 1)
    eye[...] = jnp.where(same, 1.0, 0.0).astype(BF16)


def set_column(ref, row):
    column = jnp.broadcast_to(row.astype(F32), (C, C)).T
    ref[:, :C] = column
    ref[:, C:] = column


def set_pre(block, ln_in, w_proj, b_proj, ln, w_t, bias):
    for k in range(2):
        set_column(ln.at[k], ln_in[block, k:k + 1, :])
    for k in range(5):
        cols = slice(k * C, (k + 1) * C)
        set_column(bias.at[cols], b_proj[block:block + 1, cols])
        w_t[cols, :] = w_proj[block, :, cols].astype(F32).T.astype(BF16)


def set_post(block, ln_mid, w_out, b_out, mln, wo_t, bo):
    for k in range(2):
        set_column(mln.at[k], ln_mid[block, k:k + 1, :])
    set_column(bo, b_out[block:block + 1, :])
    wo_t[...] = w_out[block].astype(F32).T.astype(BF16)


def place():
    me = lax.axis_index("dap")
    return me, me // 4, (me // 2) % 2, me % 2


def enter():
    me = lax.axis_index("dap")
    sem = pltpu.get_barrier_semaphore()
    for k in range(1, GROUP):
        pl.semaphore_signal(sem, inc=1, device_id={"dap": (me + k) % GROUP}, device_id_type=pl.DeviceIdType.MESH)


def all_in(others=GROUP - 1):
    pl.semaphore_wait(pltpu.get_barrier_semaphore(), others)


def peers():
    me, cy, cx, core = place()
    out = []
    for dy, dx in ((1, 1), (1, 0), (0, 1), (0, 0)):
        for dc in (1, 0):
            out.append((((cy + dy) % 2) * 2 + (cx + dx) % 2) * 2 + (core + dc) % 2)
    return me, out


def spread(ref, value, row):
    for h in range(2):
        ref[pl.ds(h * C * STEP + row, C, stride=STEP), :] = value[:, h * C:(h + 1) * C]


def pack_rows(stage, send_ref, slot):
    for h in range(2):
        for q in range(4):
            rows = stage[pl.ds((h * C + q * 32) * STEP, 32 * STEP), :].reshape(32, STEP, C)
            send_ref[slot, q * 32:(q + 1) * 32, :, h * C:(h + 1) * C] = rows.astype(BF16)


def move(src_ref, dst_ref, send_sem, recv_sem, dest, own):
    if own:
        return pltpu.make_async_copy(src_ref, dst_ref, recv_sem)
    return pltpu.make_async_remote_copy(src_ref, dst_ref, send_sem, recv_sem, device_id={"dap": dest}, device_id_type=pl.DeviceIdType.MESH)


def wait_sends(copies):
    for copy in copies:
        if copy.is_remote:
            copy.wait_send()


def row_copies(send_ref, out_ref, send_sem, recv_sem, slot):
    me, dests = peers()
    start = pl.multiple_of(me * ROWS + slot * STEP, STEP)
    return [
        move(send_ref.at[slot, pl.ds(pl.multiple_of(dest * CH, CH), CH)], out_ref.at[:, pl.ds(start, STEP), :],
             send_sem.at[slot, k], recv_sem, dest, k == GROUP - 1)
        for k, dest in enumerate(dests)
    ]


BCH = C // 2
BLOCK = N // 2


def by_column(kind, core):
    return core if kind else 1 - core


def pick(column, on_column, on_row):
    return column * on_column + (1 - column) * on_row


def channels(core):
    return pl.ds(pl.multiple_of(core * BCH, BCH), BCH)


def swap(lo, hi):
    first = lax.broadcasted_iota(jnp.int32, lo.shape, 1) < BLOCK // 2
    return jnp.where(first, lo, pltpu.roll(hi, BLOCK // 2, 1)), jnp.where(first, pltpu.roll(lo, BLOCK // 2, 1), hi)


def swap_core1(value):
    lo, hi = swap(value[BCH:, :BLOCK], value[BCH:, BLOCK:])
    return jnp.concatenate([value[:BCH], jnp.concatenate([lo, hi], axis=1)], axis=0)


def block_copies(kind, halves, send_ref, out_ref, send_sem, recv_sem, slot):
    me, cy, cx, core = place()
    out = []
    for k, (to, far) in enumerate(((0, 1), (1, 1), (1 - core, 0), (core, 0))):
        column = by_column(kind, to)
        y, x = cy, cx
        if far:
            y, x = (1 - cy, cx) if column else (cy, 1 - cx)
        start = pick(column, cy, cx) * 2 * ROWS + core * ROWS + slot * STEP
        src = send_ref.at[slot, pick(column, y, x), channels(to)] if halves else send_ref.at[slot, channels(to)]
        out.append(move(src, out_ref.at[:, pl.ds(pl.multiple_of(start, STEP), STEP), :], send_sem.at[slot, k], recv_sem, (y * 2 + x) * 2 + to, k == 3))
    return out


def pack_halves(stage, send_ref, slot):
    for h in range(2):
        for q in range(4):
            rows = stage[pl.ds((h * C + q * 32) * STEP, 32 * STEP), :].reshape(32, STEP, C)
            send_ref[slot, h, q * 32:(q + 1) * 32] = rows.astype(BF16)


A_ROWS = (pack_rows, functools.partial(block_copies, 0, False))
B_ROWS = (pack_rows, functools.partial(block_copies, 1, False))
ROWS_ALL = (pack_rows, row_copies)
DX_ROWS = (pack_halves, functools.partial(block_copies, 0, True))


def send_rows(step, jobs):
    for (pack, copies), stage, send_ref, out_ref, send_sem, recv_sems, k in jobs:
        pack(stage, send_ref, step)
        for copy in copies(send_ref, out_ref, send_sem, recv_sems.at[k], step):
            copy.start()
    PENDING.extend(jobs)


PENDING = []


def finish_rows(jobs):
    for (pack, copies), stage, send_ref, out_ref, send_sem, recv_sems, k in jobs:
        for slot in range(STEPS):
            wait_sends(copies(send_ref, out_ref, send_sem, recv_sems.at[k], slot))
        pltpu.make_async_copy(out_ref, out_ref, recv_sems.at[k]).wait()


OUT_FWD = (lambda c, a, b: nt(a[c], b[c]),)
IN_FWD = (lambda c, a, b: tn(a[c], b[c]),)
IN_BWD = (lambda c, a, b, dx: nt(b[c], dx[c]), lambda c, a, b, dx: nn(a[c], dx[c]))
OUT_BWD = (lambda c, a, b, dx: nn(dx[c], b[c]), lambda c, a, b, dx: tn(dx[c], a[c]))


def back_copy(job, t, k, dest, frm):
    stage, send_ref, land_ref, send_sem, recv_sem = job
    return pltpu.make_async_remote_copy(
        send_ref.at[t, dest], land_ref.at[t, :, pl.ds(pl.multiple_of(frm * CH, CH), CH), :], send_sem.at[t, k], recv_sem.at[t, frm],
        device_id={"dap": dest}, device_id_type=pl.DeviceIdType.MESH)


EARLY = 2
GROUPS = 4


class Piecewise:
    def __init__(self, source, ref, sems):
        self.source, self.ref, self.sems = source, ref, sems

    def load(self, g):
        size = self.ref.shape[0] // GROUPS
        part = pl.ds(g * size, size)
        return pltpu.make_async_copy(self.source.at[part], self.ref.at[part], self.sems.at[g])


def channel_part(products, ins, jobs):
    me, dests = peers()
    refs = [x.ref for x in ins]
    for j, (product, job) in enumerate(zip(products, jobs)):
        stage, send_ref, land_ref = job[:3]

        def body(c, carry):
            value = product(c, *refs)
            for h in range(2):
                stage[pl.ds((h * 2 + c // 8) * N * 8 + c % 8, N, stride=8), :] = value[:, h * C:(h + 1) * C]
            return carry

        for g in range(GROUPS):
            if j == 0:
                for x in ins:
                    x.load(g).wait()
            lax.fori_loop(g * (CH // GROUPS), (g + 1) * (CH // GROUPS), body, 0, unroll=True)
        if j == 0:
            all_in()
        for t in range(STEPS):
            for dest in range(GROUP):
                for h in range(2):
                    at = h * 2 * N * 8 + (dest * ROWS + t * STEP) * 8
                    lo = stage[pl.ds(at, 64), :].reshape(STEP, 8, C)
                    hi = stage[pl.ds(at + N * 8, 64), :].reshape(STEP, 8, C)
                    send_ref[t, dest, :, :, h * C:(h + 1) * C] = jnp.concatenate([lo, hi], axis=1).astype(BF16)
            for k, dest in enumerate(dests[:-1]):
                back_copy(job, t, k, dest, me).start()
            land_ref[t, :, pl.ds(pl.multiple_of(me * CH, CH), CH), :] = send_ref[t, me]


def block_sends(kind, job, t, piece=None):
    stage, send_ref, land_ref, send_sem, recv_sem = job
    me, cy, cx, core = place()
    column = by_column(kind, core)
    mine = pick(column, cy, cx)
    y, x = cy + column * (1 - 2 * cy), cx + (1 - column) * (1 - 2 * cx)
    size = BCH if piece is None else BCH // GROUPS
    at = (piece or 0) * size
    land = land_ref.at[t, mine, :, pl.ds(pl.multiple_of(core * BCH + at, size), size), :]
    out = []
    for k, (dest, member, slot) in enumerate((((y * 2 + x) * 2, pick(column, y, x) * 2, core), ((y * 2 + x) * 2 + 1, pick(column, y, x) * 2 + 1, core),
                                              (me + 1 - 2 * core, mine * 2 + 1 - core, 2))):
        out.append(pltpu.make_async_remote_copy(send_ref.at[t, member, :, pl.ds(at, size), :], land, send_sem.at[t, k], recv_sem.at[t, slot],
                                                device_id={"dap": dest}, device_id_type=pl.DeviceIdType.MESH))
    return out


def block_receives(kind, job, t):
    stage, send_ref, land_ref, send_sem, recv_sem = job
    me, cy, cx, core = place()
    out = []
    for slot, (frm, far) in enumerate(((0, 1), (1, 1), (1 - core, 0))):
        column = by_column(kind, frm)
        y, x = cy, cx
        if far:
            y, x = (1 - cy, cx) if column else (cy, 1 - cx)
        out.append(pltpu.make_async_remote_copy(send_ref.at[t, 0], land_ref.at[t, pick(column, y, x), :, channels(frm), :], send_sem.at[t, slot],
                                                recv_sem.at[t, slot], device_id={"dap": (y * 2 + x) * 2 + frm}, device_id_type=pl.DeviceIdType.MESH))
    return out


def block_part(products, kinds, ins, jobs, others=GROUP - 1):
    me, cy, cx, core = place()
    refs = [x.ref for x in ins]
    for j, (product, kind, job) in enumerate(zip(products, kinds, jobs)):
        stage, send_ref, land_ref = job[:3]
        tiles = send_ref.shape[-1] // C

        def body(c, carry):
            value = product(c, *refs)
            for h in range(tiles):
                stage[pl.ds((h * (BCH // 8) + c // 8) * BLOCK * 8 + c % 8, BLOCK, stride=8), :] = value[:, h * C:(h + 1) * C]
            return carry

        mine = pick(by_column(kind, core), cy, cx)

        def pack(t, q):
            for member in range(4):
                for h in range(tiles):
                    at = (h * (BCH // 8) + q * 2) * BLOCK * 8 + (member * ROWS + t * STEP) * 8
                    lo = stage[pl.ds(at, 64), :].reshape(STEP, 8, C)
                    hi = stage[pl.ds(at + BLOCK * 8, 64), :].reshape(STEP, 8, C)
                    send_ref[t, member, :, q * CH:(q + 1) * CH, h * C:(h + 1) * C] = jnp.concatenate([lo, hi], axis=1).astype(BF16)

        def keep(t):
            land_ref[t, mine, :, channels(core), :] = send_ref[t, mine * 2 + core]

        for g in range(GROUPS):
            if j == 0:
                for x in ins:
                    x.load(g).wait()
            lax.fori_loop(g * CH, (g + 1) * CH, body, 0, unroll=4)
            if g == j == 0:
                all_in(others)
            for t in range(EARLY):
                pack(t, g)
                for copy in block_sends(kind, job, t, g):
                    copy.start()
        for t in range(EARLY, STEPS):
            for g in range(GROUPS):
                pack(t, g)
            for copy in block_sends(kind, job, t):
                copy.start()
        for t in range(STEPS):
            keep(t)


def block_arrive(t, kinds, jobs):
    for kind, job in zip(kinds, jobs):
        for copy in block_receives(kind, job, t):
            copy.wait_recv()

    @pl.when(t == STEPS - 1)
    def _():
        for kind, job in zip(kinds, jobs):
            for slot in range(STEPS):
                for copy in block_sends(kind, job, slot):
                    copy.wait_send()


def both(land_ref, t, r):
    return land_ref[t, 0, r].astype(F32) + land_ref[t, 1, r].astype(F32)


def staged_kernel(inner, n_tri, n_in, n_const, outs, *refs):
    n_far = n_tri + n_in
    far, consts, refs = refs[:n_far], refs[n_far:n_far + n_const], refs[n_far + n_const:]
    results, refs = list(refs[:len(outs)]), refs[len(outs):]
    tri_sem, row_sem, out_sem = refs[-3:]
    rows_out = [k for k, out in enumerate(outs) if is_rows(out)]
    n_near = n_far + len(rows_out)
    refs, near = refs[:-3 - n_near], refs[-3 - n_near:-3]
    step = step_now()
    slot = (step + 1) % 2
    tris = [Piecewise(far[k], near[k], tri_sem.at[k]) for k in range(n_tri)]
    targets = [results[k] for k in rows_out]
    for k, ref in zip(rows_out, near[n_far:]):
        results[k] = ref.at[slot]

    def fetch(t, slot):
        return [pltpu.make_async_copy(block_of(whole_ref, t), ref.at[slot], row_sem.at[slot, k])
                for k, (whole_ref, ref) in enumerate(zip(far[n_tri:], near[n_tri:n_far]))]

    def store(t, slot):
        return [pltpu.make_async_copy(ref.at[slot], block_of(whole_ref, t), out_sem.at[slot, k])
                for k, (whole_ref, ref) in enumerate(zip(targets, near[n_far:]))]

    @pl.when(step == 0)
    def _():
        for g in range(GROUPS):
            for x in tris:
                x.load(g).start()
        for copy in fetch(0, 0):
            copy.start()

    @pl.when(step > 0)
    def _():
        for copy in fetch(step - 1, slot):
            copy.wait()

    @pl.when((step > 0) & (step < STEPS))
    def _():
        for copy in fetch(step, 1 - slot):
            copy.start()

    @pl.when(step > 2)
    def _():
        for copy in store(step - 3, slot):
            copy.wait()

    PENDING.clear()
    inner(*tris, *[ref.at[slot] for ref in near[n_tri:n_far]], *consts, *results, *refs)
    jobs = list(PENDING)

    @pl.when(step > 0)
    def _():
        for copy in store(step - 1, slot):
            copy.start()

    @pl.when(step == STEPS)
    def _():
        finish_rows(jobs)
        for copy in store(step - 2, 1 - slot) + store(step - 1, slot):
            copy.wait()


def block_of(ref, t):
    size = ref.shape[0] // STEPS
    return ref.at[pl.ds(t * size, size)]


def is_rows(out):
    return out not in (PRE, POST, TOT, *SENT)


def arrive(t, jobs):
    me, dests = peers()
    for job in jobs:
        for k, frm in enumerate(dests[:-1]):
            back_copy(job, t, k, frm, frm).wait_recv()

    @pl.when(t == STEPS - 1)
    def _():
        for job in jobs:
            for slot in range(STEPS):
                for k, dest in enumerate(dests[:-1]):
                    back_copy(job, slot, k, dest, me).wait_send()


def rows_loop(body):
    def step(r, carry):
        body(r)
        return carry

    lax.fori_loop(0, STEP, step, 0, unroll=UNROLL)


def pre_row(r, z_t, mask_ref, ln_ref, w_t_ref, bias_ref, g_ref, keep_ref, unit_ref, inv_ref, a_stage, b_stage):
    unit, inv, _, p = project(z_t, ln_ref, w_t_ref, bias_ref)
    unit_ref[r] = unit
    inv_ref[0, pl.ds(r, 1), :] = inv
    m = mask_ref[0, pl.ds(r, 1), :].astype(F32)
    for side, stage in ((0, a_stage), (1, b_stage)):
        s = sigmoid(p[2 * side * C:(2 * side + 1) * C])
        v = p[(2 * side + 1) * C:(2 * side + 2) * C]
        sm = s * m
        spread(stage, sm * v, r)
        keep_ref[r, 2 * side] = sm
        keep_ref[r, 2 * side + 1] = v * (1.0 - s)
    g_ref[r] = sigmoid(p[4 * C:])


def pre_kernel(z_ref, mask_ref, ln_in, w_proj, b_proj, a_ref, b_ref, g_ref, keep_ref, unit_ref, inv_ref, a_st, b_st, a_send, b_send,
               eye_ref, ln_ref, w_t_ref, bias_ref, a_ss, b_ss, rs):
    step = step_now()

    @pl.when(step == 0)
    def _():
        enter()
        set_eye(eye_ref)
        set_pre(0, ln_in, w_proj, b_proj, ln_ref, w_t_ref, bias_ref)
        all_in()

    @pl.when(step > 0)
    def _():
        t = step - 1

        @rows_loop
        def _(r):
            z_t = nt(eye_ref[...], z_ref[r])
            pre_row(r, z_t, mask_ref, ln_ref, w_t_ref, bias_ref, g_ref, keep_ref, unit_ref, inv_ref, a_st, b_st)

        send_rows(t, [(A_ROWS, a_st, a_send, a_ref, a_ss, rs, 0), (B_ROWS, b_st, b_send, b_ref, b_ss, rs, 1)])


def mid_kernel(a_in, b_in, z_ref, g0_ref, mask_ref, ln_mid, w_out, b_out, ln_in, w_proj, b_proj,
               a_ref, b_ref, g_ref, keep_ref, unit_ref, inv_ref, zm_ref, gu_ref, munit_ref, minv_ref, a_st, b_st, a_send, b_send,
               eye_ref, ln_ref, w_t_ref, bias_ref, mln_ref, wo_t_ref, bo_ref, a_ss, b_ss, rs,
               st0, se0, la0, ss0, rv0):
    step = step_now()
    jobs = [(st0, se0, la0, ss0, rv0)]

    @pl.when(step == 0)
    def _():
        enter()
        set_eye(eye_ref)
        set_pre(1, ln_in, w_proj, b_proj, ln_ref, w_t_ref, bias_ref)
        set_post(0, ln_mid, w_out, b_out, mln_ref, wo_t_ref, bo_ref)
        block_part(OUT_FWD, (0,), (a_in, b_in), jobs)

    @pl.when(step > 0)
    def _():
        t = step - 1
        block_arrive(t, (0,), jobs)

        @rows_loop
        def _(r):
            unit, inv = norm(swap_core1(jnp.concatenate([la0[t, 0, r], la0[t, 1, r]], axis=1).astype(F32)))
            munit_ref[r] = unit
            minv_ref[0, pl.ds(r, 1), :] = inv
            x_hat = (unit * mln_ref[0] + mln_ref[1]).astype(BF16)
            update = nn(wo_t_ref[...], x_hat) + bo_ref[...]
            g = g0_ref[r]
            change = g * update
            gu_ref[r] = change * (1.0 - g)
            z_new = (nt(eye_ref[...], z_ref[r]) + change).astype(BF16)
            zm_ref[r] = z_new
            pre_row(r, z_new.astype(F32), mask_ref, ln_ref, w_t_ref, bias_ref, g_ref, keep_ref, unit_ref, inv_ref, a_st, b_st)

        send_rows(t, [(ROWS_ALL, a_st, a_send, a_ref, a_ss, rs, 0), (ROWS_ALL, b_st, b_send, b_ref, b_ss, rs, 1)])


def post_back_row(unit, inv, g, dz, mln_ref, wo_ref, acc_ref, x_hat=None):
    if x_hat is None:
        x_hat = (unit * mln_ref[0] + mln_ref[1]).astype(BF16)
    d_up = dz * g
    d_up_bf = d_up.astype(BF16)
    acc_ref[0] += nt(x_hat, d_up_bf)
    acc_ref[3] += fold(d_up)
    d_hat = nn(wo_ref[...], d_up_bf).astype(BF16).astype(F32)
    acc_ref[1] += fold(d_hat * unit)
    acc_ref[2] += fold(d_hat)
    return norm_back(d_hat, unit, inv, mln_ref[0])


def put_post(grad_ref, acc_ref):
    grad_ref[0:C, :] = acc_ref[0]
    grad_ref[C:C + 8, :] = jnp.concatenate([row_sums(acc_ref[1]), row_sums(acc_ref[2]), row_sums(acc_ref[3]), jnp.zeros((5, C), F32)], axis=0)
    grad_ref[C + 8:C + HAT, :] = jnp.zeros((8, C), F32)


def turn_kernel(a_in, b_in, zm_ref, g_ref, dz_ref, ln_mid, w_out, b_out,
                dx_ref, z_out_ref, dpg_ref, grad_ref, d_st, d_send, eye_ref, mln_ref, wo_t_ref, bo_ref, acc_ref, d_ss, rs,
               st0, se0, la0, ss0, rv0):
    step = step_now()
    jobs = [(st0, se0, la0, ss0, rv0)]
    wo_ref = w_out.at[1]

    @pl.when(step == 0)
    def _():
        enter()
        set_eye(eye_ref)
        set_post(1, ln_mid, w_out, b_out, mln_ref, wo_t_ref, bo_ref)
        acc_ref[...] = jnp.zeros_like(acc_ref)
        channel_part(IN_FWD, (a_in, b_in), jobs)

    @pl.when(step > 0)
    def _():
        t = step - 1
        arrive(t, jobs)
        x_ref = la0.at[t]

        @rows_loop
        def _(r):
            dz = nt(eye_ref[...], dz_ref[r])
            g = g_ref[r]
            unit, inv = norm(x_ref[r].astype(F32))
            x_hat = (unit * mln_ref[0] + mln_ref[1]).astype(BF16)
            change = g * (nn(wo_t_ref[...], x_hat) + bo_ref[...])
            dpg_ref[r] = dz * change * (1.0 - g)
            z_out_ref[r] = (zm_ref[r].astype(F32) + change).T.astype(BF16)
            spread(d_st, post_back_row(unit, inv, g, dz, mln_ref, wo_ref, acc_ref, x_hat), r)

        @pl.when(t == STEPS - 1)
        def _():
            put_post(grad_ref, acc_ref)

        send_rows(t, [(ROWS_ALL, d_st, d_send, dx_ref, d_ss, rs, 0)])


def pre_back_row(unit, inv, keep, da, db, d_pg, ln_ref, w_ref, w_acc, b_acc, l_acc):
    z_hat = (unit * ln_ref[0] + ln_ref[1]).astype(BF16)
    parts = []
    for side, d_side in ((0, da), (1, db)):
        d_v = d_side * keep[2 * side]
        parts += [d_v * keep[2 * side + 1], d_v]
    parts.append(d_pg)
    for k, part in enumerate(parts):
        b_acc[k * C:(k + 1) * C, :] += fold(part)
    d_p = jnp.concatenate([part.astype(BF16) for part in parts], axis=0)
    w_acc[...] += nt(d_p, z_hat)
    d_hat = nn(w_ref[...], d_p).astype(BF16).astype(F32)
    l_acc[0] += fold(d_hat * unit)
    l_acc[1] += fold(d_hat)
    return norm_back(d_hat, unit, inv, ln_ref[0])


def put_pre(grad_ref, w_acc, b_acc, l_acc):
    grad_ref[0:PROJ, :] = w_acc[...]
    rows = [row_sums(b_acc[k * C:(k + 1) * C, :]) for k in range(5)]
    rows += [row_sums(l_acc[0]), row_sums(l_acc[1]), jnp.zeros((1, C), F32)]
    grad_ref[PROJ:PROJ + 8, :] = jnp.concatenate(rows, axis=0)
    grad_ref[PROJ + 8:PROJ + HAT, :] = jnp.zeros((8, C), F32)


def set_gains(ref, ln, block):
    for k in range(2):
        set_column(ref.at[k], ln[block, k:k + 1, :])


def back_kernel(a_in, b_in, dx_in, dpg1_ref, keep_ref, unit_ref, inv_ref, dz_ref, munit_ref, minv_ref, g_ref, gu_ref, ln_in, w_proj, ln_mid, w_out,
                dx_ref, dzm_ref, dpg_ref, grad1_ref, grad0_ref, d_st, d_send,
                eye_ref, ln_ref, mln_ref, w_acc, b_acc, l_acc, acc_ref, d_ss, rs,
               st0, st1, se0, se1, la0, la1, ss0, ss1, rv0, rv1):
    step = step_now()
    jobs = [(st0, se0, la0, ss0, rv0), (st1, se1, la1, ss1, rv1)]
    w_ref, wo_ref = w_proj.at[1], w_out.at[0]

    @pl.when(step == 0)
    def _():
        enter()
        set_eye(eye_ref)
        set_gains(ln_ref, ln_in, 1)
        set_gains(mln_ref, ln_mid, 0)
        for ref in (w_acc, b_acc, l_acc, acc_ref):
            ref[...] = jnp.zeros_like(ref)
        channel_part(IN_BWD, (a_in, b_in, dx_in), jobs)

    @pl.when(step > 0)
    def _():
        t = step - 1
        arrive(t, jobs)
        da_ref, db_ref = la0.at[t], la1.at[t]

        @rows_loop
        def _(r):
            at = pl.ds(r, 1)
            dzn = pre_back_row(unit_ref[r], inv_ref[0, at, :], keep_ref.at[r], da_ref[r].astype(F32), db_ref[r].astype(F32), dpg1_ref[r],
                               ln_ref, w_ref, w_acc, b_acc, l_acc)
            dzm = (nt(eye_ref[...], dz_ref[r]) + dzn).astype(BF16)
            dzm_ref[r] = dzm
            dzm = dzm.astype(F32)
            dpg_ref[r] = dzm * gu_ref[r]
            spread(d_st, swap_core1(post_back_row(munit_ref[r], minv_ref[0, at, :], g_ref[r], dzm, mln_ref, wo_ref, acc_ref)), r)

        @pl.when(t == STEPS - 1)
        def _():
            put_pre(grad1_ref, w_acc, b_acc, l_acc)
            put_post(grad0_ref, acc_ref)

        send_rows(t, [(DX_ROWS, d_st, d_send, dx_ref, d_ss, rs, 0)])


ALL = 16
EARLY_SHARE, LATE_SHARE = 64, 48


def device(o):
    return {"dp": o // GROUP, "dap": o % GROUP}


def everyone():
    dap = lax.axis_index("dap")
    me = lax.axis_index("dp") * GROUP + dap
    twin = me + 1 - dap % 2 * 2
    return me, twin, [(me + k) % ALL for k in range(1, ALL)], [(me + 2 * k) % ALL for k in range(1, GROUP)]


def enter_all():
    for to in everyone()[2]:
        pl.semaphore_signal(pltpu.get_barrier_semaphore(), inc=1, device_id=device(to), device_id_type=pl.DeviceIdType.MESH)


class Adder:
    def __init__(self, base, send_ref, got_ref, part_ref, tot_ref, sems):
        self.base, self.send_ref, self.got_ref, self.part_ref, self.tot_ref, self.sems = base, send_ref, got_ref, part_ref, tot_ref, sems
        self.size = part_ref.shape[0]

    def share(self, k, base=0):
        return pl.ds(pl.multiple_of(base + k * self.size, HAT), self.size)

    def sums(self, k):
        return self.tot_ref.at[self.share(k, self.base)]

    def remote(self, src, dst, phase, k, slot, to):
        return pltpu.make_async_remote_copy(src, dst, self.sems.at[2 * phase, k], self.sems.at[2 * phase + 1, slot], device_id=device(to),
                                            device_id_type=pl.DeviceIdType.MESH)

    def first(self, k, frm):
        other = everyone()[2][k]
        return self.remote(self.send_ref.at[self.share(other)], self.got_ref.at[frm], 0, k, frm, other)

    def second(self, k, frm):
        return self.remote(self.part_ref, self.sums(frm), 1, k, frm, everyone()[3][k])

    def third(self, k, block):
        return self.remote(self.sums(block), self.sums(block), 2, k, k, everyone()[1])

    def own(self, block):
        return self.remote(self.part_ref, self.sums(block), 2, GROUP, GROUP, everyone()[1])

    def before(self, device_number, k):
        return (device_number + ALL - 2 * (k + 1)) % ALL

    def fill(self, *packs):
        at = 0
        for ref in packs:
            self.send_ref[at:at + ref.shape[0], :] = ref[...].astype(BF16)
            at += ref.shape[0]
        self.send_ref[at:, :] = jnp.zeros((self.send_ref.shape[0] - at, C), BF16)

    def scatter(self):
        me = everyone()[0]
        for k in range(ALL - 1):
            self.first(k, me).start()
        self.got_ref[me] = self.send_ref[self.share(me), :]

    def add(self):
        me, twin, others, chips = everyone()
        for k in range(ALL - 1):
            self.first(k, others[k]).wait_recv()
        total = self.got_ref[0].astype(F32)
        for k in range(1, ALL):
            total = total + self.got_ref[k].astype(F32)
        self.part_ref[...] = total
        for k in range(GROUP - 1):
            self.second(k, me).start()
        self.own(me).start()
        self.tot_ref[self.share(me, self.base), :] = total

    def hand_on(self):
        me = everyone()[0]
        for k in range(GROUP - 1):
            self.second(k, self.before(me, k)).wait_recv()
            self.third(k, self.before(me, k)).start()

    def finish(self):
        me, twin, others, chips = everyone()
        for k in range(GROUP - 1):
            self.third(k, self.before(twin, k)).wait_recv()
        self.own(twin).wait_recv()
        self.own(me).wait_send()
        for k in range(ALL - 1):
            self.first(k, me).wait_send()
        for k in range(GROUP - 1):
            self.second(k, me).wait_send()
            self.third(k, self.before(me, k)).wait_send()


def last_kernel(a_in, b_in, dx_in, dpg_ref, keep_ref, unit_ref, inv_ref, dzm_ref, ln_in, w_proj, post0, post1, pre1,
                dz_ref, tot_out, ln_ref, w_acc, b_acc, l_acc, grad_ref, send_e, got_e, part_e, send_l, got_l, part_l, tot_ref, sems,
                st0, st1, se0, se1, la0, la1, ss0, ss1, rv0, rv1):
    step = step_now()
    jobs = [(st0, se0, la0, ss0, rv0), (st0, se1, la1, ss1, rv1)]
    w_ref = w_proj.at[0]
    early = Adder(0, send_e, got_e, part_e, tot_ref, sems.at[0])
    late = Adder(send_e.shape[0], send_l, got_l, part_l, tot_ref, sems.at[1])

    @pl.when(step == 0)
    def _():
        enter_all()
        set_gains(ln_ref, ln_in, 0)
        for ref in (w_acc, b_acc, l_acc):
            ref[...] = jnp.zeros_like(ref)
        block_part(OUT_BWD, (0, 1), (a_in, b_in, dx_in), jobs, ALL - 1)
        early.fill(post0, post1, pre1)
        early.scatter()

    @pl.when(step > 0)
    def _():
        t = step - 1
        block_arrive(t, (0, 1), jobs)

        @rows_loop
        def _(r):
            dzn = pre_back_row(unit_ref[r], inv_ref[0, pl.ds(r, 1), :], keep_ref.at[r], both(la0, t, r), both(la1, t, r), dpg_ref[r],
                               ln_ref, w_ref, w_acc, b_acc, l_acc)
            dz_ref[r] = (dzm_ref[r].astype(F32) + dzn).T.astype(BF16)

        @pl.when(t == STEPS - 1)
        def _():
            put_pre(grad_ref, w_acc, b_acc, l_acc)
            late.fill(grad_ref)
            late.scatter()
            early.add()
            late.add()
            early.hand_on()
            late.hand_on()
            early.finish()
            late.finish()
            tot_out[...] = tot_ref[...]


def split_kernel(z_in, dz_in, tot_in, z_out, dz_out, *refs):
    grads, (tot, buf, sems, tot_sem) = refs[:6], refs[6:]
    pairs = [(k, t, *pair) for t in range(STEPS) for k, pair in enumerate(((z_in, z_out), (dz_in, dz_out)))]
    loads = [pltpu.make_async_copy(block_of(src, t), buf.at[k, t], sems.at[0, k, t]) for k, t, src, dst in pairs]
    stores = [pltpu.make_async_copy(buf.at[k, t], block_of(dst, t), sems.at[1, k, t]) for k, t, src, dst in pairs]
    load_tot = pltpu.make_async_copy(tot_in, tot, tot_sem)
    for copy in [load_tot, *loads]:
        copy.start()
    load_tot.wait()
    split_grads(tot, *grads)
    for load, store in zip(loads, stores):
        load.wait()
        store.start()
    for store in stores:
        store.wait()


def split_grads(tot, d_ln_in, d_w_proj, d_b_proj, d_ln_mid, d_w_out, d_b_out):
    at = 0
    for k in range(2):
        d_w_out[k] = tot[at:at + C, :]
        d_ln_mid[k] = tot[at + C:at + C + 2, :]
        d_b_out[k:k + 1, :] = tot[at + C + 2:at + C + 3, :]
        at += C + HAT
    for k, at in enumerate((ALL * EARLY_SHARE, at)):
        for j in range(5):
            d_w_proj[k, :, j * C:(j + 1) * C] = tot[at + j * C:at + (j + 1) * C, :].T
            d_b_proj[k:k + 1, j * C:(j + 1) * C] = tot[at + PROJ + j:at + PROJ + j + 1, :]
        d_ln_in[k] = tot[at + PROJ + 5:at + PROJ + 7, :]


def finish(z_new, dz_new, total):
    shapes = ((2, 2, C), (2, C, PROJ), (2, PROJ), (2, 2, C), (2, C, C), (2, C))
    grads = [jax.ShapeDtypeStruct(shape, F32) for shape in shapes]
    far, near = pl.BlockSpec(memory_space=pl.ANY), pl.BlockSpec(memory_space=pltpu.VMEM)
    dma = pltpu.SemaphoreType.DMA
    return pl.pallas_call(
        split_kernel,
        in_specs=[far] * 3,
        out_specs=[far] * 2 + [near] * len(grads),
        out_shape=[NATIVE] * 2 + grads,
        scratch_shapes=[pltpu.VMEM(TOT.shape, F32), pltpu.VMEM((2, STEPS, STEP, N, C), BF16), dma((2, 2, STEPS)), dma],
        compiler_params=pltpu.CompilerParams(vmem_limit_bytes=VMEM_LIMIT),
        name="split",
    )(z_new, dz_new, total)


TRI = jax.ShapeDtypeStruct((CH, N, N), BF16)
BTRI = jax.ShapeDtypeStruct((BCH, BLOCK, N), BF16)
BDX = jax.ShapeDtypeStruct((BCH, BLOCK, BLOCK), BF16)
SENT = (TRI, BTRI, BDX)
ROW = jax.ShapeDtypeStruct((ROWS, C, N), BF16)
ROW32 = jax.ShapeDtypeStruct((ROWS, C, N), F32)
NATIVE = jax.ShapeDtypeStruct((ROWS, N, C), BF16)
POST = jax.ShapeDtypeStruct((C + HAT, C), F32)
PRE = jax.ShapeDtypeStruct((PROJ + HAT, C), F32)
TOT = jax.ShapeDtypeStruct((ALL * (EARLY_SHARE + LATE_SHARE), C), F32)
KEEP = jax.ShapeDtypeStruct((ROWS, 4, C, N), F32)
INV = jax.ShapeDtypeStruct((STEPS, STEP, N), F32)


def whole(array):
    zeros = (0,) * len(array.shape)
    return pl.BlockSpec(array.shape, lambda t: zeros, pipeline_mode=pl.Buffered(1))


def row_call(kernel, name, collective_id, tris, ins, consts, outs, n_back, scratch, width=0):
    n_send = sum(out in SENT for out in outs)
    packed = (STEPS, 2, C, STEP, BLOCK) if BDX in outs else (STEPS, C, STEP, N)
    dma = pltpu.SemaphoreType.DMA
    sent = [pltpu.VMEM((2 * C * STEP, C), F32)] * n_send + [pltpu.VMEM(packed, BF16)] * n_send
    sems = [dma((STEPS, GROUP))] * n_send + ([dma((n_send,))] if n_send else [])
    back = [pltpu.VMEM((4 * N * 8, C), F32)] * n_back + [pltpu.VMEM((STEPS, GROUP, STEP, CH, N), BF16)] * n_back
    back += [pltpu.VMEM((STEPS, STEP, C, N), BF16)] * n_back
    if width:
        back = [pltpu.VMEM((BCH * BLOCK * width // C if k == 0 else 8, C), F32) for k in range(n_back)]
        back += [pltpu.VMEM((STEPS, 4, STEP, BCH, width), BF16)] * n_back + [pltpu.VMEM((STEPS, 2, STEP, C, width), BF16)] * n_back
    back += [dma((STEPS, GROUP))] * (2 * n_back)
    far = pl.BlockSpec(memory_space=pl.ANY)
    rows_out = [out for out in outs if is_rows(out)]
    near = [pltpu.VMEM(x.shape, x.dtype) for x in tris]
    near += [pltpu.VMEM((2, x.shape[0] // STEPS) + x.shape[1:], x.dtype) for x in [*ins, *rows_out]]
    near += [dma((max(len(tris), 1), GROUPS)), dma((2, len(ins))), dma((2, len(rows_out)))]
    return pl.pallas_call(
        functools.partial(staged_kernel, kernel, len(tris), len(ins), len(consts), outs),
        grid=(STEPS + 1,),
        in_specs=[far] * (len(tris) + len(ins)) + [whole(x) for x in consts],
        out_specs=[pl.BlockSpec(out.shape, lambda t: (0, 0)) if out in (PRE, POST, TOT) else far for out in outs],
        out_shape=outs,
        scratch_shapes=sent + scratch + sems + back + near,
        compiler_params=pltpu.CompilerParams(dimension_semantics=("arbitrary",), vmem_limit_bytes=VMEM_LIMIT, collective_id=collective_id, has_side_effects=True),
        name=name,
    )(*tris, *ins, *consts)


def local_step(z_pair, pair_mask, dz_out, ln_in, w_proj, b_proj, ln_mid, w_out, b_out):
    z, dz = z_pair[0], dz_out[0]
    mask = pair_mask.reshape(STEPS, STEP, N)
    pre, post = [ln_in, w_proj, b_proj], [ln_mid, w_out, b_out]
    eye = [pltpu.VMEM((C, C), BF16)]
    pre_c = [pltpu.VMEM((2, C, N), F32), pltpu.VMEM((PROJ, C), BF16), pltpu.VMEM((PROJ, N), F32)]
    post_c = [pltpu.VMEM((2, C, N), F32), pltpu.VMEM((C, C), BF16), pltpu.VMEM((C, N), F32)]
    post_acc = [pltpu.VMEM((4, C, C), F32)]
    pre_acc = [pltpu.VMEM((PROJ, C), F32), pltpu.VMEM((PROJ, C), F32), pltpu.VMEM((2, C, C), F32)]

    gains = [pltpu.VMEM((2, C, N), F32)]
    kept = [TRI, TRI, ROW32, KEEP, ROW32, INV]
    a0, b0, g0, keep0, unit0, inv0 = row_call(pre_kernel, "pre0", 0, [], [z, mask], pre, [BTRI, BTRI] + kept[2:], 0, eye + pre_c)
    a1, b1, g1, keep1, unit1, inv1, zm, gu0, munit0, minv0 = row_call(
        mid_kernel, "mid", 1, [a0, b0], [z, g0, mask], post + pre, kept + [ROW, ROW32, ROW32, INV], 1, eye + pre_c + post_c, BLOCK)
    dx1, z_new, dpg1, post_g1 = row_call(
        turn_kernel, "turn", 2, [a1, b1], [zm, g1, dz], post, [TRI, NATIVE, ROW32, POST], 1, eye + post_c + post_acc)
    dx0, dzm, dpg0, pre_g1, post_g0 = row_call(
        back_kernel, "back", 3, [a1, b1, dx1], [dpg1, keep1, unit1, inv1, dz, munit0, minv0, g0, gu0], [ln_in, w_proj, ln_mid, w_out],
        [BDX, ROW, ROW32, PRE, POST], 2, eye + gains * 2 + pre_acc + post_acc)
    adders = [pltpu.VMEM(PRE.shape, F32)]
    for size in (EARLY_SHARE, LATE_SHARE):
        adders += [pltpu.VMEM((ALL * size, C), BF16), pltpu.VMEM((ALL, size, C), BF16), pltpu.VMEM((size, C), F32)]
    adders += [pltpu.VMEM(TOT.shape, F32), pltpu.SemaphoreType.DMA((2, 6, ALL))]
    dz_new, total = row_call(
        last_kernel, "last", 4, [a0, b0, dx0], [dpg0, keep0, unit0, inv0, dzm], [ln_in, w_proj, post_g0, post_g1, pre_g1],
        [NATIVE, TOT], 2, gains + pre_acc + adders, N)
    z_out, dz_pair, *grads = finish(z_new, dz_new, total)
    return z_out[None], dz_pair[None], *grads


def solution(mesh):
    row_spec = P("dp", "dap")
    return jax.shard_map(local_step, mesh=mesh, in_specs=(row_spec,) * 3 + (P(),) * 6,
                         out_specs=(row_spec,) * 2 + (P(),) * 6, check_vma=False)
```

```python
import functools

import jax
import jax.numpy as jnp
from jax import lax
from jax.experimental import pallas as pl
from jax.experimental.pallas import tpu as pltpu
from jax.sharding import PartitionSpec as P

LN_EPS = 1e-5
N = 256
C = 128
GROUP = 8
ROWS = N // GROUP
CH = C // GROUP
STEP = 8
UNROLL = 4
STEPS = ROWS // STEP
PROJ = 5 * C
HAT = 16
F32 = jnp.float32
BF16 = jnp.bfloat16
VMEM_LIMIT = 62 * 1024 * 1024


def dot(lhs, rhs, lhs_dim, rhs_dim):
    return lax.dot_general(lhs, rhs, (((lhs_dim,), (rhs_dim,)), ((), ())), preferred_element_type=F32)


nn = functools.partial(dot, lhs_dim=1, rhs_dim=0)
nt = functools.partial(dot, lhs_dim=1, rhs_dim=1)
tn = functools.partial(dot, lhs_dim=0, rhs_dim=0)


def step_now():
    return pl.program_id(0)


def mean(values):
    return jnp.mean(values, axis=0, keepdims=True)


def norm(values):
    cen = values - mean(values)
    inv = lax.rsqrt(mean(cen * cen) + LN_EPS)
    return cen * inv, inv


def norm_back(d_hat, unit, inv, gain):
    d_unit = d_hat * gain
    mean_d = mean(d_unit)
    mean_du = mean(d_unit * unit)
    return inv * (d_unit - mean_d - unit * mean_du)


def fold(values):
    return values[:, :C] + values[:, C:]


def row_sums(acc):
    return jnp.sum(acc.T, axis=0, keepdims=True)


def sigmoid(values):
    return 0.5 * jnp.tanh(0.5 * values) + 0.5


def project(z_t, ln, w_t, bias):
    unit, inv = norm(z_t)
    z_hat = (unit * ln[0] + ln[1]).astype(BF16)
    return unit, inv, z_hat, nn(w_t[...], z_hat) + bias[...]


def set_eye(eye):
    same = lax.broadcasted_iota(jnp.int32, (C, C), 0) == lax.broadcasted_iota(jnp.int32, (C, C), 1)
    eye[...] = jnp.where(same, 1.0, 0.0).astype(BF16)


def set_column(ref, row):
    column = jnp.broadcast_to(row.astype(F32), (C, C)).T
    ref[:, :C] = column
    ref[:, C:] = column


def set_pre(block, ln_in, w_proj, b_proj, ln, w_t, bias):
    for k in range(2):
        set_column(ln.at[k], ln_in[block, k:k + 1, :])
    for k in range(5):
        cols = slice(k * C, (k + 1) * C)
        set_column(bias.at[cols], b_proj[block:block + 1, cols])
        w_t[cols, :] = w_proj[block, :, cols].astype(F32).T.astype(BF16)


def set_post(block, ln_mid, w_out, b_out, mln, wo_t, bo):
    for k in range(2):
        set_column(mln.at[k], ln_mid[block, k:k + 1, :])
    set_column(bo, b_out[block:block + 1, :])
    wo_t[...] = w_out[block].astype(F32).T.astype(BF16)


def place():
    me = lax.axis_index("dap")
    return me, me // 4, (me // 2) % 2, me % 2


def enter():
    me = lax.axis_index("dap")
    sem = pltpu.get_barrier_semaphore()
    for k in range(1, GROUP):
        pl.semaphore_signal(sem, inc=1, device_id={"dap": (me + k) % GROUP}, device_id_type=pl.DeviceIdType.MESH)


def all_in(others=GROUP - 1):
    pl.semaphore_wait(pltpu.get_barrier_semaphore(), others)


def peers():
    me, cy, cx, core = place()
    out = []
    for dy, dx in ((1, 1), (1, 0), (0, 1), (0, 0)):
        for dc in (1, 0):
            out.append((((cy + dy) % 2) * 2 + (cx + dx) % 2) * 2 + (core + dc) % 2)
    return me, out


def spread(ref, value, row):
    for h in range(2):
        ref[pl.ds(h * C * STEP + row, C, stride=STEP), :] = value[:, h * C:(h + 1) * C]


def pack_rows(stage, send_ref, slot):
    for h in range(2):
        for q in range(4):
            rows = stage[pl.ds((h * C + q * 32) * STEP, 32 * STEP), :].reshape(32, STEP, C)
            send_ref[slot, q * 32:(q + 1) * 32, :, h * C:(h + 1) * C] = rows.astype(BF16)


def move(src_ref, dst_ref, send_sem, recv_sem, dest, own):
    if own:
        return pltpu.make_async_copy(src_ref, dst_ref, recv_sem)
    return pltpu.make_async_remote_copy(src_ref, dst_ref, send_sem, recv_sem, device_id={"dap": dest}, device_id_type=pl.DeviceIdType.MESH)


def wait_sends(copies):
    for copy in copies:
        if copy.is_remote:
            copy.wait_send()


def row_copies(send_ref, out_ref, send_sem, recv_sem, slot):
    me, dests = peers()
    start = pl.multiple_of(me * ROWS + slot * STEP, STEP)
    return [
        move(send_ref.at[slot, pl.ds(pl.multiple_of(dest * CH, CH), CH)], out_ref.at[:, pl.ds(start, STEP), :],
             send_sem.at[slot, k], recv_sem, dest, k == GROUP - 1)
        for k, dest in enumerate(dests)
    ]


BCH = C // 2
BLOCK = N // 2


def by_column(kind, core):
    return core if kind else 1 - core


def pick(column, on_column, on_row):
    return column * on_column + (1 - column) * on_row


def channels(core):
    return pl.ds(pl.multiple_of(core * BCH, BCH), BCH)


def swap(lo, hi):
    first = lax.broadcasted_iota(jnp.int32, lo.shape, 1) < BLOCK // 2
    return jnp.where(first, lo, pltpu.roll(hi, BLOCK // 2, 1)), jnp.where(first, pltpu.roll(lo, BLOCK // 2, 1), hi)


def swap_core1(value):
    lo, hi = swap(value[BCH:, :BLOCK], value[BCH:, BLOCK:])
    return jnp.concatenate([value[:BCH], jnp.concatenate([lo, hi], axis=1)], axis=0)


def block_copies(kind, halves, send_ref, out_ref, send_sem, recv_sem, slot):
    me, cy, cx, core = place()
    out = []
    for k, (to, far) in enumerate(((0, 1), (1, 1), (1 - core, 0), (core, 0))):
        column = by_column(kind, to)
        y, x = cy, cx
        if far:
            y, x = (1 - cy, cx) if column else (cy, 1 - cx)
        start = pick(column, cy, cx) * 2 * ROWS + core * ROWS + slot * STEP
        src = send_ref.at[slot, pick(column, y, x), channels(to)] if halves else send_ref.at[slot, channels(to)]
        out.append(move(src, out_ref.at[:, pl.ds(pl.multiple_of(start, STEP), STEP), :], send_sem.at[slot, k], recv_sem, (y * 2 + x) * 2 + to, k == 3))
    return out


def pack_halves(stage, send_ref, slot):
    for h in range(2):
        for q in range(4):
            rows = stage[pl.ds((h * C + q * 32) * STEP, 32 * STEP), :].reshape(32, STEP, C)
            send_ref[slot, h, q * 32:(q + 1) * 32] = rows.astype(BF16)


A_ROWS = (pack_rows, functools.partial(block_copies, 0, False))
B_ROWS = (pack_rows, functools.partial(block_copies, 1, False))
ROWS_ALL = (pack_rows, row_copies)
DX_ROWS = (pack_halves, functools.partial(block_copies, 0, True))


def send_rows(step, jobs):
    for (pack, copies), stage, send_ref, out_ref, send_sem, recv_sems, k in jobs:
        pack(stage, send_ref, step)
        for copy in copies(send_ref, out_ref, send_sem, recv_sems.at[k], step):
            copy.start()
    PENDING.extend(jobs)


PENDING = []


def finish_rows(jobs):
    for (pack, copies), stage, send_ref, out_ref, send_sem, recv_sems, k in jobs:
        for slot in range(STEPS):
            wait_sends(copies(send_ref, out_ref, send_sem, recv_sems.at[k], slot))
        pltpu.make_async_copy(out_ref, out_ref, recv_sems.at[k]).wait()


OUT_FWD = (lambda c, a, b: nt(a[c], b[c]),)
IN_FWD = (lambda c, a, b: tn(a[c], b[c]),)
IN_BWD = (lambda c, a, b, dx: nt(b[c], dx[c]), lambda c, a, b, dx: nn(a[c], dx[c]))
OUT_BWD = (lambda c, a, b, dx: nn(dx[c], b[c]), lambda c, a, b, dx: tn(dx[c], a[c]))


def back_copy(job, t, k, dest, frm):
    stage, send_ref, land_ref, send_sem, recv_sem = job
    return pltpu.make_async_remote_copy(
        send_ref.at[t, dest], land_ref.at[t, :, pl.ds(pl.multiple_of(frm * CH, CH), CH), :], send_sem.at[t, k], recv_sem.at[t, frm],
        device_id={"dap": dest}, device_id_type=pl.DeviceIdType.MESH)


EARLY = 1
GROUPS = 4


class Piecewise:
    def __init__(self, source, ref, sems):
        self.source, self.ref, self.sems = source, ref, sems

    def load(self, g):
        size = self.ref.shape[0] // GROUPS
        part = pl.ds(g * size, size)
        return pltpu.make_async_copy(self.source.at[part], self.ref.at[part], self.sems.at[g])


def channel_part(products, ins, jobs):
    me, dests = peers()
    refs = [x.ref for x in ins]
    for j, (product, job) in enumerate(zip(products, jobs)):
        stage, send_ref, land_ref = job[:3]

        def body(c, carry):
            value = product(c, *refs)
            for h in range(2):
                stage[pl.ds((h * 2 + c // 8) * N * 8 + c % 8, N, stride=8), :] = value[:, h * C:(h + 1) * C]
            return carry

        for g in range(GROUPS):
            if j == 0:
                for x in ins:
                    x.load(g).wait()
            lax.fori_loop(g * (CH // GROUPS), (g + 1) * (CH // GROUPS), body, 0, unroll=True)
        if j == 0:
            all_in()
        for t in range(STEPS):
            for dest in range(GROUP):
                for h in range(2):
                    at = h * 2 * N * 8 + (dest * ROWS + t * STEP) * 8
                    lo = stage[pl.ds(at, 64), :].reshape(STEP, 8, C)
                    hi = stage[pl.ds(at + N * 8, 64), :].reshape(STEP, 8, C)
                    send_ref[t, dest, :, :, h * C:(h + 1) * C] = jnp.concatenate([lo, hi], axis=1).astype(BF16)
            for k, dest in enumerate(dests[:-1]):
                back_copy(job, t, k, dest, me).start()
            land_ref[t, :, pl.ds(pl.multiple_of(me * CH, CH), CH), :] = send_ref[t, me]


def block_sends(kind, job, t, piece=None):
    stage, send_ref, land_ref, send_sem, recv_sem = job
    me, cy, cx, core = place()
    column = by_column(kind, core)
    mine = pick(column, cy, cx)
    y, x = cy + column * (1 - 2 * cy), cx + (1 - column) * (1 - 2 * cx)
    size = BCH if piece is None else BCH // GROUPS
    at = (piece or 0) * size
    land = land_ref.at[t, mine, :, pl.ds(pl.multiple_of(core * BCH + at, size), size), :]
    out = []
    for k, (dest, member, slot) in enumerate((((y * 2 + x) * 2, pick(column, y, x) * 2, core), ((y * 2 + x) * 2 + 1, pick(column, y, x) * 2 + 1, core),
                                              (me + 1 - 2 * core, mine * 2 + 1 - core, 2))):
        out.append(pltpu.make_async_remote_copy(send_ref.at[t, member, :, pl.ds(at, size), :], land, send_sem.at[t, k], recv_sem.at[t, slot],
                                                device_id={"dap": dest}, device_id_type=pl.DeviceIdType.MESH))
    return out


def block_receives(kind, job, t):
    stage, send_ref, land_ref, send_sem, recv_sem = job
    me, cy, cx, core = place()
    out = []
    for slot, (frm, far) in enumerate(((0, 1), (1, 1), (1 - core, 0))):
        column = by_column(kind, frm)
        y, x = cy, cx
        if far:
            y, x = (1 - cy, cx) if column else (cy, 1 - cx)
        out.append(pltpu.make_async_remote_copy(send_ref.at[t, 0], land_ref.at[t, pick(column, y, x), :, channels(frm), :], send_sem.at[t, slot],
                                                recv_sem.at[t, slot], device_id={"dap": (y * 2 + x) * 2 + frm}, device_id_type=pl.DeviceIdType.MESH))
    return out


def block_part(products, kinds, ins, jobs, others=GROUP - 1):
    me, cy, cx, core = place()
    refs = [x.ref for x in ins]
    for j, (product, kind, job) in enumerate(zip(products, kinds, jobs)):
        stage, send_ref, land_ref = job[:3]
        tiles = send_ref.shape[-1] // C

        def body(c, carry):
            value = product(c, *refs)
            for h in range(tiles):
                stage[pl.ds((h * (BCH // 8) + c // 8) * BLOCK * 8 + c % 8, BLOCK, stride=8), :] = value[:, h * C:(h + 1) * C]
            return carry

        mine = pick(by_column(kind, core), cy, cx)

        def pack(t, q):
            for member in range(4):
                for h in range(tiles):
                    at = (h * (BCH // 8) + q * 2) * BLOCK * 8 + (member * ROWS + t * STEP) * 8
                    lo = stage[pl.ds(at, 64), :].reshape(STEP, 8, C)
                    hi = stage[pl.ds(at + BLOCK * 8, 64), :].reshape(STEP, 8, C)
                    send_ref[t, member, :, q * CH:(q + 1) * CH, h * C:(h + 1) * C] = jnp.concatenate([lo, hi], axis=1).astype(BF16)

        def keep(t):
            land_ref[t, mine, :, channels(core), :] = send_ref[t, mine * 2 + core]

        for g in range(GROUPS):
            if j == 0:
                for x in ins:
                    x.load(g).wait()
            lax.fori_loop(g * CH, (g + 1) * CH, body, 0, unroll=4)
            if g == j == 0:
                all_in(others)
            for t in range(EARLY):
                pack(t, g)
                for copy in block_sends(kind, job, t, g):
                    copy.start()
        for t in range(EARLY, STEPS):
            for g in range(GROUPS):
                pack(t, g)
            for copy in block_sends(kind, job, t):
                copy.start()
        for t in range(STEPS):
            keep(t)


def block_arrive(t, kinds, jobs):
    for kind, job in zip(kinds, jobs):
        for copy in block_receives(kind, job, t):
            copy.wait_recv()

    @pl.when(t == STEPS - 1)
    def _():
        for kind, job in zip(kinds, jobs):
            for slot in range(STEPS):
                for copy in block_sends(kind, job, slot):
                    copy.wait_send()


def both(land_ref, t, r):
    return land_ref[t, 0, r].astype(F32) + land_ref[t, 1, r].astype(F32)


def staged_kernel(inner, n_tri, n_in, n_const, outs, *refs):
    n_far = n_tri + n_in
    far, consts, refs = refs[:n_far], refs[n_far:n_far + n_const], refs[n_far + n_const:]
    results, refs = list(refs[:len(outs)]), refs[len(outs):]
    tri_sem, row_sem, out_sem = refs[-3:]
    rows_out = [k for k, out in enumerate(outs) if is_rows(out)]
    n_near = n_far + len(rows_out)
    refs, near = refs[:-3 - n_near], refs[-3 - n_near:-3]
    step = step_now()
    slot = (step + 1) % 2
    tris = [Piecewise(far[k], near[k], tri_sem.at[k]) for k in range(n_tri)]
    targets = [results[k] for k in rows_out]
    for k, ref in zip(rows_out, near[n_far:]):
        results[k] = ref.at[slot]

    def fetch(t, slot):
        return [pltpu.make_async_copy(block_of(whole_ref, t), ref.at[slot], row_sem.at[slot, k])
                for k, (whole_ref, ref) in enumerate(zip(far[n_tri:], near[n_tri:n_far]))]

    def store(t, slot):
        return [pltpu.make_async_copy(ref.at[slot], block_of(whole_ref, t), out_sem.at[slot, k])
                for k, (whole_ref, ref) in enumerate(zip(targets, near[n_far:]))]

    @pl.when(step == 0)
    def _():
        for g in range(GROUPS):
            for x in tris:
                x.load(g).start()
        for copy in fetch(0, 0):
            copy.start()

    @pl.when(step > 0)
    def _():
        for copy in fetch(step - 1, slot):
            copy.wait()

    @pl.when((step > 0) & (step < STEPS))
    def _():
        for copy in fetch(step, 1 - slot):
            copy.start()

    @pl.when(step > 2)
    def _():
        for copy in store(step - 3, slot):
            copy.wait()

    PENDING.clear()
    inner(*tris, *[ref.at[slot] for ref in near[n_tri:n_far]], *consts, *results, *refs)
    jobs = list(PENDING)

    @pl.when(step > 0)
    def _():
        for copy in store(step - 1, slot):
            copy.start()

    @pl.when(step == STEPS)
    def _():
        finish_rows(jobs)
        for copy in store(step - 2, 1 - slot) + store(step - 1, slot):
            copy.wait()


def block_of(ref, t):
    size = ref.shape[0] // STEPS
    return ref.at[pl.ds(t * size, size)]


def is_rows(out):
    return out not in (PRE, POST, TOT, *SENT)


def arrive(t, jobs):
    me, dests = peers()
    for job in jobs:
        for k, frm in enumerate(dests[:-1]):
            back_copy(job, t, k, frm, frm).wait_recv()

    @pl.when(t == STEPS - 1)
    def _():
        for job in jobs:
            for slot in range(STEPS):
                for k, dest in enumerate(dests[:-1]):
                    back_copy(job, slot, k, dest, me).wait_send()


def rows_loop(body):
    def step(r, carry):
        body(r)
        return carry

    lax.fori_loop(0, STEP, step, 0, unroll=UNROLL)


def pre_row(r, z_t, mask_ref, ln_ref, w_t_ref, bias_ref, g_ref, keep_ref, unit_ref, inv_ref, a_stage, b_stage):
    unit, inv, _, p = project(z_t, ln_ref, w_t_ref, bias_ref)
    unit_ref[r] = unit
    inv_ref[0, pl.ds(r, 1), :] = inv
    m = mask_ref[0, pl.ds(r, 1), :].astype(F32)
    for side, stage in ((0, a_stage), (1, b_stage)):
        s = sigmoid(p[2 * side * C:(2 * side + 1) * C])
        v = p[(2 * side + 1) * C:(2 * side + 2) * C]
        sm = s * m
        spread(stage, sm * v, r)
        keep_ref[r, 2 * side] = sm
        keep_ref[r, 2 * side + 1] = v * (1.0 - s)
    g_ref[r] = sigmoid(p[4 * C:])


def pre_kernel(z_ref, mask_ref, ln_in, w_proj, b_proj, a_ref, b_ref, g_ref, keep_ref, unit_ref, inv_ref, a_st, b_st, a_send, b_send,
               eye_ref, ln_ref, w_t_ref, bias_ref, a_ss, b_ss, rs):
    step = step_now()

    @pl.when(step == 0)
    def _():
        enter()
        set_eye(eye_ref)
        set_pre(0, ln_in, w_proj, b_proj, ln_ref, w_t_ref, bias_ref)
        all_in()

    @pl.when(step > 0)
    def _():
        t = step - 1

        @rows_loop
        def _(r):
            z_t = nt(eye_ref[...], z_ref[r])
            pre_row(r, z_t, mask_ref, ln_ref, w_t_ref, bias_ref, g_ref, keep_ref, unit_ref, inv_ref, a_st, b_st)

        send_rows(t, [(A_ROWS, a_st, a_send, a_ref, a_ss, rs, 0), (B_ROWS, b_st, b_send, b_ref, b_ss, rs, 1)])


def mid_kernel(a_in, b_in, z_ref, g0_ref, mask_ref, ln_mid, w_out, b_out, ln_in, w_proj, b_proj,
               a_ref, b_ref, g_ref, keep_ref, unit_ref, inv_ref, zm_ref, gu_ref, munit_ref, minv_ref, a_st, b_st, a_send, b_send,
               eye_ref, ln_ref, w_t_ref, bias_ref, mln_ref, wo_t_ref, bo_ref, a_ss, b_ss, rs,
               st0, se0, la0, ss0, rv0):
    step = step_now()
    jobs = [(st0, se0, la0, ss0, rv0)]

    @pl.when(step == 0)
    def _():
        enter()
        set_eye(eye_ref)
        set_pre(1, ln_in, w_proj, b_proj, ln_ref, w_t_ref, bias_ref)
        set_post(0, ln_mid, w_out, b_out, mln_ref, wo_t_ref, bo_ref)
        block_part(OUT_FWD, (0,), (a_in, b_in), jobs)

    @pl.when(step > 0)
    def _():
        t = step - 1
        block_arrive(t, (0,), jobs)

        @rows_loop
        def _(r):
            unit, inv = norm(swap_core1(jnp.concatenate([la0[t, 0, r], la0[t, 1, r]], axis=1).astype(F32)))
            munit_ref[r] = unit
            minv_ref[0, pl.ds(r, 1), :] = inv
            x_hat = (unit * mln_ref[0] + mln_ref[1]).astype(BF16)
            update = nn(wo_t_ref[...], x_hat) + bo_ref[...]
            g = g0_ref[r]
            change = g * update
            gu_ref[r] = change * (1.0 - g)
            z_new = (nt(eye_ref[...], z_ref[r]) + change).astype(BF16)
            zm_ref[r] = z_new
            pre_row(r, z_new.astype(F32), mask_ref, ln_ref, w_t_ref, bias_ref, g_ref, keep_ref, unit_ref, inv_ref, a_st, b_st)

        send_rows(t, [(ROWS_ALL, a_st, a_send, a_ref, a_ss, rs, 0), (ROWS_ALL, b_st, b_send, b_ref, b_ss, rs, 1)])


def post_back_row(unit, inv, g, dz, mln_ref, wo_ref, acc_ref, x_hat=None):
    if x_hat is None:
        x_hat = (unit * mln_ref[0] + mln_ref[1]).astype(BF16)
    d_up = dz * g
    d_up_bf = d_up.astype(BF16)
    acc_ref[0] += nt(x_hat, d_up_bf)
    acc_ref[3] += fold(d_up)
    d_hat = nn(wo_ref[...], d_up_bf).astype(BF16).astype(F32)
    acc_ref[1] += fold(d_hat * unit)
    acc_ref[2] += fold(d_hat)
    return norm_back(d_hat, unit, inv, mln_ref[0])


def put_post(grad_ref, acc_ref):
    grad_ref[0:C, :] = acc_ref[0]
    grad_ref[C:C + 8, :] = jnp.concatenate([row_sums(acc_ref[1]), row_sums(acc_ref[2]), row_sums(acc_ref[3]), jnp.zeros((5, C), F32)], axis=0)
    grad_ref[C + 8:C + HAT, :] = jnp.zeros((8, C), F32)


def turn_kernel(a_in, b_in, zm_ref, g_ref, dz_ref, ln_mid, w_out, b_out,
                dx_ref, z_out_ref, dpg_ref, grad_ref, d_st, d_send, eye_ref, mln_ref, wo_t_ref, bo_ref, acc_ref, d_ss, rs,
               st0, se0, la0, ss0, rv0):
    step = step_now()
    jobs = [(st0, se0, la0, ss0, rv0)]
    wo_ref = w_out.at[1]

    @pl.when(step == 0)
    def _():
        enter()
        set_eye(eye_ref)
        set_post(1, ln_mid, w_out, b_out, mln_ref, wo_t_ref, bo_ref)
        acc_ref[...] = jnp.zeros_like(acc_ref)
        channel_part(IN_FWD, (a_in, b_in), jobs)

    @pl.when(step > 0)
    def _():
        t = step - 1
        arrive(t, jobs)
        x_ref = la0.at[t]

        @rows_loop
        def _(r):
            dz = nt(eye_ref[...], dz_ref[r])
            g = g_ref[r]
            unit, inv = norm(x_ref[r].astype(F32))
            x_hat = (unit * mln_ref[0] + mln_ref[1]).astype(BF16)
            change = g * (nn(wo_t_ref[...], x_hat) + bo_ref[...])
            dpg_ref[r] = dz * change * (1.0 - g)
            z_out_ref[r] = (zm_ref[r].astype(F32) + change).T.astype(BF16)
            spread(d_st, post_back_row(unit, inv, g, dz, mln_ref, wo_ref, acc_ref, x_hat), r)

        @pl.when(t == STEPS - 1)
        def _():
            put_post(grad_ref, acc_ref)

        send_rows(t, [(ROWS_ALL, d_st, d_send, dx_ref, d_ss, rs, 0)])


def pre_back_row(unit, inv, keep, da, db, d_pg, ln_ref, w_ref, w_acc, b_acc, l_acc):
    z_hat = (unit * ln_ref[0] + ln_ref[1]).astype(BF16)
    parts = []
    for side, d_side in ((0, da), (1, db)):
        d_v = d_side * keep[2 * side]
        parts += [d_v * keep[2 * side + 1], d_v]
    parts.append(d_pg)
    for k, part in enumerate(parts):
        b_acc[k * C:(k + 1) * C, :] += fold(part)
    d_p = jnp.concatenate([part.astype(BF16) for part in parts], axis=0)
    w_acc[...] += nt(d_p, z_hat)
    d_hat = nn(w_ref[...], d_p).astype(BF16).astype(F32)
    l_acc[0] += fold(d_hat * unit)
    l_acc[1] += fold(d_hat)
    return norm_back(d_hat, unit, inv, ln_ref[0])


def put_pre(grad_ref, w_acc, b_acc, l_acc):
    grad_ref[0:PROJ, :] = w_acc[...]
    rows = [row_sums(b_acc[k * C:(k + 1) * C, :]) for k in range(5)]
    rows += [row_sums(l_acc[0]), row_sums(l_acc[1]), jnp.zeros((1, C), F32)]
    grad_ref[PROJ:PROJ + 8, :] = jnp.concatenate(rows, axis=0)
    grad_ref[PROJ + 8:PROJ + HAT, :] = jnp.zeros((8, C), F32)


def set_gains(ref, ln, block):
    for k in range(2):
        set_column(ref.at[k], ln[block, k:k + 1, :])


def back_kernel(a_in, b_in, dx_in, dpg1_ref, keep_ref, unit_ref, inv_ref, dz_ref, munit_ref, minv_ref, g_ref, gu_ref, ln_in, w_proj, ln_mid, w_out,
                dx_ref, dzm_ref, dpg_ref, grad1_ref, grad0_ref, d_st, d_send,
                eye_ref, ln_ref, mln_ref, w_acc, b_acc, l_acc, acc_ref, d_ss, rs,
               st0, st1, se0, se1, la0, la1, ss0, ss1, rv0, rv1):
    step = step_now()
    jobs = [(st0, se0, la0, ss0, rv0), (st1, se1, la1, ss1, rv1)]
    w_ref, wo_ref = w_proj.at[1], w_out.at[0]

    @pl.when(step == 0)
    def _():
        enter()
        set_eye(eye_ref)
        set_gains(ln_ref, ln_in, 1)
        set_gains(mln_ref, ln_mid, 0)
        for ref in (w_acc, b_acc, l_acc, acc_ref):
            ref[...] = jnp.zeros_like(ref)
        channel_part(IN_BWD, (a_in, b_in, dx_in), jobs)

    @pl.when(step > 0)
    def _():
        t = step - 1
        arrive(t, jobs)
        da_ref, db_ref = la0.at[t], la1.at[t]

        @rows_loop
        def _(r):
            at = pl.ds(r, 1)
            dzn = pre_back_row(unit_ref[r], inv_ref[0, at, :], keep_ref.at[r], da_ref[r].astype(F32), db_ref[r].astype(F32), dpg1_ref[r],
                               ln_ref, w_ref, w_acc, b_acc, l_acc)
            dzm = (nt(eye_ref[...], dz_ref[r]) + dzn).astype(BF16)
            dzm_ref[r] = dzm
            dzm = dzm.astype(F32)
            dpg_ref[r] = dzm * gu_ref[r]
            spread(d_st, swap_core1(post_back_row(munit_ref[r], minv_ref[0, at, :], g_ref[r], dzm, mln_ref, wo_ref, acc_ref)), r)

        @pl.when(t == STEPS - 1)
        def _():
            put_pre(grad1_ref, w_acc, b_acc, l_acc)
            put_post(grad0_ref, acc_ref)

        send_rows(t, [(DX_ROWS, d_st, d_send, dx_ref, d_ss, rs, 0)])


ALL = 16
EARLY_SHARE, LATE_SHARE = 64, 48


def device(o):
    return {"dp": o // GROUP, "dap": o % GROUP}


def everyone():
    dap = lax.axis_index("dap")
    me = lax.axis_index("dp") * GROUP + dap
    twin = me + 1 - dap % 2 * 2
    return me, twin, [(me + k) % ALL for k in range(1, ALL)], [(me + 2 * k) % ALL for k in range(1, GROUP)]


def enter_all():
    for to in everyone()[2]:
        pl.semaphore_signal(pltpu.get_barrier_semaphore(), inc=1, device_id=device(to), device_id_type=pl.DeviceIdType.MESH)


class Adder:
    def __init__(self, base, send_ref, got_ref, part_ref, tot_ref, sems):
        self.base, self.send_ref, self.got_ref, self.part_ref, self.tot_ref, self.sems = base, send_ref, got_ref, part_ref, tot_ref, sems
        self.size = part_ref.shape[0]

    def share(self, k, base=0):
        return pl.ds(pl.multiple_of(base + k * self.size, HAT), self.size)

    def sums(self, k):
        return self.tot_ref.at[self.share(k, self.base)]

    def remote(self, src, dst, phase, k, slot, to):
        return pltpu.make_async_remote_copy(src, dst, self.sems.at[2 * phase, k], self.sems.at[2 * phase + 1, slot], device_id=device(to),
                                            device_id_type=pl.DeviceIdType.MESH)

    def first(self, k, frm):
        other = everyone()[2][k]
        return self.remote(self.send_ref.at[self.share(other)], self.got_ref.at[frm], 0, k, frm, other)

    def second(self, k, frm):
        return self.remote(self.part_ref, self.sums(frm), 1, k, frm, everyone()[3][k])

    def third(self, k, block):
        return self.remote(self.sums(block), self.sums(block), 2, k, k, everyone()[1])

    def own(self, block):
        return self.remote(self.part_ref, self.sums(block), 2, GROUP, GROUP, everyone()[1])

    def before(self, device_number, k):
        return (device_number + ALL - 2 * (k + 1)) % ALL

    def fill(self, *packs):
        at = 0
        for ref in packs:
            self.send_ref[at:at + ref.shape[0], :] = ref[...].astype(BF16)
            at += ref.shape[0]
        self.send_ref[at:, :] = jnp.zeros((self.send_ref.shape[0] - at, C), BF16)

    def scatter(self):
        me = everyone()[0]
        for k in range(ALL - 1):
            self.first(k, me).start()
        self.got_ref[me] = self.send_ref[self.share(me), :]

    def add(self):
        me, twin, others, chips = everyone()
        for k in range(ALL - 1):
            self.first(k, others[k]).wait_recv()
        total = self.got_ref[0].astype(F32)
        for k in range(1, ALL):
            total = total + self.got_ref[k].astype(F32)
        self.part_ref[...] = total
        for k in range(GROUP - 1):
            self.second(k, me).start()
        self.own(me).start()
        self.tot_ref[self.share(me, self.base), :] = total

    def hand_on(self):
        me = everyone()[0]
        for k in range(GROUP - 1):
            self.second(k, self.before(me, k)).wait_recv()
            self.third(k, self.before(me, k)).start()

    def finish(self):
        me, twin, others, chips = everyone()
        for k in range(GROUP - 1):
            self.third(k, self.before(twin, k)).wait_recv()
        self.own(twin).wait_recv()
        self.own(me).wait_send()
        for k in range(ALL - 1):
            self.first(k, me).wait_send()
        for k in range(GROUP - 1):
            self.second(k, me).wait_send()
            self.third(k, self.before(me, k)).wait_send()


def last_kernel(a_in, b_in, dx_in, dpg_ref, keep_ref, unit_ref, inv_ref, dzm_ref, ln_in, w_proj, post0, post1, pre1,
                dz_ref, tot_out, ln_ref, w_acc, b_acc, l_acc, grad_ref, send_e, got_e, part_e, send_l, got_l, part_l, tot_ref, sems,
                st0, st1, se0, se1, la0, la1, ss0, ss1, rv0, rv1):
    step = step_now()
    jobs = [(st0, se0, la0, ss0, rv0), (st0, se1, la1, ss1, rv1)]
    w_ref = w_proj.at[0]
    early = Adder(0, send_e, got_e, part_e, tot_ref, sems.at[0])
    late = Adder(send_e.shape[0], send_l, got_l, part_l, tot_ref, sems.at[1])

    @pl.when(step == 0)
    def _():
        enter_all()
        set_gains(ln_ref, ln_in, 0)
        for ref in (w_acc, b_acc, l_acc):
            ref[...] = jnp.zeros_like(ref)
        block_part(OUT_BWD, (0, 1), (a_in, b_in, dx_in), jobs, ALL - 1)
        early.fill(post0, post1, pre1)
        early.scatter()

    @pl.when(step > 0)
    def _():
        t = step - 1
        block_arrive(t, (0, 1), jobs)

        @rows_loop
        def _(r):
            dzn = pre_back_row(unit_ref[r], inv_ref[0, pl.ds(r, 1), :], keep_ref.at[r], both(la0, t, r), both(la1, t, r), dpg_ref[r],
                               ln_ref, w_ref, w_acc, b_acc, l_acc)
            dz_ref[r] = (dzm_ref[r].astype(F32) + dzn).T.astype(BF16)

        @pl.when(t == STEPS - 1)
        def _():
            put_pre(grad_ref, w_acc, b_acc, l_acc)
            late.fill(grad_ref)
            late.scatter()
            early.add()
            late.add()
            early.hand_on()
            late.hand_on()
            early.finish()
            late.finish()
            tot_out[...] = tot_ref[...]


def split_kernel(z_in, dz_in, tot_in, z_out, dz_out, *refs):
    grads, (tot, buf, sems, tot_sem) = refs[:6], refs[6:]
    pairs = [(k, t, *pair) for t in range(STEPS) for k, pair in enumerate(((z_in, z_out), (dz_in, dz_out)))]
    loads = [pltpu.make_async_copy(block_of(src, t), buf.at[k, t], sems.at[0, k, t]) for k, t, src, dst in pairs]
    stores = [pltpu.make_async_copy(buf.at[k, t], block_of(dst, t), sems.at[1, k, t]) for k, t, src, dst in pairs]
    load_tot = pltpu.make_async_copy(tot_in, tot, tot_sem)
    for copy in [load_tot, *loads]:
        copy.start()
    load_tot.wait()
    split_grads(tot, *grads)
    for load, store in zip(loads, stores):
        load.wait()
        store.start()
    for store in stores:
        store.wait()


def split_grads(tot, d_ln_in, d_w_proj, d_b_proj, d_ln_mid, d_w_out, d_b_out):
    at = 0
    for k in range(2):
        d_w_out[k] = tot[at:at + C, :]
        d_ln_mid[k] = tot[at + C:at + C + 2, :]
        d_b_out[k:k + 1, :] = tot[at + C + 2:at + C + 3, :]
        at += C + HAT
    for k, at in enumerate((ALL * EARLY_SHARE, at)):
        for j in range(5):
            d_w_proj[k, :, j * C:(j + 1) * C] = tot[at + j * C:at + (j + 1) * C, :].T
            d_b_proj[k:k + 1, j * C:(j + 1) * C] = tot[at + PROJ + j:at + PROJ + j + 1, :]
        d_ln_in[k] = tot[at + PROJ + 5:at + PROJ + 7, :]


def finish(z_new, dz_new, total):
    shapes = ((2, 2, C), (2, C, PROJ), (2, PROJ), (2, 2, C), (2, C, C), (2, C))
    grads = [jax.ShapeDtypeStruct(shape, F32) for shape in shapes]
    far, near = pl.BlockSpec(memory_space=pl.ANY), pl.BlockSpec(memory_space=pltpu.VMEM)
    dma = pltpu.SemaphoreType.DMA
    return pl.pallas_call(
        split_kernel,
        in_specs=[far] * 3,
        out_specs=[far] * 2 + [near] * len(grads),
        out_shape=[NATIVE] * 2 + grads,
        scratch_shapes=[pltpu.VMEM(TOT.shape, F32), pltpu.VMEM((2, STEPS, STEP, N, C), BF16), dma((2, 2, STEPS)), dma],
        compiler_params=pltpu.CompilerParams(vmem_limit_bytes=VMEM_LIMIT),
        name="split",
    )(z_new, dz_new, total)


TRI = jax.ShapeDtypeStruct((CH, N, N), BF16)
BTRI = jax.ShapeDtypeStruct((BCH, BLOCK, N), BF16)
BDX = jax.ShapeDtypeStruct((BCH, BLOCK, BLOCK), BF16)
SENT = (TRI, BTRI, BDX)
ROW = jax.ShapeDtypeStruct((ROWS, C, N), BF16)
ROW32 = jax.ShapeDtypeStruct((ROWS, C, N), F32)
NATIVE = jax.ShapeDtypeStruct((ROWS, N, C), BF16)
POST = jax.ShapeDtypeStruct((C + HAT, C), F32)
PRE = jax.ShapeDtypeStruct((PROJ + HAT, C), F32)
TOT = jax.ShapeDtypeStruct((ALL * (EARLY_SHARE + LATE_SHARE), C), F32)
KEEP = jax.ShapeDtypeStruct((ROWS, 4, C, N), F32)
INV = jax.ShapeDtypeStruct((STEPS, STEP, N), F32)


def whole(array):
    zeros = (0,) * len(array.shape)
    return pl.BlockSpec(array.shape, lambda t: zeros, pipeline_mode=pl.Buffered(1))


def row_call(kernel, name, collective_id, tris, ins, consts, outs, n_back, scratch, width=0):
    n_send = sum(out in SENT for out in outs)
    packed = (STEPS, 2, C, STEP, BLOCK) if BDX in outs else (STEPS, C, STEP, N)
    dma = pltpu.SemaphoreType.DMA
    sent = [pltpu.VMEM((2 * C * STEP, C), F32)] * n_send + [pltpu.VMEM(packed, BF16)] * n_send
    sems = [dma((STEPS, GROUP))] * n_send + ([dma((n_send,))] if n_send else [])
    back = [pltpu.VMEM((4 * N * 8, C), F32)] * n_back + [pltpu.VMEM((STEPS, GROUP, STEP, CH, N), BF16)] * n_back
    back += [pltpu.VMEM((STEPS, STEP, C, N), BF16)] * n_back
    if width:
        back = [pltpu.VMEM((BCH * BLOCK * width // C if k == 0 else 8, C), F32) for k in range(n_back)]
        back += [pltpu.VMEM((STEPS, 4, STEP, BCH, width), BF16)] * n_back + [pltpu.VMEM((STEPS, 2, STEP, C, width), BF16)] * n_back
    back += [dma((STEPS, GROUP))] * (2 * n_back)
    far = pl.BlockSpec(memory_space=pl.ANY)
    rows_out = [out for out in outs if is_rows(out)]
    near = [pltpu.VMEM(x.shape, x.dtype) for x in tris]
    near += [pltpu.VMEM((2, x.shape[0] // STEPS) + x.shape[1:], x.dtype) for x in [*ins, *rows_out]]
    near += [dma((max(len(tris), 1), GROUPS)), dma((2, len(ins))), dma((2, len(rows_out)))]
    return pl.pallas_call(
        functools.partial(staged_kernel, kernel, len(tris), len(ins), len(consts), outs),
        grid=(STEPS + 1,),
        in_specs=[far] * (len(tris) + len(ins)) + [whole(x) for x in consts],
        out_specs=[pl.BlockSpec(out.shape, lambda t: (0, 0)) if out in (PRE, POST, TOT) else far for out in outs],
        out_shape=outs,
        scratch_shapes=sent + scratch + sems + back + near,
        compiler_params=pltpu.CompilerParams(dimension_semantics=("arbitrary",), vmem_limit_bytes=VMEM_LIMIT, collective_id=collective_id, has_side_effects=True),
        name=name,
    )(*tris, *ins, *consts)


def local_step(z_pair, pair_mask, dz_out, ln_in, w_proj, b_proj, ln_mid, w_out, b_out):
    z, dz = z_pair[0], dz_out[0]
    mask = pair_mask.reshape(STEPS, STEP, N)
    pre, post = [ln_in, w_proj, b_proj], [ln_mid, w_out, b_out]
    eye = [pltpu.VMEM((C, C), BF16)]
    pre_c = [pltpu.VMEM((2, C, N), F32), pltpu.VMEM((PROJ, C), BF16), pltpu.VMEM((PROJ, N), F32)]
    post_c = [pltpu.VMEM((2, C, N), F32), pltpu.VMEM((C, C), BF16), pltpu.VMEM((C, N), F32)]
    post_acc = [pltpu.VMEM((4, C, C), F32)]
    pre_acc = [pltpu.VMEM((PROJ, C), F32), pltpu.VMEM((PROJ, C), F32), pltpu.VMEM((2, C, C), F32)]

    gains = [pltpu.VMEM((2, C, N), F32)]
    kept = [TRI, TRI, ROW32, KEEP, ROW32, INV]
    a0, b0, g0, keep0, unit0, inv0 = row_call(pre_kernel, "pre0", 0, [], [z, mask], pre, [BTRI, BTRI] + kept[2:], 0, eye + pre_c)
    a1, b1, g1, keep1, unit1, inv1, zm, gu0, munit0, minv0 = row_call(
        mid_kernel, "mid", 1, [a0, b0], [z, g0, mask], post + pre, kept + [ROW, ROW32, ROW32, INV], 1, eye + pre_c + post_c, BLOCK)
    dx1, z_new, dpg1, post_g1 = row_call(
        turn_kernel, "turn", 2, [a1, b1], [zm, g1, dz], post, [TRI, NATIVE, ROW32, POST], 1, eye + post_c + post_acc)
    dx0, dzm, dpg0, pre_g1, post_g0 = row_call(
        back_kernel, "back", 3, [a1, b1, dx1], [dpg1, keep1, unit1, inv1, dz, munit0, minv0, g0, gu0], [ln_in, w_proj, ln_mid, w_out],
        [BDX, ROW, ROW32, PRE, POST], 2, eye + gains * 2 + pre_acc + post_acc)
    adders = [pltpu.VMEM(PRE.shape, F32)]
    for size in (EARLY_SHARE, LATE_SHARE):
        adders += [pltpu.VMEM((ALL * size, C), BF16), pltpu.VMEM((ALL, size, C), BF16), pltpu.VMEM((size, C), F32)]
    adders += [pltpu.VMEM(TOT.shape, F32), pltpu.SemaphoreType.DMA((2, 6, ALL))]
    dz_new, total = row_call(
        last_kernel, "last", 4, [a0, b0, dx0], [dpg0, keep0, unit0, inv0, dzm], [ln_in, w_proj, post_g0, post_g1, pre_g1],
        [NATIVE, TOT], 2, gains + pre_acc + adders, N)
    z_out, dz_pair, *grads = finish(z_new, dz_new, total)
    return z_out[None], dz_pair[None], *grads


def solution(mesh):
    row_spec = P("dp", "dap")
    return jax.shard_map(local_step, mesh=mesh, in_specs=(row_spec,) * 3 + (P(),) * 6,
                         out_specs=(row_spec,) * 2 + (P(),) * 6, check_vma=False)
```
